32 devices in a mesh: fsdp: 8 (over z, x), ctx: 2 (over core), tp: 2 (over y).
Axes of the slice: x: 2, y: 2, z: 4, core: 2. Of those that a mesh axis runs over, the one named last changes fastest.
Arguments:
- hidden_in: bfloat16 [2048, 2048], P(('fsdp', 'ctx')), may hold values from -6 to 6
- segment_ids: int32 [2048], P(('fsdp', 'ctx')), may hold values from 0 to 15, never falling along the last dimension, each value on 1 to 256 neighbouring positions
- routes: int32 [2048, 8], P(('fsdp', 'ctx')), may hold values from 0 to 31, all different within a row; in each aligned block of 128 rows (0 to 127, 128 to 255, ...) at most 64 rows name the same one
- attn_gain: bfloat16 [2048], P('fsdp'), may hold values from 0.5 to 1.5
- qk_gains: bfloat16 [256], P('fsdp'), may hold values from 0.6 to 1.6
- w_query: bfloat16 [2048, 4096], P('fsdp', 'tp')
- key_projection: bfloat16 [2048, 512], P('fsdp', 'tp')
- value_projection: bfloat16 [2048, 512], P('fsdp', 'tp'), may hold values from -0.125 to 0.125
- w_out: bfloat16 [4096, 2048], P('tp', 'fsdp'), may hold values from -0.5 to 0.5
- ffn_gain: bfloat16 [2048], P('fsdp'), may hold values from 0.5 to 1.5
- w_router: bfloat16 [2048, 32], P('fsdp')
- w_gate: bfloat16 [32, 2048, 768], P(('fsdp', 'ctx'), None, 'tp'), may hold values from -0.125 to 0.125
- w_up: bfloat16 [32, 2048, 768], P(('fsdp', 'ctx'), None, 'tp'), may hold values from -0.125 to 0.125
- w_down: bfloat16 [32, 768, 2048], P(('fsdp', 'ctx'), 'tp'), may hold values from -0.625 to 0.625
- grad_out: bfloat16 [2048, 2048], P(('fsdp', 'ctx')), may hold values from -6 to 6
Outputs:
- block_out: bfloat16 [2048, 2048], P(('fsdp', 'ctx'))
- grad_in: float32 [2048, 2048], P(('fsdp', 'ctx'))
- grad_attn_gain: float32 [2048], P('fsdp')
- grad_qk_gains: float32 [256], P('fsdp')
- grad_query: float32 [2048, 4096], P('fsdp', 'tp')
- grad_key: float32 [2048, 512], P('fsdp', 'tp')
- grad_value: float32 [2048, 512], P('fsdp', 'tp')
- grad_out_proj: float32 [4096, 2048], P('tp', 'fsdp')
- grad_ffn_gain: float32 [2048], P('fsdp')
- grad_router: float32 [2048, 32], P('fsdp')
- grad_gate: float32 [32, 2048, 768], P(('fsdp', 'ctx'), None, 'tp')
- grad_up: float32 [32, 2048, 768], P(('fsdp', 'ctx'), None, 'tp')
- grad_down: float32 [32, 768, 2048], P(('fsdp', 'ctx'), 'tp')
The draws below stay inside these ranges and needn't reach their ends.
Inputs may be any that keep to these rules, and one draw needn't show every extreme that they name: `routes`: each row names 8 different experts. Within the 128 rows of one device no expert is named by more than 64 rows, and in some device one expert is named by exactly 64 rows. `segment_ids`: segment ids never fall along the tokens; a segment holds 1 to 256 tokens, and one holds exactly 256.
All inputs are finite; a program needn't handle non-finite values.
Results may differ from the reference program's by a relative error of at most 0.028.
Values may be sent and summed in bfloat16 or wider, within the bound.
A program may use at most 256 MiB of HBM per device.

```python
import math
import jax
import jax.numpy as jnp
import numpy as np
from jax import lax

MODEL_WIDTH = 2048
QUERY_HEADS = 32
KEY_VALUE_HEADS = 4
HEAD_SIZE = 128
FF = 768
TOPK = 8
TOK_DEV = 128
EXPERTS = 32
SEQUENCE_LENGTH = 256
TOTAL_TOKENS = 2048
MOST = 64
N_FSDP = 8
N_CTX = 2
N_TP = 2


def draw_w_query(key, part):
    entries = jax.random.normal(jax.random.fold_in(key, 21), (MODEL_WIDTH, QUERY_HEADS * HEAD_SIZE), jnp.float32)
    return (entries * MODEL_WIDTH ** (-0.5)).astype(jnp.bfloat16)


def draw_key_projection(key, part):
    entries = jax.random.normal(jax.random.fold_in(key, 23), (MODEL_WIDTH, KEY_VALUE_HEADS * HEAD_SIZE), jnp.float32)
    return (entries * MODEL_WIDTH ** (-0.5)).astype(jnp.bfloat16)


def draw_qk_gains(key, part):
    return jax.random.uniform(jax.random.fold_in(key, 24), (2 * HEAD_SIZE,), jnp.float32, 0.6, 1.6).astype(jnp.bfloat16)


def draw_w_router(key, part):
    column_scale = jax.random.uniform(jax.random.fold_in(key, 25), (1, EXPERTS), jnp.float32, 0.5, 2.0)
    entries = jax.random.normal(jax.random.fold_in(key, 26), (MODEL_WIDTH, EXPERTS), jnp.float32)
    return (entries * MODEL_WIDTH ** (-0.5) * column_scale).astype(jnp.bfloat16)


def block_scale(rng, extent, shards, low, largest):
    gain = 1.0
    for axis_at, blocks in shards:
        steps = jax.random.uniform(jax.random.fold_in(jax.random.fold_in(rng, 6), axis_at), (blocks,), jnp.float32, low / len(shards), largest / len(shards))
        gain = gain * jnp.repeat(jnp.exp(steps), extent[axis_at] // blocks).reshape((-1,) + (1,) * (len(extent) - 1 - axis_at))
    return gain


def length_profile(amount, total, bound, skew):
    weights = [(1 << 20) // math.isqrt(standing ** skew) + 1 for standing in range(2, amount + 1)]
    rest, given = total - bound - (amount - 1), [1] * (amount - 1)
    while rest > 0:
        free = [i for i in range(amount - 1) if given[i] < bound]
        whole, remaining = sum([weights[i] for i in free]), rest
        for i in free:
            more = min(bound - given[i], max(1, remaining * weights[i] // whole), rest)
            given[i] = given[i] + more
            rest = rest - more
    return np.array([bound] + given)


def ragged_sizes(rng, number_of, total, reach, slope):
    if number_of == 2:
        one = jax.random.randint(rng, (), max(1, total - reach), min(reach, total - 1) + 1)
        return jnp.stack([one, total - one])
    sizes = jnp.asarray(length_profile(number_of, total, reach, slope), jnp.int32)
    twos = (number_of - 1) // 2
    donor, receiver = sizes[1:1 + 2 * twos:2], sizes[2:2 + 2 * twos:2]
    room = jnp.minimum(donor - 1, reach - receiver)
    moved = jax.random.randint(jax.random.fold_in(rng, 1), (twos,), 0, 1 << 20) % (room + 1)
    sizes = sizes.at[1:1 + 2 * twos:2].set(donor - moved).at[2:2 + 2 * twos:2].set(receiver + moved)
    return sizes[jax.random.permutation(jax.random.fold_in(rng, 2), number_of)]


def routed_block(key, own, number, rows, count, top, limit, lean):
    order = jax.random.permutation(key, count)
    heavy_load, ordinary = shares(count, rows * top, limit, lean, True), shares(count, rows * top, limit, lean, False)
    places = jnp.arange(count)

    def named(sizes, rotation):
        used = int((sizes > 0).sum())
        fixed = max(1, used // 4)
        passed = fixed + (places - fixed + rotation * (used - fixed)) % max(1, count - fixed)
        return jnp.zeros((count,), jnp.int32).at[order[jnp.where(places < fixed, places, passed)]].set(jnp.asarray(sizes, jnp.int32))

    sizes = jnp.where(number % 4 == 0, named(heavy_load, number // 4), named(ordinary, number - number // 4 - 1))
    mixed = jax.random.permutation(jax.random.fold_in(own, 3), count)
    source_of, taker = mixed[0:count // 2 * 2:2], mixed[1:count // 2 * 2:2]
    margin = jnp.minimum(sizes[source_of] - 1, limit - sizes[taker]) // 2
    margin = jnp.where((source_of == order[0]) | (taker == order[0]) | (sizes[taker] == 0), 0, jnp.maximum(margin, 0))
    passed = jax.random.randint(jax.random.fold_in(own, 4), (count // 2,), 0, 1 << 20) % (margin + 1)
    sizes = sizes.at[source_of].add(-passed).at[taker].add(passed)
    labels = jnp.searchsorted(jnp.cumsum(sizes), jnp.arange(rows * top), side="right").astype(jnp.int32)
    grid = labels.reshape(top, rows).T
    grid = grid[jax.random.permutation(jax.random.fold_in(own, 1), rows)]
    rotation = jax.random.randint(jax.random.fold_in(own, 2), (rows, 1), 0, top)
    return jnp.take_along_axis(grid, (jnp.arange(top)[None, :] + rotation) % top, axis=1)


def shares(number_of, total, bound, slope, full):
    weights = [(1 << 20) // math.isqrt(rank ** slope) + 1 for rank in range(1, number_of + 1)]
    largest = bound if full else min(bound, max(-(-total // number_of), total * weights[0] // sum(weights)))
    least = 1 if total - largest >= number_of - 1 else 0
    given, rest = [largest] + [least] * (number_of - 1), total - largest - least * (number_of - 1)
    while rest > 0:
        candidates = [i for i in range(1, number_of) if given[i] < largest] or [i for i in range(1, number_of) if given[i] < bound]
        pool, left = sum([weights[i] for i in candidates]), rest
        for i in candidates:
            addition = min(bound - given[i], max(1, left * weights[i] // pool), rest)
            given[i] = given[i] + addition
            rest = rest - addition
    return np.array(given)


def noise(stream_key, extent, width, reach, pieces=(), kind=jnp.bfloat16):
    array = width * jax.random.normal(stream_key, extent, jnp.float32)
    if pieces:
        array = array * block_scale(stream_key, extent, pieces, -0.22, 0.18)
    return jnp.clip(array, -reach, reach).astype(kind)


def setup_inputs(seed: int = 0) -> dict:
    seeds = jax.random.split(jax.random.key(seed), 16)
    hidden_in = noise(seeds[0], (TOTAL_TOKENS, MODEL_WIDTH), 1.0, 6.0, ((0, 16),))
    segment_ids = jnp.searchsorted(jnp.cumsum(ragged_sizes(seeds[1], N_FSDP * N_CTX, TOTAL_TOKENS, SEQUENCE_LENGTH, 1)), jnp.arange(TOTAL_TOKENS), side="right").astype(jnp.int32)
    routes_keys = jax.random.split(jax.random.fold_in(seeds[2], 1), TOTAL_TOKENS // TOK_DEV)
    routes_turns = jax.random.permutation(jax.random.fold_in(seeds[2], 3), TOTAL_TOKENS // TOK_DEV)
    routes = jax.vmap(lambda own, number: routed_block(jax.random.fold_in(seeds[2], 2), own, number, TOK_DEV, EXPERTS, TOPK, MOST, 2))(routes_keys, routes_turns).reshape((TOTAL_TOKENS, TOPK))
    attn_gain = jnp.clip(1.0 + 0.1 * jax.random.normal(seeds[3], (MODEL_WIDTH,), jnp.float32), 0.5, 1.5).astype(jnp.bfloat16)
    qk_gains = draw_qk_gains(jax.random.fold_in(seeds[15], 71), 0)
    w_query = draw_w_query(jax.random.fold_in(seeds[15], 71), 0)
    key_projection = draw_key_projection(jax.random.fold_in(seeds[15], 71), 0)
    value_projection = noise(seeds[7], (MODEL_WIDTH, KEY_VALUE_HEADS * HEAD_SIZE), MODEL_WIDTH ** -0.5, 0.125, ((0, 8), (1, 2)))
    w_out = noise(seeds[8], (QUERY_HEADS * HEAD_SIZE, MODEL_WIDTH), HEAD_SIZE ** -0.5, 0.5, ((0, 2), (1, 8)))
    ffn_gain = jnp.clip(1.0 + 0.1 * jax.random.normal(seeds[9], (MODEL_WIDTH,), jnp.float32), 0.5, 1.5).astype(jnp.bfloat16)
    w_router = draw_w_router(jax.random.fold_in(seeds[15], 71), 0)
    w_gate = noise(seeds[11], (EXPERTS, MODEL_WIDTH, FF), MODEL_WIDTH ** -0.5, 0.125, ((0, 16), (2, 2)))
    w_up = noise(seeds[12], (EXPERTS, MODEL_WIDTH, FF), MODEL_WIDTH ** -0.5, 0.125, ((0, 16), (2, 2)))
    w_down = noise(seeds[13], (EXPERTS, FF, MODEL_WIDTH), (FF // 8) ** -0.5, 0.625, ((0, 16), (1, 2)))
    grad_out = noise(seeds[14], (TOTAL_TOKENS, MODEL_WIDTH), 1.0, 6.0, ((0, 16),))
    return dict(hidden_in=hidden_in, segment_ids=segment_ids, routes=routes, attn_gain=attn_gain, qk_gains=qk_gains, w_query=w_query, key_projection=key_projection, value_projection=value_projection, w_out=w_out, ffn_gain=ffn_gain, w_router=w_router, w_gate=w_gate, w_up=w_up, w_down=w_down, grad_out=grad_out)


eps_norm = 1e-06
rope_base = 1000000.0

def norm_forward(values, gain_row):
    inverse = lax.rsqrt(lax.optimization_barrier(jnp.mean(values * values, axis=-1, keepdims=True)) + eps_norm)
    normed = values * inverse
    return (normed * gain_row, normed, inverse)

def rms_norm_gradient(grad_scaled, normed, inverse, gain_row):
    grad_normed = grad_scaled * gain_row
    inner_mean = lax.optimization_barrier(jnp.mean(grad_normed * normed, axis=-1, keepdims=True))
    return inverse * (grad_normed - normed * inner_mean)

def rope_tables(positions):
    half_dim = HEAD_SIZE // 2
    frequencies = rope_base ** (-(jnp.arange(half_dim, dtype=jnp.float32) * 2.0) / HEAD_SIZE)
    angles = positions.astype(jnp.float32)[:, None] * frequencies[None, :]
    return (jnp.cos(angles)[:, None, :], jnp.sin(angles)[:, None, :])

def rotate(values, cosine_table, sine_values):
    half_dim = values.shape[-1] // 2
    first_half = values[..., :half_dim]
    second_half = values[..., half_dim:]
    return jnp.concatenate([first_half * cosine_table - second_half * sine_values, second_half * cosine_table + first_half * sine_values], axis=-1)

def inverse_rotation(grad_in_rot, cosine_table, sine_values):
    half_dim = grad_in_rot.shape[-1] // 2
    first_half = grad_in_rot[..., :half_dim]
    second_half = grad_in_rot[..., half_dim:]
    return jnp.concatenate([first_half * cosine_table + second_half * sine_values, second_half * cosine_table - first_half * sine_values], axis=-1)

def barrier_widen(values):
    return lax.optimization_barrier(values).astype(jnp.float32)

def attention_mask(positions, segments):
    return (positions[None, :] <= positions[:, None]) & (segments[None, :] == segments[:, None])

def attention_scores(query_seq, key_seq, allowed):
    scores = jnp.einsum('qkgd,skd->kgqs', query_seq.astype(jnp.float32), key_seq.astype(jnp.float32)) * HEAD_SIZE ** (-0.5)
    return jnp.where(allowed[None, None], scores, -jnp.inf)

def slot_index(route_rows):
    flat_routes = route_rows.reshape(-1)
    onehot = (flat_routes[:, None] == jnp.arange(EXPERTS, dtype=jnp.int32)[None, :]).astype(jnp.int32)
    rank_rows = jnp.cumsum(onehot, axis=0) - onehot
    return flat_routes * MOST + lax.optimization_barrier(jnp.sum(rank_rows * onehot, axis=1))

def expert_output(activated, down_weight):
    width_part = FF // N_TP
    summed = jnp.zeros((activated.shape[0], MODEL_WIDTH), jnp.float32)
    for split_index in range(N_TP):
        lower_edge = split_index * width_part
        partial_out = jnp.dot(activated[:, lower_edge:lower_edge + width_part], down_weight[lower_edge:lower_edge + width_part], preferred_element_type=jnp.float32)
        summed = summed + barrier_widen(partial_out.astype(jnp.bfloat16))
    return summed

def expert_input_grad(grad_gate_pre, grad_up_pre, gate_weight, up_weight):
    width_part = FF // N_TP
    summed = jnp.zeros((grad_gate_pre.shape[0], MODEL_WIDTH), jnp.float32)
    for split_index in range(N_TP):
        lower_edge = split_index * width_part
        upper_edge = lower_edge + width_part
        partial_out = jnp.dot(grad_gate_pre[:, lower_edge:upper_edge], gate_weight[:, lower_edge:upper_edge].T, preferred_element_type=jnp.float32)
        partial_out = partial_out + jnp.dot(grad_up_pre[:, lower_edge:upper_edge], up_weight[:, lower_edge:upper_edge].T, preferred_element_type=jnp.float32)
        summed = summed + barrier_widen(partial_out.astype(jnp.bfloat16))
    return summed

def reference(hidden_in, segment_ids, routes, attn_gain, qk_gains, w_query, key_projection, value_projection, w_out, ffn_gain, w_router, w_gate, w_up, w_down, grad_out):
    query_group_width = QUERY_HEADS // KEY_VALUE_HEADS
    sequence_count = TOTAL_TOKENS // SEQUENCE_LENGTH
    resid = hidden_in.astype(jnp.float32)
    gain_one = attn_gain.astype(jnp.float32)
    scaled_one, normed_one, inverse_one = norm_forward(resid, gain_one)
    hidden_first = scaled_one.astype(jnp.bfloat16)
    query_raw = jnp.dot(hidden_first, w_query, preferred_element_type=jnp.float32).reshape(TOTAL_TOKENS, QUERY_HEADS, HEAD_SIZE)
    key_projected = jnp.dot(hidden_first, key_projection, preferred_element_type=jnp.float32).reshape(TOTAL_TOKENS, KEY_VALUE_HEADS, HEAD_SIZE)
    value_matrix_rows = jnp.dot(hidden_first, value_projection, preferred_element_type=jnp.float32).astype(jnp.bfloat16)
    gain_query = qk_gains[:HEAD_SIZE].astype(jnp.float32)
    key_norm_gain = qk_gains[HEAD_SIZE:].astype(jnp.float32)
    query_normed, query_hat, query_inverse = norm_forward(query_raw, gain_query)
    key_normed, key_unit_rows, key_inverse_norm = norm_forward(key_projected, key_norm_gain)
    cosine_table, sine_values = rope_tables(jnp.arange(TOTAL_TOKENS, dtype=jnp.int32) % SEQUENCE_LENGTH)
    query_rotated = rotate(query_normed, cosine_table, sine_values).astype(jnp.bfloat16)
    key_rotated = rotate(key_normed, cosine_table, sine_values).astype(jnp.bfloat16)
    seq_positions = jnp.arange(SEQUENCE_LENGTH, dtype=jnp.int32)
    query_per_sequence = query_rotated.reshape(sequence_count, SEQUENCE_LENGTH, KEY_VALUE_HEADS, query_group_width, HEAD_SIZE)
    key_per_sequence = key_rotated.reshape(sequence_count, SEQUENCE_LENGTH, KEY_VALUE_HEADS, HEAD_SIZE)
    value_per_sequence = value_matrix_rows.reshape(sequence_count, SEQUENCE_LENGTH, KEY_VALUE_HEADS, HEAD_SIZE)
    segment_seqs = segment_ids.reshape(sequence_count, SEQUENCE_LENGTH)

    def forward_seq(seq_items):
        query_seq, key_seq, value_seq, segments = seq_items
        scores = attention_scores(query_seq, key_seq, attention_mask(seq_positions, segments))
        top_score = lax.optimization_barrier(jnp.max(scores, axis=-1, keepdims=True))
        log_total = top_score + jnp.log(lax.optimization_barrier(jnp.sum(jnp.exp(scores - top_score), axis=-1, keepdims=True)))
        weights_att = barrier_widen(jnp.exp(scores - log_total).astype(jnp.bfloat16))
        attended_seq = jnp.einsum('kgqs,skd->qkgd', weights_att, value_seq.astype(jnp.float32))
        return (attended_seq.astype(jnp.bfloat16), log_total)
    attended, log_totals = lax.map(forward_seq, (query_per_sequence, key_per_sequence, value_per_sequence, segment_seqs))
    attended = attended.reshape(TOTAL_TOKENS, QUERY_HEADS * HEAD_SIZE)
    resid_mid = resid + jnp.dot(attended, w_out, preferred_element_type=jnp.float32)
    gain_two = ffn_gain.astype(jnp.float32)
    scaled_two, normed_two, inverse_two = norm_forward(resid_mid, gain_two)
    hidden_two = scaled_two.astype(jnp.bfloat16)
    logits = jnp.dot(hidden_two, w_router, preferred_element_type=jnp.float32)
    chosen = jnp.take_along_axis(logits, routes, axis=1)
    raised = jnp.exp(chosen - lax.optimization_barrier(jnp.max(chosen, axis=1, keepdims=True)))
    route_probs = raised / lax.optimization_barrier(jnp.sum(raised, axis=1, keepdims=True))
    block_count = TOTAL_TOKENS // TOK_DEV
    per_block = TOK_DEV * TOPK
    targets = jax.vmap(slot_index)(routes.reshape(block_count, TOK_DEV, TOPK))
    assign_ids = jnp.arange(block_count * per_block, dtype=jnp.int32).reshape(block_count, per_block)
    sentinel = block_count * per_block

    def owner_table(target_row, id_row):
        return jnp.full((EXPERTS * MOST,), sentinel, jnp.int32).at[target_row].set(id_row)
    owners = jax.vmap(owner_table)(targets, assign_ids)
    owners = owners.reshape(block_count, EXPERTS, MOST).transpose(1, 0, 2).reshape(EXPERTS, block_count * MOST)
    probs_pad = jnp.concatenate([route_probs.reshape(-1), jnp.zeros((1,), jnp.float32)])
    hidden_pad = jnp.concatenate([hidden_two, jnp.zeros((1, MODEL_WIDTH), jnp.bfloat16)], axis=0)

    def forward_expert(moe_acc, expert_items):
        owner_row, gate_weight, up_weight, down_weight = expert_items
        token_row = owner_row // TOPK
        rows_in = hidden_pad[token_row]
        gate_pre = jnp.dot(rows_in, gate_weight, preferred_element_type=jnp.float32)
        up_pre = jnp.dot(rows_in, up_weight, preferred_element_type=jnp.float32)
        activated = (jax.nn.silu(gate_pre) * up_pre).astype(jnp.bfloat16)
        produced = expert_output(activated, down_weight)
        return (moe_acc.at[token_row].add(probs_pad[owner_row][:, None] * produced), None)
    moe_pad, scan_ys = lax.scan(forward_expert, jnp.zeros((TOTAL_TOKENS + 1, MODEL_WIDTH), jnp.float32), (owners, w_gate, w_up, w_down))
    block_out = (resid_mid + moe_pad[:TOTAL_TOKENS]).astype(jnp.bfloat16)
    grad_rows = grad_out.astype(jnp.float32)
    grad_pad = jnp.concatenate([grad_rows, jnp.zeros((1, MODEL_WIDTH), jnp.float32)], axis=0)

    def backward_expert(carry_pair, expert_items):
        hidden_acc, prob_acc = carry_pair
        owner_row, gate_weight, up_weight, down_weight = expert_items
        token_row = owner_row // TOPK
        rows_in = hidden_pad[token_row]
        gate_pre = jnp.dot(rows_in, gate_weight, preferred_element_type=jnp.float32)
        up_pre = jnp.dot(rows_in, up_weight, preferred_element_type=jnp.float32)
        sigmoid_gate = jax.nn.sigmoid(gate_pre)
        silu_gate = jax.nn.silu(gate_pre)
        activated = (silu_gate * up_pre).astype(jnp.bfloat16)
        produced = expert_output(activated, down_weight)
        grad_token = grad_pad[token_row]
        prob_acc = prob_acc.at[owner_row].add(lax.optimization_barrier(jnp.sum(grad_token * produced, axis=1)))
        grad_prod = (probs_pad[owner_row][:, None] * grad_token).astype(jnp.bfloat16)
        grad_act = jnp.dot(grad_prod, down_weight.T, preferred_element_type=jnp.float32)
        grad_down_e = jnp.dot(activated.T, grad_prod, preferred_element_type=jnp.float32)
        grad_gate_pre = (grad_act * up_pre * (sigmoid_gate * (1.0 + gate_pre * (1.0 - sigmoid_gate)))).astype(jnp.bfloat16)
        grad_up_pre = (grad_act * silu_gate).astype(jnp.bfloat16)
        grad_gate_e = jnp.dot(rows_in.T, grad_gate_pre, preferred_element_type=jnp.float32)
        grad_up_e = jnp.dot(rows_in.T, grad_up_pre, preferred_element_type=jnp.float32)
        hidden_acc = hidden_acc.at[token_row].add(expert_input_grad(grad_gate_pre, grad_up_pre, gate_weight, up_weight))
        return ((hidden_acc, prob_acc), (grad_gate_e, grad_up_e, grad_down_e))
    start_pair = (jnp.zeros((TOTAL_TOKENS + 1, MODEL_WIDTH), jnp.float32), jnp.zeros((TOTAL_TOKENS * TOPK + 1,), jnp.float32))
    (hidden_grad_pad, prob_grad_pad), (grad_gate, grad_up, grad_down) = lax.scan(backward_expert, start_pair, (owners, w_gate, w_up, w_down))
    grad_prob = prob_grad_pad[:TOTAL_TOKENS * TOPK].reshape(TOTAL_TOKENS, TOPK)
    grad_chosen = route_probs * (grad_prob - lax.optimization_barrier(jnp.sum(route_probs * grad_prob, axis=1, keepdims=True)))
    route_hits = (routes[:, :, None] == jnp.arange(EXPERTS, dtype=jnp.int32)[None, None, :]).astype(jnp.float32)
    grad_logits = lax.optimization_barrier(jnp.sum(route_hits * grad_chosen[:, :, None], axis=1)).astype(jnp.bfloat16)
    grad_router = jnp.dot(hidden_two.T, grad_logits, preferred_element_type=jnp.float32)
    grad_hidden_two = hidden_grad_pad[:TOTAL_TOKENS] + jnp.dot(grad_logits, w_router.T, preferred_element_type=jnp.float32)
    grad_ffn_gain = lax.optimization_barrier(jnp.sum(grad_hidden_two * normed_two, axis=0))
    grad_mid = grad_rows + rms_norm_gradient(grad_hidden_two, normed_two, inverse_two, gain_two)
    grad_proj = grad_mid.astype(jnp.bfloat16)
    grad_out_proj = jnp.dot(attended.T, grad_proj, preferred_element_type=jnp.float32)
    attended_gradient = jnp.dot(grad_proj, w_out.T, preferred_element_type=jnp.float32).astype(jnp.bfloat16)
    attended_gradient = attended_gradient.reshape(sequence_count, SEQUENCE_LENGTH, KEY_VALUE_HEADS, query_group_width, HEAD_SIZE)

    def backward_seq(seq_items):
        query_seq, key_seq, value_seq, segments, log_total, grad_seq = seq_items
        scores = attention_scores(query_seq, key_seq, attention_mask(seq_positions, segments))
        probs_att = jnp.exp(scores - log_total)
        weights_att = barrier_widen(probs_att.astype(jnp.bfloat16))
        grad_wide = grad_seq.astype(jnp.float32)
        grad_value_seq = jnp.einsum('kgqs,qkgd->skd', weights_att, grad_wide)
        grad_probs = jnp.einsum('qkgd,skd->kgqs', grad_wide, value_seq.astype(jnp.float32))
        delta_row = lax.optimization_barrier(jnp.sum(probs_att * grad_probs, axis=-1, keepdims=True))
        grad_scores = barrier_widen((probs_att * (grad_probs - delta_row) * HEAD_SIZE ** (-0.5)).astype(jnp.bfloat16))
        grad_query_seq = jnp.einsum('kgqs,skd->qkgd', grad_scores, key_seq.astype(jnp.float32))
        grad_key_seq = jnp.einsum('kgqs,qkgd->skd', grad_scores, query_seq.astype(jnp.float32))
        return (grad_query_seq, grad_key_seq, grad_value_seq)
    grad_query_rot, key_rotated_gradient, value_incoming_gradient = lax.map(backward_seq, (query_per_sequence, key_per_sequence, value_per_sequence, segment_seqs, log_totals, attended_gradient))
    grad_query_norm = inverse_rotation(grad_query_rot.reshape(TOTAL_TOKENS, QUERY_HEADS, HEAD_SIZE), cosine_table, sine_values)
    key_normed_gradient = inverse_rotation(key_rotated_gradient.reshape(TOTAL_TOKENS, KEY_VALUE_HEADS, HEAD_SIZE), cosine_table, sine_values)
    grad_qk_gains = jnp.concatenate([lax.optimization_barrier(jnp.sum(grad_query_norm * query_hat, axis=(0, 1))), lax.optimization_barrier(jnp.sum(key_normed_gradient * key_unit_rows, axis=(0, 1)))])
    grad_query_raw = rms_norm_gradient(grad_query_norm, query_hat, query_inverse, gain_query).astype(jnp.bfloat16).reshape(TOTAL_TOKENS, QUERY_HEADS * HEAD_SIZE)
    key_projected_gradient = rms_norm_gradient(key_normed_gradient, key_unit_rows, key_inverse_norm, key_norm_gain).astype(jnp.bfloat16).reshape(TOTAL_TOKENS, KEY_VALUE_HEADS * HEAD_SIZE)
    value_projected_gradient = value_incoming_gradient.reshape(TOTAL_TOKENS, KEY_VALUE_HEADS * HEAD_SIZE).astype(jnp.bfloat16)
    grad_query = jnp.dot(hidden_first.T, grad_query_raw, preferred_element_type=jnp.float32)
    grad_key = jnp.dot(hidden_first.T, key_projected_gradient, preferred_element_type=jnp.float32)
    grad_value = jnp.dot(hidden_first.T, value_projected_gradient, preferred_element_type=jnp.float32)
    grad_hidden_one = jnp.dot(grad_query_raw, w_query.T, preferred_element_type=jnp.float32)
    grad_hidden_one = grad_hidden_one + jnp.dot(key_projected_gradient, key_projection.T, preferred_element_type=jnp.float32)
    grad_hidden_one = grad_hidden_one + jnp.dot(value_projected_gradient, value_projection.T, preferred_element_type=jnp.float32)
    grad_attn_gain = lax.optimization_barrier(jnp.sum(grad_hidden_one * normed_one, axis=0))
    grad_in = grad_mid + rms_norm_gradient(grad_hidden_one, normed_one, inverse_one, gain_one)
    return (block_out, grad_in, grad_attn_gain, grad_qk_gains, grad_query, grad_key, grad_value, grad_out_proj, grad_ffn_gain, grad_router, grad_gate, grad_up, grad_down)
```

```python
import functools

import jax
import jax.numpy as jnp
from jax import lax
from jax.experimental import pallas as pl
from jax.experimental.pallas import tpu as pltpu
from jax.sharding import PartitionSpec as P

QUERY_HEADS = 32
KEY_VALUE_HEADS = 4
HEAD_SIZE = 128
TOPK = 8
MESH = pl.DeviceIdType.MESH

eps_norm = 1e-06
rope_base = 1000000.0

UP, DOWN, ACROSS, PARTNER, SIDE = range(5)


class Gather:
    def __init__(self, array, nf, form="row", half=False, rep=False, chunks=2):
        if nf > 8:
            chunks = 2 if rep else 1
        self.array, self.form, self.half, self.rep, self.chunks = array, form, half, rep, chunks
        self.shape = array.shape
        self.rows = array.shape[0] // 2 if half else array.shape[0]
        self.step = (self.rows // nf if form == "a2a" else self.rows) // chunks

    def out_shape(self, nf):
        rows, cols = self.rows, self.shape[1]
        if self.form == "col":
            return (2 * rows, nf * cols)
        if self.form == "a2a":
            return (2 * rows, cols)
        return (2 * nf * rows, cols)


def gather_kernel(nf, specs, *refs):
    n = len(specs)
    ins, outs, scratch = refs[:n], refs[n : 2 * n], refs[2 * n :]
    stage = scratch[:n]
    recv, send, local = scratch[n:]
    nz = nf // 2
    f, c, t = lax.axis_index("fsdp"), lax.axis_index("ctx"), lax.axis_index("tp")
    z, x = f // 2, lax.rem(f, 2)
    has_up, has_down = z + 1 < nz, z > 0
    device = {
        UP: (f + 2, c, t),
        DOWN: (f - 2, c, t),
        ACROSS: (z * 2 + 1 - x, c, t),
        PARTNER: (f, 1 - c, t),
        SIDE: (f, c, 1 - t),
    }
    any_a2a = any(s.form == "a2a" for s in specs)
    any_rep = any(s.rep for s in specs)
    barrier = pltpu.get_barrier_semaphore()

    def greet(dev):
        pl.semaphore_signal(barrier, 1, device_id=dev, device_id_type=MESH)

    greeted = 1
    greet(device[PARTNER])
    if any_rep:
        greet(device[SIDE])
        greeted += 1
    if any_a2a:

        def greet_far(d, carry):
            greet((lax.rem(f + d, nf), c, t))
            return carry

        lax.fori_loop(1, nf, greet_far, 0)
        pl.semaphore_wait(barrier, greeted + nf - 1)
    else:
        greet(device[ACROSS])

        @pl.when(has_up)
        def _():
            greet(device[UP])

        @pl.when(has_down)
        def _():
            greet(device[DOWN])

        pl.semaphore_wait(
            barrier, greeted + 1 + has_up.astype(jnp.int32) + has_down.astype(jnp.int32)
        )

    first = [sum(s.chunks for s in specs[:a]) for a in range(n)]

    def src(a, q, dest_f=None):
        s = specs[a]
        lo = q * s.step
        if s.half:
            lo = c * s.rows + lo
        if s.form == "a2a":
            lo = dest_f * (s.rows // nf) + lo
        return ins[a].at[pl.ds(lo, s.step)]

    def dst(a, q, bf, bc):
        s = specs[a]
        if s.form == "col":
            width = s.shape[1]
            return outs[a].at[
                pl.ds(bc * s.rows + q * s.step, s.step),
                pl.ds(pl.multiple_of(bf * width, width), width),
            ]
        rows = s.rows // nf if s.form == "a2a" else s.rows
        return outs[a].at[pl.ds((bf * 2 + bc) * rows + q * s.step, s.step)]

    def copy(a, q, bf, bc, source, kind, dev=None, slot=None):
        block = bf * 2 + bc if slot is None else slot
        return pltpu.make_async_remote_copy(
            src_ref=source,
            dst_ref=dst(a, q, bf, bc),
            send_sem=send.at[kind, block, first[a] + q],
            recv_sem=recv.at[bf * 2 + bc, first[a] + q],
            device_id=device[kind] if dev is None else dev,
            device_id_type=MESH,
        )

    def in_half(a, q):
        return (q * 2) // specs[a].chunks == t

    def both(*conds):
        conds = [k for k in conds if k is not None]
        if not conds:
            return None
        return functools.reduce(lambda u, v: u & v, conds)

    def when(cond, fn):
        if cond is None:
            fn()
        else:
            pl.when(cond)(fn)

    def go_up(a, q, dist):
        far = (dist + 1 < nz - 1) | in_half(a, q) if specs[a].rep else None
        return both(has_up, far)

    def go_down(a, q, dist):
        far = (dist + 1 < nz - 1) | in_half(a, q) if specs[a].rep else None
        return both(has_down, far)

    def go_across(a, q):
        return in_half(a, q) if specs[a].rep else None

    relays = [(a, q) for a in range(n) if specs[a].form != "a2a" for q in range(specs[a].chunks)]
    direct = [(a, q) for a in range(n) if specs[a].form == "a2a" for q in range(specs[a].chunks)]

    for a, q in relays:
        source = src(a, q)
        when(go_up(a, q, 0), lambda: copy(a, q, f, c, source, UP).start())
        when(go_down(a, q, 0), lambda: copy(a, q, f, c, source, DOWN).start())
        when(go_across(a, q), lambda: copy(a, q, f, c, source, ACROSS).start())
        copy(a, q, f, c, source, PARTNER).start()
    for a, q in direct:
        copy(a, q, f, c, src(a, q, f), PARTNER).start()

        def far_send(d, carry):
            there = lax.rem(f + d, nf)
            copy(a, q, f, c, src(a, q, there), UP, dev=(there, c, t), slot=there).start()
            return carry

        lax.fori_loop(1, nf, far_send, 0)

    def own_in(a):
        s = specs[a]
        if s.form == "a2a":
            view = ins[a].at[pl.ds(f * s.step, s.step)]
        elif s.half:
            view = ins[a].at[pl.ds(c * s.rows, s.rows)]
        else:
            view = ins[a]
        return pltpu.make_async_copy(view, stage[a], local.at[0, a])

    def own_out(a):
        s = specs[a]
        if s.form == "col":
            width = s.shape[1]
            view = outs[a].at[
                pl.ds(c * s.rows, s.rows), pl.ds(pl.multiple_of(f * width, width), width)
            ]
        else:
            rows = s.rows // nf if s.form == "a2a" else s.rows
            view = outs[a].at[pl.ds((f * 2 + c) * rows, rows)]
        return pltpu.make_async_copy(stage[a], view, local.at[1, a])

    for a in range(n):
        own_in(a).start()
    for a in range(n):
        own_in(a).wait()
        own_out(a).start()

    def arrived(a, q, bf, bc):
        copy(a, q, bf, bc, dst(a, q, bf, bc), PARTNER).wait_recv()

    def pass_on(a, q, bf, kind, cond=None):
        when(cond, lambda: copy(a, q, bf, c, dst(a, q, bf, c), kind).start())

    def column(k):
        for a, q in relays:
            rep = specs[a].rep
            came = ((k < nz - 1) | in_half(a, q)) if rep else None
            aside = (k == nz - 1) if rep else None

            def below():
                bf = (z - k) * 2 + x
                arrived(a, q, bf, c)
                pass_on(a, q, bf, UP, go_up(a, q, k))
                pass_on(a, q, bf, ACROSS, go_across(a, q))
                pass_on(a, q, bf, PARTNER)
                if rep:
                    pass_on(a, q, bf, SIDE, aside)

            def above():
                bf = (z + k) * 2 + x
                arrived(a, q, bf, c)
                pass_on(a, q, bf, DOWN, go_down(a, q, k))
                pass_on(a, q, bf, ACROSS, go_across(a, q))
                pass_on(a, q, bf, PARTNER)
                if rep:
                    pass_on(a, q, bf, SIDE, aside)

            when(both(z - k >= 0, came), below)
            when(both(z + k < nz, came), above)

    def across(k):
        for a, q in relays:
            rep = specs[a].rep

            def take(zz):
                bf = zz * 2 + 1 - x
                arrived(a, q, bf, c)
                pass_on(a, q, bf, PARTNER)
                if rep:
                    pass_on(a, q, bf, SIDE)

            mine = in_half(a, q) if rep else None
            when(both(z - k >= 0, mine), lambda: take(z - k))
            when(both(z + k < nz, k > 0, mine), lambda: take(z + k))

    def aside(k):
        for a, q in relays:
            if not specs[a].rep:
                continue
            other = jnp.logical_not(in_half(a, q))

            def take(bf):
                arrived(a, q, bf, c)
                pass_on(a, q, bf, PARTNER)

            when((z - k >= 0) & other, lambda: take((z - k) * 2 + 1 - x))
            when((z + k < nz) & (k > 0) & other, lambda: take((z + k) * 2 + 1 - x))
            when((z - k >= 0) & (k == nz - 1) & other, lambda: take((z - k) * 2 + x))
            when((z + k < nz) & (k == nz - 1) & other, lambda: take((z + k) * 2 + x))

    def step(k, carry):
        column(k)
        across(k - 1)

        @pl.when(k > 1)
        def _():
            aside(k - 2)

        return carry

    lax.fori_loop(1, nz, step, 0)
    across(nz - 1)
    if any_rep:
        aside(nz - 2)
        aside(nz - 1)

    for a, q in direct:

        def far_take(d, carry):
            there = lax.rem(f + nf - d, nf)
            arrived(a, q, there, c)
            pass_on(a, q, there, PARTNER)
            return carry

        lax.fori_loop(1, nf, far_take, 0)

    def finish(bf, carry):
        zz, xx = bf // 2, lax.rem(bf, 2)
        dist = jnp.abs(zz - z)
        here = xx == x
        for a, q in relays:
            rep = specs[a].rep
            arrived(a, q, bf, 1 - c)
            view = dst(a, q, bf, c)

            def sent(kind, cond):
                when(cond, lambda: copy(a, q, bf, c, view, kind).wait_send())

            half = in_half(a, q) if rep else None
            by_z = ((dist < nz - 1) | half) if rep else None
            sent(PARTNER, None)
            sent(UP, both(here, zz <= z, by_z, go_up(a, q, dist)))
            sent(DOWN, both(here, zz >= z, by_z, go_down(a, q, dist)))
            sent(ACROSS, both(here, by_z, go_across(a, q)))
            if rep:
                sent(SIDE, half & (jnp.logical_not(here) | (dist == nz - 1)))
        for a, q in direct:
            arrived(a, q, bf, 1 - c)
            view = dst(a, q, bf, c)
            copy(a, q, bf, c, view, PARTNER).wait_send()

            @pl.when(bf != f)
            def _():
                copy(a, q, bf, c, view, UP, slot=bf).wait_send()

        return carry

    lax.fori_loop(0, nf, finish, 0)
    for a in range(n):
        own_out(a).wait()


def plane_gather(specs, collective_id, nf):
    n = len(specs)
    total = sum(s.chunks for s in specs)

    def stage_of(s):
        rows = s.rows // nf if s.form == "a2a" else s.rows
        return pltpu.VMEM((rows, s.shape[1]), s.array.dtype)

    return pl.pallas_call(
        functools.partial(gather_kernel, nf, tuple(specs)),
        out_shape=tuple(jax.ShapeDtypeStruct(s.out_shape(nf), s.array.dtype) for s in specs),
        in_specs=[pl.BlockSpec(memory_space=pl.ANY)] * n,
        out_specs=tuple(pl.BlockSpec(memory_space=pl.ANY) for _ in specs),
        scratch_shapes=[stage_of(s) for s in specs]
        + [
            pltpu.SemaphoreType.DMA((2 * nf, total)),
            pltpu.SemaphoreType.DMA((5, 2 * nf, total)),
            pltpu.SemaphoreType.DMA((2, n)),
        ],
        compiler_params=pltpu.CompilerParams(
            collective_id=collective_id, has_side_effects=True
        ),
    )(*[s.array for s in specs])


def norm_forward(values, gain_row):
    inverse = lax.rsqrt(jnp.mean(values * values, axis=-1, keepdims=True) + eps_norm)
    normed = values * inverse
    return (normed * gain_row, normed, inverse)


def rms_norm_gradient(grad_scaled, normed, inverse, gain_row):
    grad_normed = grad_scaled * gain_row
    inner_mean = jnp.mean(grad_normed * normed, axis=-1, keepdims=True)
    return inverse * (grad_normed - normed * inner_mean)


def rope_tables(positions):
    half_dim = HEAD_SIZE // 2
    frequencies = rope_base ** (-(jnp.arange(half_dim, dtype=jnp.float32) * 2.0) / HEAD_SIZE)
    angles = positions.astype(jnp.float32)[:, None] * frequencies[None, :]
    return (jnp.cos(angles)[:, None, :], jnp.sin(angles)[:, None, :])


def rotate(values, cosine_table, sine_values):
    half_dim = values.shape[-1] // 2
    first_half = values[..., :half_dim]
    second_half = values[..., half_dim:]
    return jnp.concatenate(
        [
            first_half * cosine_table - second_half * sine_values,
            second_half * cosine_table + first_half * sine_values,
        ],
        axis=-1,
    )


def inverse_rotation(grad_in_rot, cosine_table, sine_values):
    half_dim = grad_in_rot.shape[-1] // 2
    first_half = grad_in_rot[..., :half_dim]
    second_half = grad_in_rot[..., half_dim:]
    return jnp.concatenate(
        [
            first_half * cosine_table + second_half * sine_values,
            second_half * cosine_table - first_half * sine_values,
        ],
        axis=-1,
    )


def masked_scores(query_rotated, key_rotated, allowed):
    scores = jnp.einsum(
        "qkgd,skd->kgqs", query_rotated, key_rotated, preferred_element_type=jnp.float32
    ) * HEAD_SIZE ** (-0.5)
    return jnp.where(allowed[None, None], scores, -jnp.inf)


def swap(value, axis_name):
    return lax.ppermute(value, axis_name, [(0, 1), (1, 0)])


def sum_over_tp(value):
    mine = value.astype(jnp.bfloat16)
    return mine.astype(jnp.float32) + swap(mine, "tp").astype(jnp.float32)


def block_sum(partial, nf):
    return lax.psum_scatter(partial, ("fsdp", "ctx"), scatter_dimension=0, tiled=True)


def by_shard(rows, nf):
    count, width = rows.shape
    return rows.reshape(count, nf, width // nf).transpose(1, 0, 2).reshape(nf * count, width // nf)


def on_device(
    hidden_in,
    segment_ids,
    routes,
    attn_gain,
    qk_gains,
    w_query,
    key_projection,
    value_projection,
    w_out,
    ffn_gain,
    w_router,
    w_gate,
    w_up,
    w_down,
    grad_out,
):
    tokens_dev, width_dim = hidden_in.shape
    nf = lax.axis_size("fsdp")
    devices = nf * lax.axis_size("ctx")
    local_experts = w_gate.shape[0]
    experts = local_experts * devices
    capacity = max(2, 2 * tokens_dev * TOPK // experts)
    query_group_width = QUERY_HEADS // KEY_VALUE_HEADS
    shard_width = attn_gain.shape[0]
    f_index, c_index = lax.axis_index("fsdp"), lax.axis_index("ctx")
    bf16 = jnp.bfloat16
    f32 = jnp.float32

    pieces = [w_router.reshape(-1), attn_gain, ffn_gain, qk_gains]
    flat = jnp.concatenate(pieces)
    small_rows = -(-flat.shape[0] // 2048) * 16
    small = jnp.pad(flat, (0, small_rows * 128 - flat.shape[0])).reshape(small_rows, 128)
    out_form = "row" if shard_width % 128 else "col"
    small_all, query_weight, key_weight, value_weight, out_weight, grad_all = plane_gather(
        [
            Gather(small, nf, chunks=1),
            Gather(w_query, nf, half=True, chunks=2),
            Gather(key_projection, nf, half=True, chunks=1),
            Gather(value_projection, nf, half=True, chunks=1),
            Gather(w_out, nf, form=out_form, half=True, chunks=2),
            Gather(grad_out, nf, rep=True, chunks=4),
        ],
        1,
        nf,
    )
    if out_form == "row":
        out_weight = out_weight.reshape(nf, -1, shard_width).transpose(1, 0, 2)
        out_weight = out_weight.reshape(-1, width_dim)
    small_all = small_all.reshape(nf, 2, small_rows * 128)[:, 0]
    ends = [0]
    for piece in pieces:
        ends.append(ends[-1] + piece.shape[0])
    router_weight = small_all[:, ends[0] : ends[1]].reshape(width_dim, experts)
    gain_one = small_all[:, ends[1] : ends[2]].reshape(-1).astype(f32)
    gain_two = small_all[:, ends[2] : ends[3]].reshape(-1).astype(f32)
    gain_qk = small_all[:, ends[3] : ends[4]].reshape(-1).astype(f32)
    gain_query, gain_key = gain_qk[:HEAD_SIZE], gain_qk[HEAD_SIZE:]

    kv_local = key_weight.shape[1] // HEAD_SIZE
    head_local = query_weight.shape[1] // HEAD_SIZE
    resid = hidden_in.astype(f32)
    scaled_one, normed_one, inverse_one = norm_forward(resid, gain_one)
    hidden_first = scaled_one.astype(bf16)
    query_raw = jnp.dot(hidden_first, query_weight, preferred_element_type=f32).reshape(
        tokens_dev, head_local, HEAD_SIZE
    )
    key_projected = jnp.dot(hidden_first, key_weight, preferred_element_type=f32).reshape(
        tokens_dev, kv_local, HEAD_SIZE
    )
    value_rows = jnp.dot(hidden_first, value_weight, preferred_element_type=f32).astype(bf16)
    query_normed, query_hat, query_inverse = norm_forward(query_raw, gain_query)
    key_normed, key_unit_rows, key_inverse_norm = norm_forward(key_projected, gain_key)
    own_positions = c_index * tokens_dev + jnp.arange(tokens_dev, dtype=jnp.int32)
    cosine_table, sine_values = rope_tables(own_positions)
    query_rotated = (
        rotate(query_normed, cosine_table, sine_values)
        .astype(bf16)
        .reshape(tokens_dev, kv_local, query_group_width, HEAD_SIZE)
    )
    key_rotated = rotate(key_normed, cosine_table, sine_values).astype(bf16)
    own_segments = segment_ids.astype(bf16)
    packed_kv = jnp.concatenate(
        [
            key_rotated.reshape(tokens_dev, -1),
            value_rows,
            jnp.broadcast_to(own_segments[:, None], (tokens_dev, 128)),
        ],
        axis=1,
    )
    kv_all = lax.all_gather(packed_kv, "ctx", axis=0, tiled=True)
    kv_width = kv_local * HEAD_SIZE
    key_all = kv_all[:, :kv_width].reshape(-1, kv_local, HEAD_SIZE)
    value_all = kv_all[:, kv_width : 2 * kv_width].reshape(-1, kv_local, HEAD_SIZE)
    segment_all = kv_all[:, 2 * kv_width]
    key_positions = jnp.arange(key_all.shape[0], dtype=jnp.int32)
    allowed = (key_positions[None, :] <= own_positions[:, None]) & (
        segment_all[None, :] == own_segments[:, None]
    )
    scores = masked_scores(query_rotated, key_all, allowed)
    top_score = jnp.max(scores, axis=-1, keepdims=True)
    log_total = top_score + jnp.log(jnp.sum(jnp.exp(scores - top_score), axis=-1, keepdims=True))
    weights_att = jnp.exp(scores - log_total).astype(bf16)
    attended = jnp.einsum("kgqs,skd->qkgd", weights_att, value_all, preferred_element_type=f32)
    attended = attended.astype(bf16).reshape(tokens_dev, head_local * HEAD_SIZE)
    out_partial = jnp.dot(attended, out_weight, preferred_element_type=f32)
    resid_mid = resid + sum_over_tp(out_partial)
    scaled_two, normed_two, inverse_two = norm_forward(resid_mid, gain_two)
    hidden_two = scaled_two.astype(bf16)
    logits = jnp.dot(hidden_two, router_weight, preferred_element_type=f32)
    expert_ids = jnp.arange(experts, dtype=jnp.int32)
    hits = routes[:, :, None] == expert_ids[None, None, :]
    routed = jnp.any(hits, axis=1)
    masked_logits = jnp.where(routed, logits, -jnp.inf)
    raised = jnp.where(
        routed, jnp.exp(masked_logits - jnp.max(masked_logits, axis=1, keepdims=True)), 0.0
    )
    probs = raised / jnp.sum(raised, axis=1, keepdims=True)
    marks = jnp.where(routed, probs, -1.0).T

    hidden_all, marks_all, hidden_first_slice = plane_gather(
        [
            Gather(hidden_two, nf, rep=True, chunks=4),
            Gather(marks, nf, chunks=1),
            Gather(by_shard(hidden_first, nf), nf, form="a2a", chunks=1),
        ],
        2,
        nf,
    )
    first_expert = (f_index * 2 + c_index) * local_experts
    marks_here = lax.dynamic_slice_in_dim(
        marks_all.reshape(devices, experts, tokens_dev), first_expert, local_experts, axis=1
    )
    taken = marks_here >= 0.0
    ranks = jnp.cumsum(taken.astype(jnp.int32), axis=2) - 1
    slots = jnp.arange(capacity, dtype=jnp.int32)
    chosen = taken[:, :, None, :] & (ranks[:, :, None, :] == slots[None, None, :, None])
    pick = chosen.astype(bf16)
    weight_slot = jnp.sum(jnp.where(chosen, marks_here[:, :, None, :], 0.0), axis=3)
    weight_slot = weight_slot.transpose(1, 0, 2).reshape(local_experts, devices * capacity)

    def select(rows):
        blocks = rows.reshape(devices, tokens_dev, width_dim)
        out = jnp.einsum("bjst,btd->jbsd", pick, blocks, preferred_element_type=f32)
        return out.astype(bf16).reshape(local_experts, devices * capacity, width_dim)

    def spread(rows):
        blocks = rows.reshape(local_experts, devices, capacity, width_dim)
        out = jnp.einsum("bjst,jbsd->btd", pick, blocks, preferred_element_type=f32)
        return out.astype(bf16).reshape(devices * tokens_dev, width_dim)

    rows_in = select(hidden_all)
    grad_rows_in = select(grad_all)
    gate_pre = jnp.einsum("jrd,jdf->jrf", rows_in, w_gate, preferred_element_type=f32)
    up_pre = jnp.einsum("jrd,jdf->jrf", rows_in, w_up, preferred_element_type=f32)
    sigmoid_gate = jax.nn.sigmoid(gate_pre)
    silu_gate = gate_pre * sigmoid_gate
    activated = (silu_gate * up_pre).astype(bf16)
    produced = jnp.einsum("jrf,jfd->jrd", activated, w_down, preferred_element_type=f32).astype(
        bf16
    )
    wide = produced.astype(f32)
    grad_prob_slot = jnp.sum(wide * grad_rows_in.astype(f32), axis=2)
    grad_prob_part = jnp.sum(
        jnp.where(
            chosen,
            grad_prob_slot.reshape(local_experts, devices, capacity).transpose(1, 0, 2)[..., None],
            0.0,
        ),
        axis=2,
    )
    moe_partial = spread((weight_slot[:, :, None] * wide).astype(bf16))
    grad_prod = (weight_slot[:, :, None] * grad_rows_in.astype(f32)).astype(bf16)
    grad_act = jnp.einsum("jrd,jfd->jrf", grad_prod, w_down, preferred_element_type=f32)
    grad_gate_pre = (
        grad_act * up_pre * (sigmoid_gate * (1.0 + gate_pre * (1.0 - sigmoid_gate)))
    ).astype(bf16)
    grad_up_pre = (grad_act * silu_gate).astype(bf16)
    grad_slots = jnp.einsum("jrf,jdf->jrd", grad_gate_pre, w_gate, preferred_element_type=f32)
    grad_slots = (
        grad_slots + jnp.einsum("jrf,jdf->jrd", grad_up_pre, w_up, preferred_element_type=f32)
    ).astype(bf16)
    hidden_grad_partial = spread(grad_slots)
    grad_down = jnp.einsum("jrf,jrd->jfd", activated, grad_prod, preferred_element_type=f32)
    grad_gate = jnp.einsum("jrd,jrf->jdf", rows_in, grad_gate_pre, preferred_element_type=f32)
    grad_up = jnp.einsum("jrd,jrf->jdf", rows_in, grad_up_pre, preferred_element_type=f32)

    grad_hidden_moe = sum_over_tp(block_sum(hidden_grad_partial, nf))
    grad_prob = lax.all_to_all(
        grad_prob_part, ("fsdp", "ctx"), split_axis=0, concat_axis=0, tiled=True
    ).reshape(experts, tokens_dev)
    grad_prob = grad_prob + swap(grad_prob, "tp")
    grad_prob = grad_prob.T
    block_out = (resid_mid + sum_over_tp(block_sum(moe_partial, nf))).astype(bf16)

    grad_rows = grad_out.astype(f32)
    grad_logits = (
        probs * (grad_prob - jnp.sum(probs * grad_prob, axis=1, keepdims=True))
    ).astype(bf16)
    grad_hidden_two = grad_hidden_moe + jnp.einsum(
        "te,de->td", grad_logits, router_weight, preferred_element_type=f32
    )
    grad_ffn_local = jnp.sum(grad_hidden_two * normed_two, axis=0)
    grad_mid = grad_rows + rms_norm_gradient(grad_hidden_two, normed_two, inverse_two, gain_two)
    grad_proj = grad_mid.astype(bf16)
    attended_gradient = jnp.einsum(
        "td,qd->tq", grad_proj, out_weight, preferred_element_type=f32
    ).astype(bf16)
    attended_gradient = attended_gradient.reshape(
        tokens_dev, kv_local, query_group_width, HEAD_SIZE
    )
    probs_att = jnp.exp(scores - log_total)
    grad_value_all = jnp.einsum(
        "kgqs,qkgd->skd", weights_att, attended_gradient, preferred_element_type=f32
    )
    grad_probs = jnp.einsum(
        "qkgd,skd->kgqs", attended_gradient, value_all, preferred_element_type=f32
    )
    delta_row = jnp.sum(probs_att * grad_probs, axis=-1, keepdims=True)
    grad_scores = (probs_att * (grad_probs - delta_row) * HEAD_SIZE ** (-0.5)).astype(bf16)
    grad_query_rot = jnp.einsum(
        "kgqs,skd->qkgd", grad_scores, key_all, preferred_element_type=f32
    ).reshape(tokens_dev, head_local, HEAD_SIZE)
    grad_key_all = jnp.einsum(
        "kgqs,qkgd->skd", grad_scores, query_rotated, preferred_element_type=f32
    )
    grad_kv_all = jnp.concatenate(
        [grad_key_all.reshape(-1, kv_width), grad_value_all.reshape(-1, kv_width)], axis=1
    )
    theirs = lax.dynamic_slice_in_dim(grad_kv_all, (1 - c_index) * tokens_dev, tokens_dev, axis=0)
    mine = lax.dynamic_slice_in_dim(grad_kv_all, c_index * tokens_dev, tokens_dev, axis=0)
    grad_kv = mine + swap(theirs.astype(bf16), "ctx").astype(f32)
    key_rotated_gradient = grad_kv[:, :kv_width].reshape(tokens_dev, kv_local, HEAD_SIZE)
    grad_query_norm = inverse_rotation(grad_query_rot, cosine_table, sine_values)
    key_normed_gradient = inverse_rotation(key_rotated_gradient, cosine_table, sine_values)
    grad_qk_local = jnp.concatenate(
        [
            jnp.sum(grad_query_norm * query_hat, axis=(0, 1)),
            jnp.sum(key_normed_gradient * key_unit_rows, axis=(0, 1)),
        ]
    )
    grad_query_raw = (
        rms_norm_gradient(grad_query_norm, query_hat, query_inverse, gain_query)
        .astype(bf16)
        .reshape(tokens_dev, head_local * HEAD_SIZE)
    )
    key_projected_gradient = (
        rms_norm_gradient(key_normed_gradient, key_unit_rows, key_inverse_norm, gain_key)
        .astype(bf16)
        .reshape(tokens_dev, kv_width)
    )
    value_projected_gradient = grad_kv[:, kv_width:].astype(bf16)
    grad_hidden_part = jnp.einsum(
        "tq,dq->td", grad_query_raw, query_weight, preferred_element_type=f32
    )
    grad_hidden_part = grad_hidden_part + jnp.einsum(
        "tq,dq->td", key_projected_gradient, key_weight, preferred_element_type=f32
    )
    grad_hidden_part = grad_hidden_part + jnp.einsum(
        "tq,dq->td", value_projected_gradient, value_weight, preferred_element_type=f32
    )
    grad_hidden_one = sum_over_tp(grad_hidden_part)
    grad_in = grad_mid + rms_norm_gradient(grad_hidden_one, normed_one, inverse_one, gain_one)
    grad_attn_local = jnp.sum(grad_hidden_one * normed_one, axis=0)
    grad_qk_local = grad_qk_local + swap(grad_qk_local, "tp")
    tail = jnp.concatenate([grad_attn_local, grad_ffn_local, grad_qk_local])
    tail = jnp.pad(tail, (0, -tail.shape[0] % 1024)).reshape(-1, 128)
    tail_rows = tail.shape[0]
    logit_pad = jnp.pad(grad_logits, ((0, 0), (0, -experts % 128)))

    dq_all, dk_all, dv_all, attended_all, proj_slice, logits_all, tail_all = plane_gather(
        [
            Gather(grad_query_raw, nf, chunks=2),
            Gather(key_projected_gradient, nf, chunks=1),
            Gather(value_projected_gradient, nf, chunks=1),
            Gather(attended, nf, chunks=2),
            Gather(by_shard(grad_proj, nf), nf, form="a2a", chunks=1),
            Gather(logit_pad, nf, chunks=1),
            Gather(tail, nf, chunks=1),
        ],
        3,
        nf,
    )
    over_tokens = functools.partial(
        jnp.einsum, "td,tq->dq", preferred_element_type=f32
    )
    grad_query = over_tokens(hidden_first_slice, dq_all)
    grad_key = over_tokens(hidden_first_slice, dk_all)
    grad_value = over_tokens(hidden_first_slice, dv_all)
    grad_out_proj = over_tokens(attended_all, proj_slice)
    hidden_slice = lax.dynamic_slice_in_dim(hidden_all, f_index * shard_width, shard_width, axis=1)
    grad_router = over_tokens(hidden_slice, logits_all)[:, :experts]
    tail_sum = jnp.sum(tail_all.reshape(devices, tail_rows * 128), axis=0)
    grad_attn = lax.dynamic_slice_in_dim(tail_sum, f_index * shard_width, shard_width)
    grad_ffn = lax.dynamic_slice_in_dim(tail_sum, width_dim + f_index * shard_width, shard_width)
    qk_width = qk_gains.shape[0]
    grad_qk = lax.dynamic_slice_in_dim(tail_sum, 2 * width_dim + f_index * qk_width, qk_width)
    return (
        block_out,
        grad_in,
        grad_attn,
        grad_qk,
        grad_query,
        grad_key,
        grad_value,
        grad_out_proj,
        grad_ffn,
        grad_router,
        grad_gate,
        grad_up,
        grad_down,
    )


def solution(mesh):
    return jax.shard_map(
        on_device,
        mesh=mesh,
        in_specs=(
            P(("fsdp", "ctx"), None),
            P(("fsdp", "ctx")),
            P(("fsdp", "ctx"), None),
            P("fsdp"),
            P("fsdp"),
            P("fsdp", "tp"),
            P("fsdp", "tp"),
            P("fsdp", "tp"),
            P("tp", "fsdp"),
            P("fsdp"),
            P("fsdp", None),
            P(("fsdp", "ctx"), None, "tp"),
            P(("fsdp", "ctx"), None, "tp"),
            P(("fsdp", "ctx"), "tp", None),
            P(("fsdp", "ctx"), None),
        ),
        out_specs=(
            P(("fsdp", "ctx"), None),
            P(("fsdp", "ctx"), None),
            P("fsdp"),
            P("fsdp"),
            P("fsdp", "tp"),
            P("fsdp", "tp"),
            P("fsdp", "tp"),
            P("tp", "fsdp"),
            P("fsdp"),
            P("fsdp", None),
            P(("fsdp", "ctx"), None, "tp"),
            P(("fsdp", "ctx"), None, "tp"),
            P(("fsdp", "ctx"), "tp", None),
        ),
        check_vma=False,
    )
```

```python
import functools

import jax
import jax.numpy as jnp
from jax import lax
from jax.experimental import pallas as pl
from jax.experimental.pallas import tpu as pltpu
from jax.sharding import PartitionSpec as P

QUERY_HEADS = 32
KEY_VALUE_HEADS = 4
HEAD_SIZE = 128
TOPK = 8
MESH = pl.DeviceIdType.MESH

eps_norm = 1e-06
rope_base = 1000000.0

UP, DOWN, ACROSS, PARTNER, SIDE = range(5)


class Gather:
    def __init__(self, array, nf, form="row", half=False, rep=False, chunks=2):
        if nf > 8:
            chunks = 2 if rep else 1
        self.array, self.form, self.half, self.rep, self.chunks = array, form, half, rep, chunks
        self.shape = array.shape
        self.rows = array.shape[0] // 2 if half else array.shape[0]
        self.step = (self.rows // nf if form == "a2a" else self.rows) // chunks

    def out_shape(self, nf):
        rows, cols = self.rows, self.shape[1]
        if self.form == "col":
            return (2 * rows, nf * cols)
        if self.form == "a2a":
            return (2 * rows, cols)
        return (2 * nf * rows, cols)


def gather_engine(nf, specs, ins, outs, stage, recv, send, local):
    n = len(specs)
    nz = nf // 2
    f, c, t = lax.axis_index("fsdp"), lax.axis_index("ctx"), lax.axis_index("tp")
    z, x = f // 2, lax.rem(f, 2)
    has_up, has_down = z + 1 < nz, z > 0
    device = {
        UP: (f + 2, c, t),
        DOWN: (f - 2, c, t),
        ACROSS: (z * 2 + 1 - x, c, t),
        PARTNER: (f, 1 - c, t),
        SIDE: (f, c, 1 - t),
    }
    first = [sum(s.chunks for s in specs[:a]) for a in range(n)]

    def src(a, q, dest_f=None):
        s = specs[a]
        lo = q * s.step
        if s.half:
            lo = c * s.rows + lo
        if s.form == "a2a":
            lo = dest_f * (s.rows // nf) + lo
        return ins[a].at[pl.ds(lo, s.step)]

    def dst(a, q, bf, bc):
        s = specs[a]
        if s.form == "col":
            width = s.shape[1]
            return outs[a].at[
                pl.ds(bc * s.rows + q * s.step, s.step),
                pl.ds(pl.multiple_of(bf * width, width), width),
            ]
        rows = s.rows // nf if s.form == "a2a" else s.rows
        return outs[a].at[pl.ds((bf * 2 + bc) * rows + q * s.step, s.step)]

    def copy(a, q, bf, bc, source, kind, dev=None, slot=None):
        block = bf * 2 + bc if slot is None else slot
        return pltpu.make_async_remote_copy(
            src_ref=source,
            dst_ref=dst(a, q, bf, bc),
            send_sem=send.at[kind, block, first[a] + q],
            recv_sem=recv.at[bf * 2 + bc, first[a] + q],
            device_id=device[kind] if dev is None else dev,
            device_id_type=MESH,
        )

    def in_half(a, q):
        return (q * 2) // specs[a].chunks == t

    def both(*conds):
        conds = [k for k in conds if k is not None]
        if not conds:
            return None
        return functools.reduce(lambda u, v: u & v, conds)

    def when(cond, fn):
        if cond is None:
            fn()
        else:
            pl.when(cond)(fn)

    def go_up(a, q, dist):
        far = (dist + 1 < nz - 1) | in_half(a, q) if specs[a].rep else None
        return both(has_up, far)

    def go_down(a, q, dist):
        far = (dist + 1 < nz - 1) | in_half(a, q) if specs[a].rep else None
        return both(has_down, far)

    def go_across(a, q):
        return in_half(a, q) if specs[a].rep else None

    relays = [(a, q) for a in range(n) if specs[a].form != "a2a" for q in range(specs[a].chunks)]
    direct = [(a, q) for a in range(n) if specs[a].form == "a2a" for q in range(specs[a].chunks)]

    def start():
        for a, q in relays:
            source = src(a, q)
            when(go_up(a, q, 0), lambda: copy(a, q, f, c, source, UP).start())
            when(go_down(a, q, 0), lambda: copy(a, q, f, c, source, DOWN).start())
            when(go_across(a, q), lambda: copy(a, q, f, c, source, ACROSS).start())
            copy(a, q, f, c, source, PARTNER).start()
        for a in range(n):
            own_in(a).start()
        for a in range(n):
            own_in(a).wait()
            own_out(a).start()

    def start_direct():
        for a, q in direct:
            copy(a, q, f, c, src(a, q, f), PARTNER).start()

            def far_send(d, carry):
                there = lax.rem(f + d, nf)
                copy(a, q, f, c, src(a, q, there), UP, dev=(there, c, t), slot=there).start()
                return carry

            lax.fori_loop(1, nf, far_send, 0)

    def own_in(a):
        s = specs[a]
        if s.form == "a2a":
            view = ins[a].at[pl.ds(f * s.step, s.step)]
        elif s.half:
            view = ins[a].at[pl.ds(c * s.rows, s.rows)]
        else:
            view = ins[a]
        return pltpu.make_async_copy(view, stage[a], local.at[0, a])

    def own_out(a):
        s = specs[a]
        if s.form == "col":
            width = s.shape[1]
            view = outs[a].at[
                pl.ds(c * s.rows, s.rows), pl.ds(pl.multiple_of(f * width, width), width)
            ]
        else:
            rows = s.rows // nf if s.form == "a2a" else s.rows
            view = outs[a].at[pl.ds((f * 2 + c) * rows, rows)]
        return pltpu.make_async_copy(stage[a], view, local.at[1, a])

    def arrived(a, q, bf, bc):
        copy(a, q, bf, bc, dst(a, q, bf, bc), PARTNER).wait_recv()

    def pass_on(a, q, bf, kind, cond=None):
        when(cond, lambda: copy(a, q, bf, c, dst(a, q, bf, c), kind).start())

    def column(k):
        for a, q in relays:
            rep = specs[a].rep
            came = ((k < nz - 1) | in_half(a, q)) if rep else None
            aside = (k == nz - 1) if rep else None

            def below():
                bf = (z - k) * 2 + x
                arrived(a, q, bf, c)
                pass_on(a, q, bf, UP, go_up(a, q, k))
                pass_on(a, q, bf, ACROSS, go_across(a, q))
                pass_on(a, q, bf, PARTNER)
                if rep:
                    pass_on(a, q, bf, SIDE, aside)

            def above():
                bf = (z + k) * 2 + x
                arrived(a, q, bf, c)
                pass_on(a, q, bf, DOWN, go_down(a, q, k))
                pass_on(a, q, bf, ACROSS, go_across(a, q))
                pass_on(a, q, bf, PARTNER)
                if rep:
                    pass_on(a, q, bf, SIDE, aside)

            when(both(z - k >= 0, came), below)
            when(both(z + k < nz, came), above)

    def across(k):
        for a, q in relays:
            rep = specs[a].rep

            def take(zz):
                bf = zz * 2 + 1 - x
                arrived(a, q, bf, c)
                pass_on(a, q, bf, PARTNER)
                if rep:
                    pass_on(a, q, bf, SIDE)

            mine = in_half(a, q) if rep else None
            when(both(z - k >= 0, mine), lambda: take(z - k))
            when(both(z + k < nz, k > 0, mine), lambda: take(z + k))

    def aside(k):
        for a, q in relays:
            if not specs[a].rep:
                continue
            other = jnp.logical_not(in_half(a, q))

            def take(bf):
                arrived(a, q, bf, c)
                pass_on(a, q, bf, PARTNER)

            when((z - k >= 0) & other, lambda: take((z - k) * 2 + 1 - x))
            when((z + k < nz) & (k > 0) & other, lambda: take((z + k) * 2 + 1 - x))
            when((z - k >= 0) & (k == nz - 1) & other, lambda: take((z - k) * 2 + x))
            when((z + k < nz) & (k == nz - 1) & other, lambda: take((z + k) * 2 + x))

    def step(k, carry):
        column(k)
        across(k - 1)

        @pl.when(k > 1)
        def _():
            aside(k - 2)

        return carry

    def run():
        lax.fori_loop(1, nz, step, 0)
        across(nz - 1)
        if any(s.rep for s in specs):
            aside(nz - 2)
            aside(nz - 1)

    def run_direct():
        for a, q in direct:

            def far_take(d, carry):
                there = lax.rem(f + nf - d, nf)
                arrived(a, q, there, c)
                pass_on(a, q, there, PARTNER)
                return carry

            lax.fori_loop(1, nf, far_take, 0)

    def take_partner(bf, carry):
        for a, q in relays:
            arrived(a, q, bf, 1 - c)
        return carry

    def land():
        lax.fori_loop(0, nf, take_partner, 0)
        for a in range(n):
            own_out(a).wait()

    def finish(bf, carry):
        zz, xx = bf // 2, lax.rem(bf, 2)
        dist = jnp.abs(zz - z)
        here = xx == x
        for a, q in relays:
            rep = specs[a].rep
            view = dst(a, q, bf, c)

            def sent(kind, cond):
                when(cond, lambda: copy(a, q, bf, c, view, kind).wait_send())

            half = in_half(a, q) if rep else None
            by_z = ((dist < nz - 1) | half) if rep else None
            sent(PARTNER, None)
            sent(UP, both(here, zz <= z, by_z, go_up(a, q, dist)))
            sent(DOWN, both(here, zz >= z, by_z, go_down(a, q, dist)))
            sent(ACROSS, both(here, by_z, go_across(a, q)))
            if rep:
                sent(SIDE, half & (jnp.logical_not(here) | (dist == nz - 1)))
        for a, q in direct:
            arrived(a, q, bf, 1 - c)
            view = dst(a, q, bf, c)
            copy(a, q, bf, c, view, PARTNER).wait_send()

            @pl.when(bf != f)
            def _():
                copy(a, q, bf, c, view, UP, slot=bf).wait_send()

        return carry

    def drain():
        lax.fori_loop(0, nf, finish, 0)

    return start, run, land, start_direct, run_direct, drain


def gather_kernel(nf, specs, *refs):
    n = len(specs)
    ins, outs, scratch = refs[:n], refs[n : 2 * n], refs[2 * n :]
    nz = nf // 2
    f, c, t = lax.axis_index("fsdp"), lax.axis_index("ctx"), lax.axis_index("tp")
    z, x = f // 2, lax.rem(f, 2)
    has_up, has_down = z + 1 < nz, z > 0
    device = {
        UP: (f + 2, c, t),
        DOWN: (f - 2, c, t),
        ACROSS: (z * 2 + 1 - x, c, t),
        PARTNER: (f, 1 - c, t),
        SIDE: (f, c, 1 - t),
    }
    any_a2a = any(s.form == "a2a" for s in specs)
    any_rep = any(s.rep for s in specs)
    barrier = pltpu.get_barrier_semaphore()

    def greet(dev):
        pl.semaphore_signal(barrier, 1, device_id=dev, device_id_type=MESH)

    greeted = 1
    greet(device[PARTNER])
    if any_rep:
        greet(device[SIDE])
        greeted += 1
    if any_a2a:

        def greet_far(d, carry):
            greet((lax.rem(f + d, nf), c, t))
            return carry

        lax.fori_loop(1, nf, greet_far, 0)
        pl.semaphore_wait(barrier, greeted + nf - 1)
    else:
        greet(device[ACROSS])

        @pl.when(has_up)
        def _():
            greet(device[UP])

        @pl.when(has_down)
        def _():
            greet(device[DOWN])

        pl.semaphore_wait(
            barrier, greeted + 1 + has_up.astype(jnp.int32) + has_down.astype(jnp.int32)
        )

    start, run, land, start_direct, run_direct, drain = gather_engine(
        nf, specs, ins, outs, scratch[:n], *scratch[n:]
    )
    start()
    start_direct()
    run()
    run_direct()
    land()
    drain()


def stage_of(s, nf):
    rows = s.rows // nf if s.form == "a2a" else s.rows
    return pltpu.VMEM((rows, s.shape[1]), s.array.dtype)


def plane_gather(specs, collective_id, nf):
    n = len(specs)
    total = sum(s.chunks for s in specs)

    return pl.pallas_call(
        functools.partial(gather_kernel, nf, tuple(specs)),
        out_shape=tuple(jax.ShapeDtypeStruct(s.out_shape(nf), s.array.dtype) for s in specs),
        in_specs=[pl.BlockSpec(memory_space=pl.ANY)] * n,
        out_specs=tuple(pl.BlockSpec(memory_space=pl.ANY) for _ in specs),
        scratch_shapes=[stage_of(s, nf) for s in specs]
        + [
            pltpu.SemaphoreType.DMA((2 * nf, total)),
            pltpu.SemaphoreType.DMA((5, 2 * nf, total)),
            pltpu.SemaphoreType.DMA((2, n)),
        ],
        compiler_params=pltpu.CompilerParams(
            collective_id=collective_id, has_side_effects=True
        ),
    )(*[s.array for s in specs])


CUT = 4


def expert_kernel(nf, capacity, specs, *refs):
    n = len(specs)
    ins, refs = refs[:n], refs[n:]
    (grad_all, wg_hbm, wu_hbm, wd_hbm), refs = refs[:4], refs[4:]
    gathered, refs = refs[:n], refs[n:]
    (out_part, xs_out, de_out, act_out, dg_out, du_out, grad_tok, prob_tok), refs = (
        refs[:8],
        refs[8:],
    )
    stage, refs = refs[:n], refs[n:]
    (recv, send, local), refs = refs[:3], refs[3:]
    (
        wg,
        wu,
        wd,
        x_buf,
        y_buf,
        xs,
        ys,
        de,
        pe,
        bs,
        act,
        dg,
        du,
        w_slot,
        dp_slot,
        pick,
        mk,
        rk,
        y_out,
        part,
        from_partner,
        from_across,
        from_z,
        from_side,
        dp_send,
        dp_recv,
        dp_side,
        marks_v,
        w_sem,
        load_sem,
        store_sem,
        p_send,
        p_recv,
        x_send,
        x_recv,
        z_send,
        z_recv,
        s_send,
        s_recv,
        d_send,
        d_recv,
    ) = refs
    f32, bf16 = jnp.float32, jnp.bfloat16
    nz = nf // 2
    f, c, t = lax.axis_index("fsdp"), lax.axis_index("ctx"), lax.axis_index("tp")
    z, x = f // 2, lax.rem(f, 2)
    me = f * 2 + c
    up, down = (f + 2, c, t), (f - 2, c, t)
    across_dev, partner, side = (z * 2 + 1 - x, c, t), (f, 1 - c, t), (f, c, 1 - t)
    has_up, has_down = z + 1 < nz, z > 0
    tokens = x_buf.shape[0] // 4
    width = x_buf.shape[1]
    slots = 2 * capacity
    rows_unit = 4 * capacity
    hidden = wg.shape[2]
    experts = specs[1].shape[0]
    step_rows = tokens // CUT

    barrier = pltpu.get_barrier_semaphore()

    def greet(d, carry):
        there = lax.rem(me + d, 2 * nf)
        pl.semaphore_signal(
            barrier, 1, device_id=(there // 2, lax.rem(there, 2), t), device_id_type=MESH
        )
        return carry

    lax.fori_loop(1, 2 * nf, greet, 0)
    pl.semaphore_signal(barrier, 1, device_id=side, device_id_type=MESH)
    pl.semaphore_wait(barrier, 2 * nf)

    start, run, land, start_direct, run_direct, drain = gather_engine(
        nf, specs, ins, gathered, stage, recv, send, local
    )
    start()
    weight_loads = [
        pltpu.make_async_copy(src, dst, w_sem.at[i])
        for i, (src, dst) in enumerate(((wg_hbm, wg), (wu_hbm, wu), (wd_hbm, wd)))
    ]
    for load in weight_loads:
        load.start()

    order = 0
    for at, seq in enumerate(visiting_order(nz)):
        code = sum(u * nz**i for i, u in enumerate(seq))
        order = order + code * (z == at).astype(jnp.int32)

    def unit_at(i):
        code = order
        for k in range(nz):
            code = jnp.where(i > k, code // nz, code)
        return lax.rem(code, nz)

    def load_rows(u, which):
        rows = pl.ds(pl.multiple_of(u * 4 * tokens, 4 * tokens), 4 * tokens)
        if which == 0:
            return pltpu.make_async_copy(gathered[0].at[rows], x_buf, load_sem.at[0])
        return pltpu.make_async_copy(grad_all.at[rows], y_buf, load_sem.at[1])

    load_rows(unit_at(0), 1).start()
    run()
    land()
    start_direct()
    load_rows(unit_at(0), 0).start()
    marks_in = pltpu.make_async_copy(gathered[1], marks_v, load_sem.at[2])
    marks_in.start()
    marks_in.wait()
    dp_send[...] = jnp.zeros_like(dp_send)
    first_expert = me * 2
    for b in range(2 * nf):
        for j in range(2):
            mk[2 * b + j : 2 * b + j + 1, :] = marks_v[pl.ds(b * experts + first_expert + j, 1), :]
    taken = jnp.where(mk[...] >= 0.0, 1.0, 0.0).astype(bf16)
    before = lax.broadcasted_iota(jnp.int32, (tokens, tokens), 0)
    after = lax.broadcasted_iota(jnp.int32, (tokens, tokens), 1)
    upper = jnp.where(before <= after, 1.0, 0.0).astype(bf16)
    rk[...] = jnp.dot(taken, upper, preferred_element_type=f32) - 1.0
    for load in weight_loads:
        load.wait()

    def store_unit(u):
        rows = pl.ds(pl.multiple_of(u * rows_unit, rows_unit), rows_unit)
        pairs = [(xs, xs_out), (de, de_out), (act, act_out), (dg, dg_out), (du, du_out)]
        copies = [
            pltpu.make_async_copy(src, dst.at[:, rows], store_sem.at[i])
            for i, (src, dst) in enumerate(pairs)
        ]
        out_rows = pl.ds(pl.multiple_of(u * 4 * tokens, 4 * tokens), 4 * tokens)
        copies.append(pltpu.make_async_copy(y_out, out_part.at[out_rows], store_sem.at[5]))
        return copies

    def chunk(q):
        return pl.ds(q * step_rows, step_rows)

    def p_copy(u, xx, q):
        return pltpu.make_async_remote_copy(
            src_ref=part.at[u * 4 + xx * 2 + 1 - c, chunk(q)],
            dst_ref=from_partner.at[u * 2 + xx, chunk(q)],
            send_sem=p_send.at[u * 2 + xx, q],
            recv_sem=p_recv.at[u * 2 + xx, q],
            device_id=partner,
            device_id_type=MESH,
        )

    def x_copy(u, q):
        return pltpu.make_async_remote_copy(
            src_ref=part.at[u * 4 + (1 - x) * 2 + c, chunk(q)],
            dst_ref=from_across.at[u, chunk(q)],
            send_sem=x_send.at[u, q],
            recv_sem=x_recv.at[u, q],
            device_id=across_dev,
            device_id_type=MESH,
        )

    def z_copy(u, q, way):
        return pltpu.make_async_remote_copy(
            src_ref=part.at[u * 4 + x * 2 + c, chunk(q)],
            dst_ref=from_z.at[way, u, chunk(q)],
            send_sem=z_send.at[u, q],
            recv_sem=z_recv.at[way, u, q],
            device_id=up if way == 0 else down,
            device_id_type=MESH,
        )

    def z_wait(u, q, way):
        pltpu.make_async_remote_copy(
            src_ref=part.at[me, chunk(q)],
            dst_ref=from_z.at[way, u, chunk(q)],
            send_sem=z_send.at[u, q],
            recv_sem=z_recv.at[way, u, q],
            device_id=partner,
            device_id_type=MESH,
        ).wait_recv()

    def s_copy(q):
        return pltpu.make_async_remote_copy(
            src_ref=part.at[me, chunk(q)],
            dst_ref=from_side.at[chunk(q)],
            send_sem=s_send.at[q],
            recv_sem=s_recv.at[q],
            device_id=side,
            device_id_type=MESH,
        )

    def d_copy(b, source=None):
        return pltpu.make_async_remote_copy(
            src_ref=dp_send.at[b],
            dst_ref=dp_recv.at[me if source is None else source],
            send_sem=d_send.at[b],
            recv_sem=d_recv.at[me if source is None else source],
            device_id=(b // 2, lax.rem(b, 2), t),
            device_id_type=MESH,
        )

    def compute(i, u):
        load_rows(u, 0).wait()
        load_rows(u, 1).wait()

        @pl.when(i > 0)
        def _():
            for cp in store_unit(unit_at(i - 1)):
                cp.wait()

        slot_ids = lax.broadcasted_iota(jnp.int32, (capacity, tokens), 0).astype(f32)
        for b in range(4):
            for j in range(2):
                row = pl.ds(2 * (u * 4 + b) + j, 1)
                mark = mk[row, :]
                hit = (rk[row, :] == slot_ids) & (mark >= 0.0)
                pick[b, j * capacity : (j + 1) * capacity, :] = jnp.where(hit, 1.0, 0.0)
                w_slot[j, b * capacity : (b + 1) * capacity, :] = jnp.sum(
                    jnp.where(hit, mark, 0.0), axis=1, keepdims=True
                )
        tile = 512
        for b in range(4):
            chosen = pick[b].astype(bf16)
            for k in range(width // tile):
                cols = slice(k * tile, (k + 1) * tile)
                got = jnp.dot(
                    chosen, x_buf[b * tokens : (b + 1) * tokens, cols], preferred_element_type=f32
                ).astype(bf16)
                gy = jnp.dot(
                    chosen, y_buf[b * tokens : (b + 1) * tokens, cols], preferred_element_type=f32
                )
                for j in range(2):
                    to = slice(b * capacity, (b + 1) * capacity)
                    of = slice(j * capacity, (j + 1) * capacity)
                    xs[j, to, cols] = got[of]
                    ys[j, to, cols] = gy[of].astype(bf16)
                    de[j, to, cols] = (w_slot[j, to, :] * gy[of]).astype(bf16)

        @pl.when(i + 1 < nz)
        def _():
            load_rows(unit_at(i + 1), 0).start()
            load_rows(unit_at(i + 1), 1).start()

        def expert(j, carry):
            gate = jnp.dot(xs[j], wg[j], preferred_element_type=f32)
            upv = jnp.dot(xs[j], wu[j], preferred_element_type=f32)
            sig = 1.0 / (1.0 + jnp.exp(-gate))
            silu = gate * sig
            act[j] = (silu * upv).astype(bf16)
            grad_act = lax.dot_general(
                de[j], wd[j], (((1,), (1,)), ((), ())), preferred_element_type=f32
            )
            dg[j] = (grad_act * upv * (sig * (1.0 + gate * (1.0 - sig)))).astype(bf16)
            du[j] = (grad_act * silu).astype(bf16)
            total = jnp.zeros((rows_unit, 1), f32)
            for k in range(width // tile):
                cols = slice(k * tile, (k + 1) * tile)
                made = jnp.dot(act[j], wd[j, :, cols], preferred_element_type=f32)
                made = made.astype(bf16).astype(f32)
                total = total + jnp.sum(made * ys[j, :, cols].astype(f32), axis=1, keepdims=True)
                weighted = (w_slot[j] * made).astype(bf16)
                back = lax.dot_general(
                    dg[j], wg[j, cols, :], (((1,), (1,)), ((), ())), preferred_element_type=f32
                ) + lax.dot_general(
                    du[j], wu[j, cols, :], (((1,), (1,)), ((), ())), preferred_element_type=f32
                )
                back = back.astype(bf16)
                for b in range(4):
                    of = slice(b * capacity, (b + 1) * capacity)
                    to = pl.ds(pl.multiple_of(j * capacity, capacity), capacity)
                    pe[b, to, cols] = weighted[of]
                    bs[b, to, cols] = back[of]
            for b in range(4):
                to = pl.ds(pl.multiple_of(j * capacity, capacity), capacity)
                dp_slot[b, to, :] = total[b * capacity : (b + 1) * capacity]
            return carry

        lax.fori_loop(0, 2, expert, 0)

        def spread(b):
            chosen = pick[b]
            back = jnp.transpose(chosen).astype(bf16)
            for k in range(width // tile):
                cols = slice(k * tile, (k + 1) * tile)
                part[u * 4 + b, :, cols] = jnp.dot(
                    back, bs[b, :, cols], preferred_element_type=f32
                ).astype(bf16)

        for b in range(4):
            spread(b)
        for xx in range(2):
            for q in range(CUT):
                p_copy(u, xx, q).start()
        for b in range(4):
            back = jnp.transpose(pick[b]).astype(bf16)
            for k in range(width // tile):
                cols = slice(k * tile, (k + 1) * tile)
                y_out[b * tokens : (b + 1) * tokens, cols] = jnp.dot(
                    back, pe[b, :, cols], preferred_element_type=f32
                ).astype(bf16)
            for j in range(2):
                of = slice(j * capacity, (j + 1) * capacity)
                dp_send[u * 4 + b, j : j + 1, :] = jnp.sum(
                    pick[b, of, :] * dp_slot[b, of, :], axis=0, keepdims=True
                )
        for cp in store_unit(u):
            cp.start()
        for b in range(4):
            bb = u * 4 + b

            @pl.when(bb != me)
            def _():
                d_copy(bb).start()

    def wide(ref):
        return ref.astype(f32)

    def to_across(u):
        for q in range(CUT):
            for xx in range(2):
                p_copy(u, xx, q).wait_recv()
            blk = u * 4 + (1 - x) * 2 + c
            part[blk, chunk(q)] = (
                wide(part[blk, chunk(q)]) + wide(from_partner[u * 2 + 1 - x, chunk(q)])
            ).astype(bf16)
            x_copy(u, q).start()

    def along(u):
        blk = u * 4 + x * 2 + c
        for q in range(CUT):
            x_copy(u, q).wait_recv()

            def total():
                return (
                    wide(part[blk, chunk(q)])
                    + wide(from_partner[u * 2 + x, chunk(q)])
                    + wide(from_across[u, chunk(q)])
                )

            def hop(way, has_before):
                @pl.when(has_before)
                def _():
                    z_wait(u, q, way)
                    part[blk, chunk(q)] = (total() + wide(from_z[way, u, chunk(q)])).astype(bf16)

                @pl.when(jnp.logical_not(has_before))
                def _():
                    part[blk, chunk(q)] = total().astype(bf16)

                z_copy(u, q, way).start()

            @pl.when(u > z)
            def _():
                hop(0, has_down)

            @pl.when(u < z)
            def _():
                hop(1, has_up)

            @pl.when(u == z)
            def _():
                grad_tok[chunk(q)] = total()

                @pl.when(has_down)
                def _():
                    z_wait(u, q, 0)
                    grad_tok[chunk(q)] = grad_tok[chunk(q)] + wide(from_z[0, u, chunk(q)])

                @pl.when(has_up)
                def _():
                    z_wait(u, q, 1)
                    grad_tok[chunk(q)] = grad_tok[chunk(q)] + wide(from_z[1, u, chunk(q)])

                part[blk, chunk(q)] = grad_tok[chunk(q)].astype(bf16)
                s_copy(q).start()

    def unit(i, carry):
        u = unit_at(i)
        compute(i, u)

        @pl.when(i > 0)
        def _():
            along(unit_at(i - 1))

        to_across(u)
        return carry

    lax.fori_loop(0, nz, unit, 0)
    along(z)

    dp_recv[me] = dp_send[me]

    def take_prob(d, carry):
        d_copy(me, lax.rem(me + d, 2 * nf)).wait_recv()
        return carry

    lax.fori_loop(1, 2 * nf, take_prob, 0)
    swap_prob = pltpu.make_async_remote_copy(
        src_ref=dp_recv,
        dst_ref=dp_side,
        send_sem=s_send.at[CUT],
        recv_sem=s_recv.at[CUT],
        device_id=side,
        device_id_type=MESH,
    )
    swap_prob.start()
    run_direct()
    for q in range(CUT):
        s_copy(q).wait_recv()
        grad_tok[chunk(q)] = wide(part[me, chunk(q)]) + wide(from_side[chunk(q)])
    swap_prob.wait_recv()
    prob_tok[...] = dp_recv[...] + dp_side[...]

    for cp in store_unit(z):
        cp.wait()
    swap_prob.wait_send()

    def ends(u, carry):
        for q in range(CUT):
            for xx in range(2):
                p_copy(u, xx, q).wait_send()
            x_copy(u, q).wait_send()

            @pl.when(u > z)
            def _():
                z_copy(u, q, 0).wait_send()

            @pl.when(u < z)
            def _():
                z_copy(u, q, 1).wait_send()

        for b in range(4):

            @pl.when(u * 4 + b != me)
            def _():
                d_copy(u * 4 + b).wait_send()

        return carry

    lax.fori_loop(0, nz, ends, 0)
    for q in range(CUT):
        s_copy(q).wait_send()

    drain()


def visiting_order(nz):
    rows = []
    for at in range(nz):
        rows.append(sorted(range(nz), key=lambda u: (-abs(u - at), u if at < nz // 2 else -u)))
    return rows


def expert_pass(hidden_two, marks, hidden_slices, grad_all, w_gate, w_up, w_down, capacity, nf):
    specs = [
        Gather(hidden_two, nf, rep=True, chunks=4),
        Gather(marks, nf, chunks=1),
        Gather(hidden_slices, nf, form="a2a", chunks=1),
    ]
    n = len(specs)
    f32, bf16 = jnp.float32, jnp.bfloat16
    tokens, width = hidden_two.shape
    nz = nf // 2
    total = sum(s.chunks for s in specs)
    hidden = w_gate.shape[2]
    rows = 2 * nf * capacity
    unit_rows = 4 * capacity
    slots = 2 * capacity
    any_spec = pl.BlockSpec(memory_space=pl.ANY)
    vmem = pl.BlockSpec(memory_space=pltpu.VMEM)
    dma = pltpu.SemaphoreType.DMA
    outs = [jax.ShapeDtypeStruct(s.out_shape(nf), s.array.dtype) for s in specs] + [
        jax.ShapeDtypeStruct((2 * nf * tokens, width), bf16),
        jax.ShapeDtypeStruct((2, rows, width), bf16),
        jax.ShapeDtypeStruct((2, rows, width), bf16),
        jax.ShapeDtypeStruct((2, rows, hidden), bf16),
        jax.ShapeDtypeStruct((2, rows, hidden), bf16),
        jax.ShapeDtypeStruct((2, rows, hidden), bf16),
        jax.ShapeDtypeStruct((tokens, width), f32),
        jax.ShapeDtypeStruct((2 * nf, 8, tokens), f32),
    ]
    result = pl.pallas_call(
        functools.partial(expert_kernel, nf, capacity, tuple(specs)),
        out_shape=tuple(outs),
        in_specs=[any_spec] * (n + 4),
        out_specs=tuple([any_spec] * (n + 6) + [vmem, vmem]),
        scratch_shapes=[stage_of(s, nf) for s in specs]
        + [dma((2 * nf, total)), dma((5, 2 * nf, total)), dma((2, n))]
        + [
            pltpu.VMEM(w_gate.shape, bf16),
            pltpu.VMEM(w_up.shape, bf16),
            pltpu.VMEM(w_down.shape, bf16),
            pltpu.VMEM((4 * tokens, width), bf16),
            pltpu.VMEM((4 * tokens, width), bf16),
            pltpu.VMEM((2, unit_rows, width), bf16),
            pltpu.VMEM((2, unit_rows, width), bf16),
            pltpu.VMEM((2, unit_rows, width), bf16),
            pltpu.VMEM((4, slots, width), bf16),
            pltpu.VMEM((4, slots, width), bf16),
            pltpu.VMEM((2, unit_rows, hidden), bf16),
            pltpu.VMEM((2, unit_rows, hidden), bf16),
            pltpu.VMEM((2, unit_rows, hidden), bf16),
            pltpu.VMEM((2, unit_rows, 1), f32),
            pltpu.VMEM((4, slots, 1), f32),
            pltpu.VMEM((4, slots, tokens), f32),
            pltpu.VMEM((4 * nf, tokens), f32),
            pltpu.VMEM((4 * nf, tokens), f32),
            pltpu.VMEM((4 * tokens, width), bf16),
            pltpu.VMEM((2 * nf, tokens, width), bf16),
            pltpu.VMEM((nf, tokens, width), bf16),
            pltpu.VMEM((nz, tokens, width), bf16),
            pltpu.VMEM((2, nz, tokens, width), bf16),
            pltpu.VMEM((tokens, width), bf16),
            pltpu.VMEM((2 * nf, 8, tokens), f32),
            pltpu.VMEM((2 * nf, 8, tokens), f32),
            pltpu.VMEM((2 * nf, 8, tokens), f32),
            pltpu.VMEM(specs[1].out_shape(nf), f32),
            dma((3,)),
            dma((3,)),
            dma((6,)),
            dma((nf, CUT)),
            dma((nf, CUT)),
            dma((nz, CUT)),
            dma((nz, CUT)),
            dma((nz, CUT)),
            dma((2, nz, CUT)),
            dma((CUT + 1,)),
            dma((CUT + 1,)),
            dma((2 * nf,)),
            dma((2 * nf,)),
        ],
        compiler_params=pltpu.CompilerParams(
            collective_id=7, has_side_effects=True, vmem_limit_bytes=67043328
        ),
    )(*[s.array for s in specs], grad_all, w_gate, w_up, w_down)
    hidden_all, _, hidden_slice = result[:3]
    return (hidden_all, hidden_slice) + tuple(result[3:])


def norm_forward(values, gain_row):
    inverse = lax.rsqrt(jnp.mean(values * values, axis=-1, keepdims=True) + eps_norm)
    normed = values * inverse
    return (normed * gain_row, normed, inverse)


def rms_norm_gradient(grad_scaled, normed, inverse, gain_row):
    grad_normed = grad_scaled * gain_row
    inner_mean = jnp.mean(grad_normed * normed, axis=-1, keepdims=True)
    return inverse * (grad_normed - normed * inner_mean)


def rope_tables(positions):
    half_dim = HEAD_SIZE // 2
    frequencies = rope_base ** (-(jnp.arange(half_dim, dtype=jnp.float32) * 2.0) / HEAD_SIZE)
    angles = positions.astype(jnp.float32)[:, None] * frequencies[None, :]
    return (jnp.cos(angles)[:, None, :], jnp.sin(angles)[:, None, :])


def rotate(values, cosine_table, sine_values):
    half_dim = values.shape[-1] // 2
    first_half = values[..., :half_dim]
    second_half = values[..., half_dim:]
    return jnp.concatenate(
        [
            first_half * cosine_table - second_half * sine_values,
            second_half * cosine_table + first_half * sine_values,
        ],
        axis=-1,
    )


def inverse_rotation(grad_in_rot, cosine_table, sine_values):
    half_dim = grad_in_rot.shape[-1] // 2
    first_half = grad_in_rot[..., :half_dim]
    second_half = grad_in_rot[..., half_dim:]
    return jnp.concatenate(
        [
            first_half * cosine_table + second_half * sine_values,
            second_half * cosine_table - first_half * sine_values,
        ],
        axis=-1,
    )


def masked_scores(query_rotated, key_rotated, allowed):
    scores = jnp.einsum(
        "qkgd,skd->kgqs", query_rotated, key_rotated, preferred_element_type=jnp.float32
    ) * HEAD_SIZE ** (-0.5)
    return jnp.where(allowed[None, None], scores, -jnp.inf)


def swap(value, axis_name):
    return lax.ppermute(value, axis_name, [(0, 1), (1, 0)])


def sum_over_tp(value):
    mine = value.astype(jnp.bfloat16)
    return mine.astype(jnp.float32) + swap(mine, "tp").astype(jnp.float32)


def block_sum(partial, nf):
    return lax.psum_scatter(partial, ("fsdp", "ctx"), scatter_dimension=0, tiled=True)


def by_shard(rows, nf):
    count, width = rows.shape
    return rows.reshape(count, nf, width // nf).transpose(1, 0, 2).reshape(nf * count, width // nf)


def on_device(
    hidden_in,
    segment_ids,
    routes,
    attn_gain,
    qk_gains,
    w_query,
    key_projection,
    value_projection,
    w_out,
    ffn_gain,
    w_router,
    w_gate,
    w_up,
    w_down,
    grad_out,
):
    tokens_dev, width_dim = hidden_in.shape
    nf = lax.axis_size("fsdp")
    devices = nf * lax.axis_size("ctx")
    local_experts = w_gate.shape[0]
    experts = local_experts * devices
    capacity = max(2, 2 * tokens_dev * TOPK // experts)
    query_group_width = QUERY_HEADS // KEY_VALUE_HEADS
    shard_width = attn_gain.shape[0]
    f_index, c_index = lax.axis_index("fsdp"), lax.axis_index("ctx")
    bf16 = jnp.bfloat16
    f32 = jnp.float32

    pieces = [w_router.reshape(-1), attn_gain, ffn_gain, qk_gains]
    flat = jnp.concatenate(pieces)
    small_rows = -(-flat.shape[0] // 2048) * 16
    small = jnp.pad(flat, (0, small_rows * 128 - flat.shape[0])).reshape(small_rows, 128)
    out_form = "row" if shard_width % 128 else "col"
    small_all, query_weight, key_weight, value_weight, out_weight, grad_all = plane_gather(
        [
            Gather(small, nf, chunks=1),
            Gather(w_query, nf, half=True, chunks=2),
            Gather(key_projection, nf, half=True, chunks=1),
            Gather(value_projection, nf, half=True, chunks=1),
            Gather(w_out, nf, form=out_form, half=True, chunks=2),
            Gather(grad_out, nf, rep=True, chunks=4),
        ],
        1,
        nf,
    )
    if out_form == "row":
        out_weight = out_weight.reshape(nf, -1, shard_width).transpose(1, 0, 2)
        out_weight = out_weight.reshape(-1, width_dim)
    small_all = small_all.reshape(nf, 2, small_rows * 128)[:, 0]
    ends = [0]
    for piece in pieces:
        ends.append(ends[-1] + piece.shape[0])
    router_weight = small_all[:, ends[0] : ends[1]].reshape(width_dim, experts)
    gain_one = small_all[:, ends[1] : ends[2]].reshape(-1).astype(f32)
    gain_two = small_all[:, ends[2] : ends[3]].reshape(-1).astype(f32)
    gain_qk = small_all[:, ends[3] : ends[4]].reshape(-1).astype(f32)
    gain_query, gain_key = gain_qk[:HEAD_SIZE], gain_qk[HEAD_SIZE:]

    kv_local = key_weight.shape[1] // HEAD_SIZE
    head_local = query_weight.shape[1] // HEAD_SIZE
    resid = hidden_in.astype(f32)
    scaled_one, normed_one, inverse_one = norm_forward(resid, gain_one)
    hidden_first = scaled_one.astype(bf16)
    query_raw = jnp.dot(hidden_first, query_weight, preferred_element_type=f32).reshape(
        tokens_dev, head_local, HEAD_SIZE
    )
    key_projected = jnp.dot(hidden_first, key_weight, preferred_element_type=f32).reshape(
        tokens_dev, kv_local, HEAD_SIZE
    )
    value_rows = jnp.dot(hidden_first, value_weight, preferred_element_type=f32).astype(bf16)
    query_normed, query_hat, query_inverse = norm_forward(query_raw, gain_query)
    key_normed, key_unit_rows, key_inverse_norm = norm_forward(key_projected, gain_key)
    own_positions = c_index * tokens_dev + jnp.arange(tokens_dev, dtype=jnp.int32)
    cosine_table, sine_values = rope_tables(own_positions)
    query_rotated = (
        rotate(query_normed, cosine_table, sine_values)
        .astype(bf16)
        .reshape(tokens_dev, kv_local, query_group_width, HEAD_SIZE)
    )
    key_rotated = rotate(key_normed, cosine_table, sine_values).astype(bf16)
    own_segments = segment_ids.astype(bf16)
    packed_kv = jnp.concatenate(
        [
            key_rotated.reshape(tokens_dev, -1),
            value_rows,
            jnp.broadcast_to(own_segments[:, None], (tokens_dev, 128)),
        ],
        axis=1,
    )
    kv_all = lax.all_gather(packed_kv, "ctx", axis=0, tiled=True)
    kv_width = kv_local * HEAD_SIZE
    key_all = kv_all[:, :kv_width].reshape(-1, kv_local, HEAD_SIZE)
    value_all = kv_all[:, kv_width : 2 * kv_width].reshape(-1, kv_local, HEAD_SIZE)
    segment_all = kv_all[:, 2 * kv_width]
    key_positions = jnp.arange(key_all.shape[0], dtype=jnp.int32)
    allowed = (key_positions[None, :] <= own_positions[:, None]) & (
        segment_all[None, :] == own_segments[:, None]
    )
    scores = masked_scores(query_rotated, key_all, allowed)
    top_score = jnp.max(scores, axis=-1, keepdims=True)
    log_total = top_score + jnp.log(jnp.sum(jnp.exp(scores - top_score), axis=-1, keepdims=True))
    weights_att = jnp.exp(scores - log_total).astype(bf16)
    attended = jnp.einsum("kgqs,skd->qkgd", weights_att, value_all, preferred_element_type=f32)
    attended = attended.astype(bf16).reshape(tokens_dev, head_local * HEAD_SIZE)
    out_partial = jnp.dot(attended, out_weight, preferred_element_type=f32)
    resid_mid = resid + sum_over_tp(out_partial)
    scaled_two, normed_two, inverse_two = norm_forward(resid_mid, gain_two)
    hidden_two = scaled_two.astype(bf16)
    logits = jnp.dot(hidden_two, router_weight, preferred_element_type=f32)
    expert_ids = jnp.arange(experts, dtype=jnp.int32)
    hits = routes[:, :, None] == expert_ids[None, None, :]
    routed = jnp.any(hits, axis=1)
    masked_logits = jnp.where(routed, logits, -jnp.inf)
    raised = jnp.where(
        routed, jnp.exp(masked_logits - jnp.max(masked_logits, axis=1, keepdims=True)), 0.0
    )
    probs = raised / jnp.sum(raised, axis=1, keepdims=True)
    marks = jnp.where(routed, probs, -1.0).T

    if nf == 8:
        (
            hidden_all,
            hidden_first_slice,
            moe_partial,
            rows_in,
            grad_prod,
            activated,
            grad_gate_pre,
            grad_up_pre,
            grad_hidden_moe,
            grad_prob,
        ) = expert_pass(
            hidden_two,
            marks,
            by_shard(hidden_first, nf),
            grad_all,
            w_gate,
            w_up,
            w_down,
            capacity,
            nf,
        )
        grad_prob = grad_prob.reshape(devices, 8, tokens_dev)[:, :local_experts]
        grad_prob = grad_prob.reshape(experts, tokens_dev).T
    else:
        hidden_all, marks_all, hidden_first_slice = plane_gather(
            [
                Gather(hidden_two, nf, rep=True, chunks=4),
                Gather(marks, nf, chunks=1),
                Gather(by_shard(hidden_first, nf), nf, form="a2a", chunks=1),
            ],
            2,
            nf,
        )
        first_expert = (f_index * 2 + c_index) * local_experts
        marks_here = lax.dynamic_slice_in_dim(
            marks_all.reshape(devices, experts, tokens_dev), first_expert, local_experts, axis=1
        )
        taken = marks_here >= 0.0
        ranks = jnp.cumsum(taken.astype(jnp.int32), axis=2) - 1
        slots = jnp.arange(capacity, dtype=jnp.int32)
        chosen = taken[:, :, None, :] & (ranks[:, :, None, :] == slots[None, None, :, None])
        pick = chosen.astype(bf16)
        weight_slot = jnp.sum(jnp.where(chosen, marks_here[:, :, None, :], 0.0), axis=3)
        weight_slot = weight_slot.transpose(1, 0, 2).reshape(local_experts, devices * capacity)

        def select(rows):
            blocks = rows.reshape(devices, tokens_dev, width_dim)
            out = jnp.einsum("bjst,btd->jbsd", pick, blocks, preferred_element_type=f32)
            return out.astype(bf16).reshape(local_experts, devices * capacity, width_dim)

        def spread(rows):
            blocks = rows.reshape(local_experts, devices, capacity, width_dim)
            out = jnp.einsum("bjst,jbsd->btd", pick, blocks, preferred_element_type=f32)
            return out.astype(bf16).reshape(devices * tokens_dev, width_dim)

        rows_in = select(hidden_all)
        grad_rows_in = select(grad_all)
        gate_pre = jnp.einsum("jrd,jdf->jrf", rows_in, w_gate, preferred_element_type=f32)
        up_pre = jnp.einsum("jrd,jdf->jrf", rows_in, w_up, preferred_element_type=f32)
        sigmoid_gate = jax.nn.sigmoid(gate_pre)
        silu_gate = gate_pre * sigmoid_gate
        activated = (silu_gate * up_pre).astype(bf16)
        produced = jnp.einsum("jrf,jfd->jrd", activated, w_down, preferred_element_type=f32).astype(
            bf16
        )
        wide = produced.astype(f32)
        grad_prob_slot = jnp.sum(wide * grad_rows_in.astype(f32), axis=2)
        grad_prob_part = jnp.sum(
            jnp.where(
                chosen,
                grad_prob_slot.reshape(local_experts, devices, capacity).transpose(1, 0, 2)[..., None],
                0.0,
            ),
            axis=2,
        )
        moe_partial = spread((weight_slot[:, :, None] * wide).astype(bf16))
        grad_prod = (weight_slot[:, :, None] * grad_rows_in.astype(f32)).astype(bf16)
        grad_act = jnp.einsum("jrd,jfd->jrf", grad_prod, w_down, preferred_element_type=f32)
        grad_gate_pre = (
            grad_act * up_pre * (sigmoid_gate * (1.0 + gate_pre * (1.0 - sigmoid_gate)))
        ).astype(bf16)
        grad_up_pre = (grad_act * silu_gate).astype(bf16)
        grad_slots = jnp.einsum("jrf,jdf->jrd", grad_gate_pre, w_gate, preferred_element_type=f32)
        grad_slots = (
            grad_slots + jnp.einsum("jrf,jdf->jrd", grad_up_pre, w_up, preferred_element_type=f32)
        ).astype(bf16)
        hidden_grad_partial = spread(grad_slots)

        grad_hidden_moe = sum_over_tp(block_sum(hidden_grad_partial, nf))
        grad_prob = lax.all_to_all(
            grad_prob_part, ("fsdp", "ctx"), split_axis=0, concat_axis=0, tiled=True
        ).reshape(experts, tokens_dev)
        grad_prob = grad_prob + swap(grad_prob, "tp")
        grad_prob = grad_prob.T
    grad_down = jnp.einsum("jrf,jrd->jfd", activated, grad_prod, preferred_element_type=f32)
    grad_gate = jnp.einsum("jrd,jrf->jdf", rows_in, grad_gate_pre, preferred_element_type=f32)
    grad_up = jnp.einsum("jrd,jrf->jdf", rows_in, grad_up_pre, preferred_element_type=f32)

    block_out = (resid_mid + sum_over_tp(block_sum(moe_partial, nf))).astype(bf16)

    grad_rows = grad_out.astype(f32)
    grad_logits = (
        probs * (grad_prob - jnp.sum(probs * grad_prob, axis=1, keepdims=True))
    ).astype(bf16)
    grad_hidden_two = grad_hidden_moe + jnp.einsum(
        "te,de->td", grad_logits, router_weight, preferred_element_type=f32
    )
    grad_ffn_local = jnp.sum(grad_hidden_two * normed_two, axis=0)
    grad_mid = grad_rows + rms_norm_gradient(grad_hidden_two, normed_two, inverse_two, gain_two)
    grad_proj = grad_mid.astype(bf16)
    attended_gradient = jnp.einsum(
        "td,qd->tq", grad_proj, out_weight, preferred_element_type=f32
    ).astype(bf16)
    attended_gradient = attended_gradient.reshape(
        tokens_dev, kv_local, query_group_width, HEAD_SIZE
    )
    probs_att = jnp.exp(scores - log_total)
    grad_value_all = jnp.einsum(
        "kgqs,qkgd->skd", weights_att, attended_gradient, preferred_element_type=f32
    )
    grad_probs = jnp.einsum(
        "qkgd,skd->kgqs", attended_gradient, value_all, preferred_element_type=f32
    )
    delta_row = jnp.sum(probs_att * grad_probs, axis=-1, keepdims=True)
    grad_scores = (probs_att * (grad_probs - delta_row) * HEAD_SIZE ** (-0.5)).astype(bf16)
    grad_query_rot = jnp.einsum(
        "kgqs,skd->qkgd", grad_scores, key_all, preferred_element_type=f32
    ).reshape(tokens_dev, head_local, HEAD_SIZE)
    grad_key_all = jnp.einsum(
        "kgqs,qkgd->skd", grad_scores, query_rotated, preferred_element_type=f32
    )
    grad_kv_all = jnp.concatenate(
        [grad_key_all.reshape(-1, kv_width), grad_value_all.reshape(-1, kv_width)], axis=1
    )
    theirs = lax.dynamic_slice_in_dim(grad_kv_all, (1 - c_index) * tokens_dev, tokens_dev, axis=0)
    mine = lax.dynamic_slice_in_dim(grad_kv_all, c_index * tokens_dev, tokens_dev, axis=0)
    grad_kv = mine + swap(theirs.astype(bf16), "ctx").astype(f32)
    key_rotated_gradient = grad_kv[:, :kv_width].reshape(tokens_dev, kv_local, HEAD_SIZE)
    grad_query_norm = inverse_rotation(grad_query_rot, cosine_table, sine_values)
    key_normed_gradient = inverse_rotation(key_rotated_gradient, cosine_table, sine_values)
    grad_qk_local = jnp.concatenate(
        [
            jnp.sum(grad_query_norm * query_hat, axis=(0, 1)),
            jnp.sum(key_normed_gradient * key_unit_rows, axis=(0, 1)),
        ]
    )
    grad_query_raw = (
        rms_norm_gradient(grad_query_norm, query_hat, query_inverse, gain_query)
        .astype(bf16)
        .reshape(tokens_dev, head_local * HEAD_SIZE)
    )
    key_projected_gradient = (
        rms_norm_gradient(key_normed_gradient, key_unit_rows, key_inverse_norm, gain_key)
        .astype(bf16)
        .reshape(tokens_dev, kv_width)
    )
    value_projected_gradient = grad_kv[:, kv_width:].astype(bf16)
    grad_hidden_part = jnp.einsum(
        "tq,dq->td", grad_query_raw, query_weight, preferred_element_type=f32
    )
    grad_hidden_part = grad_hidden_part + jnp.einsum(
        "tq,dq->td", key_projected_gradient, key_weight, preferred_element_type=f32
    )
    grad_hidden_part = grad_hidden_part + jnp.einsum(
        "tq,dq->td", value_projected_gradient, value_weight, preferred_element_type=f32
    )
    grad_hidden_one = sum_over_tp(grad_hidden_part)
    grad_in = grad_mid + rms_norm_gradient(grad_hidden_one, normed_one, inverse_one, gain_one)
    grad_attn_local = jnp.sum(grad_hidden_one * normed_one, axis=0)
    grad_qk_local = grad_qk_local + swap(grad_qk_local, "tp")
    tail = jnp.concatenate([grad_attn_local, grad_ffn_local, grad_qk_local])
    tail = jnp.pad(tail, (0, -tail.shape[0] % 1024)).reshape(-1, 128)
    tail_rows = tail.shape[0]
    logit_pad = jnp.pad(grad_logits, ((0, 0), (0, -experts % 128)))

    dq_all, dk_all, dv_all, attended_all, proj_slice, logits_all, tail_all = plane_gather(
        [
            Gather(grad_query_raw, nf, chunks=2),
            Gather(key_projected_gradient, nf, chunks=1),
            Gather(value_projected_gradient, nf, chunks=1),
            Gather(attended, nf, chunks=2),
            Gather(by_shard(grad_proj, nf), nf, form="a2a", chunks=1),
            Gather(logit_pad, nf, chunks=1),
            Gather(tail, nf, chunks=1),
        ],
        3,
        nf,
    )
    over_tokens = functools.partial(
        jnp.einsum, "td,tq->dq", preferred_element_type=f32
    )
    grad_query = over_tokens(hidden_first_slice, dq_all)
    grad_key = over_tokens(hidden_first_slice, dk_all)
    grad_value = over_tokens(hidden_first_slice, dv_all)
    grad_out_proj = over_tokens(attended_all, proj_slice)
    hidden_slice = lax.dynamic_slice_in_dim(hidden_all, f_index * shard_width, shard_width, axis=1)
    grad_router = over_tokens(hidden_slice, logits_all)[:, :experts]
    tail_sum = jnp.sum(tail_all.reshape(devices, tail_rows * 128), axis=0)
    grad_attn = lax.dynamic_slice_in_dim(tail_sum, f_index * shard_width, shard_width)
    grad_ffn = lax.dynamic_slice_in_dim(tail_sum, width_dim + f_index * shard_width, shard_width)
    qk_width = qk_gains.shape[0]
    grad_qk = lax.dynamic_slice_in_dim(tail_sum, 2 * width_dim + f_index * qk_width, qk_width)
    return (
        block_out,
        grad_in,
        grad_attn,
        grad_qk,
        grad_query,
        grad_key,
        grad_value,
        grad_out_proj,
        grad_ffn,
        grad_router,
        grad_gate,
        grad_up,
        grad_down,
    )


def solution(mesh):
    return jax.shard_map(
        on_device,
        mesh=mesh,
        in_specs=(
            P(("fsdp", "ctx"), None),
            P(("fsdp", "ctx")),
            P(("fsdp", "ctx"), None),
            P("fsdp"),
            P("fsdp"),
            P("fsdp", "tp"),
            P("fsdp", "tp"),
            P("fsdp", "tp"),
            P("tp", "fsdp"),
            P("fsdp"),
            P("fsdp", None),
            P(("fsdp", "ctx"), None, "tp"),
            P(("fsdp", "ctx"), None, "tp"),
            P(("fsdp", "ctx"), "tp", None),
            P(("fsdp", "ctx"), None),
        ),
        out_specs=(
            P(("fsdp", "ctx"), None),
            P(("fsdp", "ctx"), None),
            P("fsdp"),
            P("fsdp"),
            P("fsdp", "tp"),
            P("fsdp", "tp"),
            P("fsdp", "tp"),
            P("tp", "fsdp"),
            P("fsdp"),
            P("fsdp", None),
            P(("fsdp", "ctx"), None, "tp"),
            P(("fsdp", "ctx"), None, "tp"),
            P(("fsdp", "ctx"), "tp", None),
        ),
        check_vma=False,
    )
```

```python
import functools

import jax
import jax.numpy as jnp
from jax import lax
from jax.experimental import pallas as pl
from jax.experimental.pallas import tpu as pltpu
from jax.sharding import PartitionSpec as P

QUERY_HEADS = 32
KEY_VALUE_HEADS = 4
HEAD_SIZE = 128
TOPK = 8
MESH = pl.DeviceIdType.MESH

eps_norm = 1e-06
rope_base = 1000000.0

UP, DOWN, ACROSS, PARTNER, SIDE = range(5)


class Gather:
    def __init__(self, array, nf, form="row", half=False, rep=False, chunks=2):
        if nf > 8:
            chunks = 2 if rep else 1
        self.array, self.form, self.half, self.rep, self.chunks = array, form, half, rep, chunks
        self.shape = array.shape
        self.rows = array.shape[0] // 2 if half else array.shape[0]
        self.step = (self.rows // nf if form == "a2a" else self.rows) // chunks

    def out_shape(self, nf):
        rows, cols = self.rows, self.shape[1]
        if self.form == "col":
            return (2 * rows, nf * cols)
        if self.form == "a2a":
            return (2 * rows, cols)
        return (2 * nf * rows, cols)


def gather_engine(nf, specs, ins, outs, stage, recv, send, local):
    n = len(specs)
    nz = nf // 2
    f, c, t = lax.axis_index("fsdp"), lax.axis_index("ctx"), lax.axis_index("tp")
    z, x = f // 2, lax.rem(f, 2)
    has_up, has_down = z + 1 < nz, z > 0
    device = {
        UP: (f + 2, c, t),
        DOWN: (f - 2, c, t),
        ACROSS: (z * 2 + 1 - x, c, t),
        PARTNER: (f, 1 - c, t),
        SIDE: (f, c, 1 - t),
    }
    first = [sum(s.chunks for s in specs[:a]) for a in range(n)]

    def src(a, q, dest_f=None):
        s = specs[a]
        lo = row_chunk(a, q) * s.step
        if s.half:
            lo = c * s.rows + lo
        if s.form == "a2a":
            lo = dest_f * (s.rows // nf) + lo
        return ins[a].at[pl.ds(lo, s.step)]

    def dst(a, q, bf, bc):
        s = specs[a]
        if s.form == "col":
            width = s.shape[1]
            return outs[a].at[
                pl.ds(bc * s.rows + row_chunk(a, q) * s.step, s.step),
                pl.ds(pl.multiple_of(bf * width, width), width),
            ]
        rows = s.rows // nf if s.form == "a2a" else s.rows
        return outs[a].at[pl.ds((bf * 2 + bc) * rows + row_chunk(a, q) * s.step, s.step)]

    def copy(a, q, bf, bc, source, kind, dev=None, slot=None):
        block = bf * 2 + bc if slot is None else slot
        return pltpu.make_async_remote_copy(
            src_ref=source,
            dst_ref=dst(a, q, bf, bc),
            send_sem=send.at[kind, block, first[a] + row_chunk(a, q)],
            recv_sem=recv.at[bf * 2 + bc, first[a] + row_chunk(a, q)],
            device_id=device[kind] if dev is None else dev,
            device_id_type=MESH,
        )

    def row_chunk(a, q):
        n_chunks = specs[a].chunks
        if not specs[a].rep:
            return q
        return lax.rem(q + t * (n_chunks // 2), n_chunks)

    def in_half(a, q):
        return 2 * q < specs[a].chunks

    def both(*conds):
        if any(k is False for k in conds):
            return False
        conds = [k for k in conds if k is not None and k is not True]
        if not conds:
            return None
        return functools.reduce(lambda u, v: u & v, conds)

    def when(cond, fn):
        if cond is None or cond is True:
            fn()
        elif cond is not False:
            pl.when(cond)(fn)

    def go_up(a, q, dist):
        far = dist + 1 < nz - 1 if specs[a].rep and not in_half(a, q) else None
        return both(has_up, far)

    def go_down(a, q, dist):
        far = dist + 1 < nz - 1 if specs[a].rep and not in_half(a, q) else None
        return both(has_down, far)

    def go_across(a, q):
        return in_half(a, q) if specs[a].rep else None

    relays = [(a, q) for a in range(n) if specs[a].form != "a2a" for q in range(specs[a].chunks)]
    direct = [(a, q) for a in range(n) if specs[a].form == "a2a" for q in range(specs[a].chunks)]

    def start(only=None):
        only = range(n) if only is None else only
        for a, q in relays:
            if a not in only:
                continue
            source = src(a, q)
            when(go_up(a, q, 0), lambda: copy(a, q, f, c, source, UP).start())
            when(go_down(a, q, 0), lambda: copy(a, q, f, c, source, DOWN).start())
            when(go_across(a, q), lambda: copy(a, q, f, c, source, ACROSS).start())
            copy(a, q, f, c, source, PARTNER).start()
        own_start([a for a in only if specs[a].form != "a2a"])

    def own_start(only):
        for a in only:
            own_in(a).start()
        for a in only:
            own_in(a).wait()
            own_out(a).start()

    def start_direct():
        own_start(sorted({a for a, _ in direct}))
        for a, q in direct:
            copy(a, q, f, c, src(a, q, f), PARTNER).start()

            def far_send(d, carry):
                there = lax.rem(f + d, nf)
                copy(a, q, f, c, src(a, q, there), UP, dev=(there, c, t), slot=there).start()
                return carry

            lax.fori_loop(1, nf, far_send, 0)

    def own_in(a):
        s = specs[a]
        if s.form == "a2a":
            view = ins[a].at[pl.ds(f * s.step, s.step)]
        elif s.half:
            view = ins[a].at[pl.ds(c * s.rows, s.rows)]
        else:
            view = ins[a]
        return pltpu.make_async_copy(view, stage[a], local.at[0, a])

    def own_out(a):
        s = specs[a]
        if s.form == "col":
            width = s.shape[1]
            view = outs[a].at[
                pl.ds(c * s.rows, s.rows), pl.ds(pl.multiple_of(f * width, width), width)
            ]
        else:
            rows = s.rows // nf if s.form == "a2a" else s.rows
            view = outs[a].at[pl.ds((f * 2 + c) * rows, rows)]
        return pltpu.make_async_copy(stage[a], view, local.at[1, a])

    def arrived(a, q, bf, bc):
        copy(a, q, bf, bc, dst(a, q, bf, bc), PARTNER).wait_recv()

    def pass_on(a, q, bf, kind, cond=None):
        when(cond, lambda: copy(a, q, bf, c, dst(a, q, bf, c), kind).start())

    pair = z + 1 - 2 * lax.rem(z, 2)
    even = lax.rem(z, 2) == 0

    def shared(a, q):
        return not specs[a].rep and specs[a].chunks > 1 and 2 * q >= specs[a].chunks

    def column(k, a, q):
        rep = specs[a].rep
        came = k < nz - 1 if rep and not in_half(a, q) else None
        far = (k == nz - 1) if rep and in_half(a, q) else False

        def take(zz, kind, onward):
            bf = zz * 2 + x
            arrived(a, q, bf, c)
            pass_on(a, q, bf, kind, onward)
            cross = (zz != pair) if shared(a, q) else go_across(a, q)
            pass_on(a, q, bf, ACROSS, cross)
            pass_on(a, q, bf, PARTNER)
            if rep:
                pass_on(a, q, bf, SIDE, far)

        when(both(z - k >= 0, came), lambda: take(z - k, UP, go_up(a, q, k)))
        when(both(z + k < nz, came), lambda: take(z + k, DOWN, go_down(a, q, k)))

    def across(k, a, q):
        rep = specs[a].rep
        mine = in_half(a, q) if rep else None

        def take(zz):
            bf = zz * 2 + 1 - x
            arrived(a, q, bf, c)
            pass_on(a, q, bf, PARTNER)
            if rep:
                pass_on(a, q, bf, SIDE)
            if shared(a, q):
                pass_on(a, q, bf, UP, (zz == z) & even)
                pass_on(a, q, bf, DOWN, (zz == z) & jnp.logical_not(even))

        when(both(z - k >= 0, mine), lambda: take(z - k))
        when(both(z + k < nz, k > 0, mine), lambda: take(z + k))

    def aside(k, a, q):
        if not specs[a].rep:
            return
        if in_half(a, q):
            return

        def take(bf):
            arrived(a, q, bf, c)
            pass_on(a, q, bf, PARTNER)

        when((z - k >= 0), lambda: take((z - k) * 2 + 1 - x))
        when((z + k < nz) & (k > 0), lambda: take((z + k) * 2 + 1 - x))
        when((z - k >= 0) & (k == nz - 1), lambda: take((z - k) * 2 + x))
        when((z + k < nz) & (k == nz - 1), lambda: take((z + k) * 2 + x))

    count = len(relays)
    lag = 2

    def late(fn, k, i):
        if i >= 0:
            fn(k, *relays[i])
        else:
            pl.when(k > 1)(lambda: fn(k - 1, *relays[count + i]))

    by_chunk = all(specs[a].rep for a, _ in relays)

    def step(k, carry):
        if not by_chunk:
            for a, q in relays:
                column(k, a, q)
            for a, q in relays:
                across(k - 1, a, q)

            @pl.when(k > 1)
            def _():
                for a, q in relays:
                    aside(k - 2, a, q)

            return carry
        for i, (a, q) in enumerate(relays):
            column(k, a, q)
            pl.when(k == 1)(lambda: across(0, a, q))
            late(across, k, i - lag)
            if i >= lag:
                pl.when(k == 1)(lambda: aside(0, *relays[i - lag]))
            late(aside, k, i - 2 * lag)

        @pl.when(k == 1)
        def _():
            for a, q in relays[count - lag :]:
                aside(0, a, q)

        return carry

    def run(hook=None):
        def body(k, carry):
            step(k, carry)
            if hook is not None:
                hook(k)
            return carry

        lax.fori_loop(1, nz, body, 0)
        for a, q in relays[count - lag if by_chunk else 0 :]:
            across(nz - 1, a, q)
        if not by_chunk:
            for a, q in relays:
                aside(nz - 2, a, q)
        for a, q in relays[count - 2 * lag if by_chunk else 0 :]:
            aside(nz - 1, a, q)

    def run_direct():
        for a, q in direct:

            def far_take(d, carry):
                there = lax.rem(f + nf - d, nf)
                arrived(a, q, there, c)
                pass_on(a, q, there, PARTNER)
                return carry

            lax.fori_loop(1, nf, far_take, 0)

    def take_partner(bf, carry):
        for a, q in relays:
            arrived(a, q, bf, 1 - c)
        return carry

    def land():
        lax.fori_loop(0, nf, take_partner, 0)
        for a in range(n):
            if specs[a].form != "a2a":
                own_out(a).wait()

    def finish(bf, carry):
        zz, xx = bf // 2, lax.rem(bf, 2)
        dist = jnp.abs(zz - z)
        here = xx == x
        for a, q in relays:
            rep = specs[a].rep
            view = dst(a, q, bf, c)

            def sent(kind, cond):
                when(cond, lambda: copy(a, q, bf, c, view, kind).wait_send())

            half = in_half(a, q) if rep else None
            by_z = dist < nz - 1 if rep and not half else None
            sent(PARTNER, None)
            sent(UP, both(here, zz <= z, by_z, go_up(a, q, dist)))
            sent(DOWN, both(here, zz >= z, by_z, go_down(a, q, dist)))
            cross = (zz != pair) if shared(a, q) else go_across(a, q)
            sent(ACROSS, both(here, by_z, cross))
            if shared(a, q):
                there = jnp.logical_not(here) & (zz == z)
                sent(UP, there & even)
                sent(DOWN, there & jnp.logical_not(even))
            if rep and half:
                sent(SIDE, jnp.logical_not(here) | (dist == nz - 1))
        for a, q in direct:
            arrived(a, q, bf, 1 - c)
            view = dst(a, q, bf, c)
            copy(a, q, bf, c, view, PARTNER).wait_send()

            @pl.when(bf != f)
            def _():
                copy(a, q, bf, c, view, UP, slot=bf).wait_send()

        return carry

    def drain():
        lax.fori_loop(0, nf, finish, 0)
        for a in range(n):
            if specs[a].form == "a2a":
                own_out(a).wait()

    return start, run, land, start_direct, run_direct, drain


def gather_kernel(nf, specs, *refs):
    n = len(specs)
    ins, outs, scratch = refs[:n], refs[n : 2 * n], refs[2 * n :]
    nz = nf // 2
    f, c, t = lax.axis_index("fsdp"), lax.axis_index("ctx"), lax.axis_index("tp")
    z, x = f // 2, lax.rem(f, 2)
    has_up, has_down = z + 1 < nz, z > 0
    device = {
        UP: (f + 2, c, t),
        DOWN: (f - 2, c, t),
        ACROSS: (z * 2 + 1 - x, c, t),
        PARTNER: (f, 1 - c, t),
        SIDE: (f, c, 1 - t),
    }
    any_a2a = any(s.form == "a2a" for s in specs)
    any_rep = any(s.rep for s in specs)
    barrier = pltpu.get_barrier_semaphore()

    def greet(dev):
        pl.semaphore_signal(barrier, 1, device_id=dev, device_id_type=MESH)

    greeted = 1
    greet(device[PARTNER])
    if any_rep:
        greet(device[SIDE])
        greeted += 1
    if any_a2a:

        def greet_far(d, carry):
            greet((lax.rem(f + d, nf), c, t))
            return carry

        lax.fori_loop(1, nf, greet_far, 0)
        pl.semaphore_wait(barrier, greeted + nf - 1)
    else:
        greet(device[ACROSS])

        @pl.when(has_up)
        def _():
            greet(device[UP])

        @pl.when(has_down)
        def _():
            greet(device[DOWN])

        pl.semaphore_wait(
            barrier, greeted + 1 + has_up.astype(jnp.int32) + has_down.astype(jnp.int32)
        )

    start, run, land, start_direct, run_direct, drain = gather_engine(
        nf, specs, ins, outs, scratch[:n], *scratch[n:]
    )
    start()
    start_direct()
    run()
    run_direct()
    land()
    drain()


def stage_of(s, nf):
    rows = s.rows // nf if s.form == "a2a" else s.rows
    return pltpu.VMEM((rows, s.shape[1]), s.array.dtype)


def plane_gather(specs, collective_id, nf):
    n = len(specs)
    total = sum(s.chunks for s in specs)

    return pl.pallas_call(
        functools.partial(gather_kernel, nf, tuple(specs)),
        out_shape=tuple(jax.ShapeDtypeStruct(s.out_shape(nf), s.array.dtype) for s in specs),
        in_specs=[pl.BlockSpec(memory_space=pl.ANY)] * n,
        out_specs=tuple(pl.BlockSpec(memory_space=pl.ANY) for _ in specs),
        scratch_shapes=[stage_of(s, nf) for s in specs]
        + [
            pltpu.SemaphoreType.DMA((2 * nf, total)),
            pltpu.SemaphoreType.DMA((5, 2 * nf, total)),
            pltpu.SemaphoreType.DMA((2, n)),
        ],
        compiler_params=pltpu.CompilerParams(
            collective_id=collective_id, has_side_effects=True
        ),
    )(*[s.array for s in specs])


CUT = 4


def expert_kernel(nf, capacity, specs, *refs):
    n = len(specs)
    ins, refs = refs[:n], refs[n:]
    (grad_all, wg_hbm, wu_hbm, wd_hbm), refs = refs[:4], refs[4:]
    gathered, refs = refs[:n], refs[n:]
    (out_part, xs_out, de_out, act_out, dg_out, du_out, grad_tok, prob_tok), refs = (
        refs[:8],
        refs[8:],
    )
    stage, refs = refs[:n], refs[n:]
    (recv, send, local), refs = refs[:3], refs[3:]
    (
        wg,
        wu,
        wd,
        x_buf,
        y_buf,
        xs,
        ys,
        de,
        pe,
        bs,
        act,
        dg,
        du,
        w_slot,
        dp_slot,
        pick,
        mk,
        rk,
        y_out,
        part,
        from_partner,
        from_across,
        from_z,
        from_side,
        dp_send,
        dp_recv,
        dp_side,
        marks_v,
        w_sem,
        load_sem,
        store_sem,
        p_send,
        p_recv,
        x_send,
        x_recv,
        z_send,
        z_recv,
        s_send,
        s_recv,
        d_send,
        d_recv,
    ) = refs
    f32, bf16 = jnp.float32, jnp.bfloat16
    nz = nf // 2
    f, c, t = lax.axis_index("fsdp"), lax.axis_index("ctx"), lax.axis_index("tp")
    z, x = f // 2, lax.rem(f, 2)
    me = f * 2 + c
    up, down = (f + 2, c, t), (f - 2, c, t)
    across_dev, partner, side = (z * 2 + 1 - x, c, t), (f, 1 - c, t), (f, c, 1 - t)
    has_up, has_down = z + 1 < nz, z > 0
    tokens = x_buf.shape[0] // 4
    width = x_buf.shape[1]
    slots = 2 * capacity
    rows_unit = 4 * capacity
    hidden = wg.shape[2]
    experts = specs[1].shape[0]
    step_rows = tokens // CUT

    barrier = pltpu.get_barrier_semaphore()

    def greet(d, carry):
        there = lax.rem(me + d, 2 * nf)
        pl.semaphore_signal(
            barrier, 1, device_id=(there // 2, lax.rem(there, 2), t), device_id_type=MESH
        )
        return carry

    lax.fori_loop(1, 2 * nf, greet, 0)
    pl.semaphore_signal(barrier, 1, device_id=side, device_id_type=MESH)
    pl.semaphore_wait(barrier, 2 * nf)

    start, run, land, start_direct, run_direct, drain = gather_engine(
        nf, specs, ins, gathered, stage, recv, send, local
    )
    start()
    weight_loads = [
        pltpu.make_async_copy(src, dst, w_sem.at[i])
        for i, (src, dst) in enumerate(((wg_hbm, wg), (wu_hbm, wu), (wd_hbm, wd)))
    ]
    for load in weight_loads:
        load.start()

    order = 0
    for at, seq in enumerate(visiting_order(nz)):
        code = sum(u * nz**i for i, u in enumerate(seq))
        order = order + code * (z == at).astype(jnp.int32)

    def unit_at(i):
        code = order
        for k in range(nz):
            code = jnp.where(i > k, code // nz, code)
        return lax.rem(code, nz)

    def load_rows(u, which):
        rows = pl.ds(pl.multiple_of(u * 4 * tokens, 4 * tokens), 4 * tokens)
        if which == 0:
            return pltpu.make_async_copy(gathered[0].at[rows], x_buf, load_sem.at[0])
        return pltpu.make_async_copy(grad_all.at[rows], y_buf, load_sem.at[1])

    load_rows(unit_at(0), 1).start()
    run()
    land()
    start_direct()
    load_rows(unit_at(0), 0).start()
    marks_in = pltpu.make_async_copy(gathered[1], marks_v, load_sem.at[2])
    marks_in.start()
    marks_in.wait()
    dp_send[...] = jnp.zeros_like(dp_send)
    first_expert = me * 2
    for b in range(2 * nf):
        for j in range(2):
            mk[2 * b + j : 2 * b + j + 1, :] = marks_v[pl.ds(b * experts + first_expert + j, 1), :]
    taken = jnp.where(mk[...] >= 0.0, 1.0, 0.0).astype(bf16)
    before = lax.broadcasted_iota(jnp.int32, (tokens, tokens), 0)
    after = lax.broadcasted_iota(jnp.int32, (tokens, tokens), 1)
    upper = jnp.where(before <= after, 1.0, 0.0).astype(bf16)
    rk[...] = jnp.dot(taken, upper, preferred_element_type=f32) - 1.0
    for load in weight_loads:
        load.wait()

    def store_unit(u):
        rows = pl.ds(pl.multiple_of(u * rows_unit, rows_unit), rows_unit)
        pairs = [(xs, xs_out), (de, de_out), (act, act_out), (dg, dg_out), (du, du_out)]
        copies = [
            pltpu.make_async_copy(src, dst.at[:, rows], store_sem.at[i])
            for i, (src, dst) in enumerate(pairs)
        ]
        out_rows = pl.ds(pl.multiple_of(u * 4 * tokens, 4 * tokens), 4 * tokens)
        copies.append(pltpu.make_async_copy(y_out, out_part.at[out_rows], store_sem.at[5]))
        return copies

    def chunk(q):
        return pl.ds(q * step_rows, step_rows)

    def p_copy(u, xx, q):
        return pltpu.make_async_remote_copy(
            src_ref=part.at[u * 4 + xx * 2 + 1 - c, chunk(q)],
            dst_ref=from_partner.at[u * 2 + xx, chunk(q)],
            send_sem=p_send.at[u * 2 + xx, q],
            recv_sem=p_recv.at[u * 2 + xx, q],
            device_id=partner,
            device_id_type=MESH,
        )

    def x_copy(u, q):
        return pltpu.make_async_remote_copy(
            src_ref=part.at[u * 4 + (1 - x) * 2 + c, chunk(q)],
            dst_ref=from_across.at[u, chunk(q)],
            send_sem=x_send.at[u, q],
            recv_sem=x_recv.at[u, q],
            device_id=across_dev,
            device_id_type=MESH,
        )

    def z_copy(u, q, way):
        return pltpu.make_async_remote_copy(
            src_ref=part.at[u * 4 + x * 2 + c, chunk(q)],
            dst_ref=from_z.at[way, u, chunk(q)],
            send_sem=z_send.at[u, q],
            recv_sem=z_recv.at[way, u, q],
            device_id=up if way == 0 else down,
            device_id_type=MESH,
        )

    def z_wait(u, q, way):
        pltpu.make_async_remote_copy(
            src_ref=part.at[me, chunk(q)],
            dst_ref=from_z.at[way, u, chunk(q)],
            send_sem=z_send.at[u, q],
            recv_sem=z_recv.at[way, u, q],
            device_id=partner,
            device_id_type=MESH,
        ).wait_recv()

    def s_copy(q):
        return pltpu.make_async_remote_copy(
            src_ref=part.at[me, chunk(q)],
            dst_ref=from_side.at[chunk(q)],
            send_sem=s_send.at[q],
            recv_sem=s_recv.at[q],
            device_id=side,
            device_id_type=MESH,
        )

    def d_copy(b, source=None):
        return pltpu.make_async_remote_copy(
            src_ref=dp_send.at[b],
            dst_ref=dp_recv.at[me if source is None else source],
            send_sem=d_send.at[b],
            recv_sem=d_recv.at[me if source is None else source],
            device_id=(b // 2, lax.rem(b, 2), t),
            device_id_type=MESH,
        )

    def compute(i, u):
        load_rows(u, 0).wait()
        load_rows(u, 1).wait()

        @pl.when(i > 0)
        def _():
            for cp in store_unit(unit_at(i - 1)):
                cp.wait()

        slot_ids = lax.broadcasted_iota(jnp.int32, (capacity, tokens), 0).astype(f32)
        for b in range(4):
            for j in range(2):
                row = pl.ds(2 * (u * 4 + b) + j, 1)
                mark = mk[row, :]
                hit = (rk[row, :] == slot_ids) & (mark >= 0.0)
                pick[b, j * capacity : (j + 1) * capacity, :] = jnp.where(hit, 1.0, 0.0)
                w_slot[j, b * capacity : (b + 1) * capacity, :] = jnp.sum(
                    jnp.where(hit, mark, 0.0), axis=1, keepdims=True
                )
        tile = 512
        for b in range(4):
            chosen = pick[b].astype(bf16)
            for k in range(width // tile):
                cols = slice(k * tile, (k + 1) * tile)
                got = jnp.dot(
                    chosen, x_buf[b * tokens : (b + 1) * tokens, cols], preferred_element_type=f32
                ).astype(bf16)
                gy = jnp.dot(
                    chosen, y_buf[b * tokens : (b + 1) * tokens, cols], preferred_element_type=f32
                )
                for j in range(2):
                    to = slice(b * capacity, (b + 1) * capacity)
                    of = slice(j * capacity, (j + 1) * capacity)
                    xs[j, to, cols] = got[of]
                    ys[j, to, cols] = gy[of].astype(bf16)
                    de[j, to, cols] = (w_slot[j, to, :] * gy[of]).astype(bf16)

        @pl.when(i + 1 < nz)
        def _():
            load_rows(unit_at(i + 1), 0).start()
            load_rows(unit_at(i + 1), 1).start()

        def expert(j, carry):
            gate = jnp.dot(xs[j], wg[j], preferred_element_type=f32)
            upv = jnp.dot(xs[j], wu[j], preferred_element_type=f32)
            sig = 1.0 / (1.0 + jnp.exp(-gate))
            silu = gate * sig
            act[j] = (silu * upv).astype(bf16)
            grad_act = lax.dot_general(
                de[j], wd[j], (((1,), (1,)), ((), ())), preferred_element_type=f32
            )
            dg[j] = (grad_act * upv * (sig * (1.0 + gate * (1.0 - sig)))).astype(bf16)
            du[j] = (grad_act * silu).astype(bf16)
            total = jnp.zeros((rows_unit, 1), f32)
            for k in range(width // tile):
                cols = slice(k * tile, (k + 1) * tile)
                made = jnp.dot(act[j], wd[j, :, cols], preferred_element_type=f32)
                made = made.astype(bf16).astype(f32)
                total = total + jnp.sum(made * ys[j, :, cols].astype(f32), axis=1, keepdims=True)
                weighted = (w_slot[j] * made).astype(bf16)
                back = lax.dot_general(
                    dg[j], wg[j, cols, :], (((1,), (1,)), ((), ())), preferred_element_type=f32
                ) + lax.dot_general(
                    du[j], wu[j, cols, :], (((1,), (1,)), ((), ())), preferred_element_type=f32
                )
                back = back.astype(bf16)
                for b in range(4):
                    of = slice(b * capacity, (b + 1) * capacity)
                    to = pl.ds(pl.multiple_of(j * capacity, capacity), capacity)
                    pe[b, to, cols] = weighted[of]
                    bs[b, to, cols] = back[of]
            for b in range(4):
                to = pl.ds(pl.multiple_of(j * capacity, capacity), capacity)
                dp_slot[b, to, :] = total[b * capacity : (b + 1) * capacity]
            return carry

        lax.fori_loop(0, 2, expert, 0)

        def spread(b):
            chosen = pick[b]
            back = jnp.transpose(chosen).astype(bf16)
            for k in range(width // tile):
                cols = slice(k * tile, (k + 1) * tile)
                part[u * 4 + b, :, cols] = jnp.dot(
                    back, bs[b, :, cols], preferred_element_type=f32
                ).astype(bf16)

        for b in range(4):
            spread(b)
        for xx in range(2):
            for q in range(CUT):
                p_copy(u, xx, q).start()
        for b in range(4):
            back = jnp.transpose(pick[b]).astype(bf16)
            for k in range(width // tile):
                cols = slice(k * tile, (k + 1) * tile)
                y_out[b * tokens : (b + 1) * tokens, cols] = jnp.dot(
                    back, pe[b, :, cols], preferred_element_type=f32
                ).astype(bf16)
            for j in range(2):
                of = slice(j * capacity, (j + 1) * capacity)
                dp_send[u * 4 + b, j : j + 1, :] = jnp.sum(
                    pick[b, of, :] * dp_slot[b, of, :], axis=0, keepdims=True
                )
        for cp in store_unit(u):
            cp.start()
        for b in range(4):
            bb = u * 4 + b

            @pl.when(bb != me)
            def _():
                d_copy(bb).start()

    def wide(ref):
        return ref.astype(f32)

    def to_across(u):
        for q in range(CUT):
            for xx in range(2):
                p_copy(u, xx, q).wait_recv()
            blk = u * 4 + (1 - x) * 2 + c
            part[blk, chunk(q)] = (
                wide(part[blk, chunk(q)]) + wide(from_partner[u * 2 + 1 - x, chunk(q)])
            ).astype(bf16)
            x_copy(u, q).start()

    def along(u):
        blk = u * 4 + x * 2 + c
        for q in range(CUT):
            x_copy(u, q).wait_recv()

            def total():
                return (
                    wide(part[blk, chunk(q)])
                    + wide(from_partner[u * 2 + x, chunk(q)])
                    + wide(from_across[u, chunk(q)])
                )

            def hop(way, has_before):
                @pl.when(has_before)
                def _():
                    z_wait(u, q, way)
                    part[blk, chunk(q)] = (total() + wide(from_z[way, u, chunk(q)])).astype(bf16)

                @pl.when(jnp.logical_not(has_before))
                def _():
                    part[blk, chunk(q)] = total().astype(bf16)

                z_copy(u, q, way).start()

            @pl.when(u > z)
            def _():
                hop(0, has_down)

            @pl.when(u < z)
            def _():
                hop(1, has_up)

            @pl.when(u == z)
            def _():
                grad_tok[chunk(q)] = total()

                @pl.when(has_down)
                def _():
                    z_wait(u, q, 0)
                    grad_tok[chunk(q)] = grad_tok[chunk(q)] + wide(from_z[0, u, chunk(q)])

                @pl.when(has_up)
                def _():
                    z_wait(u, q, 1)
                    grad_tok[chunk(q)] = grad_tok[chunk(q)] + wide(from_z[1, u, chunk(q)])

                part[blk, chunk(q)] = grad_tok[chunk(q)].astype(bf16)
                s_copy(q).start()

    def unit(i, carry):
        u = unit_at(i)
        compute(i, u)

        @pl.when(i > 0)
        def _():
            along(unit_at(i - 1))

        to_across(u)
        return carry

    lax.fori_loop(0, nz, unit, 0)
    along(z)

    dp_recv[me] = dp_send[me]

    def take_prob(d, carry):
        d_copy(me, lax.rem(me + d, 2 * nf)).wait_recv()
        return carry

    lax.fori_loop(1, 2 * nf, take_prob, 0)
    swap_prob = pltpu.make_async_remote_copy(
        src_ref=dp_recv,
        dst_ref=dp_side,
        send_sem=s_send.at[CUT],
        recv_sem=s_recv.at[CUT],
        device_id=side,
        device_id_type=MESH,
    )
    swap_prob.start()
    run_direct()
    for q in range(CUT):
        s_copy(q).wait_recv()
        grad_tok[chunk(q)] = wide(part[me, chunk(q)]) + wide(from_side[chunk(q)])
    swap_prob.wait_recv()
    prob_tok[...] = dp_recv[...] + dp_side[...]

    for cp in store_unit(z):
        cp.wait()
    swap_prob.wait_send()

    def ends(u, carry):
        for q in range(CUT):
            for xx in range(2):
                p_copy(u, xx, q).wait_send()
            x_copy(u, q).wait_send()

            @pl.when(u > z)
            def _():
                z_copy(u, q, 0).wait_send()

            @pl.when(u < z)
            def _():
                z_copy(u, q, 1).wait_send()

        for b in range(4):

            @pl.when(u * 4 + b != me)
            def _():
                d_copy(u * 4 + b).wait_send()

        return carry

    lax.fori_loop(0, nz, ends, 0)
    for q in range(CUT):
        s_copy(q).wait_send()

    drain()


def visiting_order(nz):
    rows = []
    for at in range(nz):
        rows.append(sorted(range(nz), key=lambda u: (-abs(u - at), u if at < nz // 2 else -u)))
    return rows


def expert_pass(hidden_two, marks, hidden_slices, grad_all, w_gate, w_up, w_down, capacity, nf):
    specs = [
        Gather(hidden_two, nf, rep=True, chunks=4),
        Gather(marks, nf, rep=True, chunks=2),
        Gather(hidden_slices, nf, form="a2a", chunks=1),
    ]
    n = len(specs)
    f32, bf16 = jnp.float32, jnp.bfloat16
    tokens, width = hidden_two.shape
    nz = nf // 2
    total = sum(s.chunks for s in specs)
    hidden = w_gate.shape[2]
    rows = 2 * nf * capacity
    unit_rows = 4 * capacity
    slots = 2 * capacity
    any_spec = pl.BlockSpec(memory_space=pl.ANY)
    vmem = pl.BlockSpec(memory_space=pltpu.VMEM)
    dma = pltpu.SemaphoreType.DMA
    outs = [jax.ShapeDtypeStruct(s.out_shape(nf), s.array.dtype) for s in specs] + [
        jax.ShapeDtypeStruct((2 * nf * tokens, width), bf16),
        jax.ShapeDtypeStruct((2, rows, width), bf16),
        jax.ShapeDtypeStruct((2, rows, width), bf16),
        jax.ShapeDtypeStruct((2, rows, hidden), bf16),
        jax.ShapeDtypeStruct((2, rows, hidden), bf16),
        jax.ShapeDtypeStruct((2, rows, hidden), bf16),
        jax.ShapeDtypeStruct((tokens, width), f32),
        jax.ShapeDtypeStruct((2 * nf, 8, tokens), f32),
    ]
    result = pl.pallas_call(
        functools.partial(expert_kernel, nf, capacity, tuple(specs)),
        out_shape=tuple(outs),
        in_specs=[any_spec] * (n + 4),
        out_specs=tuple([any_spec] * (n + 6) + [vmem, vmem]),
        scratch_shapes=[stage_of(s, nf) for s in specs]
        + [dma((2 * nf, total)), dma((5, 2 * nf, total)), dma((2, n))]
        + [
            pltpu.VMEM(w_gate.shape, bf16),
            pltpu.VMEM(w_up.shape, bf16),
            pltpu.VMEM(w_down.shape, bf16),
            pltpu.VMEM((4 * tokens, width), bf16),
            pltpu.VMEM((4 * tokens, width), bf16),
            pltpu.VMEM((2, unit_rows, width), bf16),
            pltpu.VMEM((2, unit_rows, width), bf16),
            pltpu.VMEM((2, unit_rows, width), bf16),
            pltpu.VMEM((4, slots, width), bf16),
            pltpu.VMEM((4, slots, width), bf16),
            pltpu.VMEM((2, unit_rows, hidden), bf16),
            pltpu.VMEM((2, unit_rows, hidden), bf16),
            pltpu.VMEM((2, unit_rows, hidden), bf16),
            pltpu.VMEM((2, unit_rows, 1), f32),
            pltpu.VMEM((4, slots, 1), f32),
            pltpu.VMEM((4, slots, tokens), f32),
            pltpu.VMEM((4 * nf, tokens), f32),
            pltpu.VMEM((4 * nf, tokens), f32),
            pltpu.VMEM((4 * tokens, width), bf16),
            pltpu.VMEM((2 * nf, tokens, width), bf16),
            pltpu.VMEM((nf, tokens, width), bf16),
            pltpu.VMEM((nz, tokens, width), bf16),
            pltpu.VMEM((2, nz, tokens, width), bf16),
            pltpu.VMEM((tokens, width), bf16),
            pltpu.VMEM((2 * nf, 8, tokens), f32),
            pltpu.VMEM((2 * nf, 8, tokens), f32),
            pltpu.VMEM((2 * nf, 8, tokens), f32),
            pltpu.VMEM(specs[1].out_shape(nf), f32),
            dma((3,)),
            dma((3,)),
            dma((6,)),
            dma((nf, CUT)),
            dma((nf, CUT)),
            dma((nz, CUT)),
            dma((nz, CUT)),
            dma((nz, CUT)),
            dma((2, nz, CUT)),
            dma((CUT + 1,)),
            dma((CUT + 1,)),
            dma((2 * nf,)),
            dma((2 * nf,)),
        ],
        compiler_params=pltpu.CompilerParams(
            collective_id=7, has_side_effects=True, vmem_limit_bytes=67043328
        ),
    )(*[s.array for s in specs], grad_all, w_gate, w_up, w_down)
    hidden_all, _, hidden_slice = result[:3]
    return (hidden_all, hidden_slice) + tuple(result[3:])


NT = (((1,), (1,)), ((), ()))
TN = (((0,), (0,)), ((), ()))


def backward_kernel(nf, specs, *refs):
    n = len(specs)
    (
        attended,
        dh2_moe,
        grad_prob,
        probs,
        router,
        x_in,
        x_mid,
        gains,
        grad_out,
        wo_hbm,
        wq_hbm,
        wk_hbm,
        wv_hbm,
        q_raw,
        k_raw,
        q_rot,
        keys,
        values,
        bias,
        lse,
        trig,
        out_part,
    ), refs = refs[:22], refs[22:]
    gathered, grad_in, block_out, refs = refs[:n], refs[n], refs[n + 1], refs[n + 2 :]
    stage, refs = refs[:n], refs[n:]
    (recv, send, local), refs = refs[:3], refs[3:]
    (
        w_big,
        w_key,
        w_value,
        dx1,
        dh2,
        d_out,
        d_out_slices,
        d_attn,
        d_query,
        d_key,
        d_value,
        logit,
        tail,
        dk_acc,
        dv_acc,
        qk_acc,
        kv_send,
        kv_recv,
        dh1,
        dh1_side,
        qk_side,
        row_sum,
        w_sem,
        kv_sem,
        side_send,
        side_recv,
        sum_own,
        sum_total,
        sum_bufs,
        sum_sems,
    ) = refs[:28] + (refs[28:32], refs[32:])
    f32, bf16 = jnp.float32, jnp.bfloat16
    f, c, t = lax.axis_index("fsdp"), lax.axis_index("ctx"), lax.axis_index("tp")
    partner, side = (f, 1 - c, t), (f, c, 1 - t)
    tokens, width = x_in.shape
    experts = probs.shape[1]
    scale = HEAD_SIZE ** (-0.5)

    barrier = pltpu.get_barrier_semaphore()

    def greet(d, carry):
        pl.semaphore_signal(
            barrier, 1, device_id=(lax.rem(f + d, nf), c, t), device_id_type=MESH
        )
        return carry

    lax.fori_loop(1, nf, greet, 0)
    for dev in (partner, side):
        pl.semaphore_signal(barrier, 1, device_id=dev, device_id_type=MESH)
    pl.semaphore_wait(barrier, nf + 1)

    ins = (attended, d_query, d_key, d_value, logit, tail, d_out_slices)
    start, run, land, start_direct, run_direct, drain = gather_engine(
        nf, specs, ins, gathered, stage, recv, send, local
    )
    nz = nf // 2
    order = visit_code(nz, f // 2)
    own_loads, to_partner, to_across, along, finish_sum, drain_sum = token_sum(
        nf, out_part, sum_own, sum_total, sum_bufs, sum_sems
    )
    for cp in own_loads:
        cp.start()
    lax.fori_loop(0, nz, lambda i, carry: to_partner(visit(order, nz, i), carry), 0)
    start((0,))

    def load(src, dst, i):
        return pltpu.make_async_copy(src, dst, w_sem.at[i])

    load(wo_hbm, w_big, 0).start()
    load(wk_hbm, w_key, 1).start()
    load(wv_hbm, w_value, 2).start()

    logit[...] = jnp.zeros_like(logit)
    pr = probs[...]
    gp = grad_prob[...]
    dl = (pr * (gp - jnp.sum(pr * gp, axis=1, keepdims=True))).astype(bf16)
    logit[:, :experts] = dl
    tile = 512
    for k in range(width // tile):
        cols = slice(k * tile, (k + 1) * tile)
        dh2[:, cols] = dh2_moe[:, cols] + lax.dot_general(
            dl, router[cols, :], NT, preferred_element_type=f32
        )
    gain_one, gain_two = gains[0:1, :], gains[1:2, :]
    gain_query, gain_key = gains[2:3, :HEAD_SIZE], gains[2:3, HEAD_SIZE : 2 * HEAD_SIZE]
    row_sum[...] = jnp.zeros_like(row_sum)
    part_rows = 16

    def norm_two(i, carry):
        rows = pl.ds(pl.multiple_of(i * part_rows, part_rows), part_rows)
        x1 = x_mid[rows]
        r2 = lax.rsqrt(jnp.mean(x1 * x1, axis=1, keepdims=True) + eps_norm)
        n2 = x1 * r2
        g = dh2[rows]
        row_sum[1:2, :] += jnp.sum(g * n2, axis=0, keepdims=True)
        scaled = g * gain_two
        mean = jnp.mean(scaled * n2, axis=1, keepdims=True)
        out = grad_out[rows].astype(f32) + r2 * (scaled - n2 * mean)
        dx1[rows] = out
        d_out[rows] = out.astype(bf16)
        return carry

    lax.fori_loop(0, tokens // part_rows, norm_two, 0)
    shard = width // nf
    for k in range(nf):
        d_out_slices[k * tokens : (k + 1) * tokens, :] = d_out[:, k * shard : (k + 1) * shard]

    load(wo_hbm, w_big, 0).wait()
    heads_width = d_attn.shape[1]
    tile = 256
    for k in range(heads_width // tile):
        cols = slice(k * tile, (k + 1) * tile)
        d_attn[:, cols] = lax.dot_general(
            d_out[...], w_big[cols, :], NT, preferred_element_type=f32
        ).astype(bf16)
    load(wq_hbm, w_big, 0).start()
    for cp in own_loads:
        cp.wait()
    lax.fori_loop(0, nz, lambda i, carry: to_across(visit(order, nz, i), carry), 0)
    dk_acc[...] = jnp.zeros_like(dk_acc)
    dv_acc[...] = jnp.zeros_like(dv_acc)
    qk_acc[...] = jnp.zeros_like(qk_acc)
    group = QUERY_HEADS // KEY_VALUE_HEADS

    def unrope(g):
        return g * trig[0] + pltpu.roll(g, HEAD_SIZE // 2, 1) * trig[1]

    def norm_back(g, raw, gain):
        inv = lax.rsqrt(jnp.mean(raw * raw, axis=1, keepdims=True) + eps_norm)
        hat = raw * inv
        scaled = g * gain
        mean = jnp.mean(scaled * hat, axis=1, keepdims=True)
        return jnp.sum(g * hat, axis=0, keepdims=True), inv * (scaled - hat * mean)

    def head(h, carry):
        cols = pl.ds(pl.multiple_of(h * HEAD_SIZE, HEAD_SIZE), HEAD_SIZE)
        kv_cols = pl.ds(pl.multiple_of((h // group) * HEAD_SIZE, HEAD_SIZE), HEAD_SIZE)
        q, key, value, da = q_rot[:, cols], keys[:, kv_cols], values[:, kv_cols], d_attn[:, cols]
        s = lax.dot_general(q, key, NT, preferred_element_type=f32) * scale + bias[...]
        prob = jnp.exp(s - lse[h])
        dp = lax.dot_general(da, value, NT, preferred_element_type=f32)
        delta = jnp.sum(prob * dp, axis=1, keepdims=True)
        ds = (prob * (dp - delta) * scale).astype(bf16)
        dk_acc[:, kv_cols] += lax.dot_general(ds, q, TN, preferred_element_type=f32)
        dv_acc[:, kv_cols] += lax.dot_general(
            prob.astype(bf16), da, TN, preferred_element_type=f32
        )
        dq = unrope(jnp.dot(ds, key, preferred_element_type=f32))
        gain_grad, dq = norm_back(dq, q_raw[:, cols], gain_query)
        qk_acc[0:1, :] += gain_grad
        d_query[:, cols] = dq.astype(bf16)
        return carry

    lax.fori_loop(0, heads_width // HEAD_SIZE, head, 0)

    kv_width = dk_acc.shape[1]
    theirs = pl.ds(pl.multiple_of((1 - c) * tokens, tokens), tokens)
    mine = pl.ds(pl.multiple_of(c * tokens, tokens), tokens)
    kv_send[:, :kv_width] = dk_acc[theirs].astype(bf16)
    kv_send[:, kv_width:] = dv_acc[theirs].astype(bf16)
    swap_kv = pltpu.make_async_remote_copy(
        src_ref=kv_send,
        dst_ref=kv_recv,
        send_sem=kv_sem.at[0],
        recv_sem=kv_sem.at[1],
        device_id=partner,
        device_id_type=MESH,
    )
    swap_kv.start()
    start((1, 4))
    start_direct()
    swap_kv.wait()
    for kv in range(kv_width // HEAD_SIZE):
        cols = slice(kv * HEAD_SIZE, (kv + 1) * HEAD_SIZE)
        g = dk_acc[mine, cols] + kv_recv[:, cols].astype(f32)
        gain_grad, dk = norm_back(unrope(g), k_raw[:, cols], gain_key)
        qk_acc[1:2, :] += gain_grad
        d_key[:, cols] = dk.astype(bf16)
    d_value[...] = (dv_acc[mine] + kv_recv[:, kv_width:].astype(f32)).astype(bf16)
    start((2, 3))

    def to_side(src, dst, i):
        return pltpu.make_async_remote_copy(
            src_ref=src,
            dst_ref=dst,
            send_sem=side_send.at[i],
            recv_sem=side_recv.at[i],
            device_id=side,
            device_id_type=MESH,
        )

    swap_qk = to_side(qk_acc, qk_side, 4)
    swap_qk.start()
    load(wq_hbm, w_big, 0).wait()
    load(wk_hbm, w_key, 1).wait()
    load(wv_hbm, w_value, 2).wait()
    quarter = width // 4

    def dh1_copy(i):
        cols = pl.ds(i * quarter, quarter)
        return to_side(dh1.at[:, cols], dh1_side.at[:, cols], i)

    for k in range(width // tile):
        rows = slice(k * tile, (k + 1) * tile)
        total = lax.dot_general(d_query[...], w_big[rows, :], NT, preferred_element_type=f32)
        total = total + lax.dot_general(d_key[...], w_key[rows, :], NT, preferred_element_type=f32)
        total = total + lax.dot_general(
            d_value[...], w_value[rows, :], NT, preferred_element_type=f32
        )
        dh1[:, rows] = total.astype(bf16)
        if (k + 1) * tile % quarter == 0:
            dh1_copy((k + 1) * tile // quarter - 1).start()
    for i in range(4):
        dh1_copy(i).wait_recv()
    swap_qk.wait_recv()

    def norm_one(i, carry):
        rows = pl.ds(pl.multiple_of(i * part_rows, part_rows), part_rows)
        x0 = x_in[rows].astype(f32)
        r1 = lax.rsqrt(jnp.mean(x0 * x0, axis=1, keepdims=True) + eps_norm)
        n1 = x0 * r1
        g = dh1[rows].astype(f32) + dh1_side[rows].astype(f32)
        row_sum[0:1, :] += jnp.sum(g * n1, axis=0, keepdims=True)
        scaled = g * gain_one
        mean = jnp.mean(scaled * n1, axis=1, keepdims=True)
        grad_in[rows] = dx1[rows] + r1 * (scaled - n1 * mean)
        return carry

    lax.fori_loop(0, tokens // part_rows, norm_one, 0)
    lanes = width // 128
    tail[...] = jnp.zeros_like(tail)
    for which in range(2):
        for k in range(lanes):
            row = which * lanes + k
            tail[row : row + 1, :] = row_sum[which : which + 1, k * 128 : (k + 1) * 128]
    tail[2 * lanes : 2 * lanes + 2, :] = qk_acc[0:2, :] + qk_side[0:2, :]
    start((5,))
    run(lambda k: along(visit(order, nz, k - 1)))
    along(f // 2)
    run_direct()
    land()

    def put_out(rows, value):
        block_out[rows] = (x_mid[rows] + value).astype(bf16)

    finish_sum(put_out)
    drain()
    drain_sum()
    for i in range(4):
        dh1_copy(i).wait_send()
    swap_qk.wait_send()


def visit_code(nz, z):
    order = 0
    for at, seq in enumerate(visiting_order(nz)):
        code = sum(u * nz**i for i, u in enumerate(seq))
        order = order + code * (z == at).astype(jnp.int32)
    return order


def visit(code, nz, i):
    for k in range(nz):
        code = jnp.where(i > k, code // nz, code)
    return lax.rem(code, nz)


SUM_CUT = 2


def token_sum(nf, partial, own, total_ref, bufs, sems):
    from_partner, from_across, from_z, from_side = bufs
    load_sem, p_send, p_recv, x_send, x_recv, z_send, z_recv, s_send, s_recv = sems
    nz = nf // 2
    f, c, t = lax.axis_index("fsdp"), lax.axis_index("ctx"), lax.axis_index("tp")
    z, x = f // 2, lax.rem(f, 2)
    has_up, has_down = z + 1 < nz, z > 0
    up, down = (f + 2, c, t), (f - 2, c, t)
    across_dev, partner, side = (z * 2 + 1 - x, c, t), (f, 1 - c, t), (f, c, 1 - t)
    tokens = total_ref.shape[0]
    rows = tokens // SUM_CUT
    bf16 = jnp.bfloat16

    def chunk(q):
        return pl.ds(q * rows, rows)

    def remote(src, dst, send, recv, dev):
        return pltpu.make_async_remote_copy(
            src_ref=src,
            dst_ref=dst,
            send_sem=send,
            recv_sem=recv,
            device_id=dev,
            device_id_type=MESH,
        )

    own_loads = [
        pltpu.make_async_copy(
            partial.at[pl.ds((2 * b + c) * tokens, tokens)], own.at[b], load_sem.at[b]
        )
        for b in range(nf)
    ]

    def p_copy(u, xx, q):
        b = u * 2 + xx
        return remote(
            partial.at[pl.ds((2 * b + 1 - c) * tokens + q * rows, rows)],
            from_partner.at[b, chunk(q)],
            p_send.at[b, q],
            p_recv.at[b, q],
            partner,
        )

    def x_copy(u, q):
        return remote(
            own.at[u * 2 + 1 - x, chunk(q)],
            from_across.at[u, chunk(q)],
            x_send.at[u, q],
            x_recv.at[u, q],
            across_dev,
        )

    def z_copy(u, q, way, dev):
        return remote(
            own.at[u * 2 + x, chunk(q)],
            from_z.at[way, u, chunk(q)],
            z_send.at[u, q],
            z_recv.at[way, u, q],
            dev,
        )

    def s_copy(q):
        return remote(
            own.at[f, chunk(q)], from_side.at[chunk(q)], s_send.at[q], s_recv.at[q], side
        )

    def wide(value):
        return value.astype(jnp.float32)

    def to_partner(u, carry):
        for xx in range(2):
            for q in range(SUM_CUT):
                p_copy(u, xx, q).start()
        return carry

    def to_across(u, carry):
        b = u * 2 + 1 - x
        for q in range(SUM_CUT):
            for xx in range(2):
                p_copy(u, xx, q).wait_recv()
            own[b, chunk(q)] = (wide(own[b, chunk(q)]) + wide(from_partner[b, chunk(q)])).astype(
                bf16
            )
            x_copy(u, q).start()
        return carry

    def along(u):
        b = u * 2 + x
        for q in range(SUM_CUT):
            x_copy(u, q).wait_recv()
            total_ref[chunk(q)] = (
                wide(own[b, chunk(q)])
                + wide(from_partner[b, chunk(q)])
                + wide(from_across[u, chunk(q)])
            )

            @pl.when((u >= z) & has_down)
            def _():
                z_copy(u, q, 0, partner).wait_recv()
                total_ref[chunk(q)] += wide(from_z[0, u, chunk(q)])

            @pl.when((u <= z) & has_up)
            def _():
                z_copy(u, q, 1, partner).wait_recv()
                total_ref[chunk(q)] += wide(from_z[1, u, chunk(q)])

            own[b, chunk(q)] = total_ref[chunk(q)].astype(bf16)

            @pl.when(u > z)
            def _():
                z_copy(u, q, 0, up).start()

            @pl.when(u < z)
            def _():
                z_copy(u, q, 1, down).start()

            @pl.when(u == z)
            def _():
                s_copy(q).start()

    def finish_sum(put):
        for q in range(SUM_CUT):
            s_copy(q).wait_recv()
            put(chunk(q), wide(own[f, chunk(q)]) + wide(from_side[chunk(q)]))

    def drain_sum():
        def ends(u, carry):
            for q in range(SUM_CUT):
                for xx in range(2):
                    p_copy(u, xx, q).wait_send()
                x_copy(u, q).wait_send()

                @pl.when(u != z)
                def _():
                    z_copy(u, q, 0, partner).wait_send()

            return carry

        lax.fori_loop(0, nz, ends, 0)
        for q in range(SUM_CUT):
            s_copy(q).wait_send()

    return own_loads, to_partner, to_across, along, finish_sum, drain_sum


def backward_pass(nf, arrays, attended, shapes):
    f32, bf16 = jnp.float32, jnp.bfloat16
    tokens, width, heads_width, kv_width, keys = shapes
    tail_rows = -(-(2 * width // 128 + 2) // 8) * 8
    shape = jax.ShapeDtypeStruct
    specs = [
        Gather(attended, nf, chunks=2),
        Gather(shape((tokens, heads_width), bf16), nf, chunks=2),
        Gather(shape((tokens, kv_width), bf16), nf, chunks=1),
        Gather(shape((tokens, kv_width), bf16), nf, chunks=1),
        Gather(shape((tokens, 128), bf16), nf, chunks=1),
        Gather(shape((tail_rows, 128), f32), nf, chunks=1),
        Gather(shape((nf * tokens, width // nf), bf16), nf, form="a2a", chunks=1),
    ]
    n = len(specs)
    total = sum(s.chunks for s in specs)
    any_spec = pl.BlockSpec(memory_space=pl.ANY)
    vmem = pl.BlockSpec(memory_space=pltpu.VMEM)
    dma = pltpu.SemaphoreType.DMA
    in_any = {0, 9, 10, 11, 12, 21}
    nz = nf // 2
    return pl.pallas_call(
        functools.partial(backward_kernel, nf, tuple(specs)),
        out_shape=tuple(shape(s.out_shape(nf), s.array.dtype) for s in specs)
        + (shape((tokens, width), f32), shape((tokens, width), bf16)),
        in_specs=[any_spec if i in in_any else vmem for i in range(22)],
        out_specs=tuple([any_spec] * n + [vmem, vmem]),
        scratch_shapes=[stage_of(s, nf) for s in specs]
        + [dma((2 * nf, total)), dma((5, 2 * nf, total)), dma((2, n))]
        + [
            pltpu.VMEM((width, max(width, heads_width)), bf16),
            pltpu.VMEM((width, kv_width), bf16),
            pltpu.VMEM((width, kv_width), bf16),
            pltpu.VMEM((tokens, width), f32),
            pltpu.VMEM((tokens, width), f32),
            pltpu.VMEM((tokens, width), bf16),
            pltpu.VMEM((nf * tokens, width // nf), bf16),
            pltpu.VMEM((tokens, heads_width), bf16),
            pltpu.VMEM((tokens, heads_width), bf16),
            pltpu.VMEM((tokens, kv_width), bf16),
            pltpu.VMEM((tokens, kv_width), bf16),
            pltpu.VMEM((tokens, 128), bf16),
            pltpu.VMEM((tail_rows, 128), f32),
            pltpu.VMEM((keys, kv_width), f32),
            pltpu.VMEM((keys, kv_width), f32),
            pltpu.VMEM((8, 128), f32),
            pltpu.VMEM((tokens, 2 * kv_width), bf16),
            pltpu.VMEM((tokens, 2 * kv_width), bf16),
            pltpu.VMEM((tokens, width), bf16),
            pltpu.VMEM((tokens, width), bf16),
            pltpu.VMEM((8, 128), f32),
            pltpu.VMEM((2, width), f32),
            dma((3,)),
            dma((2,)),
            dma((5,)),
            dma((5,)),
            pltpu.VMEM((nf, tokens, width), bf16),
            pltpu.VMEM((tokens, width), f32),
            pltpu.VMEM((nf, tokens, width), bf16),
            pltpu.VMEM((nz, tokens, width), bf16),
            pltpu.VMEM((2, nz, tokens, width), bf16),
            pltpu.VMEM((tokens, width), bf16),
            dma((nf,)),
            dma((nf, SUM_CUT)),
            dma((nf, SUM_CUT)),
            dma((nz, SUM_CUT)),
            dma((nz, SUM_CUT)),
            dma((nz, SUM_CUT)),
            dma((2, nz, SUM_CUT)),
            dma((SUM_CUT,)),
            dma((SUM_CUT,)),
        ],
        compiler_params=pltpu.CompilerParams(
            collective_id=8, has_side_effects=True, vmem_limit_bytes=67043328
        ),
    )(attended, *arrays)


def norm_forward(values, gain_row):
    inverse = lax.rsqrt(jnp.mean(values * values, axis=-1, keepdims=True) + eps_norm)
    normed = values * inverse
    return (normed * gain_row, normed, inverse)


def rms_norm_gradient(grad_scaled, normed, inverse, gain_row):
    grad_normed = grad_scaled * gain_row
    inner_mean = jnp.mean(grad_normed * normed, axis=-1, keepdims=True)
    return inverse * (grad_normed - normed * inner_mean)


def rope_tables(positions):
    half_dim = HEAD_SIZE // 2
    frequencies = rope_base ** (-(jnp.arange(half_dim, dtype=jnp.float32) * 2.0) / HEAD_SIZE)
    angles = positions.astype(jnp.float32)[:, None] * frequencies[None, :]
    return (jnp.cos(angles)[:, None, :], jnp.sin(angles)[:, None, :])


def rotate(values, cosine_table, sine_values):
    half_dim = values.shape[-1] // 2
    first_half = values[..., :half_dim]
    second_half = values[..., half_dim:]
    return jnp.concatenate(
        [
            first_half * cosine_table - second_half * sine_values,
            second_half * cosine_table + first_half * sine_values,
        ],
        axis=-1,
    )


def inverse_rotation(grad_in_rot, cosine_table, sine_values):
    half_dim = grad_in_rot.shape[-1] // 2
    first_half = grad_in_rot[..., :half_dim]
    second_half = grad_in_rot[..., half_dim:]
    return jnp.concatenate(
        [
            first_half * cosine_table + second_half * sine_values,
            second_half * cosine_table - first_half * sine_values,
        ],
        axis=-1,
    )


def masked_scores(query_rotated, key_rotated, allowed):
    scores = jnp.einsum(
        "qkgd,skd->kgqs", query_rotated, key_rotated, preferred_element_type=jnp.float32
    ) * HEAD_SIZE ** (-0.5)
    return jnp.where(allowed[None, None], scores, -jnp.inf)


def swap(value, axis_name):
    return lax.ppermute(value, axis_name, [(0, 1), (1, 0)])


def sum_over_tp(value):
    mine = value.astype(jnp.bfloat16)
    return mine.astype(jnp.float32) + swap(mine, "tp").astype(jnp.float32)


def block_sum(partial, nf):
    return lax.psum_scatter(partial, ("fsdp", "ctx"), scatter_dimension=0, tiled=True)


def by_shard(rows, nf):
    count, width = rows.shape
    return rows.reshape(count, nf, width // nf).transpose(1, 0, 2).reshape(nf * count, width // nf)


def on_device(
    hidden_in,
    segment_ids,
    routes,
    attn_gain,
    qk_gains,
    w_query,
    key_projection,
    value_projection,
    w_out,
    ffn_gain,
    w_router,
    w_gate,
    w_up,
    w_down,
    grad_out,
):
    tokens_dev, width_dim = hidden_in.shape
    nf = lax.axis_size("fsdp")
    devices = nf * lax.axis_size("ctx")
    local_experts = w_gate.shape[0]
    experts = local_experts * devices
    capacity = max(2, 2 * tokens_dev * TOPK // experts)
    query_group_width = QUERY_HEADS // KEY_VALUE_HEADS
    shard_width = attn_gain.shape[0]
    f_index, c_index = lax.axis_index("fsdp"), lax.axis_index("ctx")
    bf16 = jnp.bfloat16
    f32 = jnp.float32

    pieces = [w_router.reshape(-1), attn_gain, ffn_gain, qk_gains]
    flat = jnp.concatenate(pieces)
    small_rows = -(-flat.shape[0] // 2048) * 16
    small = jnp.pad(flat, (0, small_rows * 128 - flat.shape[0])).reshape(small_rows, 128)
    out_form = "row" if shard_width % 128 else "col"
    small_all, query_weight, key_weight, value_weight, out_weight, grad_all = plane_gather(
        [
            Gather(small, nf, chunks=1),
            Gather(w_query, nf, half=True, chunks=2),
            Gather(key_projection, nf, half=True, chunks=1),
            Gather(value_projection, nf, half=True, chunks=1),
            Gather(w_out, nf, form=out_form, half=True, chunks=2),
            Gather(grad_out, nf, rep=True, chunks=4),
        ],
        1,
        nf,
    )
    if out_form == "row":
        out_weight = out_weight.reshape(nf, -1, shard_width).transpose(1, 0, 2)
        out_weight = out_weight.reshape(-1, width_dim)
    small_all = small_all.reshape(nf, 2, small_rows * 128)[:, 0]
    ends = [0]
    for piece in pieces:
        ends.append(ends[-1] + piece.shape[0])
    router_weight = small_all[:, ends[0] : ends[1]].reshape(width_dim, experts)
    gain_one = small_all[:, ends[1] : ends[2]].reshape(-1).astype(f32)
    gain_two = small_all[:, ends[2] : ends[3]].reshape(-1).astype(f32)
    gain_qk = small_all[:, ends[3] : ends[4]].reshape(-1).astype(f32)
    gain_query, gain_key = gain_qk[:HEAD_SIZE], gain_qk[HEAD_SIZE:]

    kv_local = key_weight.shape[1] // HEAD_SIZE
    head_local = query_weight.shape[1] // HEAD_SIZE
    resid = hidden_in.astype(f32)
    scaled_one, normed_one, inverse_one = norm_forward(resid, gain_one)
    hidden_first = scaled_one.astype(bf16)
    query_raw = jnp.dot(hidden_first, query_weight, preferred_element_type=f32).reshape(
        tokens_dev, head_local, HEAD_SIZE
    )
    key_projected = jnp.dot(hidden_first, key_weight, preferred_element_type=f32).reshape(
        tokens_dev, kv_local, HEAD_SIZE
    )
    value_rows = jnp.dot(hidden_first, value_weight, preferred_element_type=f32).astype(bf16)
    query_normed, query_hat, query_inverse = norm_forward(query_raw, gain_query)
    key_normed, key_unit_rows, key_inverse_norm = norm_forward(key_projected, gain_key)
    own_positions = c_index * tokens_dev + jnp.arange(tokens_dev, dtype=jnp.int32)
    cosine_table, sine_values = rope_tables(own_positions)
    query_rotated = (
        rotate(query_normed, cosine_table, sine_values)
        .astype(bf16)
        .reshape(tokens_dev, kv_local, query_group_width, HEAD_SIZE)
    )
    key_rotated = rotate(key_normed, cosine_table, sine_values).astype(bf16)
    own_segments = segment_ids.astype(bf16)
    packed_kv = jnp.concatenate(
        [
            key_rotated.reshape(tokens_dev, -1),
            value_rows,
            jnp.broadcast_to(own_segments[:, None], (tokens_dev, 128)),
        ],
        axis=1,
    )
    kv_all = lax.all_gather(packed_kv, "ctx", axis=0, tiled=True)
    kv_width = kv_local * HEAD_SIZE
    key_all = kv_all[:, :kv_width].reshape(-1, kv_local, HEAD_SIZE)
    value_all = kv_all[:, kv_width : 2 * kv_width].reshape(-1, kv_local, HEAD_SIZE)
    segment_all = kv_all[:, 2 * kv_width]
    key_positions = jnp.arange(key_all.shape[0], dtype=jnp.int32)
    allowed = (key_positions[None, :] <= own_positions[:, None]) & (
        segment_all[None, :] == own_segments[:, None]
    )
    scores = masked_scores(query_rotated, key_all, allowed)
    top_score = jnp.max(scores, axis=-1, keepdims=True)
    log_total = top_score + jnp.log(jnp.sum(jnp.exp(scores - top_score), axis=-1, keepdims=True))
    weights_att = jnp.exp(scores - log_total).astype(bf16)
    attended = jnp.einsum("kgqs,skd->qkgd", weights_att, value_all, preferred_element_type=f32)
    attended = attended.astype(bf16).reshape(tokens_dev, head_local * HEAD_SIZE)
    out_partial = jnp.dot(attended, out_weight, preferred_element_type=f32)
    resid_mid = resid + sum_over_tp(out_partial)
    scaled_two, normed_two, inverse_two = norm_forward(resid_mid, gain_two)
    hidden_two = scaled_two.astype(bf16)
    logits = jnp.dot(hidden_two, router_weight, preferred_element_type=f32)
    expert_ids = jnp.arange(experts, dtype=jnp.int32)
    hits = routes[:, :, None] == expert_ids[None, None, :]
    routed = jnp.any(hits, axis=1)
    masked_logits = jnp.where(routed, logits, -jnp.inf)
    raised = jnp.where(
        routed, jnp.exp(masked_logits - jnp.max(masked_logits, axis=1, keepdims=True)), 0.0
    )
    probs = raised / jnp.sum(raised, axis=1, keepdims=True)
    marks = jnp.where(routed, probs, -1.0).T

    if nf == 8:
        (
            hidden_all,
            hidden_first_slice,
            moe_partial,
            rows_in,
            grad_prod,
            activated,
            grad_gate_pre,
            grad_up_pre,
            grad_hidden_moe,
            grad_prob,
        ) = expert_pass(
            hidden_two,
            marks,
            by_shard(hidden_first, nf),
            grad_all,
            w_gate,
            w_up,
            w_down,
            capacity,
            nf,
        )
        grad_prob = grad_prob.reshape(devices, 8, tokens_dev)[:, :local_experts]
        grad_prob = grad_prob.reshape(experts, tokens_dev).T
    else:
        hidden_all, marks_all, hidden_first_slice = plane_gather(
            [
                Gather(hidden_two, nf, rep=True, chunks=4),
                Gather(marks, nf, chunks=1),
                Gather(by_shard(hidden_first, nf), nf, form="a2a", chunks=1),
            ],
            2,
            nf,
        )
        first_expert = (f_index * 2 + c_index) * local_experts
        marks_here = lax.dynamic_slice_in_dim(
            marks_all.reshape(devices, experts, tokens_dev), first_expert, local_experts, axis=1
        )
        taken = marks_here >= 0.0
        ranks = jnp.cumsum(taken.astype(jnp.int32), axis=2) - 1
        slots = jnp.arange(capacity, dtype=jnp.int32)
        chosen = taken[:, :, None, :] & (ranks[:, :, None, :] == slots[None, None, :, None])
        pick = chosen.astype(bf16)
        weight_slot = jnp.sum(jnp.where(chosen, marks_here[:, :, None, :], 0.0), axis=3)
        weight_slot = weight_slot.transpose(1, 0, 2).reshape(local_experts, devices * capacity)

        def select(rows):
            blocks = rows.reshape(devices, tokens_dev, width_dim)
            out = jnp.einsum("bjst,btd->jbsd", pick, blocks, preferred_element_type=f32)
            return out.astype(bf16).reshape(local_experts, devices * capacity, width_dim)

        def spread(rows):
            blocks = rows.reshape(local_experts, devices, capacity, width_dim)
            out = jnp.einsum("bjst,jbsd->btd", pick, blocks, preferred_element_type=f32)
            return out.astype(bf16).reshape(devices * tokens_dev, width_dim)

        rows_in = select(hidden_all)
        grad_rows_in = select(grad_all)
        gate_pre = jnp.einsum("jrd,jdf->jrf", rows_in, w_gate, preferred_element_type=f32)
        up_pre = jnp.einsum("jrd,jdf->jrf", rows_in, w_up, preferred_element_type=f32)
        sigmoid_gate = jax.nn.sigmoid(gate_pre)
        silu_gate = gate_pre * sigmoid_gate
        activated = (silu_gate * up_pre).astype(bf16)
        produced = jnp.einsum("jrf,jfd->jrd", activated, w_down, preferred_element_type=f32).astype(
            bf16
        )
        wide = produced.astype(f32)
        grad_prob_slot = jnp.sum(wide * grad_rows_in.astype(f32), axis=2)
        grad_prob_part = jnp.sum(
            jnp.where(
                chosen,
                grad_prob_slot.reshape(local_experts, devices, capacity).transpose(1, 0, 2)[..., None],
                0.0,
            ),
            axis=2,
        )
        moe_partial = spread((weight_slot[:, :, None] * wide).astype(bf16))
        grad_prod = (weight_slot[:, :, None] * grad_rows_in.astype(f32)).astype(bf16)
        grad_act = jnp.einsum("jrd,jfd->jrf", grad_prod, w_down, preferred_element_type=f32)
        grad_gate_pre = (
            grad_act * up_pre * (sigmoid_gate * (1.0 + gate_pre * (1.0 - sigmoid_gate)))
        ).astype(bf16)
        grad_up_pre = (grad_act * silu_gate).astype(bf16)
        grad_slots = jnp.einsum("jrf,jdf->jrd", grad_gate_pre, w_gate, preferred_element_type=f32)
        grad_slots = (
            grad_slots + jnp.einsum("jrf,jdf->jrd", grad_up_pre, w_up, preferred_element_type=f32)
        ).astype(bf16)
        hidden_grad_partial = spread(grad_slots)

        grad_hidden_moe = sum_over_tp(block_sum(hidden_grad_partial, nf))
        grad_prob = lax.all_to_all(
            grad_prob_part, ("fsdp", "ctx"), split_axis=0, concat_axis=0, tiled=True
        ).reshape(experts, tokens_dev)
        grad_prob = grad_prob + swap(grad_prob, "tp")
        grad_prob = grad_prob.T
    grad_down = jnp.einsum("jrf,jrd->jfd", activated, grad_prod, preferred_element_type=f32)
    grad_gate = jnp.einsum("jrd,jrf->jdf", rows_in, grad_gate_pre, preferred_element_type=f32)
    grad_up = jnp.einsum("jrd,jrf->jdf", rows_in, grad_up_pre, preferred_element_type=f32)

    if nf == 8:
        gains = jnp.stack([gain_one, gain_two, jnp.pad(gain_qk, (0, width_dim - gain_qk.shape[0]))])
        cosine_row, sine_row = cosine_table[:, 0], sine_values[:, 0]
        trig = jnp.stack(
            [
                jnp.concatenate([cosine_row, cosine_row], axis=1),
                jnp.concatenate([sine_row, -sine_row], axis=1),
            ]
        )
        operands = (
            grad_hidden_moe,
            grad_prob,
            probs,
            router_weight,
            hidden_in,
            resid_mid,
            gains,
            grad_out,
            out_weight,
            query_weight,
            key_weight,
            value_weight,
            query_raw.reshape(tokens_dev, -1),
            key_projected.reshape(tokens_dev, -1),
            query_rotated.reshape(tokens_dev, -1),
            key_all.reshape(-1, kv_width),
            value_all.reshape(-1, kv_width),
            jnp.where(allowed, 0.0, -jnp.inf),
            log_total.reshape(head_local, tokens_dev, 1),
            trig,
            moe_partial,
        )
        shapes = (tokens_dev, width_dim, head_local * HEAD_SIZE, kv_width, key_all.shape[0])
        (
            attended_all,
            dq_all,
            dk_all,
            dv_all,
            logits_all,
            tail_all,
            proj_slice,
            grad_in,
            block_out,
        ) = backward_pass(nf, operands, attended, shapes)
        tail_rows = tail_all.shape[0] // devices
    else:
        block_out = (resid_mid + sum_over_tp(block_sum(moe_partial, nf))).astype(bf16)

        grad_rows = grad_out.astype(f32)
        grad_logits = (
            probs * (grad_prob - jnp.sum(probs * grad_prob, axis=1, keepdims=True))
        ).astype(bf16)
        grad_hidden_two = grad_hidden_moe + jnp.einsum(
            "te,de->td", grad_logits, router_weight, preferred_element_type=f32
        )
        grad_ffn_local = jnp.sum(grad_hidden_two * normed_two, axis=0)
        grad_mid = grad_rows + rms_norm_gradient(grad_hidden_two, normed_two, inverse_two, gain_two)
        grad_proj = grad_mid.astype(bf16)
        attended_gradient = jnp.einsum(
            "td,qd->tq", grad_proj, out_weight, preferred_element_type=f32
        ).astype(bf16)
        attended_gradient = attended_gradient.reshape(
            tokens_dev, kv_local, query_group_width, HEAD_SIZE
        )
        probs_att = jnp.exp(scores - log_total)
        grad_value_all = jnp.einsum(
            "kgqs,qkgd->skd", weights_att, attended_gradient, preferred_element_type=f32
        )
        grad_probs = jnp.einsum(
            "qkgd,skd->kgqs", attended_gradient, value_all, preferred_element_type=f32
        )
        delta_row = jnp.sum(probs_att * grad_probs, axis=-1, keepdims=True)
        grad_scores = (probs_att * (grad_probs - delta_row) * HEAD_SIZE ** (-0.5)).astype(bf16)
        grad_query_rot = jnp.einsum(
            "kgqs,skd->qkgd", grad_scores, key_all, preferred_element_type=f32
        ).reshape(tokens_dev, head_local, HEAD_SIZE)
        grad_key_all = jnp.einsum(
            "kgqs,qkgd->skd", grad_scores, query_rotated, preferred_element_type=f32
        )
        grad_kv_all = jnp.concatenate(
            [grad_key_all.reshape(-1, kv_width), grad_value_all.reshape(-1, kv_width)], axis=1
        )
        theirs = lax.dynamic_slice_in_dim(grad_kv_all, (1 - c_index) * tokens_dev, tokens_dev, axis=0)
        mine = lax.dynamic_slice_in_dim(grad_kv_all, c_index * tokens_dev, tokens_dev, axis=0)
        grad_kv = mine + swap(theirs.astype(bf16), "ctx").astype(f32)
        key_rotated_gradient = grad_kv[:, :kv_width].reshape(tokens_dev, kv_local, HEAD_SIZE)
        grad_query_norm = inverse_rotation(grad_query_rot, cosine_table, sine_values)
        key_normed_gradient = inverse_rotation(key_rotated_gradient, cosine_table, sine_values)
        grad_qk_local = jnp.concatenate(
            [
                jnp.sum(grad_query_norm * query_hat, axis=(0, 1)),
                jnp.sum(key_normed_gradient * key_unit_rows, axis=(0, 1)),
            ]
        )
        grad_query_raw = (
            rms_norm_gradient(grad_query_norm, query_hat, query_inverse, gain_query)
            .astype(bf16)
            .reshape(tokens_dev, head_local * HEAD_SIZE)
        )
        key_projected_gradient = (
            rms_norm_gradient(key_normed_gradient, key_unit_rows, key_inverse_norm, gain_key)
            .astype(bf16)
            .reshape(tokens_dev, kv_width)
        )
        value_projected_gradient = grad_kv[:, kv_width:].astype(bf16)
        grad_hidden_part = jnp.einsum(
            "tq,dq->td", grad_query_raw, query_weight, preferred_element_type=f32
        )
        grad_hidden_part = grad_hidden_part + jnp.einsum(
            "tq,dq->td", key_projected_gradient, key_weight, preferred_element_type=f32
        )
        grad_hidden_part = grad_hidden_part + jnp.einsum(
            "tq,dq->td", value_projected_gradient, value_weight, preferred_element_type=f32
        )
        grad_hidden_one = sum_over_tp(grad_hidden_part)
        grad_in = grad_mid + rms_norm_gradient(grad_hidden_one, normed_one, inverse_one, gain_one)
        grad_attn_local = jnp.sum(grad_hidden_one * normed_one, axis=0)
        grad_qk_local = grad_qk_local + swap(grad_qk_local, "tp")
        tail = jnp.concatenate([grad_attn_local, grad_ffn_local, grad_qk_local])
        tail = jnp.pad(tail, (0, -tail.shape[0] % 1024)).reshape(-1, 128)
        tail_rows = tail.shape[0]
        logit_pad = jnp.pad(grad_logits, ((0, 0), (0, -experts % 128)))

        dq_all, dk_all, dv_all, attended_all, proj_slice, logits_all, tail_all = plane_gather(
            [
                Gather(grad_query_raw, nf, chunks=2),
                Gather(key_projected_gradient, nf, chunks=1),
                Gather(value_projected_gradient, nf, chunks=1),
                Gather(attended, nf, chunks=2),
                Gather(by_shard(grad_proj, nf), nf, form="a2a", chunks=1),
                Gather(logit_pad, nf, chunks=1),
                Gather(tail, nf, chunks=1),
            ],
            3,
            nf,
        )
    over_tokens = functools.partial(
        jnp.einsum, "td,tq->dq", preferred_element_type=f32
    )
    grad_query = over_tokens(hidden_first_slice, dq_all)
    grad_key = over_tokens(hidden_first_slice, dk_all)
    grad_value = over_tokens(hidden_first_slice, dv_all)
    grad_out_proj = over_tokens(attended_all, proj_slice)
    hidden_slice = lax.dynamic_slice_in_dim(hidden_all, f_index * shard_width, shard_width, axis=1)
    grad_router = over_tokens(hidden_slice, logits_all)[:, :experts]
    tail_sum = jnp.sum(tail_all.reshape(devices, tail_rows * 128), axis=0)
    grad_attn = lax.dynamic_slice_in_dim(tail_sum, f_index * shard_width, shard_width)
    grad_ffn = lax.dynamic_slice_in_dim(tail_sum, width_dim + f_index * shard_width, shard_width)
    qk_width = qk_gains.shape[0]
    grad_qk = lax.dynamic_slice_in_dim(tail_sum, 2 * width_dim + f_index * qk_width, qk_width)
    return (
        block_out,
        grad_in,
        grad_attn,
        grad_qk,
        grad_query,
        grad_key,
        grad_value,
        grad_out_proj,
        grad_ffn,
        grad_router,
        grad_gate,
        grad_up,
        grad_down,
    )


def solution(mesh):
    return jax.shard_map(
        on_device,
        mesh=mesh,
        in_specs=(
            P(("fsdp", "ctx"), None),
            P(("fsdp", "ctx")),
            P(("fsdp", "ctx"), None),
            P("fsdp"),
            P("fsdp"),
            P("fsdp", "tp"),
            P("fsdp", "tp"),
            P("fsdp", "tp"),
            P("tp", "fsdp"),
            P("fsdp"),
            P("fsdp", None),
            P(("fsdp", "ctx"), None, "tp"),
            P(("fsdp", "ctx"), None, "tp"),
            P(("fsdp", "ctx"), "tp", None),
            P(("fsdp", "ctx"), None),
        ),
        out_specs=(
            P(("fsdp", "ctx"), None),
            P(("fsdp", "ctx"), None),
            P("fsdp"),
            P("fsdp"),
            P("fsdp", "tp"),
            P("fsdp", "tp"),
            P("fsdp", "tp"),
            P("tp", "fsdp"),
            P("fsdp"),
            P("fsdp", None),
            P(("fsdp", "ctx"), None, "tp"),
            P(("fsdp", "ctx"), None, "tp"),
            P(("fsdp", "ctx"), "tp", None),
        ),
        check_vma=False,
    )
```

```python
import functools

import jax
import jax.numpy as jnp
from jax import lax
from jax.experimental import pallas as pl
from jax.experimental.pallas import tpu as pltpu
from jax.sharding import PartitionSpec as P

QUERY_HEADS = 32
KEY_VALUE_HEADS = 4
HEAD_SIZE = 128
TOPK = 8
MESH = pl.DeviceIdType.MESH

eps_norm = 1e-06
rope_base = 1000000.0

UP, DOWN, ACROSS, PARTNER, SIDE = range(5)


class Gather:
    def __init__(self, array, nf, form="row", half=False, rep=False, chunks=2):
        if nf > 8:
            chunks = 2 if rep else 1
        self.array, self.form, self.half, self.rep, self.chunks = array, form, half, rep, chunks
        self.shape = array.shape
        self.rows = array.shape[0] // 2 if half else array.shape[0]
        self.step = (self.rows // nf if form == "a2a" else self.rows) // chunks

    def out_shape(self, nf):
        rows, cols = self.rows, self.shape[1]
        if self.form == "col":
            return (2 * rows, nf * cols)
        if self.form == "a2a":
            return (2 * rows, cols)
        return (2 * nf * rows, cols)


def gather_engine(nf, specs, ins, outs, stage, recv, send, local):
    n = len(specs)
    nz = nf // 2
    f, c, t = lax.axis_index("fsdp"), lax.axis_index("ctx"), lax.axis_index("tp")
    z, x = f // 2, lax.rem(f, 2)
    has_up, has_down = z + 1 < nz, z > 0
    device = {
        UP: (f + 2, c, t),
        DOWN: (f - 2, c, t),
        ACROSS: (z * 2 + 1 - x, c, t),
        PARTNER: (f, 1 - c, t),
        SIDE: (f, c, 1 - t),
    }
    first = [sum(s.chunks for s in specs[:a]) for a in range(n)]

    def src(a, q, dest_f=None):
        s = specs[a]
        lo = row_chunk(a, q) * s.step
        if s.half:
            lo = c * s.rows + lo
        if s.form == "a2a":
            lo = dest_f * (s.rows // nf) + lo
        return ins[a].at[pl.ds(lo, s.step)]

    def dst(a, q, bf, bc):
        s = specs[a]
        if s.form == "col":
            width = s.shape[1]
            return outs[a].at[
                pl.ds(bc * s.rows + row_chunk(a, q) * s.step, s.step),
                pl.ds(pl.multiple_of(bf * width, width), width),
            ]
        rows = s.rows // nf if s.form == "a2a" else s.rows
        return outs[a].at[pl.ds((bf * 2 + bc) * rows + row_chunk(a, q) * s.step, s.step)]

    def copy(a, q, bf, bc, source, kind, dev=None, slot=None):
        block = bf * 2 + bc if slot is None else slot
        return pltpu.make_async_remote_copy(
            src_ref=source,
            dst_ref=dst(a, q, bf, bc),
            send_sem=send.at[kind, block, first[a] + row_chunk(a, q)],
            recv_sem=recv.at[bf * 2 + bc, first[a] + row_chunk(a, q)],
            device_id=device[kind] if dev is None else dev,
            device_id_type=MESH,
        )

    def row_chunk(a, q):
        n_chunks = specs[a].chunks
        if not specs[a].rep:
            return q
        return lax.rem(q + t * (n_chunks // 2), n_chunks)

    def in_half(a, q):
        return 2 * q < specs[a].chunks

    def both(*conds):
        if any(k is False for k in conds):
            return False
        conds = [k for k in conds if k is not None and k is not True]
        if not conds:
            return None
        return functools.reduce(lambda u, v: u & v, conds)

    def when(cond, fn):
        if cond is None or cond is True:
            fn()
        elif cond is not False:
            pl.when(cond)(fn)

    def go_up(a, q, dist):
        far = dist + 1 < nz - 1 if specs[a].rep and not in_half(a, q) else None
        return both(has_up, far)

    def go_down(a, q, dist):
        far = dist + 1 < nz - 1 if specs[a].rep and not in_half(a, q) else None
        return both(has_down, far)

    def go_across(a, q):
        return in_half(a, q) if specs[a].rep else None

    relays = [(a, q) for a in range(n) if specs[a].form != "a2a" for q in range(specs[a].chunks)]
    direct = [(a, q) for a in range(n) if specs[a].form == "a2a" for q in range(specs[a].chunks)]

    def start(only=None):
        only = range(n) if only is None else only
        for a, q in relays:
            if a not in only:
                continue
            source = src(a, q)
            when(go_up(a, q, 0), lambda: copy(a, q, f, c, source, UP).start())
            when(go_down(a, q, 0), lambda: copy(a, q, f, c, source, DOWN).start())
            when(go_across(a, q), lambda: copy(a, q, f, c, source, ACROSS).start())
            copy(a, q, f, c, source, PARTNER).start()
        own_start([a for a in only if specs[a].form != "a2a"])

    def own_start(only):
        for a in only:
            own_in(a).start()
        for a in only:
            own_in(a).wait()
            own_out(a).start()

    def start_direct():
        own_start(sorted({a for a, _ in direct}))
        for a, q in direct:
            copy(a, q, f, c, src(a, q, f), PARTNER).start()

            def far_send(d, carry):
                there = lax.rem(f + d, nf)
                copy(a, q, f, c, src(a, q, there), UP, dev=(there, c, t), slot=there).start()
                return carry

            lax.fori_loop(1, nf, far_send, 0)

    def own_in(a):
        s = specs[a]
        if s.form == "a2a":
            view = ins[a].at[pl.ds(f * s.step, s.step)]
        elif s.half:
            view = ins[a].at[pl.ds(c * s.rows, s.rows)]
        else:
            view = ins[a]
        return pltpu.make_async_copy(view, stage[a], local.at[0, a])

    def own_out(a):
        s = specs[a]
        if s.form == "col":
            width = s.shape[1]
            view = outs[a].at[
                pl.ds(c * s.rows, s.rows), pl.ds(pl.multiple_of(f * width, width), width)
            ]
        else:
            rows = s.rows // nf if s.form == "a2a" else s.rows
            view = outs[a].at[pl.ds((f * 2 + c) * rows, rows)]
        return pltpu.make_async_copy(stage[a], view, local.at[1, a])

    def arrived(a, q, bf, bc):
        copy(a, q, bf, bc, dst(a, q, bf, bc), PARTNER).wait_recv()

    def pass_on(a, q, bf, kind, cond=None):
        when(cond, lambda: copy(a, q, bf, c, dst(a, q, bf, c), kind).start())

    pair = z + 1 - 2 * lax.rem(z, 2)
    even = lax.rem(z, 2) == 0

    def shared(a, q):
        return not specs[a].rep and specs[a].chunks > 1 and 2 * q >= specs[a].chunks

    def column(k, a, q):
        rep = specs[a].rep
        came = k < nz - 1 if rep and not in_half(a, q) else None
        far = (k == nz - 1) if rep and in_half(a, q) else False

        def take(zz, kind, onward):
            bf = zz * 2 + x
            arrived(a, q, bf, c)
            pass_on(a, q, bf, kind, onward)
            cross = (zz != pair) if shared(a, q) else go_across(a, q)
            pass_on(a, q, bf, ACROSS, cross)
            pass_on(a, q, bf, PARTNER)
            if rep:
                pass_on(a, q, bf, SIDE, far)

        when(both(z - k >= 0, came), lambda: take(z - k, UP, go_up(a, q, k)))
        when(both(z + k < nz, came), lambda: take(z + k, DOWN, go_down(a, q, k)))

    def across(k, a, q):
        rep = specs[a].rep
        mine = in_half(a, q) if rep else None

        def take(zz):
            bf = zz * 2 + 1 - x
            arrived(a, q, bf, c)
            pass_on(a, q, bf, PARTNER)
            if rep:
                pass_on(a, q, bf, SIDE)
            if shared(a, q):
                pass_on(a, q, bf, UP, (zz == z) & even)
                pass_on(a, q, bf, DOWN, (zz == z) & jnp.logical_not(even))

        when(both(z - k >= 0, mine), lambda: take(z - k))
        when(both(z + k < nz, k > 0, mine), lambda: take(z + k))

    def aside(k, a, q):
        if not specs[a].rep:
            return
        if in_half(a, q):
            return

        def take(bf):
            arrived(a, q, bf, c)
            pass_on(a, q, bf, PARTNER)

        when((z - k >= 0), lambda: take((z - k) * 2 + 1 - x))
        when((z + k < nz) & (k > 0), lambda: take((z + k) * 2 + 1 - x))
        when((z - k >= 0) & (k == nz - 1), lambda: take((z - k) * 2 + x))
        when((z + k < nz) & (k == nz - 1), lambda: take((z + k) * 2 + x))

    count = len(relays)
    lag = 2

    def late(fn, k, i):
        if i >= 0:
            fn(k, *relays[i])
        else:
            pl.when(k > 1)(lambda: fn(k - 1, *relays[count + i]))

    by_chunk = all(specs[a].rep for a, _ in relays)

    def step(k, carry):
        if not by_chunk:
            for a, q in relays:
                column(k, a, q)
            for a, q in relays:
                across(k - 1, a, q)

            @pl.when(k > 1)
            def _():
                for a, q in relays:
                    aside(k - 2, a, q)

            return carry
        for i, (a, q) in enumerate(relays):
            column(k, a, q)
            pl.when(k == 1)(lambda: across(0, a, q))
            late(across, k, i - lag)
            if i >= lag:
                pl.when(k == 1)(lambda: aside(0, *relays[i - lag]))
            late(aside, k, i - 2 * lag)

        @pl.when(k == 1)
        def _():
            for a, q in relays[count - lag :]:
                aside(0, a, q)

        return carry

    def run(hook=None):
        def body(k, carry):
            step(k, carry)
            if hook is not None:
                hook(k)
            return carry

        lax.fori_loop(1, nz, body, 0)
        for a, q in relays[count - lag if by_chunk else 0 :]:
            across(nz - 1, a, q)
        if not by_chunk:
            for a, q in relays:
                aside(nz - 2, a, q)
        for a, q in relays[count - 2 * lag if by_chunk else 0 :]:
            aside(nz - 1, a, q)

    def step_of(k, only):
        some = [(a, q) for a, q in relays if a in only]
        for a, q in some:
            column(k, a, q)
        for a, q in some:
            across(k - 1, a, q)

        if k > 1:
            for a, q in some:
                aside(k - 2, a, q)

    def edge_of(only):
        some = [(a, q) for a, q in relays if a in only]
        for a, q in some:
            across(nz - 1, a, q)
        for a, q in some:
            aside(nz - 2, a, q)
        for a, q in some:
            aside(nz - 1, a, q)

    def land_of(only):
        def take(bf, carry):
            for a, q in relays:
                if a in only:
                    arrived(a, q, bf, 1 - c)
            return carry

        lax.fori_loop(0, nf, take, 0)
        for a in only:
            own_out(a).wait()

    def run_direct():
        for a, q in direct:

            def far_take(d, carry):
                there = lax.rem(f + nf - d, nf)
                arrived(a, q, there, c)
                pass_on(a, q, there, PARTNER)
                return carry

            lax.fori_loop(1, nf, far_take, 0)

    def take_partner(bf, carry):
        for a, q in relays:
            arrived(a, q, bf, 1 - c)
        return carry

    def land():
        lax.fori_loop(0, nf, take_partner, 0)
        for a in range(n):
            if specs[a].form != "a2a":
                own_out(a).wait()

    def finish(bf, carry):
        zz, xx = bf // 2, lax.rem(bf, 2)
        dist = jnp.abs(zz - z)
        here = xx == x
        for a, q in relays:
            rep = specs[a].rep
            view = dst(a, q, bf, c)

            def sent(kind, cond):
                when(cond, lambda: copy(a, q, bf, c, view, kind).wait_send())

            half = in_half(a, q) if rep else None
            by_z = dist < nz - 1 if rep and not half else None
            sent(PARTNER, None)
            sent(UP, both(here, zz <= z, by_z, go_up(a, q, dist)))
            sent(DOWN, both(here, zz >= z, by_z, go_down(a, q, dist)))
            cross = (zz != pair) if shared(a, q) else go_across(a, q)
            sent(ACROSS, both(here, by_z, cross))
            if shared(a, q):
                there = jnp.logical_not(here) & (zz == z)
                sent(UP, there & even)
                sent(DOWN, there & jnp.logical_not(even))
            if rep and half:
                sent(SIDE, jnp.logical_not(here) | (dist == nz - 1))
        for a, q in direct:
            arrived(a, q, bf, 1 - c)
            view = dst(a, q, bf, c)
            copy(a, q, bf, c, view, PARTNER).wait_send()

            @pl.when(bf != f)
            def _():
                copy(a, q, bf, c, view, UP, slot=bf).wait_send()

        return carry

    def drain():
        lax.fori_loop(0, nf, finish, 0)
        for a in range(n):
            if specs[a].form == "a2a":
                own_out(a).wait()

    return start, run, land, start_direct, run_direct, drain, step_of, edge_of, land_of


def gather_kernel(nf, specs, *refs):
    n = len(specs)
    ins, outs, scratch = refs[:n], refs[n : 2 * n], refs[2 * n :]
    nz = nf // 2
    f, c, t = lax.axis_index("fsdp"), lax.axis_index("ctx"), lax.axis_index("tp")
    z, x = f // 2, lax.rem(f, 2)
    has_up, has_down = z + 1 < nz, z > 0
    device = {
        UP: (f + 2, c, t),
        DOWN: (f - 2, c, t),
        ACROSS: (z * 2 + 1 - x, c, t),
        PARTNER: (f, 1 - c, t),
        SIDE: (f, c, 1 - t),
    }
    any_a2a = any(s.form == "a2a" for s in specs)
    any_rep = any(s.rep for s in specs)
    barrier = pltpu.get_barrier_semaphore()

    def greet(dev):
        pl.semaphore_signal(barrier, 1, device_id=dev, device_id_type=MESH)

    greeted = 1
    greet(device[PARTNER])
    if any_rep:
        greet(device[SIDE])
        greeted += 1
    if any_a2a:

        def greet_far(d, carry):
            greet((lax.rem(f + d, nf), c, t))
            return carry

        lax.fori_loop(1, nf, greet_far, 0)
        pl.semaphore_wait(barrier, greeted + nf - 1)
    else:
        greet(device[ACROSS])

        @pl.when(has_up)
        def _():
            greet(device[UP])

        @pl.when(has_down)
        def _():
            greet(device[DOWN])

        pl.semaphore_wait(
            barrier, greeted + 1 + has_up.astype(jnp.int32) + has_down.astype(jnp.int32)
        )

    start, run, land, start_direct, run_direct, drain, *_ = gather_engine(
        nf, specs, ins, outs, scratch[:n], *scratch[n:]
    )
    start()
    start_direct()
    run()
    run_direct()
    land()
    drain()


def stage_of(s, nf):
    rows = s.rows // nf if s.form == "a2a" else s.rows
    return pltpu.VMEM((rows, s.shape[1]), s.array.dtype)


def plane_gather(specs, collective_id, nf):
    n = len(specs)
    total = sum(s.chunks for s in specs)

    return pl.pallas_call(
        functools.partial(gather_kernel, nf, tuple(specs)),
        out_shape=tuple(jax.ShapeDtypeStruct(s.out_shape(nf), s.array.dtype) for s in specs),
        in_specs=[pl.BlockSpec(memory_space=pl.ANY)] * n,
        out_specs=tuple(pl.BlockSpec(memory_space=pl.ANY) for _ in specs),
        scratch_shapes=[stage_of(s, nf) for s in specs]
        + [
            pltpu.SemaphoreType.DMA((2 * nf, total)),
            pltpu.SemaphoreType.DMA((5, 2 * nf, total)),
            pltpu.SemaphoreType.DMA((2, n)),
        ],
        compiler_params=pltpu.CompilerParams(
            collective_id=collective_id, has_side_effects=True
        ),
    )(*[s.array for s in specs])


CUT = 4


def expert_kernel(nf, capacity, specs, *refs):
    n = len(specs)
    ins, refs = refs[:n], refs[n:]
    (grad_all, wg_hbm, wu_hbm, wd_hbm), refs = refs[:4], refs[4:]
    gathered, refs = refs[:n], refs[n:]
    (out_part, xs_out, de_out, act_out, dg_out, du_out, grad_tok, prob_tok), refs = (
        refs[:8],
        refs[8:],
    )
    stage, refs = refs[:n], refs[n:]
    (recv, send, local), refs = refs[:3], refs[3:]
    (
        wg,
        wu,
        wd,
        x_buf,
        y_buf,
        xs,
        ys,
        de,
        pe,
        bs,
        act,
        dg,
        du,
        w_slot,
        dp_slot,
        pick,
        mk,
        rk,
        y_out,
        part,
        from_partner,
        from_across,
        from_z,
        from_side,
        dp_send,
        dp_recv,
        dp_side,
        marks_v,
        w_sem,
        load_sem,
        store_sem,
        p_send,
        p_recv,
        x_send,
        x_recv,
        z_send,
        z_recv,
        s_send,
        s_recv,
        d_send,
        d_recv,
    ) = refs
    f32, bf16 = jnp.float32, jnp.bfloat16
    nz = nf // 2
    f, c, t = lax.axis_index("fsdp"), lax.axis_index("ctx"), lax.axis_index("tp")
    z, x = f // 2, lax.rem(f, 2)
    me = f * 2 + c
    up, down = (f + 2, c, t), (f - 2, c, t)
    across_dev, partner, side = (z * 2 + 1 - x, c, t), (f, 1 - c, t), (f, c, 1 - t)
    has_up, has_down = z + 1 < nz, z > 0
    tokens = x_buf.shape[0] // 4
    width = x_buf.shape[1]
    slots = 2 * capacity
    rows_unit = 4 * capacity
    hidden = wg.shape[2]
    experts = specs[1].shape[0]
    step_rows = tokens // CUT

    barrier = pltpu.get_barrier_semaphore()

    def greet(d, carry):
        there = lax.rem(me + d, 2 * nf)
        pl.semaphore_signal(
            barrier, 1, device_id=(there // 2, lax.rem(there, 2), t), device_id_type=MESH
        )
        return carry

    lax.fori_loop(1, 2 * nf, greet, 0)
    pl.semaphore_signal(barrier, 1, device_id=side, device_id_type=MESH)
    pl.semaphore_wait(barrier, 2 * nf)

    start, run, land, start_direct, run_direct, drain, *_ = gather_engine(
        nf, specs, ins, gathered, stage, recv, send, local
    )
    start()
    weight_loads = [
        pltpu.make_async_copy(src, dst, w_sem.at[i])
        for i, (src, dst) in enumerate(((wg_hbm, wg), (wu_hbm, wu), (wd_hbm, wd)))
    ]
    for load in weight_loads:
        load.start()

    order = 0
    for at, seq in enumerate(visiting_order(nz)):
        code = sum(u * nz**i for i, u in enumerate(seq))
        order = order + code * (z == at).astype(jnp.int32)

    def unit_at(i):
        code = order
        for k in range(nz):
            code = jnp.where(i > k, code // nz, code)
        return lax.rem(code, nz)

    def load_rows(u, which):
        rows = pl.ds(pl.multiple_of(u * 4 * tokens, 4 * tokens), 4 * tokens)
        if which == 0:
            return pltpu.make_async_copy(gathered[0].at[rows], x_buf, load_sem.at[0])
        return pltpu.make_async_copy(grad_all.at[rows], y_buf, load_sem.at[1])

    load_rows(unit_at(0), 1).start()
    run()
    land()
    start_direct()
    load_rows(unit_at(0), 0).start()
    marks_in = pltpu.make_async_copy(gathered[1], marks_v, load_sem.at[2])
    marks_in.start()
    marks_in.wait()
    dp_send[...] = jnp.zeros_like(dp_send)
    first_expert = me * 2
    for b in range(2 * nf):
        for j in range(2):
            mk[2 * b + j : 2 * b + j + 1, :] = marks_v[pl.ds(b * experts + first_expert + j, 1), :]
    taken = jnp.where(mk[...] >= 0.0, 1.0, 0.0).astype(bf16)
    before = lax.broadcasted_iota(jnp.int32, (tokens, tokens), 0)
    after = lax.broadcasted_iota(jnp.int32, (tokens, tokens), 1)
    upper = jnp.where(before <= after, 1.0, 0.0).astype(bf16)
    rk[...] = jnp.dot(taken, upper, preferred_element_type=f32) - 1.0
    for load in weight_loads:
        load.wait()

    def store_unit(u):
        rows = pl.ds(pl.multiple_of(u * rows_unit, rows_unit), rows_unit)
        pairs = [(xs, xs_out), (de, de_out), (act, act_out), (dg, dg_out), (du, du_out)]
        copies = [
            pltpu.make_async_copy(src, dst.at[:, rows], store_sem.at[i])
            for i, (src, dst) in enumerate(pairs)
        ]
        out_rows = pl.ds(pl.multiple_of(u * 4 * tokens, 4 * tokens), 4 * tokens)
        copies.append(pltpu.make_async_copy(y_out, out_part.at[out_rows], store_sem.at[5]))
        return copies

    def chunk(q):
        return pl.ds(q * step_rows, step_rows)

    def p_copy(u, xx, q):
        return pltpu.make_async_remote_copy(
            src_ref=part.at[u * 4 + xx * 2 + 1 - c, chunk(q)],
            dst_ref=from_partner.at[u * 2 + xx, chunk(q)],
            send_sem=p_send.at[u * 2 + xx, q],
            recv_sem=p_recv.at[u * 2 + xx, q],
            device_id=partner,
            device_id_type=MESH,
        )

    def x_copy(u, q):
        return pltpu.make_async_remote_copy(
            src_ref=part.at[u * 4 + (1 - x) * 2 + c, chunk(q)],
            dst_ref=from_across.at[u, chunk(q)],
            send_sem=x_send.at[u, q],
            recv_sem=x_recv.at[u, q],
            device_id=across_dev,
            device_id_type=MESH,
        )

    def z_copy(u, q, way):
        return pltpu.make_async_remote_copy(
            src_ref=part.at[u * 4 + x * 2 + c, chunk(q)],
            dst_ref=from_z.at[way, u, chunk(q)],
            send_sem=z_send.at[u, q],
            recv_sem=z_recv.at[way, u, q],
            device_id=up if way == 0 else down,
            device_id_type=MESH,
        )

    def z_wait(u, q, way):
        pltpu.make_async_remote_copy(
            src_ref=part.at[me, chunk(q)],
            dst_ref=from_z.at[way, u, chunk(q)],
            send_sem=z_send.at[u, q],
            recv_sem=z_recv.at[way, u, q],
            device_id=partner,
            device_id_type=MESH,
        ).wait_recv()

    def s_copy(q):
        return pltpu.make_async_remote_copy(
            src_ref=part.at[me, chunk(q)],
            dst_ref=from_side.at[chunk(q)],
            send_sem=s_send.at[q],
            recv_sem=s_recv.at[q],
            device_id=side,
            device_id_type=MESH,
        )

    def d_copy(b, source=None):
        return pltpu.make_async_remote_copy(
            src_ref=dp_send.at[b],
            dst_ref=dp_recv.at[me if source is None else source],
            send_sem=d_send.at[b],
            recv_sem=d_recv.at[me if source is None else source],
            device_id=(b // 2, lax.rem(b, 2), t),
            device_id_type=MESH,
        )

    def compute(i, u):
        load_rows(u, 0).wait()
        load_rows(u, 1).wait()

        @pl.when(i > 0)
        def _():
            for cp in store_unit(unit_at(i - 1)):
                cp.wait()

        slot_ids = lax.broadcasted_iota(jnp.int32, (capacity, tokens), 0).astype(f32)
        for b in range(4):
            for j in range(2):
                row = pl.ds(2 * (u * 4 + b) + j, 1)
                mark = mk[row, :]
                hit = (rk[row, :] == slot_ids) & (mark >= 0.0)
                pick[b, j * capacity : (j + 1) * capacity, :] = jnp.where(hit, 1.0, 0.0)
                w_slot[j, b * capacity : (b + 1) * capacity, :] = jnp.sum(
                    jnp.where(hit, mark, 0.0), axis=1, keepdims=True
                )
        tile = 512
        for b in range(4):
            chosen = pick[b].astype(bf16)
            for k in range(width // tile):
                cols = slice(k * tile, (k + 1) * tile)
                got = jnp.dot(
                    chosen, x_buf[b * tokens : (b + 1) * tokens, cols], preferred_element_type=f32
                ).astype(bf16)
                gy = jnp.dot(
                    chosen, y_buf[b * tokens : (b + 1) * tokens, cols], preferred_element_type=f32
                )
                for j in range(2):
                    to = slice(b * capacity, (b + 1) * capacity)
                    of = slice(j * capacity, (j + 1) * capacity)
                    xs[j, to, cols] = got[of]
                    ys[j, to, cols] = gy[of].astype(bf16)
                    de[j, to, cols] = (w_slot[j, to, :] * gy[of]).astype(bf16)

        @pl.when(i + 1 < nz)
        def _():
            load_rows(unit_at(i + 1), 0).start()
            load_rows(unit_at(i + 1), 1).start()

        def expert(j, carry):
            gate = jnp.dot(xs[j], wg[j], preferred_element_type=f32)
            upv = jnp.dot(xs[j], wu[j], preferred_element_type=f32)
            sig = 1.0 / (1.0 + jnp.exp(-gate))
            silu = gate * sig
            act[j] = (silu * upv).astype(bf16)
            grad_act = lax.dot_general(
                de[j], wd[j], (((1,), (1,)), ((), ())), preferred_element_type=f32
            )
            dg[j] = (grad_act * upv * (sig * (1.0 + gate * (1.0 - sig)))).astype(bf16)
            du[j] = (grad_act * silu).astype(bf16)
            total = jnp.zeros((rows_unit, 1), f32)
            for k in range(width // tile):
                cols = slice(k * tile, (k + 1) * tile)
                made = jnp.dot(act[j], wd[j, :, cols], preferred_element_type=f32)
                made = made.astype(bf16).astype(f32)
                total = total + jnp.sum(made * ys[j, :, cols].astype(f32), axis=1, keepdims=True)
                weighted = (w_slot[j] * made).astype(bf16)
                back = lax.dot_general(
                    dg[j], wg[j, cols, :], (((1,), (1,)), ((), ())), preferred_element_type=f32
                ) + lax.dot_general(
                    du[j], wu[j, cols, :], (((1,), (1,)), ((), ())), preferred_element_type=f32
                )
                back = back.astype(bf16)
                for b in range(4):
                    of = slice(b * capacity, (b + 1) * capacity)
                    to = pl.ds(pl.multiple_of(j * capacity, capacity), capacity)
                    pe[b, to, cols] = weighted[of]
                    bs[b, to, cols] = back[of]
            for b in range(4):
                to = pl.ds(pl.multiple_of(j * capacity, capacity), capacity)
                dp_slot[b, to, :] = total[b * capacity : (b + 1) * capacity]
            return carry

        lax.fori_loop(0, 2, expert, 0)

        def spread(b):
            chosen = pick[b]
            back = jnp.transpose(chosen).astype(bf16)
            for k in range(width // tile):
                cols = slice(k * tile, (k + 1) * tile)
                part[u * 4 + b, :, cols] = jnp.dot(
                    back, bs[b, :, cols], preferred_element_type=f32
                ).astype(bf16)

        for b in range(4):
            spread(b)
        for xx in range(2):
            for q in range(CUT):
                p_copy(u, xx, q).start()
        for b in range(4):
            back = jnp.transpose(pick[b]).astype(bf16)
            for k in range(width // tile):
                cols = slice(k * tile, (k + 1) * tile)
                y_out[b * tokens : (b + 1) * tokens, cols] = jnp.dot(
                    back, pe[b, :, cols], preferred_element_type=f32
                ).astype(bf16)
            for j in range(2):
                of = slice(j * capacity, (j + 1) * capacity)
                dp_send[u * 4 + b, j : j + 1, :] = jnp.sum(
                    pick[b, of, :] * dp_slot[b, of, :], axis=0, keepdims=True
                )
        for cp in store_unit(u):
            cp.start()
        for b in range(4):
            bb = u * 4 + b

            @pl.when(bb != me)
            def _():
                d_copy(bb).start()

    def wide(ref):
        return ref.astype(f32)

    def to_across(u):
        for q in range(CUT):
            for xx in range(2):
                p_copy(u, xx, q).wait_recv()
            blk = u * 4 + (1 - x) * 2 + c
            part[blk, chunk(q)] = (
                wide(part[blk, chunk(q)]) + wide(from_partner[u * 2 + 1 - x, chunk(q)])
            ).astype(bf16)
            x_copy(u, q).start()

    def along(u):
        blk = u * 4 + x * 2 + c
        for q in range(CUT):
            x_copy(u, q).wait_recv()

            def total():
                return (
                    wide(part[blk, chunk(q)])
                    + wide(from_partner[u * 2 + x, chunk(q)])
                    + wide(from_across[u, chunk(q)])
                )

            def hop(way, has_before):
                @pl.when(has_before)
                def _():
                    z_wait(u, q, way)
                    part[blk, chunk(q)] = (total() + wide(from_z[way, u, chunk(q)])).astype(bf16)

                @pl.when(jnp.logical_not(has_before))
                def _():
                    part[blk, chunk(q)] = total().astype(bf16)

                z_copy(u, q, way).start()

            @pl.when(u > z)
            def _():
                hop(0, has_down)

            @pl.when(u < z)
            def _():
                hop(1, has_up)

            @pl.when(u == z)
            def _():
                grad_tok[chunk(q)] = total()

                @pl.when(has_down)
                def _():
                    z_wait(u, q, 0)
                    grad_tok[chunk(q)] = grad_tok[chunk(q)] + wide(from_z[0, u, chunk(q)])

                @pl.when(has_up)
                def _():
                    z_wait(u, q, 1)
                    grad_tok[chunk(q)] = grad_tok[chunk(q)] + wide(from_z[1, u, chunk(q)])

                part[blk, chunk(q)] = grad_tok[chunk(q)].astype(bf16)
                s_copy(q).start()

    def unit(i, carry):
        u = unit_at(i)
        compute(i, u)

        @pl.when(i > 0)
        def _():
            along(unit_at(i - 1))

        to_across(u)
        return carry

    lax.fori_loop(0, nz, unit, 0)
    along(z)

    dp_recv[me] = dp_send[me]

    def take_prob(d, carry):
        d_copy(me, lax.rem(me + d, 2 * nf)).wait_recv()
        return carry

    lax.fori_loop(1, 2 * nf, take_prob, 0)
    swap_prob = pltpu.make_async_remote_copy(
        src_ref=dp_recv,
        dst_ref=dp_side,
        send_sem=s_send.at[CUT],
        recv_sem=s_recv.at[CUT],
        device_id=side,
        device_id_type=MESH,
    )
    swap_prob.start()
    run_direct()
    for q in range(CUT):
        s_copy(q).wait_recv()
        grad_tok[chunk(q)] = wide(part[me, chunk(q)]) + wide(from_side[chunk(q)])
    swap_prob.wait_recv()
    prob_tok[...] = dp_recv[...] + dp_side[...]

    for cp in store_unit(z):
        cp.wait()
    swap_prob.wait_send()

    def ends(u, carry):
        for q in range(CUT):
            for xx in range(2):
                p_copy(u, xx, q).wait_send()
            x_copy(u, q).wait_send()

            @pl.when(u > z)
            def _():
                z_copy(u, q, 0).wait_send()

            @pl.when(u < z)
            def _():
                z_copy(u, q, 1).wait_send()

        for b in range(4):

            @pl.when(u * 4 + b != me)
            def _():
                d_copy(u * 4 + b).wait_send()

        return carry

    lax.fori_loop(0, nz, ends, 0)
    for q in range(CUT):
        s_copy(q).wait_send()

    drain()


def visiting_order(nz):
    rows = []
    for at in range(nz):
        rows.append(sorted(range(nz), key=lambda u: (-abs(u - at), u if at < nz // 2 else -u)))
    return rows


def expert_pass(hidden_two, marks, hidden_slices, grad_all, w_gate, w_up, w_down, capacity, nf):
    specs = [
        Gather(hidden_two, nf, rep=True, chunks=4),
        Gather(marks, nf, rep=True, chunks=2),
        Gather(hidden_slices, nf, form="a2a", chunks=1),
    ]
    n = len(specs)
    f32, bf16 = jnp.float32, jnp.bfloat16
    tokens, width = hidden_two.shape
    nz = nf // 2
    total = sum(s.chunks for s in specs)
    hidden = w_gate.shape[2]
    rows = 2 * nf * capacity
    unit_rows = 4 * capacity
    slots = 2 * capacity
    any_spec = pl.BlockSpec(memory_space=pl.ANY)
    vmem = pl.BlockSpec(memory_space=pltpu.VMEM)
    dma = pltpu.SemaphoreType.DMA
    outs = [jax.ShapeDtypeStruct(s.out_shape(nf), s.array.dtype) for s in specs] + [
        jax.ShapeDtypeStruct((2 * nf * tokens, width), bf16),
        jax.ShapeDtypeStruct((2, rows, width), bf16),
        jax.ShapeDtypeStruct((2, rows, width), bf16),
        jax.ShapeDtypeStruct((2, rows, hidden), bf16),
        jax.ShapeDtypeStruct((2, rows, hidden), bf16),
        jax.ShapeDtypeStruct((2, rows, hidden), bf16),
        jax.ShapeDtypeStruct((tokens, width), f32),
        jax.ShapeDtypeStruct((2 * nf, 8, tokens), f32),
    ]
    result = pl.pallas_call(
        functools.partial(expert_kernel, nf, capacity, tuple(specs)),
        out_shape=tuple(outs),
        in_specs=[any_spec] * (n + 4),
        out_specs=tuple([any_spec] * (n + 6) + [vmem, vmem]),
        scratch_shapes=[stage_of(s, nf) for s in specs]
        + [dma((2 * nf, total)), dma((5, 2 * nf, total)), dma((2, n))]
        + [
            pltpu.VMEM(w_gate.shape, bf16),
            pltpu.VMEM(w_up.shape, bf16),
            pltpu.VMEM(w_down.shape, bf16),
            pltpu.VMEM((4 * tokens, width), bf16),
            pltpu.VMEM((4 * tokens, width), bf16),
            pltpu.VMEM((2, unit_rows, width), bf16),
            pltpu.VMEM((2, unit_rows, width), bf16),
            pltpu.VMEM((2, unit_rows, width), bf16),
            pltpu.VMEM((4, slots, width), bf16),
            pltpu.VMEM((4, slots, width), bf16),
            pltpu.VMEM((2, unit_rows, hidden), bf16),
            pltpu.VMEM((2, unit_rows, hidden), bf16),
            pltpu.VMEM((2, unit_rows, hidden), bf16),
            pltpu.VMEM((2, unit_rows, 1), f32),
            pltpu.VMEM((4, slots, 1), f32),
            pltpu.VMEM((4, slots, tokens), f32),
            pltpu.VMEM((4 * nf, tokens), f32),
            pltpu.VMEM((4 * nf, tokens), f32),
            pltpu.VMEM((4 * tokens, width), bf16),
            pltpu.VMEM((2 * nf, tokens, width), bf16),
            pltpu.VMEM((nf, tokens, width), bf16),
            pltpu.VMEM((nz, tokens, width), bf16),
            pltpu.VMEM((2, nz, tokens, width), bf16),
            pltpu.VMEM((tokens, width), bf16),
            pltpu.VMEM((2 * nf, 8, tokens), f32),
            pltpu.VMEM((2 * nf, 8, tokens), f32),
            pltpu.VMEM((2 * nf, 8, tokens), f32),
            pltpu.VMEM(specs[1].out_shape(nf), f32),
            dma((3,)),
            dma((3,)),
            dma((6,)),
            dma((nf, CUT)),
            dma((nf, CUT)),
            dma((nz, CUT)),
            dma((nz, CUT)),
            dma((nz, CUT)),
            dma((2, nz, CUT)),
            dma((CUT + 1,)),
            dma((CUT + 1,)),
            dma((2 * nf,)),
            dma((2 * nf,)),
        ],
        compiler_params=pltpu.CompilerParams(
            collective_id=7, has_side_effects=True, vmem_limit_bytes=67043328
        ),
    )(*[s.array for s in specs], grad_all, w_gate, w_up, w_down)
    hidden_all, _, hidden_slice = result[:3]
    return (hidden_all, hidden_slice) + tuple(result[3:])


NT = (((1,), (1,)), ((), ()))
TN = (((0,), (0,)), ((), ()))
NN = (((1,), (0,)), ((), ()))


def backward_kernel(nf, specs, *refs):
    n = len(specs)
    (
        attended,
        dh2_moe,
        grad_prob,
        probs,
        router,
        x_in,
        x_mid,
        gains,
        grad_out,
        wo_hbm,
        wq_hbm,
        wk_hbm,
        wv_hbm,
        q_raw,
        k_raw,
        q_rot,
        keys,
        values,
        bias,
        lse,
        trig,
        out_part,
    ), refs = refs[:22], refs[22:]
    gathered, grad_in, block_out, refs = refs[:n], refs[n], refs[n + 1], refs[n + 2 :]
    stage, refs = refs[:n], refs[n:]
    (recv, send, local), refs = refs[:3], refs[3:]
    (
        w_big,
        w_key,
        w_value,
        dx1,
        dh2,
        d_out,
        d_out_slices,
        d_attn,
        d_query,
        d_key,
        d_value,
        logit,
        tail,
        dk_acc,
        dv_acc,
        qk_acc,
        kv_send,
        kv_recv,
        dh1,
        dh1_side,
        qk_side,
        row_sum,
        w_sem,
        kv_sem,
        side_send,
        side_recv,
        sum_own,
        sum_total,
        sum_bufs,
        sum_sems,
    ) = refs[:28] + (refs[28:32], refs[32:])
    f32, bf16 = jnp.float32, jnp.bfloat16
    f, c, t = lax.axis_index("fsdp"), lax.axis_index("ctx"), lax.axis_index("tp")
    partner, side = (f, 1 - c, t), (f, c, 1 - t)
    tokens, width = x_in.shape
    experts = probs.shape[1]
    scale = HEAD_SIZE ** (-0.5)

    barrier = pltpu.get_barrier_semaphore()

    def greet(d, carry):
        pl.semaphore_signal(
            barrier, 1, device_id=(lax.rem(f + d, nf), c, t), device_id_type=MESH
        )
        return carry

    lax.fori_loop(1, nf, greet, 0)
    for dev in (partner, side):
        pl.semaphore_signal(barrier, 1, device_id=dev, device_id_type=MESH)
    pl.semaphore_wait(barrier, nf + 1)

    ins = (attended, d_query, d_key, d_value, logit, tail, d_out_slices)
    start, run, land, start_direct, run_direct, drain, step_of, edge_of, _ = gather_engine(
        nf, specs, ins, gathered, stage, recv, send, local
    )
    early, late = (0,), (1, 2, 3, 4, 5)
    nz = nf // 2
    order = visit_code(nz, f // 2)
    own_loads, to_partner, to_across, along, finish_sum, drain_sum = token_sum(
        nf, out_part, sum_own, sum_total, sum_bufs, sum_sems
    )
    for cp in own_loads:
        cp.start()
    lax.fori_loop(0, nz, lambda i, carry: to_partner(visit(order, nz, i), carry), 0)
    start((0,))

    def load(src, dst, i):
        return pltpu.make_async_copy(src, dst, w_sem.at[i])

    load(wo_hbm, w_big, 0).start()
    load(wk_hbm, w_key, 1).start()
    load(wv_hbm, w_value, 2).start()

    logit[...] = jnp.zeros_like(logit)
    pr = probs[...]
    gp = grad_prob[...]
    dl = (pr * (gp - jnp.sum(pr * gp, axis=1, keepdims=True))).astype(bf16)
    logit[:, :experts] = dl
    tile = 512
    for k in range(width // tile):
        cols = slice(k * tile, (k + 1) * tile)
        dh2[:, cols] = dh2_moe[:, cols] + lax.dot_general(
            dl, router[:, cols], NN, preferred_element_type=f32
        )
    gain_one, gain_two = gains[0:1, :], gains[1:2, :]
    gain_query, gain_key = gains[2:3, :HEAD_SIZE], gains[2:3, HEAD_SIZE : 2 * HEAD_SIZE]
    row_sum[...] = jnp.zeros_like(row_sum)
    part_rows = 16

    def norm_two(i, carry):
        rows = pl.ds(pl.multiple_of(i * part_rows, part_rows), part_rows)
        x1 = x_mid[rows]
        r2 = lax.rsqrt(jnp.mean(x1 * x1, axis=1, keepdims=True) + eps_norm)
        n2 = x1 * r2
        g = dh2[rows]
        row_sum[1:2, :] += jnp.sum(g * n2, axis=0, keepdims=True)
        scaled = g * gain_two
        mean = jnp.mean(scaled * n2, axis=1, keepdims=True)
        out = grad_out[rows].astype(f32) + r2 * (scaled - n2 * mean)
        dx1[rows] = out
        d_out[rows] = out.astype(bf16)
        return carry

    lax.fori_loop(0, tokens // part_rows, norm_two, 0)
    shard = width // nf
    for k in range(nf):
        d_out_slices[k * tokens : (k + 1) * tokens, :] = d_out[:, k * shard : (k + 1) * shard]

    load(wo_hbm, w_big, 0).wait()
    heads_width = d_attn.shape[1]
    tile = 256
    for k in range(heads_width // tile):
        cols = slice(k * tile, (k + 1) * tile)
        d_attn[:, cols] = lax.dot_general(
            d_out[...], w_big[cols, :], NT, preferred_element_type=f32
        ).astype(bf16)
    load(wq_hbm, w_big, 0).start()
    for cp in own_loads:
        cp.wait()
    for i in range(2):
        to_across(visit(order, nz, i), 0)
    step_of(1, early)
    dk_acc[...] = jnp.zeros_like(dk_acc)
    dv_acc[...] = jnp.zeros_like(dv_acc)
    qk_acc[...] = jnp.zeros_like(qk_acc)
    group = QUERY_HEADS // KEY_VALUE_HEADS

    def unrope(g):
        return g * trig[0] + pltpu.roll(g, HEAD_SIZE // 2, 1) * trig[1]

    def norm_back(g, raw, gain):
        inv = lax.rsqrt(jnp.mean(raw * raw, axis=1, keepdims=True) + eps_norm)
        hat = raw * inv
        scaled = g * gain
        mean = jnp.mean(scaled * hat, axis=1, keepdims=True)
        return jnp.sum(g * hat, axis=0, keepdims=True), inv * (scaled - hat * mean)

    def head(h, carry):
        cols = pl.ds(pl.multiple_of(h * HEAD_SIZE, HEAD_SIZE), HEAD_SIZE)
        kv_cols = pl.ds(pl.multiple_of((h // group) * HEAD_SIZE, HEAD_SIZE), HEAD_SIZE)
        q, key, value, da = q_rot[:, cols], keys[:, kv_cols], values[:, kv_cols], d_attn[:, cols]
        s = lax.dot_general(q, key, NT, preferred_element_type=f32) * scale + bias[...]
        prob = jnp.exp(s - lse[h])
        dp = lax.dot_general(da, value, NT, preferred_element_type=f32)
        delta = jnp.sum(prob * dp, axis=1, keepdims=True)
        ds = (prob * (dp - delta) * scale).astype(bf16)
        dk_acc[:, kv_cols] += lax.dot_general(ds, q, TN, preferred_element_type=f32)
        dv_acc[:, kv_cols] += lax.dot_general(
            prob.astype(bf16), da, TN, preferred_element_type=f32
        )
        dq = unrope(jnp.dot(ds, key, preferred_element_type=f32))
        gain_grad, dq = norm_back(dq, q_raw[:, cols], gain_query)
        qk_acc[0:1, :] += gain_grad
        d_query[:, cols] = dq.astype(bf16)
        return carry

    heads = heads_width // HEAD_SIZE
    lax.fori_loop(0, heads // 2, head, 0)
    for i in range(2, nz):
        to_across(visit(order, nz, i), 0)
    step_of(2, early)
    lax.fori_loop(heads // 2, heads, head, 0)

    kv_width = dk_acc.shape[1]
    theirs = pl.ds(pl.multiple_of((1 - c) * tokens, tokens), tokens)
    mine = pl.ds(pl.multiple_of(c * tokens, tokens), tokens)
    kv_send[:, :kv_width] = dk_acc[theirs].astype(bf16)
    kv_send[:, kv_width:] = dv_acc[theirs].astype(bf16)
    swap_kv = pltpu.make_async_remote_copy(
        src_ref=kv_send,
        dst_ref=kv_recv,
        send_sem=kv_sem.at[0],
        recv_sem=kv_sem.at[1],
        device_id=partner,
        device_id_type=MESH,
    )
    swap_kv.start()
    start((1, 4))
    start_direct()
    swap_kv.wait()
    for kv in range(kv_width // HEAD_SIZE):
        cols = slice(kv * HEAD_SIZE, (kv + 1) * HEAD_SIZE)
        g = dk_acc[mine, cols] + kv_recv[:, cols].astype(f32)
        gain_grad, dk = norm_back(unrope(g), k_raw[:, cols], gain_key)
        qk_acc[1:2, :] += gain_grad
        d_key[:, cols] = dk.astype(bf16)
    d_value[...] = (dv_acc[mine] + kv_recv[:, kv_width:].astype(f32)).astype(bf16)
    start((2, 3))

    def to_side(src, dst, i):
        return pltpu.make_async_remote_copy(
            src_ref=src,
            dst_ref=dst,
            send_sem=side_send.at[i],
            recv_sem=side_recv.at[i],
            device_id=side,
            device_id_type=MESH,
        )

    swap_qk = to_side(qk_acc, qk_side, 4)
    swap_qk.start()
    load(wq_hbm, w_big, 0).wait()
    load(wk_hbm, w_key, 1).wait()
    load(wv_hbm, w_value, 2).wait()
    quarter = width // 4

    def dh1_copy(i):
        cols = pl.ds(i * quarter, quarter)
        return to_side(dh1.at[:, cols], dh1_side.at[:, cols], i)

    for k in range(width // tile):
        rows = slice(k * tile, (k + 1) * tile)
        total = lax.dot_general(d_query[...], w_big[rows, :], NT, preferred_element_type=f32)
        total = total + lax.dot_general(d_key[...], w_key[rows, :], NT, preferred_element_type=f32)
        total = total + lax.dot_general(
            d_value[...], w_value[rows, :], NT, preferred_element_type=f32
        )
        dh1[:, rows] = total.astype(bf16)
        if (k + 1) * tile % quarter == 0:
            dh1_copy((k + 1) * tile // quarter - 1).start()
    step_of(3, early)
    along(visit(order, nz, 0))
    for i in range(4):
        dh1_copy(i).wait_recv()
    swap_qk.wait_recv()

    def norm_one(i, carry):
        rows = pl.ds(pl.multiple_of(i * part_rows, part_rows), part_rows)
        x0 = x_in[rows].astype(f32)
        r1 = lax.rsqrt(jnp.mean(x0 * x0, axis=1, keepdims=True) + eps_norm)
        n1 = x0 * r1
        g = dh1[rows].astype(f32) + dh1_side[rows].astype(f32)
        row_sum[0:1, :] += jnp.sum(g * n1, axis=0, keepdims=True)
        scaled = g * gain_one
        mean = jnp.mean(scaled * n1, axis=1, keepdims=True)
        grad_in[rows] = dx1[rows] + r1 * (scaled - n1 * mean)
        return carry

    lax.fori_loop(0, tokens // part_rows, norm_one, 0)
    lanes = width // 128
    tail[...] = jnp.zeros_like(tail)
    for which in range(2):
        for k in range(lanes):
            row = which * lanes + k
            tail[row : row + 1, :] = row_sum[which : which + 1, k * 128 : (k + 1) * 128]
    tail[2 * lanes : 2 * lanes + 2, :] = qk_acc[0:2, :] + qk_side[0:2, :]
    start((5,))
    step_of(1, late)
    edge_of(early)
    along(visit(order, nz, 1))
    step_of(2, late)
    along(visit(order, nz, 2))
    step_of(3, late)
    edge_of(late)
    along(f // 2)
    run_direct()
    land()

    def put_out(rows, value):
        block_out[rows] = (x_mid[rows] + value).astype(bf16)

    finish_sum(put_out)
    drain()
    drain_sum()
    for i in range(4):
        dh1_copy(i).wait_send()
    swap_qk.wait_send()


def visit_code(nz, z):
    order = 0
    for at, seq in enumerate(visiting_order(nz)):
        code = sum(u * nz**i for i, u in enumerate(seq))
        order = order + code * (z == at).astype(jnp.int32)
    return order


def visit(code, nz, i):
    for k in range(nz):
        code = jnp.where(i > k, code // nz, code)
    return lax.rem(code, nz)


SUM_CUT = 2


def token_sum(nf, partial, own, total_ref, bufs, sems):
    from_partner, from_across, from_z, from_side = bufs
    load_sem, p_send, p_recv, x_send, x_recv, z_send, z_recv, s_send, s_recv = sems
    nz = nf // 2
    f, c, t = lax.axis_index("fsdp"), lax.axis_index("ctx"), lax.axis_index("tp")
    z, x = f // 2, lax.rem(f, 2)
    has_up, has_down = z + 1 < nz, z > 0
    up, down = (f + 2, c, t), (f - 2, c, t)
    across_dev, partner, side = (z * 2 + 1 - x, c, t), (f, 1 - c, t), (f, c, 1 - t)
    tokens = total_ref.shape[0]
    rows = tokens // SUM_CUT
    bf16 = jnp.bfloat16

    def chunk(q):
        return pl.ds(q * rows, rows)

    def remote(src, dst, send, recv, dev):
        return pltpu.make_async_remote_copy(
            src_ref=src,
            dst_ref=dst,
            send_sem=send,
            recv_sem=recv,
            device_id=dev,
            device_id_type=MESH,
        )

    own_loads = [
        pltpu.make_async_copy(
            partial.at[pl.ds((2 * b + c) * tokens, tokens)], own.at[b], load_sem.at[b]
        )
        for b in range(nf)
    ]

    def p_copy(u, xx, q):
        b = u * 2 + xx
        return remote(
            partial.at[pl.ds((2 * b + 1 - c) * tokens + q * rows, rows)],
            from_partner.at[b, chunk(q)],
            p_send.at[b, q],
            p_recv.at[b, q],
            partner,
        )

    def x_copy(u, q):
        return remote(
            own.at[u * 2 + 1 - x, chunk(q)],
            from_across.at[u, chunk(q)],
            x_send.at[u, q],
            x_recv.at[u, q],
            across_dev,
        )

    def z_copy(u, q, way, dev):
        return remote(
            own.at[u * 2 + x, chunk(q)],
            from_z.at[way, u, chunk(q)],
            z_send.at[u, q],
            z_recv.at[way, u, q],
            dev,
        )

    def s_copy(q):
        return remote(
            own.at[f, chunk(q)], from_side.at[chunk(q)], s_send.at[q], s_recv.at[q], side
        )

    def wide(value):
        return value.astype(jnp.float32)

    def to_partner(u, carry):
        for xx in range(2):
            for q in range(SUM_CUT):
                p_copy(u, xx, q).start()
        return carry

    def to_across(u, carry):
        b = u * 2 + 1 - x
        for q in range(SUM_CUT):
            for xx in range(2):
                p_copy(u, xx, q).wait_recv()
            own[b, chunk(q)] = (wide(own[b, chunk(q)]) + wide(from_partner[b, chunk(q)])).astype(
                bf16
            )
            x_copy(u, q).start()
        return carry

    def along(u):
        b = u * 2 + x
        for q in range(SUM_CUT):
            x_copy(u, q).wait_recv()
            total_ref[chunk(q)] = (
                wide(own[b, chunk(q)])
                + wide(from_partner[b, chunk(q)])
                + wide(from_across[u, chunk(q)])
            )

            @pl.when((u >= z) & has_down)
            def _():
                z_copy(u, q, 0, partner).wait_recv()
                total_ref[chunk(q)] += wide(from_z[0, u, chunk(q)])

            @pl.when((u <= z) & has_up)
            def _():
                z_copy(u, q, 1, partner).wait_recv()
                total_ref[chunk(q)] += wide(from_z[1, u, chunk(q)])

            own[b, chunk(q)] = total_ref[chunk(q)].astype(bf16)

            @pl.when(u > z)
            def _():
                z_copy(u, q, 0, up).start()

            @pl.when(u < z)
            def _():
                z_copy(u, q, 1, down).start()

            @pl.when(u == z)
            def _():
                s_copy(q).start()

    def finish_sum(put):
        for q in range(SUM_CUT):
            s_copy(q).wait_recv()
            put(chunk(q), wide(own[f, chunk(q)]) + wide(from_side[chunk(q)]))

    def drain_sum():
        def ends(u, carry):
            for q in range(SUM_CUT):
                for xx in range(2):
                    p_copy(u, xx, q).wait_send()
                x_copy(u, q).wait_send()

                @pl.when(u != z)
                def _():
                    z_copy(u, q, 0, partner).wait_send()

            return carry

        lax.fori_loop(0, nz, ends, 0)
        for q in range(SUM_CUT):
            s_copy(q).wait_send()

    return own_loads, to_partner, to_across, along, finish_sum, drain_sum


def backward_pass(nf, arrays, attended, shapes):
    f32, bf16 = jnp.float32, jnp.bfloat16
    tokens, width, heads_width, kv_width, keys = shapes
    tail_rows = -(-(2 * width // 128 + 2) // 8) * 8
    shape = jax.ShapeDtypeStruct
    specs = [
        Gather(attended, nf, chunks=2),
        Gather(shape((tokens, heads_width), bf16), nf, chunks=2),
        Gather(shape((tokens, kv_width), bf16), nf, chunks=1),
        Gather(shape((tokens, kv_width), bf16), nf, chunks=1),
        Gather(shape((tokens, 128), bf16), nf, chunks=1),
        Gather(shape((tail_rows, 128), f32), nf, chunks=1),
        Gather(shape((nf * tokens, width // nf), bf16), nf, form="a2a", chunks=1),
    ]
    n = len(specs)
    total = sum(s.chunks for s in specs)
    any_spec = pl.BlockSpec(memory_space=pl.ANY)
    vmem = pl.BlockSpec(memory_space=pltpu.VMEM)
    dma = pltpu.SemaphoreType.DMA
    in_any = {0, 9, 10, 11, 12, 21}
    nz = nf // 2
    return pl.pallas_call(
        functools.partial(backward_kernel, nf, tuple(specs)),
        out_shape=tuple(shape(s.out_shape(nf), s.array.dtype) for s in specs)
        + (shape((tokens, width), f32), shape((tokens, width), bf16)),
        in_specs=[any_spec if i in in_any else vmem for i in range(22)],
        out_specs=tuple([any_spec] * n + [vmem, vmem]),
        scratch_shapes=[stage_of(s, nf) for s in specs]
        + [dma((2 * nf, total)), dma((5, 2 * nf, total)), dma((2, n))]
        + [
            pltpu.VMEM((width, max(width, heads_width)), bf16),
            pltpu.VMEM((width, kv_width), bf16),
            pltpu.VMEM((width, kv_width), bf16),
            pltpu.VMEM((tokens, width), f32),
            pltpu.VMEM((tokens, width), f32),
            pltpu.VMEM((tokens, width), bf16),
            pltpu.VMEM((nf * tokens, width // nf), bf16),
            pltpu.VMEM((tokens, heads_width), bf16),
            pltpu.VMEM((tokens, heads_width), bf16),
            pltpu.VMEM((tokens, kv_width), bf16),
            pltpu.VMEM((tokens, kv_width), bf16),
            pltpu.VMEM((tokens, 128), bf16),
            pltpu.VMEM((tail_rows, 128), f32),
            pltpu.VMEM((keys, kv_width), f32),
            pltpu.VMEM((keys, kv_width), f32),
            pltpu.VMEM((8, 128), f32),
            pltpu.VMEM((tokens, 2 * kv_width), bf16),
            pltpu.VMEM((tokens, 2 * kv_width), bf16),
            pltpu.VMEM((tokens, width), bf16),
            pltpu.VMEM((tokens, width), bf16),
            pltpu.VMEM((8, 128), f32),
            pltpu.VMEM((2, width), f32),
            dma((3,)),
            dma((2,)),
            dma((5,)),
            dma((5,)),
            pltpu.VMEM((nf, tokens, width), bf16),
            pltpu.VMEM((tokens, width), f32),
            pltpu.VMEM((nf, tokens, width), bf16),
            pltpu.VMEM((nz, tokens, width), bf16),
            pltpu.VMEM((2, nz, tokens, width), bf16),
            pltpu.VMEM((tokens, width), bf16),
            dma((nf,)),
            dma((nf, SUM_CUT)),
            dma((nf, SUM_CUT)),
            dma((nz, SUM_CUT)),
            dma((nz, SUM_CUT)),
            dma((nz, SUM_CUT)),
            dma((2, nz, SUM_CUT)),
            dma((SUM_CUT,)),
            dma((SUM_CUT,)),
        ],
        compiler_params=pltpu.CompilerParams(
            collective_id=8, has_side_effects=True, vmem_limit_bytes=67043328
        ),
    )(attended, *arrays)


def forward_kernel(nf, specs, *refs):
    n = len(specs)
    ins, refs = refs[:n], refs[n:]
    (x_in, segments, routed, trig), refs = refs[:4], refs[4:]
    gathered, refs = refs[:n], refs[n:]
    (
        hidden,
        hidden_slices,
        marks,
        probs,
        x_mid,
        attended,
        q_raw,
        k_raw,
        q_rot,
        keys,
        values,
        bias,
        lse,
        gains,
        router,
    ), refs = refs[:15], refs[15:]
    stage, refs = refs[:n], refs[n:]
    (recv, send, local), refs = refs[:3], refs[3:]
    (
        w_big,
        w_key,
        w_value,
        small,
        hidden_one,
        kv_all,
        part,
        part_side,
        square,
        w_sem,
        kv_sem,
        side_send,
        side_recv,
    ) = refs
    f32, bf16 = jnp.float32, jnp.bfloat16
    nz = nf // 2
    f, c, t = lax.axis_index("fsdp"), lax.axis_index("ctx"), lax.axis_index("tp")
    z, x = f // 2, lax.rem(f, 2)
    partner, side = (f, 1 - c, t), (f, c, 1 - t)
    has_up, has_down = z + 1 < nz, z > 0
    tokens, width = x_in.shape
    experts = routed.shape[1]
    heads_width = q_raw.shape[1]
    kv_width = k_raw.shape[1]
    scale = HEAD_SIZE ** (-0.5)
    barrier = pltpu.get_barrier_semaphore()

    def greet(dev):
        pl.semaphore_signal(barrier, 1, device_id=dev, device_id_type=MESH)

    for dev in (partner, side, (z * 2 + 1 - x, c, t)):
        greet(dev)

    @pl.when(has_up)
    def _():
        greet((f + 2, c, t))

    @pl.when(has_down)
    def _():
        greet((f - 2, c, t))

    pl.semaphore_wait(barrier, 3 + has_up.astype(jnp.int32) + has_down.astype(jnp.int32))
    start, _, _, _, _, drain, step_of, edge_of, land_of = gather_engine(
        nf, specs, ins, gathered, stage, recv, send, local
    )
    first, second, third = (0, 1, 2, 3), (4,), (5,)
    start(first)
    for k in range(1, nz):
        step_of(k, first)
    start(second)
    edge_of(first)
    land_of(first)

    def load(src, dst, i):
        return pltpu.make_async_copy(src, dst, w_sem.at[i])

    small_load = load(gathered[0], small, 3)
    small_load.start()
    load(gathered[2], w_key, 1).start()
    load(gathered[3], w_value, 2).start()
    load(gathered[1], w_big, 0).start()
    small_load.wait()

    size = specs[0].rows
    halves = width // nf // 128
    qk_sum = [jnp.zeros((1, 128), f32), jnp.zeros((1, 128), f32)]
    for k in range(nf):
        base = 2 * k * size
        for h in range(halves):
            cols = slice((k * halves + h) * 128, (k * halves + h + 1) * 128)
            router[:, cols] = small[base + h * experts : base + (h + 1) * experts, :]
            at = base + halves * experts
            for g in range(2):
                row = at + g * halves + h
                gains[g : g + 1, cols] = small[row : row + 1, :].astype(f32)
        at = base + halves * experts + 2 * halves
        for h in range(2):
            qk_sum[h] = qk_sum[h] + small[at + h : at + h + 1, :].astype(f32)
    gains[2:3, :] = jnp.zeros((1, width), f32)
    for h in range(2):
        gains[2:3, h * 128 : (h + 1) * 128] = qk_sum[h]
    gain_one, gain_two = gains[0:1, :], gains[1:2, :]
    gain_query, gain_key = qk_sum
    part_rows = 16

    def norm_one(i, carry):
        rows = pl.ds(pl.multiple_of(i * part_rows, part_rows), part_rows)
        x0 = x_in[rows].astype(f32)
        r1 = lax.rsqrt(jnp.mean(x0 * x0, axis=1, keepdims=True) + eps_norm)
        hidden_one[rows] = (x0 * r1 * gain_one).astype(bf16)
        return carry

    lax.fori_loop(0, tokens // part_rows, norm_one, 0)
    shard = width // nf
    for k in range(nf):
        hidden_slices[k * tokens : (k + 1) * tokens, :] = hidden_one[:, k * shard : (k + 1) * shard]

    def norm_rope(raw, gain):
        inv = lax.rsqrt(jnp.mean(raw * raw, axis=1, keepdims=True) + eps_norm)
        normed = raw * inv * gain
        turned = normed * trig[0] - pltpu.roll(normed, HEAD_SIZE // 2, 1) * trig[1]
        return turned.astype(bf16)

    load(gathered[2], w_key, 1).wait()
    load(gathered[3], w_value, 2).wait()
    mine = pl.ds(pl.multiple_of(c * tokens, tokens), tokens)
    k_raw[...] = jnp.dot(hidden_one[...], w_key[...], preferred_element_type=f32)
    kv_all[mine, kv_width : 2 * kv_width] = jnp.dot(
        hidden_one[...], w_value[...], preferred_element_type=f32
    ).astype(bf16)
    for kv in range(kv_width // HEAD_SIZE):
        cols = slice(kv * HEAD_SIZE, (kv + 1) * HEAD_SIZE)
        kv_all[mine, cols] = norm_rope(k_raw[:, cols], gain_key)
    kv_all[mine, 2 * kv_width :] = segments[...]
    swap_kv = pltpu.make_async_remote_copy(
        src_ref=kv_all.at[mine],
        dst_ref=kv_all.at[mine],
        send_sem=kv_sem.at[0],
        recv_sem=kv_sem.at[1],
        device_id=partner,
        device_id_type=MESH,
    )
    swap_kv.start()
    step_of(1, second)
    load(gathered[1], w_big, 0).wait()
    tile = 256
    for k in range(heads_width // tile):
        cols = slice(k * tile, (k + 1) * tile)
        q_raw[:, cols] = jnp.dot(hidden_one[...], w_big[:, cols], preferred_element_type=f32)
    swap_kv.wait()
    keys[...] = kv_all[:, :kv_width]
    values[...] = kv_all[:, kv_width : 2 * kv_width]
    span = kv_all.shape[0]
    theirs = jnp.transpose(kv_all[:, 2 * kv_width :].astype(f32))
    own = segments[...].astype(f32)
    query_at = c * tokens + lax.broadcasted_iota(jnp.int32, (tokens, 128), 0)
    for h in range(span // 128):
        cols = slice(h * 128, (h + 1) * 128)
        key_at = h * 128 + lax.broadcasted_iota(jnp.int32, (tokens, 128), 1)
        allowed = (key_at <= query_at) & (theirs[:, cols] == own)
        bias[:, cols] = jnp.where(allowed, 0.0, -jnp.inf)
    step_of(2, second)
    group = QUERY_HEADS // KEY_VALUE_HEADS

    def head(h, carry):
        cols = pl.ds(pl.multiple_of(h * HEAD_SIZE, HEAD_SIZE), HEAD_SIZE)
        kv_cols = pl.ds(pl.multiple_of((h // group) * HEAD_SIZE, HEAD_SIZE), HEAD_SIZE)
        q = norm_rope(q_raw[:, cols], gain_query)
        q_rot[:, cols] = q
        s = lax.dot_general(q, keys[:, kv_cols], NT, preferred_element_type=f32) * scale
        s = s + bias[...]
        top = jnp.max(s, axis=1, keepdims=True)
        total = top + jnp.log(jnp.sum(jnp.exp(s - top), axis=1, keepdims=True))
        lse[h] = total
        prob = jnp.exp(s - total).astype(bf16)
        attended[:, cols] = jnp.dot(
            prob, values[:, kv_cols], preferred_element_type=f32
        ).astype(bf16)
        return carry

    heads = heads_width // HEAD_SIZE
    lax.fori_loop(0, heads // 2, head, 0)
    step_of(3, second)
    start(third)
    lax.fori_loop(heads // 2, heads, head, 0)
    edge_of(second)
    land_of(second)
    load(gathered[4], w_big, 0).start()
    step_of(1, third)
    load(gathered[4], w_big, 0).wait()
    quarter = width // 4

    def side_copy(i):
        cols = pl.ds(i * quarter, quarter)
        return pltpu.make_async_remote_copy(
            src_ref=part.at[:, cols],
            dst_ref=part_side.at[:, cols],
            send_sem=side_send.at[i],
            recv_sem=side_recv.at[i],
            device_id=side,
            device_id_type=MESH,
        )

    for k in range(width // tile):
        cols = slice(k * tile, (k + 1) * tile)
        part[:, cols] = jnp.dot(
            attended[...], w_big[:, cols], preferred_element_type=f32
        ).astype(bf16)
        if (k + 1) * tile % quarter == 0:
            side_copy((k + 1) * tile // quarter - 1).start()
    step_of(2, third)
    for i in range(4):
        side_copy(i).wait_recv()

    def norm_two(i, carry):
        rows = pl.ds(pl.multiple_of(i * part_rows, part_rows), part_rows)
        x1 = x_in[rows].astype(f32) + (part[rows].astype(f32) + part_side[rows].astype(f32))
        x_mid[rows] = x1
        r2 = lax.rsqrt(jnp.mean(x1 * x1, axis=1, keepdims=True) + eps_norm)
        hidden[rows] = (x1 * r2 * gain_two).astype(bf16)
        return carry

    lax.fori_loop(0, tokens // part_rows, norm_two, 0)
    logits = lax.dot_general(hidden[...], router[...], NT, preferred_element_type=f32)
    on = routed[...] > 0.0
    kept = jnp.where(on, logits, -jnp.inf)
    raised = jnp.where(on, jnp.exp(kept - jnp.max(kept, axis=1, keepdims=True)), 0.0)
    shares = raised / jnp.sum(raised, axis=1, keepdims=True)
    probs[...] = shares
    square[...] = jnp.zeros_like(square)
    square[:, :experts] = jnp.where(on, shares, -1.0)
    marks[...] = jnp.transpose(square[...])[:experts, :]
    step_of(3, third)
    edge_of(third)
    land_of(third)
    drain()
    for i in range(4):
        side_copy(i).wait_send()


def forward_pass(nf, arrays, operands, shapes):
    f32, bf16 = jnp.float32, jnp.bfloat16
    small, w_query, key_projection, value_projection, w_out, grad_out = arrays
    tokens, width, heads_width, kv_width, experts = shapes
    specs = [
        Gather(small, nf, chunks=1),
        Gather(w_query, nf, half=True, chunks=2),
        Gather(key_projection, nf, half=True, chunks=1),
        Gather(value_projection, nf, half=True, chunks=1),
        Gather(w_out, nf, form="col", half=True, chunks=2),
        Gather(grad_out, nf, rep=True, chunks=4),
    ]
    n = len(specs)
    total = sum(s.chunks for s in specs)
    any_spec = pl.BlockSpec(memory_space=pl.ANY)
    vmem = pl.BlockSpec(memory_space=pltpu.VMEM)
    dma = pltpu.SemaphoreType.DMA
    shape = jax.ShapeDtypeStruct
    span = 2 * tokens
    made = [
        shape((tokens, width), bf16),
        shape((nf * tokens, width // nf), bf16),
        shape((experts, tokens), f32),
        shape((tokens, experts), f32),
        shape((tokens, width), f32),
        shape((tokens, heads_width), bf16),
        shape((tokens, heads_width), f32),
        shape((tokens, kv_width), f32),
        shape((tokens, heads_width), bf16),
        shape((span, kv_width), bf16),
        shape((span, kv_width), bf16),
        shape((tokens, span), f32),
        shape((heads_width // HEAD_SIZE, tokens, 1), f32),
        shape((3, width), f32),
        shape((experts, width), bf16),
    ]
    return pl.pallas_call(
        functools.partial(forward_kernel, nf, tuple(specs)),
        out_shape=tuple(shape(s.out_shape(nf), s.array.dtype) for s in specs) + tuple(made),
        in_specs=[any_spec] * n + [vmem] * 4,
        out_specs=tuple([any_spec] * n + [vmem] * len(made)),
        scratch_shapes=[stage_of(s, nf) for s in specs]
        + [dma((2 * nf, total)), dma((5, 2 * nf, total)), dma((2, n))]
        + [
            pltpu.VMEM((width, max(width, heads_width)), bf16),
            pltpu.VMEM((width, kv_width), bf16),
            pltpu.VMEM((width, kv_width), bf16),
            pltpu.VMEM(specs[0].out_shape(nf), bf16),
            pltpu.VMEM((tokens, width), bf16),
            pltpu.VMEM((span, 2 * kv_width + 128), bf16),
            pltpu.VMEM((tokens, width), bf16),
            pltpu.VMEM((tokens, width), bf16),
            pltpu.VMEM((tokens, 128), f32),
            dma((4,)),
            dma((2,)),
            dma((4,)),
            dma((4,)),
        ],
        compiler_params=pltpu.CompilerParams(
            collective_id=9, has_side_effects=True, vmem_limit_bytes=67043328
        ),
    )(*arrays, *operands)


def norm_forward(values, gain_row):
    inverse = lax.rsqrt(jnp.mean(values * values, axis=-1, keepdims=True) + eps_norm)
    normed = values * inverse
    return (normed * gain_row, normed, inverse)


def rms_norm_gradient(grad_scaled, normed, inverse, gain_row):
    grad_normed = grad_scaled * gain_row
    inner_mean = jnp.mean(grad_normed * normed, axis=-1, keepdims=True)
    return inverse * (grad_normed - normed * inner_mean)


def rope_tables(positions):
    half_dim = HEAD_SIZE // 2
    frequencies = rope_base ** (-(jnp.arange(half_dim, dtype=jnp.float32) * 2.0) / HEAD_SIZE)
    angles = positions.astype(jnp.float32)[:, None] * frequencies[None, :]
    return (jnp.cos(angles)[:, None, :], jnp.sin(angles)[:, None, :])


def rotate(values, cosine_table, sine_values):
    half_dim = values.shape[-1] // 2
    first_half = values[..., :half_dim]
    second_half = values[..., half_dim:]
    return jnp.concatenate(
        [
            first_half * cosine_table - second_half * sine_values,
            second_half * cosine_table + first_half * sine_values,
        ],
        axis=-1,
    )


def inverse_rotation(grad_in_rot, cosine_table, sine_values):
    half_dim = grad_in_rot.shape[-1] // 2
    first_half = grad_in_rot[..., :half_dim]
    second_half = grad_in_rot[..., half_dim:]
    return jnp.concatenate(
        [
            first_half * cosine_table + second_half * sine_values,
            second_half * cosine_table - first_half * sine_values,
        ],
        axis=-1,
    )


def masked_scores(query_rotated, key_rotated, allowed):
    scores = jnp.einsum(
        "qkgd,skd->kgqs", query_rotated, key_rotated, preferred_element_type=jnp.float32
    ) * HEAD_SIZE ** (-0.5)
    return jnp.where(allowed[None, None], scores, -jnp.inf)


def swap(value, axis_name):
    return lax.ppermute(value, axis_name, [(0, 1), (1, 0)])


def sum_over_tp(value):
    mine = value.astype(jnp.bfloat16)
    return mine.astype(jnp.float32) + swap(mine, "tp").astype(jnp.float32)


def block_sum(partial, nf):
    return lax.psum_scatter(partial, ("fsdp", "ctx"), scatter_dimension=0, tiled=True)


def by_shard(rows, nf):
    count, width = rows.shape
    return rows.reshape(count, nf, width // nf).transpose(1, 0, 2).reshape(nf * count, width // nf)


def on_device(
    hidden_in,
    segment_ids,
    routes,
    attn_gain,
    qk_gains,
    w_query,
    key_projection,
    value_projection,
    w_out,
    ffn_gain,
    w_router,
    w_gate,
    w_up,
    w_down,
    grad_out,
):
    tokens_dev, width_dim = hidden_in.shape
    nf = lax.axis_size("fsdp")
    devices = nf * lax.axis_size("ctx")
    local_experts = w_gate.shape[0]
    experts = local_experts * devices
    capacity = max(2, 2 * tokens_dev * TOPK // experts)
    query_group_width = QUERY_HEADS // KEY_VALUE_HEADS
    shard_width = attn_gain.shape[0]
    f_index, c_index = lax.axis_index("fsdp"), lax.axis_index("ctx")
    bf16 = jnp.bfloat16
    f32 = jnp.float32

    if nf == 8:
        halves = shard_width // 128
        turned = w_router.T.reshape(experts, halves, 128).transpose(1, 0, 2).reshape(-1, 128)
        qk_row = lax.dynamic_update_slice(
            jnp.zeros((256,), bf16), qk_gains, (f_index * qk_gains.shape[0],)
        )
        small = jnp.concatenate(
            [
                turned,
                attn_gain.reshape(-1, 128),
                ffn_gain.reshape(-1, 128),
                qk_row.reshape(-1, 128),
            ]
        )
        small = jnp.pad(small, ((0, -small.shape[0] % 16), (0, 0)))
        own_positions = c_index * tokens_dev + jnp.arange(tokens_dev, dtype=jnp.int32)
        cosine_table, sine_values = rope_tables(own_positions)
        cosine_row, sine_row = cosine_table[:, 0], sine_values[:, 0]
        trig = jnp.stack(
            [
                jnp.concatenate([cosine_row, cosine_row], axis=1),
                jnp.concatenate([sine_row, -sine_row], axis=1),
            ]
        )
        segment_wide = jnp.broadcast_to(segment_ids.astype(bf16)[:, None], (tokens_dev, 128))
        expert_ids = jnp.arange(experts, dtype=jnp.int32)
        hits = routes[:, :, None] == expert_ids[None, None, :]
        routed = jnp.any(hits, axis=1).astype(f32)
        heads_width, kv_width = w_query.shape[1], key_projection.shape[1]
        shapes = (tokens_dev, width_dim, heads_width, kv_width, experts)
        (
            _,
            query_weight,
            key_weight,
            value_weight,
            out_weight,
            grad_all,
            hidden_two,
            hidden_slices,
            marks,
            probs,
            resid_mid,
            attended,
            query_raw,
            key_projected,
            query_rotated,
            key_all,
            value_all,
            bias,
            log_total,
            gains,
            router_rows,
        ) = forward_pass(
            nf,
            (small, w_query, key_projection, value_projection, w_out, grad_out),
            (hidden_in, segment_wide, routed, trig),
            shapes,
        )
    else:
        pieces = [w_router.reshape(-1), attn_gain, ffn_gain, qk_gains]
        flat = jnp.concatenate(pieces)
        small_rows = -(-flat.shape[0] // 2048) * 16
        small = jnp.pad(flat, (0, small_rows * 128 - flat.shape[0])).reshape(small_rows, 128)
        out_form = "row" if shard_width % 128 else "col"
        small_all, query_weight, key_weight, value_weight, out_weight, grad_all = plane_gather(
            [
                Gather(small, nf, chunks=1),
                Gather(w_query, nf, half=True, chunks=2),
                Gather(key_projection, nf, half=True, chunks=1),
                Gather(value_projection, nf, half=True, chunks=1),
                Gather(w_out, nf, form=out_form, half=True, chunks=2),
                Gather(grad_out, nf, rep=True, chunks=4),
            ],
            1,
            nf,
        )
        if out_form == "row":
            out_weight = out_weight.reshape(nf, -1, shard_width).transpose(1, 0, 2)
            out_weight = out_weight.reshape(-1, width_dim)
        small_all = small_all.reshape(nf, 2, small_rows * 128)[:, 0]
        ends = [0]
        for piece in pieces:
            ends.append(ends[-1] + piece.shape[0])
        router_weight = small_all[:, ends[0] : ends[1]].reshape(width_dim, experts)
        gain_one = small_all[:, ends[1] : ends[2]].reshape(-1).astype(f32)
        gain_two = small_all[:, ends[2] : ends[3]].reshape(-1).astype(f32)
        gain_qk = small_all[:, ends[3] : ends[4]].reshape(-1).astype(f32)
        gain_query, gain_key = gain_qk[:HEAD_SIZE], gain_qk[HEAD_SIZE:]

        kv_local = key_weight.shape[1] // HEAD_SIZE
        head_local = query_weight.shape[1] // HEAD_SIZE
        resid = hidden_in.astype(f32)
        scaled_one, normed_one, inverse_one = norm_forward(resid, gain_one)
        hidden_first = scaled_one.astype(bf16)
        query_raw = jnp.dot(hidden_first, query_weight, preferred_element_type=f32).reshape(
            tokens_dev, head_local, HEAD_SIZE
        )
        key_projected = jnp.dot(hidden_first, key_weight, preferred_element_type=f32).reshape(
            tokens_dev, kv_local, HEAD_SIZE
        )
        value_rows = jnp.dot(hidden_first, value_weight, preferred_element_type=f32).astype(bf16)
        query_normed, query_hat, query_inverse = norm_forward(query_raw, gain_query)
        key_normed, key_unit_rows, key_inverse_norm = norm_forward(key_projected, gain_key)
        own_positions = c_index * tokens_dev + jnp.arange(tokens_dev, dtype=jnp.int32)
        cosine_table, sine_values = rope_tables(own_positions)
        query_rotated = (
            rotate(query_normed, cosine_table, sine_values)
            .astype(bf16)
            .reshape(tokens_dev, kv_local, query_group_width, HEAD_SIZE)
        )
        key_rotated = rotate(key_normed, cosine_table, sine_values).astype(bf16)
        own_segments = segment_ids.astype(bf16)
        packed_kv = jnp.concatenate(
            [
                key_rotated.reshape(tokens_dev, -1),
                value_rows,
                jnp.broadcast_to(own_segments[:, None], (tokens_dev, 128)),
            ],
            axis=1,
        )
        kv_all = lax.all_gather(packed_kv, "ctx", axis=0, tiled=True)
        kv_width = kv_local * HEAD_SIZE
        key_all = kv_all[:, :kv_width].reshape(-1, kv_local, HEAD_SIZE)
        value_all = kv_all[:, kv_width : 2 * kv_width].reshape(-1, kv_local, HEAD_SIZE)
        segment_all = kv_all[:, 2 * kv_width]
        key_positions = jnp.arange(key_all.shape[0], dtype=jnp.int32)
        allowed = (key_positions[None, :] <= own_positions[:, None]) & (
            segment_all[None, :] == own_segments[:, None]
        )
        scores = masked_scores(query_rotated, key_all, allowed)
        top_score = jnp.max(scores, axis=-1, keepdims=True)
        log_total = top_score + jnp.log(jnp.sum(jnp.exp(scores - top_score), axis=-1, keepdims=True))
        weights_att = jnp.exp(scores - log_total).astype(bf16)
        attended = jnp.einsum("kgqs,skd->qkgd", weights_att, value_all, preferred_element_type=f32)
        attended = attended.astype(bf16).reshape(tokens_dev, head_local * HEAD_SIZE)
        out_partial = jnp.dot(attended, out_weight, preferred_element_type=f32)
        resid_mid = resid + sum_over_tp(out_partial)
        scaled_two, normed_two, inverse_two = norm_forward(resid_mid, gain_two)
        hidden_two = scaled_two.astype(bf16)
        logits = jnp.dot(hidden_two, router_weight, preferred_element_type=f32)
        expert_ids = jnp.arange(experts, dtype=jnp.int32)
        hits = routes[:, :, None] == expert_ids[None, None, :]
        routed = jnp.any(hits, axis=1)
        masked_logits = jnp.where(routed, logits, -jnp.inf)
        raised = jnp.where(
            routed, jnp.exp(masked_logits - jnp.max(masked_logits, axis=1, keepdims=True)), 0.0
        )
        probs = raised / jnp.sum(raised, axis=1, keepdims=True)
        marks = jnp.where(routed, probs, -1.0).T
    if nf == 8:
        (
            hidden_all,
            hidden_first_slice,
            moe_partial,
            rows_in,
            grad_prod,
            activated,
            grad_gate_pre,
            grad_up_pre,
            grad_hidden_moe,
            grad_prob,
        ) = expert_pass(
            hidden_two,
            marks,
            hidden_slices,
            grad_all,
            w_gate,
            w_up,
            w_down,
            capacity,
            nf,
        )
        grad_prob = grad_prob.reshape(devices, 8, tokens_dev)[:, :local_experts]
        grad_prob = grad_prob.reshape(experts, tokens_dev).T
    else:
        hidden_all, marks_all, hidden_first_slice = plane_gather(
            [
                Gather(hidden_two, nf, rep=True, chunks=4),
                Gather(marks, nf, chunks=1),
                Gather(by_shard(hidden_first, nf), nf, form="a2a", chunks=1),
            ],
            2,
            nf,
        )
        first_expert = (f_index * 2 + c_index) * local_experts
        marks_here = lax.dynamic_slice_in_dim(
            marks_all.reshape(devices, experts, tokens_dev), first_expert, local_experts, axis=1
        )
        taken = marks_here >= 0.0
        ranks = jnp.cumsum(taken.astype(jnp.int32), axis=2) - 1
        slots = jnp.arange(capacity, dtype=jnp.int32)
        chosen = taken[:, :, None, :] & (ranks[:, :, None, :] == slots[None, None, :, None])
        pick = chosen.astype(bf16)
        weight_slot = jnp.sum(jnp.where(chosen, marks_here[:, :, None, :], 0.0), axis=3)
        weight_slot = weight_slot.transpose(1, 0, 2).reshape(local_experts, devices * capacity)

        def select(rows):
            blocks = rows.reshape(devices, tokens_dev, width_dim)
            out = jnp.einsum("bjst,btd->jbsd", pick, blocks, preferred_element_type=f32)
            return out.astype(bf16).reshape(local_experts, devices * capacity, width_dim)

        def spread(rows):
            blocks = rows.reshape(local_experts, devices, capacity, width_dim)
            out = jnp.einsum("bjst,jbsd->btd", pick, blocks, preferred_element_type=f32)
            return out.astype(bf16).reshape(devices * tokens_dev, width_dim)

        rows_in = select(hidden_all)
        grad_rows_in = select(grad_all)
        gate_pre = jnp.einsum("jrd,jdf->jrf", rows_in, w_gate, preferred_element_type=f32)
        up_pre = jnp.einsum("jrd,jdf->jrf", rows_in, w_up, preferred_element_type=f32)
        sigmoid_gate = jax.nn.sigmoid(gate_pre)
        silu_gate = gate_pre * sigmoid_gate
        activated = (silu_gate * up_pre).astype(bf16)
        produced = jnp.einsum("jrf,jfd->jrd", activated, w_down, preferred_element_type=f32).astype(
            bf16
        )
        wide = produced.astype(f32)
        grad_prob_slot = jnp.sum(wide * grad_rows_in.astype(f32), axis=2)
        grad_prob_part = jnp.sum(
            jnp.where(
                chosen,
                grad_prob_slot.reshape(local_experts, devices, capacity).transpose(1, 0, 2)[..., None],
                0.0,
            ),
            axis=2,
        )
        moe_partial = spread((weight_slot[:, :, None] * wide).astype(bf16))
        grad_prod = (weight_slot[:, :, None] * grad_rows_in.astype(f32)).astype(bf16)
        grad_act = jnp.einsum("jrd,jfd->jrf", grad_prod, w_down, preferred_element_type=f32)
        grad_gate_pre = (
            grad_act * up_pre * (sigmoid_gate * (1.0 + gate_pre * (1.0 - sigmoid_gate)))
        ).astype(bf16)
        grad_up_pre = (grad_act * silu_gate).astype(bf16)
        grad_slots = jnp.einsum("jrf,jdf->jrd", grad_gate_pre, w_gate, preferred_element_type=f32)
        grad_slots = (
            grad_slots + jnp.einsum("jrf,jdf->jrd", grad_up_pre, w_up, preferred_element_type=f32)
        ).astype(bf16)
        hidden_grad_partial = spread(grad_slots)

        grad_hidden_moe = sum_over_tp(block_sum(hidden_grad_partial, nf))
        grad_prob = lax.all_to_all(
            grad_prob_part, ("fsdp", "ctx"), split_axis=0, concat_axis=0, tiled=True
        ).reshape(experts, tokens_dev)
        grad_prob = grad_prob + swap(grad_prob, "tp")
        grad_prob = grad_prob.T
    grad_down = jnp.einsum("jrf,jrd->jfd", activated, grad_prod, preferred_element_type=f32)
    grad_gate = jnp.einsum("jrd,jrf->jdf", rows_in, grad_gate_pre, preferred_element_type=f32)
    grad_up = jnp.einsum("jrd,jrf->jdf", rows_in, grad_up_pre, preferred_element_type=f32)

    if nf == 8:
        operands = (
            grad_hidden_moe,
            grad_prob,
            probs,
            router_rows,
            hidden_in,
            resid_mid,
            gains,
            grad_out,
            out_weight,
            query_weight,
            key_weight,
            value_weight,
            query_raw,
            key_projected,
            query_rotated,
            key_all,
            value_all,
            bias,
            log_total,
            trig,
            moe_partial,
        )
        shapes = (tokens_dev, width_dim, heads_width, kv_width, key_all.shape[0])
        (
            attended_all,
            dq_all,
            dk_all,
            dv_all,
            logits_all,
            tail_all,
            proj_slice,
            grad_in,
            block_out,
        ) = backward_pass(nf, operands, attended, shapes)
        tail_rows = tail_all.shape[0] // devices
    else:
        block_out = (resid_mid + sum_over_tp(block_sum(moe_partial, nf))).astype(bf16)

        grad_rows = grad_out.astype(f32)
        grad_logits = (
            probs * (grad_prob - jnp.sum(probs * grad_prob, axis=1, keepdims=True))
        ).astype(bf16)
        grad_hidden_two = grad_hidden_moe + jnp.einsum(
            "te,de->td", grad_logits, router_weight, preferred_element_type=f32
        )
        grad_ffn_local = jnp.sum(grad_hidden_two * normed_two, axis=0)
        grad_mid = grad_rows + rms_norm_gradient(grad_hidden_two, normed_two, inverse_two, gain_two)
        grad_proj = grad_mid.astype(bf16)
        attended_gradient = jnp.einsum(
            "td,qd->tq", grad_proj, out_weight, preferred_element_type=f32
        ).astype(bf16)
        attended_gradient = attended_gradient.reshape(
            tokens_dev, kv_local, query_group_width, HEAD_SIZE
        )
        probs_att = jnp.exp(scores - log_total)
        grad_value_all = jnp.einsum(
            "kgqs,qkgd->skd", weights_att, attended_gradient, preferred_element_type=f32
        )
        grad_probs = jnp.einsum(
            "qkgd,skd->kgqs", attended_gradient, value_all, preferred_element_type=f32
        )
        delta_row = jnp.sum(probs_att * grad_probs, axis=-1, keepdims=True)
        grad_scores = (probs_att * (grad_probs - delta_row) * HEAD_SIZE ** (-0.5)).astype(bf16)
        grad_query_rot = jnp.einsum(
            "kgqs,skd->qkgd", grad_scores, key_all, preferred_element_type=f32
        ).reshape(tokens_dev, head_local, HEAD_SIZE)
        grad_key_all = jnp.einsum(
            "kgqs,qkgd->skd", grad_scores, query_rotated, preferred_element_type=f32
        )
        grad_kv_all = jnp.concatenate(
            [grad_key_all.reshape(-1, kv_width), grad_value_all.reshape(-1, kv_width)], axis=1
        )
        theirs = lax.dynamic_slice_in_dim(grad_kv_all, (1 - c_index) * tokens_dev, tokens_dev, axis=0)
        mine = lax.dynamic_slice_in_dim(grad_kv_all, c_index * tokens_dev, tokens_dev, axis=0)
        grad_kv = mine + swap(theirs.astype(bf16), "ctx").astype(f32)
        key_rotated_gradient = grad_kv[:, :kv_width].reshape(tokens_dev, kv_local, HEAD_SIZE)
        grad_query_norm = inverse_rotation(grad_query_rot, cosine_table, sine_values)
        key_normed_gradient = inverse_rotation(key_rotated_gradient, cosine_table, sine_values)
        grad_qk_local = jnp.concatenate(
            [
                jnp.sum(grad_query_norm * query_hat, axis=(0, 1)),
                jnp.sum(key_normed_gradient * key_unit_rows, axis=(0, 1)),
            ]
        )
        grad_query_raw = (
            rms_norm_gradient(grad_query_norm, query_hat, query_inverse, gain_query)
            .astype(bf16)
            .reshape(tokens_dev, head_local * HEAD_SIZE)
        )
        key_projected_gradient = (
            rms_norm_gradient(key_normed_gradient, key_unit_rows, key_inverse_norm, gain_key)
            .astype(bf16)
            .reshape(tokens_dev, kv_width)
        )
        value_projected_gradient = grad_kv[:, kv_width:].astype(bf16)
        grad_hidden_part = jnp.einsum(
            "tq,dq->td", grad_query_raw, query_weight, preferred_element_type=f32
        )
        grad_hidden_part = grad_hidden_part + jnp.einsum(
            "tq,dq->td", key_projected_gradient, key_weight, preferred_element_type=f32
        )
        grad_hidden_part = grad_hidden_part + jnp.einsum(
            "tq,dq->td", value_projected_gradient, value_weight, preferred_element_type=f32
        )
        grad_hidden_one = sum_over_tp(grad_hidden_part)
        grad_in = grad_mid + rms_norm_gradient(grad_hidden_one, normed_one, inverse_one, gain_one)
        grad_attn_local = jnp.sum(grad_hidden_one * normed_one, axis=0)
        grad_qk_local = grad_qk_local + swap(grad_qk_local, "tp")
        tail = jnp.concatenate([grad_attn_local, grad_ffn_local, grad_qk_local])
        tail = jnp.pad(tail, (0, -tail.shape[0] % 1024)).reshape(-1, 128)
        tail_rows = tail.shape[0]
        logit_pad = jnp.pad(grad_logits, ((0, 0), (0, -experts % 128)))

        dq_all, dk_all, dv_all, attended_all, proj_slice, logits_all, tail_all = plane_gather(
            [
                Gather(grad_query_raw, nf, chunks=2),
                Gather(key_projected_gradient, nf, chunks=1),
                Gather(value_projected_gradient, nf, chunks=1),
                Gather(attended, nf, chunks=2),
                Gather(by_shard(grad_proj, nf), nf, form="a2a", chunks=1),
                Gather(logit_pad, nf, chunks=1),
                Gather(tail, nf, chunks=1),
            ],
            3,
            nf,
        )
    over_tokens = functools.partial(
        jnp.einsum, "td,tq->dq", preferred_element_type=f32
    )
    grad_query = over_tokens(hidden_first_slice, dq_all)
    grad_key = over_tokens(hidden_first_slice, dk_all)
    grad_value = over_tokens(hidden_first_slice, dv_all)
    grad_out_proj = over_tokens(attended_all, proj_slice)
    hidden_slice = lax.dynamic_slice_in_dim(hidden_all, f_index * shard_width, shard_width, axis=1)
    grad_router = over_tokens(hidden_slice, logits_all)[:, :experts]
    tail_sum = jnp.sum(tail_all.reshape(devices, tail_rows * 128), axis=0)
    grad_attn = lax.dynamic_slice_in_dim(tail_sum, f_index * shard_width, shard_width)
    grad_ffn = lax.dynamic_slice_in_dim(tail_sum, width_dim + f_index * shard_width, shard_width)
    qk_width = qk_gains.shape[0]
    grad_qk = lax.dynamic_slice_in_dim(tail_sum, 2 * width_dim + f_index * qk_width, qk_width)
    return (
        block_out,
        grad_in,
        grad_attn,
        grad_qk,
        grad_query,
        grad_key,
        grad_value,
        grad_out_proj,
        grad_ffn,
        grad_router,
        grad_gate,
        grad_up,
        grad_down,
    )


def solution(mesh):
    return jax.shard_map(
        on_device,
        mesh=mesh,
        in_specs=(
            P(("fsdp", "ctx"), None),
            P(("fsdp", "ctx")),
            P(("fsdp", "ctx"), None),
            P("fsdp"),
            P("fsdp"),
            P("fsdp", "tp"),
            P("fsdp", "tp"),
            P("fsdp", "tp"),
            P("tp", "fsdp"),
            P("fsdp"),
            P("fsdp", None),
            P(("fsdp", "ctx"), None, "tp"),
            P(("fsdp", "ctx"), None, "tp"),
            P(("fsdp", "ctx"), "tp", None),
            P(("fsdp", "ctx"), None),
        ),
        out_specs=(
            P(("fsdp", "ctx"), None),
            P(("fsdp", "ctx"), None),
            P("fsdp"),
            P("fsdp"),
            P("fsdp", "tp"),
            P("fsdp", "tp"),
            P("fsdp", "tp"),
            P("tp", "fsdp"),
            P("fsdp"),
            P("fsdp", None),
            P(("fsdp", "ctx"), None, "tp"),
            P(("fsdp", "ctx"), None, "tp"),
            P(("fsdp", "ctx"), "tp", None),
        ),
        check_vma=False,
    )
```

```python
import functools

import jax
import jax.numpy as jnp
from jax import lax
from jax.experimental import pallas as pl
from jax.experimental.pallas import tpu as pltpu
from jax.sharding import PartitionSpec as P

QUERY_HEADS = 32
KEY_VALUE_HEADS = 4
HEAD_SIZE = 128
TOPK = 8
MESH = pl.DeviceIdType.MESH

eps_norm = 1e-06
rope_base = 1000000.0

UP, DOWN, ACROSS, PARTNER, SIDE = range(5)


class Gather:
    def __init__(self, array, nf, form="row", half=False, rep=False, chunks=2):
        if nf > 8:
            chunks = 2 if rep else 1
        self.array, self.form, self.half, self.rep, self.chunks = array, form, half, rep, chunks
        self.shape = array.shape
        self.rows = array.shape[0] // 2 if half else array.shape[0]
        self.step = (self.rows // nf if form == "a2a" else self.rows) // chunks

    def out_shape(self, nf):
        rows, cols = self.rows, self.shape[1]
        if self.form == "col":
            return (2 * rows, nf * cols)
        if self.form == "a2a":
            return (2 * rows, cols)
        return (2 * nf * rows, cols)


def gather_engine(nf, specs, ins, outs, stage, recv, send, local):
    n = len(specs)
    nz = nf // 2
    f, c, t = lax.axis_index("fsdp"), lax.axis_index("ctx"), lax.axis_index("tp")
    z, x = f // 2, lax.rem(f, 2)
    has_up, has_down = z + 1 < nz, z > 0
    device = {
        UP: (f + 2, c, t),
        DOWN: (f - 2, c, t),
        ACROSS: (z * 2 + 1 - x, c, t),
        PARTNER: (f, 1 - c, t),
        SIDE: (f, c, 1 - t),
    }
    first = [sum(s.chunks for s in specs[:a]) for a in range(n)]

    def src(a, q, dest_f=None):
        s = specs[a]
        lo = row_chunk(a, q) * s.step
        if s.half:
            lo = c * s.rows + lo
        if s.form == "a2a":
            lo = dest_f * (s.rows // nf) + lo
        return ins[a].at[pl.ds(lo, s.step)]

    def dst(a, q, bf, bc):
        s = specs[a]
        if s.form == "col":
            width = s.shape[1]
            return outs[a].at[
                pl.ds(bc * s.rows + row_chunk(a, q) * s.step, s.step),
                pl.ds(pl.multiple_of(bf * width, width), width),
            ]
        rows = s.rows // nf if s.form == "a2a" else s.rows
        return outs[a].at[pl.ds((bf * 2 + bc) * rows + row_chunk(a, q) * s.step, s.step)]

    def copy(a, q, bf, bc, source, kind, dev=None, slot=None):
        block = bf * 2 + bc if slot is None else slot
        return pltpu.make_async_remote_copy(
            src_ref=source,
            dst_ref=dst(a, q, bf, bc),
            send_sem=send.at[kind, block, first[a] + row_chunk(a, q)],
            recv_sem=recv.at[bf * 2 + bc, first[a] + row_chunk(a, q)],
            device_id=device[kind] if dev is None else dev,
            device_id_type=MESH,
        )

    def row_chunk(a, q):
        n_chunks = specs[a].chunks
        if not specs[a].rep:
            return q
        return lax.rem(q + t * (n_chunks // 2), n_chunks)

    def in_half(a, q):
        return 2 * q < specs[a].chunks

    def both(*conds):
        if any(k is False for k in conds):
            return False
        conds = [k for k in conds if k is not None and k is not True]
        if not conds:
            return None
        return functools.reduce(lambda u, v: u & v, conds)

    def when(cond, fn):
        if cond is None or cond is True:
            fn()
        elif cond is not False:
            pl.when(cond)(fn)

    def go_up(a, q, dist):
        far = dist + 1 < nz - 1 if specs[a].rep and not in_half(a, q) else None
        return both(has_up, far)

    def go_down(a, q, dist):
        far = dist + 1 < nz - 1 if specs[a].rep and not in_half(a, q) else None
        return both(has_down, far)

    def go_across(a, q):
        return in_half(a, q) if specs[a].rep else None

    relays = [(a, q) for a in range(n) if specs[a].form != "a2a" for q in range(specs[a].chunks)]
    direct = [(a, q) for a in range(n) if specs[a].form == "a2a" for q in range(specs[a].chunks)]

    def start(only=None):
        only = range(n) if only is None else only
        for a, q in relays:
            if a not in only:
                continue
            source = src(a, q)
            when(go_up(a, q, 0), lambda: copy(a, q, f, c, source, UP).start())
            when(go_down(a, q, 0), lambda: copy(a, q, f, c, source, DOWN).start())
            when(go_across(a, q), lambda: copy(a, q, f, c, source, ACROSS).start())
            copy(a, q, f, c, source, PARTNER).start()
        own_start([a for a in only if specs[a].form != "a2a"])

    def own_start(only):
        for a in only:
            own_in(a).start()
        for a in only:
            own_in(a).wait()
            own_out(a).start()

    def start_direct():
        own_start(sorted({a for a, _ in direct}))
        for a, q in direct:
            copy(a, q, f, c, src(a, q, f), PARTNER).start()

            def far_send(d, carry):
                there = lax.rem(f + d, nf)
                copy(a, q, f, c, src(a, q, there), UP, dev=(there, c, t), slot=there).start()
                return carry

            lax.fori_loop(1, nf, far_send, 0)

    def own_in(a):
        s = specs[a]
        if s.form == "a2a":
            view = ins[a].at[pl.ds(f * s.step, s.step)]
        elif s.half:
            view = ins[a].at[pl.ds(c * s.rows, s.rows)]
        else:
            view = ins[a]
        return pltpu.make_async_copy(view, stage[a], local.at[0, a])

    def own_out(a):
        s = specs[a]
        if s.form == "col":
            width = s.shape[1]
            view = outs[a].at[
                pl.ds(c * s.rows, s.rows), pl.ds(pl.multiple_of(f * width, width), width)
            ]
        else:
            rows = s.rows // nf if s.form == "a2a" else s.rows
            view = outs[a].at[pl.ds((f * 2 + c) * rows, rows)]
        return pltpu.make_async_copy(stage[a], view, local.at[1, a])

    def arrived(a, q, bf, bc):
        copy(a, q, bf, bc, dst(a, q, bf, bc), PARTNER).wait_recv()

    def pass_on(a, q, bf, kind, cond=None):
        when(cond, lambda: copy(a, q, bf, c, dst(a, q, bf, c), kind).start())

    pair = z + 1 - 2 * lax.rem(z, 2)
    even = lax.rem(z, 2) == 0

    def shared(a, q):
        return not specs[a].rep and specs[a].chunks > 1 and 2 * q >= specs[a].chunks

    def column(k, a, q):
        rep = specs[a].rep
        came = k < nz - 1 if rep and not in_half(a, q) else None
        far = (k == nz - 1) if rep and in_half(a, q) else False

        def take(zz, kind, onward):
            bf = zz * 2 + x
            arrived(a, q, bf, c)
            pass_on(a, q, bf, kind, onward)
            cross = (zz != pair) if shared(a, q) else go_across(a, q)
            pass_on(a, q, bf, ACROSS, cross)
            pass_on(a, q, bf, PARTNER)
            if rep:
                pass_on(a, q, bf, SIDE, far)

        when(both(z - k >= 0, came), lambda: take(z - k, UP, go_up(a, q, k)))
        when(both(z + k < nz, came), lambda: take(z + k, DOWN, go_down(a, q, k)))

    def across(k, a, q):
        rep = specs[a].rep
        mine = in_half(a, q) if rep else None

        def take(zz):
            bf = zz * 2 + 1 - x
            arrived(a, q, bf, c)
            pass_on(a, q, bf, PARTNER)
            if rep:
                pass_on(a, q, bf, SIDE)
            if shared(a, q):
                pass_on(a, q, bf, UP, (zz == z) & even)
                pass_on(a, q, bf, DOWN, (zz == z) & jnp.logical_not(even))

        when(both(z - k >= 0, mine), lambda: take(z - k))
        when(both(z + k < nz, k > 0, mine), lambda: take(z + k))

    def aside(k, a, q):
        if not specs[a].rep:
            return
        if in_half(a, q):
            return

        def take(bf):
            arrived(a, q, bf, c)
            pass_on(a, q, bf, PARTNER)

        when((z - k >= 0), lambda: take((z - k) * 2 + 1 - x))
        when((z + k < nz) & (k > 0), lambda: take((z + k) * 2 + 1 - x))
        when((z - k >= 0) & (k == nz - 1), lambda: take((z - k) * 2 + x))
        when((z + k < nz) & (k == nz - 1), lambda: take((z + k) * 2 + x))

    count = len(relays)
    lag = 2

    def late(fn, k, i):
        if i >= 0:
            fn(k, *relays[i])
        else:
            pl.when(k > 1)(lambda: fn(k - 1, *relays[count + i]))

    by_chunk = all(specs[a].rep for a, _ in relays)

    def step(k, carry):
        if not by_chunk:
            for a, q in relays:
                column(k, a, q)
            for a, q in relays:
                across(k - 1, a, q)

            @pl.when(k > 1)
            def _():
                for a, q in relays:
                    aside(k - 2, a, q)

            return carry
        for i, (a, q) in enumerate(relays):
            column(k, a, q)
            pl.when(k == 1)(lambda: across(0, a, q))
            late(across, k, i - lag)
            if i >= lag:
                pl.when(k == 1)(lambda: aside(0, *relays[i - lag]))
            late(aside, k, i - 2 * lag)

        @pl.when(k == 1)
        def _():
            for a, q in relays[count - lag :]:
                aside(0, a, q)

        return carry

    def run(hook=None):
        def body(k, carry):
            step(k, carry)
            if hook is not None:
                hook(k)
            return carry

        lax.fori_loop(1, nz, body, 0)
        for a, q in relays[count - lag if by_chunk else 0 :]:
            across(nz - 1, a, q)
        if not by_chunk:
            for a, q in relays:
                aside(nz - 2, a, q)
        for a, q in relays[count - 2 * lag if by_chunk else 0 :]:
            aside(nz - 1, a, q)

    def step_of(k, only):
        some = [(a, q) for a, q in relays if a in only]
        for a, q in some:
            column(k, a, q)
        for a, q in some:
            across(k - 1, a, q)

        if k > 1:
            for a, q in some:
                aside(k - 2, a, q)

    def edge_of(only):
        some = [(a, q) for a, q in relays if a in only]
        for a, q in some:
            across(nz - 1, a, q)
        for a, q in some:
            aside(nz - 2, a, q)
        for a, q in some:
            aside(nz - 1, a, q)

    def land_of(only):
        def take(bf, carry):
            for a, q in relays:
                if a in only:
                    arrived(a, q, bf, 1 - c)
            return carry

        lax.fori_loop(0, nf, take, 0)
        for a in only:
            own_out(a).wait()

    def run_direct():
        for a, q in direct:

            def far_take(d, carry):
                there = lax.rem(f + nf - d, nf)
                arrived(a, q, there, c)
                pass_on(a, q, there, PARTNER)
                return carry

            lax.fori_loop(1, nf, far_take, 0)

    def take_partner(bf, carry):
        for a, q in relays:
            arrived(a, q, bf, 1 - c)
        return carry

    def land():
        lax.fori_loop(0, nf, take_partner, 0)
        for a in range(n):
            if specs[a].form != "a2a":
                own_out(a).wait()

    def finish(bf, carry):
        zz, xx = bf // 2, lax.rem(bf, 2)
        dist = jnp.abs(zz - z)
        here = xx == x
        for a, q in relays:
            rep = specs[a].rep
            view = dst(a, q, bf, c)

            def sent(kind, cond):
                when(cond, lambda: copy(a, q, bf, c, view, kind).wait_send())

            half = in_half(a, q) if rep else None
            by_z = dist < nz - 1 if rep and not half else None
            sent(PARTNER, None)
            sent(UP, both(here, zz <= z, by_z, go_up(a, q, dist)))
            sent(DOWN, both(here, zz >= z, by_z, go_down(a, q, dist)))
            cross = (zz != pair) if shared(a, q) else go_across(a, q)
            sent(ACROSS, both(here, by_z, cross))
            if shared(a, q):
                there = jnp.logical_not(here) & (zz == z)
                sent(UP, there & even)
                sent(DOWN, there & jnp.logical_not(even))
            if rep and half:
                sent(SIDE, jnp.logical_not(here) | (dist == nz - 1))
        for a, q in direct:
            arrived(a, q, bf, 1 - c)
            view = dst(a, q, bf, c)
            copy(a, q, bf, c, view, PARTNER).wait_send()

            @pl.when(bf != f)
            def _():
                copy(a, q, bf, c, view, UP, slot=bf).wait_send()

        return carry

    def drain():
        lax.fori_loop(0, nf, finish, 0)
        for a in range(n):
            if specs[a].form == "a2a":
                own_out(a).wait()

    return start, run, land, start_direct, run_direct, drain, step_of, edge_of, land_of


def gather_kernel(nf, specs, *refs):
    n = len(specs)
    ins, outs, scratch = refs[:n], refs[n : 2 * n], refs[2 * n :]
    nz = nf // 2
    f, c, t = lax.axis_index("fsdp"), lax.axis_index("ctx"), lax.axis_index("tp")
    z, x = f // 2, lax.rem(f, 2)
    has_up, has_down = z + 1 < nz, z > 0
    device = {
        UP: (f + 2, c, t),
        DOWN: (f - 2, c, t),
        ACROSS: (z * 2 + 1 - x, c, t),
        PARTNER: (f, 1 - c, t),
        SIDE: (f, c, 1 - t),
    }
    any_a2a = any(s.form == "a2a" for s in specs)
    any_rep = any(s.rep for s in specs)
    barrier = pltpu.get_barrier_semaphore()

    def greet(dev):
        pl.semaphore_signal(barrier, 1, device_id=dev, device_id_type=MESH)

    greeted = 1
    greet(device[PARTNER])
    if any_rep:
        greet(device[SIDE])
        greeted += 1
    if any_a2a:

        def greet_far(d, carry):
            greet((lax.rem(f + d, nf), c, t))
            return carry

        lax.fori_loop(1, nf, greet_far, 0)
        pl.semaphore_wait(barrier, greeted + nf - 1)
    else:
        greet(device[ACROSS])

        @pl.when(has_up)
        def _():
            greet(device[UP])

        @pl.when(has_down)
        def _():
            greet(device[DOWN])

        pl.semaphore_wait(
            barrier, greeted + 1 + has_up.astype(jnp.int32) + has_down.astype(jnp.int32)
        )

    start, run, land, start_direct, run_direct, drain, *_ = gather_engine(
        nf, specs, ins, outs, scratch[:n], *scratch[n:]
    )
    start()
    start_direct()
    run()
    run_direct()
    land()
    drain()


def stage_of(s, nf):
    rows = s.rows // nf if s.form == "a2a" else s.rows
    return pltpu.VMEM((rows, s.shape[1]), s.array.dtype)


def plane_gather(specs, collective_id, nf):
    n = len(specs)
    total = sum(s.chunks for s in specs)

    return pl.pallas_call(
        functools.partial(gather_kernel, nf, tuple(specs)),
        out_shape=tuple(jax.ShapeDtypeStruct(s.out_shape(nf), s.array.dtype) for s in specs),
        in_specs=[pl.BlockSpec(memory_space=pl.ANY)] * n,
        out_specs=tuple(pl.BlockSpec(memory_space=pl.ANY) for _ in specs),
        scratch_shapes=[stage_of(s, nf) for s in specs]
        + [
            pltpu.SemaphoreType.DMA((2 * nf, total)),
            pltpu.SemaphoreType.DMA((5, 2 * nf, total)),
            pltpu.SemaphoreType.DMA((2, n)),
        ],
        compiler_params=pltpu.CompilerParams(
            collective_id=collective_id, has_side_effects=True
        ),
    )(*[s.array for s in specs])


CUT = 4


def expert_kernel(nf, capacity, specs, *refs):
    n = len(specs)
    ins, refs = refs[:n], refs[n:]
    (grad_all, wg_hbm, wu_hbm, wd_hbm), refs = refs[:4], refs[4:]
    gathered, refs = refs[:n], refs[n:]
    (out_part, xs_out, de_out, act_out, dg_out, du_out, grad_tok, prob_tok), refs = (
        refs[:8],
        refs[8:],
    )
    stage, refs = refs[:n], refs[n:]
    (recv, send, local), refs = refs[:3], refs[3:]
    (
        wg,
        wu,
        wd,
        x_buf,
        y_buf,
        xs,
        ys,
        de,
        pe,
        bs,
        act,
        dg,
        du,
        w_slot,
        dp_slot,
        pick,
        mk,
        rk,
        y_out,
        part,
        from_partner,
        from_across,
        from_z,
        from_side,
        dp_send,
        dp_recv,
        dp_side,
        marks_v,
        w_sem,
        load_sem,
        store_sem,
        p_send,
        p_recv,
        x_send,
        x_recv,
        z_send,
        z_recv,
        s_send,
        s_recv,
        d_send,
        d_recv,
    ) = refs
    f32, bf16 = jnp.float32, jnp.bfloat16
    nz = nf // 2
    f, c, t = lax.axis_index("fsdp"), lax.axis_index("ctx"), lax.axis_index("tp")
    z, x = f // 2, lax.rem(f, 2)
    me = f * 2 + c
    up, down = (f + 2, c, t), (f - 2, c, t)
    across_dev, partner, side = (z * 2 + 1 - x, c, t), (f, 1 - c, t), (f, c, 1 - t)
    has_up, has_down = z + 1 < nz, z > 0
    tokens = x_buf.shape[0] // 4
    width = x_buf.shape[1]
    slots = 2 * capacity
    rows_unit = 4 * capacity
    hidden = wg.shape[2]
    experts = specs[1].shape[0]
    step_rows = tokens // CUT

    barrier = pltpu.get_barrier_semaphore()

    def greet(d, carry):
        there = lax.rem(me + d, 2 * nf)
        pl.semaphore_signal(
            barrier, 1, device_id=(there // 2, lax.rem(there, 2), t), device_id_type=MESH
        )
        return carry

    lax.fori_loop(1, 2 * nf, greet, 0)
    pl.semaphore_signal(barrier, 1, device_id=side, device_id_type=MESH)
    pl.semaphore_wait(barrier, 2 * nf)

    start, run, land, start_direct, run_direct, drain, *_ = gather_engine(
        nf, specs, ins, gathered, stage, recv, send, local
    )
    start()
    weight_loads = [
        pltpu.make_async_copy(src, dst, w_sem.at[i])
        for i, (src, dst) in enumerate(((wg_hbm, wg), (wu_hbm, wu), (wd_hbm, wd)))
    ]
    for load in weight_loads:
        load.start()

    order = 0
    for at, seq in enumerate(visiting_order(nz)):
        code = sum(u * nz**i for i, u in enumerate(seq))
        order = order + code * (z == at).astype(jnp.int32)

    def unit_at(i):
        code = order
        for k in range(nz):
            code = jnp.where(i > k, code // nz, code)
        return lax.rem(code, nz)

    def load_rows(u, which):
        rows = pl.ds(pl.multiple_of(u * 4 * tokens, 4 * tokens), 4 * tokens)
        if which == 0:
            return pltpu.make_async_copy(gathered[0].at[rows], x_buf, load_sem.at[0])
        return pltpu.make_async_copy(grad_all.at[rows], y_buf, load_sem.at[1])

    load_rows(unit_at(0), 1).start()
    run()
    land()
    start_direct()
    load_rows(unit_at(0), 0).start()
    marks_in = pltpu.make_async_copy(gathered[1], marks_v, load_sem.at[2])
    marks_in.start()
    marks_in.wait()
    dp_send[...] = jnp.zeros_like(dp_send)
    first_expert = me * 2
    for b in range(2 * nf):
        for j in range(2):
            mk[2 * b + j : 2 * b + j + 1, :] = marks_v[pl.ds(b * experts + first_expert + j, 1), :]
    taken = jnp.where(mk[...] >= 0.0, 1.0, 0.0).astype(bf16)
    before = lax.broadcasted_iota(jnp.int32, (tokens, tokens), 0)
    after = lax.broadcasted_iota(jnp.int32, (tokens, tokens), 1)
    upper = jnp.where(before <= after, 1.0, 0.0).astype(bf16)
    rk[...] = jnp.dot(taken, upper, preferred_element_type=f32) - 1.0
    for load in weight_loads:
        load.wait()

    def store_unit(u):
        rows = pl.ds(pl.multiple_of(u * rows_unit, rows_unit), rows_unit)
        pairs = [(xs, xs_out), (de, de_out), (act, act_out), (dg, dg_out), (du, du_out)]
        copies = [
            pltpu.make_async_copy(src, dst.at[:, rows], store_sem.at[i])
            for i, (src, dst) in enumerate(pairs)
        ]
        out_rows = pl.ds(pl.multiple_of(u * 4 * tokens, 4 * tokens), 4 * tokens)
        copies.append(pltpu.make_async_copy(y_out, out_part.at[out_rows], store_sem.at[5]))
        return copies

    def chunk(q):
        return pl.ds(q * step_rows, step_rows)

    def p_copy(u, xx, q):
        return pltpu.make_async_remote_copy(
            src_ref=part.at[u * 4 + xx * 2 + 1 - c, chunk(q)],
            dst_ref=from_partner.at[u * 2 + xx, chunk(q)],
            send_sem=p_send.at[u * 2 + xx, q],
            recv_sem=p_recv.at[u * 2 + xx, q],
            device_id=partner,
            device_id_type=MESH,
        )

    def x_copy(u, q):
        return pltpu.make_async_remote_copy(
            src_ref=part.at[u * 4 + (1 - x) * 2 + c, chunk(q)],
            dst_ref=from_across.at[u, chunk(q)],
            send_sem=x_send.at[u, q],
            recv_sem=x_recv.at[u, q],
            device_id=across_dev,
            device_id_type=MESH,
        )

    def z_copy(u, q, way):
        return pltpu.make_async_remote_copy(
            src_ref=part.at[u * 4 + x * 2 + c, chunk(q)],
            dst_ref=from_z.at[way, u, chunk(q)],
            send_sem=z_send.at[u, q],
            recv_sem=z_recv.at[way, u, q],
            device_id=up if way == 0 else down,
            device_id_type=MESH,
        )

    def z_wait(u, q, way):
        pltpu.make_async_remote_copy(
            src_ref=part.at[me, chunk(q)],
            dst_ref=from_z.at[way, u, chunk(q)],
            send_sem=z_send.at[u, q],
            recv_sem=z_recv.at[way, u, q],
            device_id=partner,
            device_id_type=MESH,
        ).wait_recv()

    def s_copy(q):
        return pltpu.make_async_remote_copy(
            src_ref=part.at[me, chunk(q)],
            dst_ref=from_side.at[chunk(q)],
            send_sem=s_send.at[q],
            recv_sem=s_recv.at[q],
            device_id=side,
            device_id_type=MESH,
        )

    def d_copy(b, source=None):
        return pltpu.make_async_remote_copy(
            src_ref=dp_send.at[b],
            dst_ref=dp_recv.at[me if source is None else source],
            send_sem=d_send.at[b],
            recv_sem=d_recv.at[me if source is None else source],
            device_id=(b // 2, lax.rem(b, 2), t),
            device_id_type=MESH,
        )

    def compute(i, u):
        load_rows(u, 0).wait()
        load_rows(u, 1).wait()

        @pl.when(i > 0)
        def _():
            for cp in store_unit(unit_at(i - 1)):
                cp.wait()

        slot_ids = lax.broadcasted_iota(jnp.int32, (capacity, tokens), 0).astype(f32)
        for b in range(4):
            for j in range(2):
                row = pl.ds(2 * (u * 4 + b) + j, 1)
                mark = mk[row, :]
                hit = (rk[row, :] == slot_ids) & (mark >= 0.0)
                pick[b, j * capacity : (j + 1) * capacity, :] = jnp.where(hit, 1.0, 0.0)
                w_slot[j, b * capacity : (b + 1) * capacity, :] = jnp.sum(
                    jnp.where(hit, mark, 0.0), axis=1, keepdims=True
                )
        tile = 512
        for b in range(4):
            chosen = pick[b].astype(bf16)
            for k in range(width // tile):
                cols = slice(k * tile, (k + 1) * tile)
                got = jnp.dot(
                    chosen, x_buf[b * tokens : (b + 1) * tokens, cols], preferred_element_type=f32
                ).astype(bf16)
                gy = jnp.dot(
                    chosen, y_buf[b * tokens : (b + 1) * tokens, cols], preferred_element_type=f32
                )
                for j in range(2):
                    to = slice(b * capacity, (b + 1) * capacity)
                    of = slice(j * capacity, (j + 1) * capacity)
                    xs[j, to, cols] = got[of]
                    ys[j, to, cols] = gy[of].astype(bf16)
                    de[j, to, cols] = (w_slot[j, to, :] * gy[of]).astype(bf16)

        @pl.when(i + 1 < nz)
        def _():
            load_rows(unit_at(i + 1), 0).start()
            load_rows(unit_at(i + 1), 1).start()

        def expert(j, carry):
            gate = jnp.dot(xs[j], wg[j], preferred_element_type=f32)
            upv = jnp.dot(xs[j], wu[j], preferred_element_type=f32)
            sig = 1.0 / (1.0 + jnp.exp(-gate))
            silu = gate * sig
            act[j] = (silu * upv).astype(bf16)
            grad_act = lax.dot_general(
                de[j], wd[j], (((1,), (1,)), ((), ())), preferred_element_type=f32
            )
            dg[j] = (grad_act * upv * (sig * (1.0 + gate * (1.0 - sig)))).astype(bf16)
            du[j] = (grad_act * silu).astype(bf16)
            total = jnp.zeros((rows_unit, 1), f32)
            for k in range(width // tile):
                cols = slice(k * tile, (k + 1) * tile)
                made = jnp.dot(act[j], wd[j, :, cols], preferred_element_type=f32)
                made = made.astype(bf16).astype(f32)
                total = total + jnp.sum(made * ys[j, :, cols].astype(f32), axis=1, keepdims=True)
                weighted = (w_slot[j] * made).astype(bf16)
                back = lax.dot_general(
                    dg[j], wg[j, cols, :], (((1,), (1,)), ((), ())), preferred_element_type=f32
                ) + lax.dot_general(
                    du[j], wu[j, cols, :], (((1,), (1,)), ((), ())), preferred_element_type=f32
                )
                back = back.astype(bf16)
                for b in range(4):
                    of = slice(b * capacity, (b + 1) * capacity)
                    to = pl.ds(pl.multiple_of(j * capacity, capacity), capacity)
                    pe[b, to, cols] = weighted[of]
                    bs[b, to, cols] = back[of]
            for b in range(4):
                to = pl.ds(pl.multiple_of(j * capacity, capacity), capacity)
                dp_slot[b, to, :] = total[b * capacity : (b + 1) * capacity]
            return carry

        lax.fori_loop(0, 2, expert, 0)

        def spread(b):
            chosen = pick[b]
            back = jnp.transpose(chosen).astype(bf16)
            for k in range(width // tile):
                cols = slice(k * tile, (k + 1) * tile)
                part[u * 4 + b, :, cols] = jnp.dot(
                    back, bs[b, :, cols], preferred_element_type=f32
                ).astype(bf16)

        for b in range(4):
            spread(b)
        for xx in range(2):
            for q in range(CUT):
                p_copy(u, xx, q).start()
        for b in range(4):
            back = jnp.transpose(pick[b]).astype(bf16)
            for k in range(width // tile):
                cols = slice(k * tile, (k + 1) * tile)
                y_out[b * tokens : (b + 1) * tokens, cols] = jnp.dot(
                    back, pe[b, :, cols], preferred_element_type=f32
                ).astype(bf16)
            for j in range(2):
                of = slice(j * capacity, (j + 1) * capacity)
                dp_send[u * 4 + b, j : j + 1, :] = jnp.sum(
                    pick[b, of, :] * dp_slot[b, of, :], axis=0, keepdims=True
                )
        for cp in store_unit(u):
            cp.start()
        for b in range(4):
            bb = u * 4 + b

            @pl.when(bb != me)
            def _():
                d_copy(bb).start()

    def wide(ref):
        return ref.astype(f32)

    def to_across(u):
        for q in range(CUT):
            for xx in range(2):
                p_copy(u, xx, q).wait_recv()
            blk = u * 4 + (1 - x) * 2 + c
            part[blk, chunk(q)] = (
                wide(part[blk, chunk(q)]) + wide(from_partner[u * 2 + 1 - x, chunk(q)])
            ).astype(bf16)
            x_copy(u, q).start()

    def along(u):
        blk = u * 4 + x * 2 + c
        for q in range(CUT):
            x_copy(u, q).wait_recv()

            def total():
                return (
                    wide(part[blk, chunk(q)])
                    + wide(from_partner[u * 2 + x, chunk(q)])
                    + wide(from_across[u, chunk(q)])
                )

            def hop(way, has_before):
                @pl.when(has_before)
                def _():
                    z_wait(u, q, way)
                    part[blk, chunk(q)] = (total() + wide(from_z[way, u, chunk(q)])).astype(bf16)

                @pl.when(jnp.logical_not(has_before))
                def _():
                    part[blk, chunk(q)] = total().astype(bf16)

                z_copy(u, q, way).start()

            @pl.when(u > z)
            def _():
                hop(0, has_down)

            @pl.when(u < z)
            def _():
                hop(1, has_up)

            @pl.when(u == z)
            def _():
                grad_tok[chunk(q)] = total()

                @pl.when(has_down)
                def _():
                    z_wait(u, q, 0)
                    grad_tok[chunk(q)] = grad_tok[chunk(q)] + wide(from_z[0, u, chunk(q)])

                @pl.when(has_up)
                def _():
                    z_wait(u, q, 1)
                    grad_tok[chunk(q)] = grad_tok[chunk(q)] + wide(from_z[1, u, chunk(q)])

                part[blk, chunk(q)] = grad_tok[chunk(q)].astype(bf16)
                s_copy(q).start()

    def unit(i, carry):
        u = unit_at(i)
        compute(i, u)

        @pl.when(i > 0)
        def _():
            along(unit_at(i - 1))

        to_across(u)
        return carry

    lax.fori_loop(0, nz, unit, 0)
    along(z)

    dp_recv[me] = dp_send[me]

    def take_prob(d, carry):
        d_copy(me, lax.rem(me + d, 2 * nf)).wait_recv()
        return carry

    lax.fori_loop(1, 2 * nf, take_prob, 0)
    swap_prob = pltpu.make_async_remote_copy(
        src_ref=dp_recv,
        dst_ref=dp_side,
        send_sem=s_send.at[CUT],
        recv_sem=s_recv.at[CUT],
        device_id=side,
        device_id_type=MESH,
    )
    swap_prob.start()
    run_direct()
    for q in range(CUT):
        s_copy(q).wait_recv()
        grad_tok[chunk(q)] = wide(part[me, chunk(q)]) + wide(from_side[chunk(q)])
    swap_prob.wait_recv()
    prob_tok[...] = dp_recv[...] + dp_side[...]

    for cp in store_unit(z):
        cp.wait()
    swap_prob.wait_send()

    def ends(u, carry):
        for q in range(CUT):
            for xx in range(2):
                p_copy(u, xx, q).wait_send()
            x_copy(u, q).wait_send()

            @pl.when(u > z)
            def _():
                z_copy(u, q, 0).wait_send()

            @pl.when(u < z)
            def _():
                z_copy(u, q, 1).wait_send()

        for b in range(4):

            @pl.when(u * 4 + b != me)
            def _():
                d_copy(u * 4 + b).wait_send()

        return carry

    lax.fori_loop(0, nz, ends, 0)
    for q in range(CUT):
        s_copy(q).wait_send()

    drain()


def visiting_order(nz):
    rows = []
    for at in range(nz):
        rows.append(sorted(range(nz), key=lambda u: (-abs(u - at), u if at < nz // 2 else -u)))
    return rows


def expert_pass(hidden_two, marks, hidden_slices, grad_all, w_gate, w_up, w_down, capacity, nf):
    specs = [
        Gather(hidden_two, nf, rep=True, chunks=4),
        Gather(marks, nf, rep=True, chunks=2),
        Gather(hidden_slices, nf, form="a2a", chunks=1),
    ]
    n = len(specs)
    f32, bf16 = jnp.float32, jnp.bfloat16
    tokens, width = hidden_two.shape
    nz = nf // 2
    total = sum(s.chunks for s in specs)
    hidden = w_gate.shape[2]
    rows = 2 * nf * capacity
    unit_rows = 4 * capacity
    slots = 2 * capacity
    any_spec = pl.BlockSpec(memory_space=pl.ANY)
    vmem = pl.BlockSpec(memory_space=pltpu.VMEM)
    dma = pltpu.SemaphoreType.DMA
    outs = [jax.ShapeDtypeStruct(s.out_shape(nf), s.array.dtype) for s in specs] + [
        jax.ShapeDtypeStruct((2 * nf * tokens, width), bf16),
        jax.ShapeDtypeStruct((2, rows, width), bf16),
        jax.ShapeDtypeStruct((2, rows, width), bf16),
        jax.ShapeDtypeStruct((2, rows, hidden), bf16),
        jax.ShapeDtypeStruct((2, rows, hidden), bf16),
        jax.ShapeDtypeStruct((2, rows, hidden), bf16),
        jax.ShapeDtypeStruct((tokens, width), f32),
        jax.ShapeDtypeStruct((2 * nf, 8, tokens), f32),
    ]
    result = pl.pallas_call(
        functools.partial(expert_kernel, nf, capacity, tuple(specs)),
        out_shape=tuple(outs),
        in_specs=[any_spec] * (n + 4),
        out_specs=tuple([any_spec] * (n + 6) + [vmem, vmem]),
        scratch_shapes=[stage_of(s, nf) for s in specs]
        + [dma((2 * nf, total)), dma((5, 2 * nf, total)), dma((2, n))]
        + [
            pltpu.VMEM(w_gate.shape, bf16),
            pltpu.VMEM(w_up.shape, bf16),
            pltpu.VMEM(w_down.shape, bf16),
            pltpu.VMEM((4 * tokens, width), bf16),
            pltpu.VMEM((4 * tokens, width), bf16),
            pltpu.VMEM((2, unit_rows, width), bf16),
            pltpu.VMEM((2, unit_rows, width), bf16),
            pltpu.VMEM((2, unit_rows, width), bf16),
            pltpu.VMEM((4, slots, width), bf16),
            pltpu.VMEM((4, slots, width), bf16),
            pltpu.VMEM((2, unit_rows, hidden), bf16),
            pltpu.VMEM((2, unit_rows, hidden), bf16),
            pltpu.VMEM((2, unit_rows, hidden), bf16),
            pltpu.VMEM((2, unit_rows, 1), f32),
            pltpu.VMEM((4, slots, 1), f32),
            pltpu.VMEM((4, slots, tokens), f32),
            pltpu.VMEM((4 * nf, tokens), f32),
            pltpu.VMEM((4 * nf, tokens), f32),
            pltpu.VMEM((4 * tokens, width), bf16),
            pltpu.VMEM((2 * nf, tokens, width), bf16),
            pltpu.VMEM((nf, tokens, width), bf16),
            pltpu.VMEM((nz, tokens, width), bf16),
            pltpu.VMEM((2, nz, tokens, width), bf16),
            pltpu.VMEM((tokens, width), bf16),
            pltpu.VMEM((2 * nf, 8, tokens), f32),
            pltpu.VMEM((2 * nf, 8, tokens), f32),
            pltpu.VMEM((2 * nf, 8, tokens), f32),
            pltpu.VMEM(specs[1].out_shape(nf), f32),
            dma((3,)),
            dma((3,)),
            dma((6,)),
            dma((nf, CUT)),
            dma((nf, CUT)),
            dma((nz, CUT)),
            dma((nz, CUT)),
            dma((nz, CUT)),
            dma((2, nz, CUT)),
            dma((CUT + 1,)),
            dma((CUT + 1,)),
            dma((2 * nf,)),
            dma((2 * nf,)),
        ],
        compiler_params=pltpu.CompilerParams(
            collective_id=7, has_side_effects=True, vmem_limit_bytes=67043328
        ),
    )(*[s.array for s in specs], grad_all, w_gate, w_up, w_down)
    hidden_all, _, hidden_slice = result[:3]
    return (hidden_all, hidden_slice) + tuple(result[3:])


NT = (((1,), (1,)), ((), ()))
TN = (((0,), (0,)), ((), ()))
NN = (((1,), (0,)), ((), ()))


def backward_kernel(nf, specs, *refs):
    n = len(specs)
    (
        attended,
        dh2_moe,
        grad_prob,
        probs,
        router,
        x_in,
        x_mid,
        gains,
        grad_out,
        wo_hbm,
        wq_hbm,
        wk_hbm,
        wv_hbm,
        q_raw,
        k_raw,
        q_rot,
        keys,
        values,
        bias,
        lse,
        trig,
        out_part,
    ), refs = refs[:22], refs[22:]
    gathered, grad_in, block_out, refs = refs[:n], refs[n], refs[n + 1], refs[n + 2 :]
    stage, refs = refs[:n], refs[n:]
    (recv, send, local), refs = refs[:3], refs[3:]
    (
        w_big,
        w_key,
        w_value,
        dx1,
        dh2,
        d_out,
        d_out_slices,
        d_attn,
        d_query,
        d_key,
        d_value,
        logit,
        tail,
        dk_acc,
        dv_acc,
        qk_acc,
        kv_send,
        kv_recv,
        dh1,
        dh1_side,
        qk_side,
        row_sum,
        w_sem,
        kv_sem,
        side_send,
        side_recv,
        sum_own,
        sum_total,
        sum_bufs,
        sum_sems,
    ) = refs[:28] + (refs[28:33], refs[33:])
    f32, bf16 = jnp.float32, jnp.bfloat16
    f, c, t = lax.axis_index("fsdp"), lax.axis_index("ctx"), lax.axis_index("tp")
    partner, side = (f, 1 - c, t), (f, c, 1 - t)
    tokens, width = x_in.shape
    experts = probs.shape[1]
    scale = HEAD_SIZE ** (-0.5)

    barrier = pltpu.get_barrier_semaphore()

    def greet(d, carry):
        pl.semaphore_signal(
            barrier, 1, device_id=(lax.rem(f + d, nf), c, t), device_id_type=MESH
        )
        return carry

    lax.fori_loop(1, nf, greet, 0)
    for dev in (partner, side):
        pl.semaphore_signal(barrier, 1, device_id=dev, device_id_type=MESH)
    pl.semaphore_wait(barrier, nf + 1)

    ins = (attended, d_query, d_key, d_value, logit, tail, d_out_slices)
    start, run, land, start_direct, run_direct, drain, step_of, edge_of, _ = gather_engine(
        nf, specs, ins, gathered, stage, recv, send, local
    )
    early, late = (0,), (1, 2, 3, 4, 5)
    nz = nf // 2
    order = visit_code(nz, f // 2)
    own_loads, to_partner, to_side, to_across, along, finish_sum, drain_sum = token_sum(
        nf, out_part, sum_own, sum_total, sum_bufs, sum_sems
    )
    for cp in own_loads:
        cp.start()
    lax.fori_loop(0, nz, lambda i, carry: to_partner(visit(order, nz, i), carry), 0)
    start((0,))

    def load(src, dst, i):
        return pltpu.make_async_copy(src, dst, w_sem.at[i])

    load(wo_hbm, w_big, 0).start()
    load(wk_hbm, w_key, 1).start()
    load(wv_hbm, w_value, 2).start()

    logit[...] = jnp.zeros_like(logit)
    pr = probs[...]
    gp = grad_prob[...]
    dl = (pr * (gp - jnp.sum(pr * gp, axis=1, keepdims=True))).astype(bf16)
    logit[:, :experts] = dl
    tile = 512
    for k in range(width // tile):
        cols = slice(k * tile, (k + 1) * tile)
        dh2[:, cols] = dh2_moe[:, cols] + lax.dot_general(
            dl, router[:, cols], NN, preferred_element_type=f32
        )
    gain_one, gain_two = gains[0:1, :], gains[1:2, :]
    gain_query, gain_key = gains[2:3, :HEAD_SIZE], gains[2:3, HEAD_SIZE : 2 * HEAD_SIZE]
    row_sum[...] = jnp.zeros_like(row_sum)
    part_rows = 16

    def norm_two(i, carry):
        rows = pl.ds(pl.multiple_of(i * part_rows, part_rows), part_rows)
        x1 = x_mid[rows]
        r2 = lax.rsqrt(jnp.mean(x1 * x1, axis=1, keepdims=True) + eps_norm)
        n2 = x1 * r2
        g = dh2[rows]
        row_sum[1:2, :] += jnp.sum(g * n2, axis=0, keepdims=True)
        scaled = g * gain_two
        mean = jnp.mean(scaled * n2, axis=1, keepdims=True)
        out = grad_out[rows].astype(f32) + r2 * (scaled - n2 * mean)
        dx1[rows] = out
        d_out[rows] = out.astype(bf16)
        return carry

    lax.fori_loop(0, tokens // part_rows, norm_two, 0)
    for cp in own_loads:
        cp.wait()
    lax.fori_loop(0, nz, lambda i, carry: to_side(visit(order, nz, i), carry), 0)
    shard = width // nf
    for k in range(nf):
        d_out_slices[k * tokens : (k + 1) * tokens, :] = d_out[:, k * shard : (k + 1) * shard]

    load(wo_hbm, w_big, 0).wait()
    heads_width = d_attn.shape[1]
    tile = 256
    for k in range(heads_width // tile):
        cols = slice(k * tile, (k + 1) * tile)
        d_attn[:, cols] = lax.dot_general(
            d_out[...], w_big[cols, :], NT, preferred_element_type=f32
        ).astype(bf16)
    load(wq_hbm, w_big, 0).start()
    step_of(1, early)
    to_across(visit(order, nz, 0))
    dk_acc[...] = jnp.zeros_like(dk_acc)
    dv_acc[...] = jnp.zeros_like(dv_acc)
    qk_acc[...] = jnp.zeros_like(qk_acc)
    group = QUERY_HEADS // KEY_VALUE_HEADS

    def unrope(g):
        return g * trig[0] + pltpu.roll(g, HEAD_SIZE // 2, 1) * trig[1]

    def norm_back(g, raw, gain):
        inv = lax.rsqrt(jnp.mean(raw * raw, axis=1, keepdims=True) + eps_norm)
        hat = raw * inv
        scaled = g * gain
        mean = jnp.mean(scaled * hat, axis=1, keepdims=True)
        return jnp.sum(g * hat, axis=0, keepdims=True), inv * (scaled - hat * mean)

    def head(h, carry):
        cols = pl.ds(pl.multiple_of(h * HEAD_SIZE, HEAD_SIZE), HEAD_SIZE)
        kv_cols = pl.ds(pl.multiple_of((h // group) * HEAD_SIZE, HEAD_SIZE), HEAD_SIZE)
        q, key, value, da = q_rot[:, cols], keys[:, kv_cols], values[:, kv_cols], d_attn[:, cols]
        s = lax.dot_general(q, key, NT, preferred_element_type=f32) * scale + bias[...]
        prob = jnp.exp(s - lse[h])
        dp = lax.dot_general(da, value, NT, preferred_element_type=f32)
        delta = jnp.sum(prob * dp, axis=1, keepdims=True)
        ds = (prob * (dp - delta) * scale).astype(bf16)
        dk_acc[:, kv_cols] += lax.dot_general(ds, q, TN, preferred_element_type=f32)
        dv_acc[:, kv_cols] += lax.dot_general(
            prob.astype(bf16), da, TN, preferred_element_type=f32
        )
        dq = unrope(jnp.dot(ds, key, preferred_element_type=f32))
        gain_grad, dq = norm_back(dq, q_raw[:, cols], gain_query)
        qk_acc[0:1, :] += gain_grad
        d_query[:, cols] = dq.astype(bf16)
        return carry

    heads = heads_width // HEAD_SIZE
    lax.fori_loop(0, heads // 2, head, 0)
    to_across(visit(order, nz, 1))
    step_of(2, early)
    lax.fori_loop(heads // 2, heads, head, 0)

    kv_width = dk_acc.shape[1]
    theirs = pl.ds(pl.multiple_of((1 - c) * tokens, tokens), tokens)
    mine = pl.ds(pl.multiple_of(c * tokens, tokens), tokens)
    kv_send[:, :kv_width] = dk_acc[theirs].astype(bf16)
    kv_send[:, kv_width:] = dv_acc[theirs].astype(bf16)
    swap_kv = pltpu.make_async_remote_copy(
        src_ref=kv_send,
        dst_ref=kv_recv,
        send_sem=kv_sem.at[0],
        recv_sem=kv_sem.at[1],
        device_id=partner,
        device_id_type=MESH,
    )
    swap_kv.start()
    start((1, 4))
    start_direct()
    swap_kv.wait()
    for kv in range(kv_width // HEAD_SIZE):
        cols = slice(kv * HEAD_SIZE, (kv + 1) * HEAD_SIZE)
        g = dk_acc[mine, cols] + kv_recv[:, cols].astype(f32)
        gain_grad, dk = norm_back(unrope(g), k_raw[:, cols], gain_key)
        qk_acc[1:2, :] += gain_grad
        d_key[:, cols] = dk.astype(bf16)
    d_value[...] = (dv_acc[mine] + kv_recv[:, kv_width:].astype(f32)).astype(bf16)
    start((2, 3))
    to_across(visit(order, nz, 2))
    along(visit(order, nz, 0))

    def to_side(src, dst, i):
        return pltpu.make_async_remote_copy(
            src_ref=src,
            dst_ref=dst,
            send_sem=side_send.at[i],
            recv_sem=side_recv.at[i],
            device_id=side,
            device_id_type=MESH,
        )

    swap_qk = to_side(qk_acc, qk_side, 4)
    swap_qk.start()
    load(wq_hbm, w_big, 0).wait()
    load(wk_hbm, w_key, 1).wait()
    load(wv_hbm, w_value, 2).wait()
    quarter = width // 4

    def dh1_copy(i):
        cols = pl.ds(i * quarter, quarter)
        return to_side(dh1.at[:, cols], dh1_side.at[:, cols], i)

    for k in range(width // tile):
        rows = slice(k * tile, (k + 1) * tile)
        total = lax.dot_general(d_query[...], w_big[rows, :], NT, preferred_element_type=f32)
        total = total + lax.dot_general(d_key[...], w_key[rows, :], NT, preferred_element_type=f32)
        total = total + lax.dot_general(
            d_value[...], w_value[rows, :], NT, preferred_element_type=f32
        )
        dh1[:, rows] = total.astype(bf16)
        if (k + 1) * tile % quarter == 0:
            dh1_copy((k + 1) * tile // quarter - 1).start()
    to_across(visit(order, nz, 3))
    step_of(3, early)
    along(visit(order, nz, 1))
    for i in range(4):
        dh1_copy(i).wait_recv()
    swap_qk.wait_recv()

    def norm_one(i, carry):
        rows = pl.ds(pl.multiple_of(i * part_rows, part_rows), part_rows)
        x0 = x_in[rows].astype(f32)
        r1 = lax.rsqrt(jnp.mean(x0 * x0, axis=1, keepdims=True) + eps_norm)
        n1 = x0 * r1
        g = dh1[rows].astype(f32) + dh1_side[rows].astype(f32)
        row_sum[0:1, :] += jnp.sum(g * n1, axis=0, keepdims=True)
        scaled = g * gain_one
        mean = jnp.mean(scaled * n1, axis=1, keepdims=True)
        grad_in[rows] = dx1[rows] + r1 * (scaled - n1 * mean)
        return carry

    lax.fori_loop(0, tokens // part_rows, norm_one, 0)
    lanes = width // 128
    tail[...] = jnp.zeros_like(tail)
    for which in range(2):
        for k in range(lanes):
            row = which * lanes + k
            tail[row : row + 1, :] = row_sum[which : which + 1, k * 128 : (k + 1) * 128]
    tail[2 * lanes : 2 * lanes + 2, :] = qk_acc[0:2, :] + qk_side[0:2, :]
    start((5,))
    step_of(1, late)
    along(visit(order, nz, 2))
    edge_of(early)
    step_of(2, late)
    along(f // 2)
    step_of(3, late)
    edge_of(late)
    run_direct()
    land()

    def put_out(rows, cols, value):
        block_out[rows, cols] = (x_mid[rows, cols] + value).astype(bf16)

    finish_sum(put_out)
    drain()
    drain_sum()
    for i in range(4):
        dh1_copy(i).wait_send()
    swap_qk.wait_send()


def visit_code(nz, z):
    order = 0
    for at, seq in enumerate(visiting_order(nz)):
        code = sum(u * nz**i for i, u in enumerate(seq))
        order = order + code * (z == at).astype(jnp.int32)
    return order


def visit(code, nz, i):
    for k in range(nz):
        code = jnp.where(i > k, code // nz, code)
    return lax.rem(code, nz)


SUM_CUT = 2


def token_sum(nf, partial, own, total_ref, bufs, sems):
    from_partner, from_side, from_across, from_z, last_half = bufs
    (
        load_sem,
        p_send,
        p_recv,
        y_send,
        y_recv,
        x_send,
        x_recv,
        z_send,
        z_recv,
        s_send,
        s_recv,
    ) = sems
    nz = nf // 2
    f, c, t = lax.axis_index("fsdp"), lax.axis_index("ctx"), lax.axis_index("tp")
    z, x = f // 2, lax.rem(f, 2)
    has_up, has_down = z + 1 < nz, z > 0
    up, down = (f + 2, c, t), (f - 2, c, t)
    across_dev, partner, side = (z * 2 + 1 - x, c, t), (f, 1 - c, t), (f, c, 1 - t)
    tokens, half = total_ref.shape
    rows = tokens // SUM_CUT
    bf16 = jnp.bfloat16
    kept = pl.ds(pl.multiple_of(t * half, half), half)
    given = pl.ds(pl.multiple_of((1 - t) * half, half), half)

    def chunk(q):
        return pl.ds(q * rows, rows)

    def remote(src, dst, send, recv, dev):
        return pltpu.make_async_remote_copy(
            src_ref=src,
            dst_ref=dst,
            send_sem=send,
            recv_sem=recv,
            device_id=dev,
            device_id_type=MESH,
        )

    own_loads = [
        pltpu.make_async_copy(
            partial.at[pl.ds((2 * b + c) * tokens, tokens)], own.at[b], load_sem.at[b]
        )
        for b in range(nf)
    ]

    def p_copy(b, q):
        return remote(
            partial.at[pl.ds((2 * b + 1 - c) * tokens + q * rows, rows)],
            from_partner.at[b, chunk(q)],
            p_send.at[b, q],
            p_recv.at[b, q],
            partner,
        )

    def y_copy(b, q):
        return remote(
            own.at[b, chunk(q), given],
            from_side.at[b, chunk(q)],
            y_send.at[b, q],
            y_recv.at[b, q],
            side,
        )

    def x_copy(u, q):
        return remote(
            own.at[u * 2 + 1 - x, chunk(q), kept],
            from_across.at[u, chunk(q)],
            x_send.at[u, q],
            x_recv.at[u, q],
            across_dev,
        )

    def z_copy(u, q, way, dev):
        return remote(
            own.at[u * 2 + x, chunk(q), kept],
            from_z.at[way, u, chunk(q)],
            z_send.at[u, q],
            z_recv.at[way, u, q],
            dev,
        )

    def s_copy(q):
        return remote(
            own.at[f, chunk(q), kept], last_half.at[chunk(q)], s_send.at[q], s_recv.at[q], side
        )

    def wide(value):
        return value.astype(jnp.float32)

    def to_partner(u, carry):
        for xx in range(2):
            for q in range(SUM_CUT):
                p_copy(u * 2 + xx, q).start()
        return carry

    def to_side(u, carry):
        for xx in range(2):
            b = u * 2 + xx
            for q in range(SUM_CUT):
                p_copy(b, q).wait_recv()
                own[b, chunk(q)] = (
                    wide(own[b, chunk(q)]) + wide(from_partner[b, chunk(q)])
                ).astype(bf16)
                y_copy(b, q).start()
        return carry

    def to_across(u):
        b = u * 2 + 1 - x
        for q in range(SUM_CUT):
            y_copy(b, q).wait_recv()
            own[b, chunk(q), kept] = (
                wide(own[b, chunk(q), kept]) + wide(from_side[b, chunk(q)])
            ).astype(bf16)
            x_copy(u, q).start()

    def along(u):
        b = u * 2 + x
        for q in range(SUM_CUT):
            y_copy(b, q).wait_recv()
            x_copy(u, q).wait_recv()
            total_ref[chunk(q)] = (
                wide(own[b, chunk(q), kept])
                + wide(from_side[b, chunk(q)])
                + wide(from_across[u, chunk(q)])
            )

            @pl.when((u >= z) & has_down)
            def _():
                z_copy(u, q, 0, partner).wait_recv()
                total_ref[chunk(q)] += wide(from_z[0, u, chunk(q)])

            @pl.when((u <= z) & has_up)
            def _():
                z_copy(u, q, 1, partner).wait_recv()
                total_ref[chunk(q)] += wide(from_z[1, u, chunk(q)])

            own[b, chunk(q), kept] = total_ref[chunk(q)].astype(bf16)

            @pl.when(u > z)
            def _():
                z_copy(u, q, 0, up).start()

            @pl.when(u < z)
            def _():
                z_copy(u, q, 1, down).start()

            @pl.when(u == z)
            def _():
                s_copy(q).start()

    def finish_sum(put):
        for q in range(SUM_CUT):
            put(chunk(q), kept, wide(own[f, chunk(q), kept]))
            s_copy(q).wait_recv()
            put(chunk(q), given, wide(last_half[chunk(q)]))

    def drain_sum():
        def ends(u, carry):
            for q in range(SUM_CUT):
                for xx in range(2):
                    p_copy(u * 2 + xx, q).wait_send()
                    y_copy(u * 2 + xx, q).wait_send()
                x_copy(u, q).wait_send()

                @pl.when(u != z)
                def _():
                    z_copy(u, q, 0, partner).wait_send()

            return carry

        lax.fori_loop(0, nz, ends, 0)
        for q in range(SUM_CUT):
            s_copy(q).wait_send()

    return own_loads, to_partner, to_side, to_across, along, finish_sum, drain_sum


def backward_pass(nf, arrays, attended, shapes):
    f32, bf16 = jnp.float32, jnp.bfloat16
    tokens, width, heads_width, kv_width, keys = shapes
    tail_rows = -(-(2 * width // 128 + 2) // 8) * 8
    shape = jax.ShapeDtypeStruct
    specs = [
        Gather(attended, nf, chunks=2),
        Gather(shape((tokens, heads_width), bf16), nf, chunks=2),
        Gather(shape((tokens, kv_width), bf16), nf, chunks=1),
        Gather(shape((tokens, kv_width), bf16), nf, chunks=1),
        Gather(shape((tokens, 128), bf16), nf, chunks=1),
        Gather(shape((tail_rows, 128), f32), nf, chunks=1),
        Gather(shape((nf * tokens, width // nf), bf16), nf, form="a2a", chunks=1),
    ]
    n = len(specs)
    total = sum(s.chunks for s in specs)
    any_spec = pl.BlockSpec(memory_space=pl.ANY)
    vmem = pl.BlockSpec(memory_space=pltpu.VMEM)
    dma = pltpu.SemaphoreType.DMA
    in_any = {0, 9, 10, 11, 12, 21}
    nz = nf // 2
    return pl.pallas_call(
        functools.partial(backward_kernel, nf, tuple(specs)),
        out_shape=tuple(shape(s.out_shape(nf), s.array.dtype) for s in specs)
        + (shape((tokens, width), f32), shape((tokens, width), bf16)),
        in_specs=[any_spec if i in in_any else vmem for i in range(22)],
        out_specs=tuple([any_spec] * n + [vmem, vmem]),
        scratch_shapes=[stage_of(s, nf) for s in specs]
        + [dma((2 * nf, total)), dma((5, 2 * nf, total)), dma((2, n))]
        + [
            pltpu.VMEM((width, max(width, heads_width)), bf16),
            pltpu.VMEM((width, kv_width), bf16),
            pltpu.VMEM((width, kv_width), bf16),
            pltpu.VMEM((tokens, width), f32),
            pltpu.VMEM((tokens, width), f32),
            pltpu.VMEM((tokens, width), bf16),
            pltpu.VMEM((nf * tokens, width // nf), bf16),
            pltpu.VMEM((tokens, heads_width), bf16),
            pltpu.VMEM((tokens, heads_width), bf16),
            pltpu.VMEM((tokens, kv_width), bf16),
            pltpu.VMEM((tokens, kv_width), bf16),
            pltpu.VMEM((tokens, 128), bf16),
            pltpu.VMEM((tail_rows, 128), f32),
            pltpu.VMEM((keys, kv_width), f32),
            pltpu.VMEM((keys, kv_width), f32),
            pltpu.VMEM((8, 128), f32),
            pltpu.VMEM((tokens, 2 * kv_width), bf16),
            pltpu.VMEM((tokens, 2 * kv_width), bf16),
            pltpu.VMEM((tokens, width), bf16),
            pltpu.VMEM((tokens, width), bf16),
            pltpu.VMEM((8, 128), f32),
            pltpu.VMEM((2, width), f32),
            dma((3,)),
            dma((2,)),
            dma((5,)),
            dma((5,)),
            pltpu.VMEM((nf, tokens, width), bf16),
            pltpu.VMEM((tokens, width // 2), f32),
            pltpu.VMEM((nf, tokens, width), bf16),
            pltpu.VMEM((nf, tokens, width // 2), bf16),
            pltpu.VMEM((nz, tokens, width // 2), bf16),
            pltpu.VMEM((2, nz, tokens, width // 2), bf16),
            pltpu.VMEM((tokens, width // 2), bf16),
            dma((nf,)),
            dma((nf, SUM_CUT)),
            dma((nf, SUM_CUT)),
            dma((nf, SUM_CUT)),
            dma((nf, SUM_CUT)),
            dma((nz, SUM_CUT)),
            dma((nz, SUM_CUT)),
            dma((nz, SUM_CUT)),
            dma((2, nz, SUM_CUT)),
            dma((SUM_CUT,)),
            dma((SUM_CUT,)),
        ],
        compiler_params=pltpu.CompilerParams(
            collective_id=8, has_side_effects=True, vmem_limit_bytes=67043328
        ),
    )(attended, *arrays)


def forward_kernel(nf, specs, *refs):
    n = len(specs)
    ins, refs = refs[:n], refs[n:]
    (x_in, segments, routed, trig), refs = refs[:4], refs[4:]
    gathered, refs = refs[:n], refs[n:]
    (
        hidden,
        hidden_slices,
        marks,
        probs,
        x_mid,
        attended,
        q_raw,
        k_raw,
        q_rot,
        keys,
        values,
        bias,
        lse,
        gains,
        router,
    ), refs = refs[:15], refs[15:]
    stage, refs = refs[:n], refs[n:]
    (recv, send, local), refs = refs[:3], refs[3:]
    (
        w_big,
        w_key,
        w_value,
        small,
        hidden_one,
        kv_all,
        part,
        part_side,
        square,
        w_sem,
        kv_sem,
        side_send,
        side_recv,
    ) = refs
    f32, bf16 = jnp.float32, jnp.bfloat16
    nz = nf // 2
    f, c, t = lax.axis_index("fsdp"), lax.axis_index("ctx"), lax.axis_index("tp")
    z, x = f // 2, lax.rem(f, 2)
    partner, side = (f, 1 - c, t), (f, c, 1 - t)
    has_up, has_down = z + 1 < nz, z > 0
    tokens, width = x_in.shape
    experts = routed.shape[1]
    heads_width = q_raw.shape[1]
    kv_width = k_raw.shape[1]
    scale = HEAD_SIZE ** (-0.5)
    barrier = pltpu.get_barrier_semaphore()

    def greet(dev):
        pl.semaphore_signal(barrier, 1, device_id=dev, device_id_type=MESH)

    for dev in (partner, side, (z * 2 + 1 - x, c, t)):
        greet(dev)

    @pl.when(has_up)
    def _():
        greet((f + 2, c, t))

    @pl.when(has_down)
    def _():
        greet((f - 2, c, t))

    pl.semaphore_wait(barrier, 3 + has_up.astype(jnp.int32) + has_down.astype(jnp.int32))
    start, _, _, _, _, drain, step_of, edge_of, land_of = gather_engine(
        nf, specs, ins, gathered, stage, recv, send, local
    )
    first, second, third = (0, 1, 2, 3), (4,), (5,)
    start(first)
    for k in range(1, nz):
        step_of(k, first)
    start(second)
    edge_of(first)
    land_of(first)

    def load(src, dst, i):
        return pltpu.make_async_copy(src, dst, w_sem.at[i])

    small_load = load(gathered[0], small, 3)
    small_load.start()
    load(gathered[2], w_key, 1).start()
    load(gathered[3], w_value, 2).start()
    load(gathered[1], w_big, 0).start()
    small_load.wait()

    size = specs[0].rows
    halves = width // nf // 128
    qk_sum = [jnp.zeros((1, 128), f32), jnp.zeros((1, 128), f32)]
    for k in range(nf):
        base = 2 * k * size
        for h in range(halves):
            cols = slice((k * halves + h) * 128, (k * halves + h + 1) * 128)
            router[:, cols] = small[base + h * experts : base + (h + 1) * experts, :]
            at = base + halves * experts
            for g in range(2):
                row = at + g * halves + h
                gains[g : g + 1, cols] = small[row : row + 1, :].astype(f32)
        at = base + halves * experts + 2 * halves
        for h in range(2):
            qk_sum[h] = qk_sum[h] + small[at + h : at + h + 1, :].astype(f32)
    gains[2:3, :] = jnp.zeros((1, width), f32)
    for h in range(2):
        gains[2:3, h * 128 : (h + 1) * 128] = qk_sum[h]
    gain_one, gain_two = gains[0:1, :], gains[1:2, :]
    gain_query, gain_key = qk_sum
    part_rows = 16

    def norm_one(i, carry):
        rows = pl.ds(pl.multiple_of(i * part_rows, part_rows), part_rows)
        x0 = x_in[rows].astype(f32)
        r1 = lax.rsqrt(jnp.mean(x0 * x0, axis=1, keepdims=True) + eps_norm)
        hidden_one[rows] = (x0 * r1 * gain_one).astype(bf16)
        return carry

    lax.fori_loop(0, tokens // part_rows, norm_one, 0)
    shard = width // nf
    for k in range(nf):
        hidden_slices[k * tokens : (k + 1) * tokens, :] = hidden_one[:, k * shard : (k + 1) * shard]

    def norm_rope(raw, gain):
        inv = lax.rsqrt(jnp.mean(raw * raw, axis=1, keepdims=True) + eps_norm)
        normed = raw * inv * gain
        turned = normed * trig[0] - pltpu.roll(normed, HEAD_SIZE // 2, 1) * trig[1]
        return turned.astype(bf16)

    load(gathered[2], w_key, 1).wait()
    load(gathered[3], w_value, 2).wait()
    mine = pl.ds(pl.multiple_of(c * tokens, tokens), tokens)
    k_raw[...] = jnp.dot(hidden_one[...], w_key[...], preferred_element_type=f32)
    kv_all[mine, kv_width : 2 * kv_width] = jnp.dot(
        hidden_one[...], w_value[...], preferred_element_type=f32
    ).astype(bf16)
    for kv in range(kv_width // HEAD_SIZE):
        cols = slice(kv * HEAD_SIZE, (kv + 1) * HEAD_SIZE)
        kv_all[mine, cols] = norm_rope(k_raw[:, cols], gain_key)
    kv_all[mine, 2 * kv_width :] = segments[...]
    swap_kv = pltpu.make_async_remote_copy(
        src_ref=kv_all.at[mine],
        dst_ref=kv_all.at[mine],
        send_sem=kv_sem.at[0],
        recv_sem=kv_sem.at[1],
        device_id=partner,
        device_id_type=MESH,
    )
    swap_kv.start()
    step_of(1, second)
    load(gathered[1], w_big, 0).wait()
    tile = 256
    for k in range(heads_width // tile):
        cols = slice(k * tile, (k + 1) * tile)
        q_raw[:, cols] = jnp.dot(hidden_one[...], w_big[:, cols], preferred_element_type=f32)
    swap_kv.wait()
    keys[...] = kv_all[:, :kv_width]
    values[...] = kv_all[:, kv_width : 2 * kv_width]
    span = kv_all.shape[0]
    theirs = jnp.transpose(kv_all[:, 2 * kv_width :].astype(f32))
    own = segments[...].astype(f32)
    query_at = c * tokens + lax.broadcasted_iota(jnp.int32, (tokens, 128), 0)
    for h in range(span // 128):
        cols = slice(h * 128, (h + 1) * 128)
        key_at = h * 128 + lax.broadcasted_iota(jnp.int32, (tokens, 128), 1)
        allowed = (key_at <= query_at) & (theirs[:, cols] == own)
        bias[:, cols] = jnp.where(allowed, 0.0, -jnp.inf)
    step_of(2, second)
    group = QUERY_HEADS // KEY_VALUE_HEADS

    def head(h, carry):
        cols = pl.ds(pl.multiple_of(h * HEAD_SIZE, HEAD_SIZE), HEAD_SIZE)
        kv_cols = pl.ds(pl.multiple_of((h // group) * HEAD_SIZE, HEAD_SIZE), HEAD_SIZE)
        q = norm_rope(q_raw[:, cols], gain_query)
        q_rot[:, cols] = q
        s = lax.dot_general(q, keys[:, kv_cols], NT, preferred_element_type=f32) * scale
        s = s + bias[...]
        top = jnp.max(s, axis=1, keepdims=True)
        total = top + jnp.log(jnp.sum(jnp.exp(s - top), axis=1, keepdims=True))
        lse[h] = total
        prob = jnp.exp(s - total).astype(bf16)
        attended[:, cols] = jnp.dot(
            prob, values[:, kv_cols], preferred_element_type=f32
        ).astype(bf16)
        return carry

    heads = heads_width // HEAD_SIZE
    lax.fori_loop(0, heads // 2, head, 0)
    step_of(3, second)
    start(third)
    lax.fori_loop(heads // 2, heads, head, 0)
    edge_of(second)
    land_of(second)
    load(gathered[4], w_big, 0).start()
    step_of(1, third)
    load(gathered[4], w_big, 0).wait()
    quarter = width // 4

    def side_copy(i):
        cols = pl.ds(i * quarter, quarter)
        return pltpu.make_async_remote_copy(
            src_ref=part.at[:, cols],
            dst_ref=part_side.at[:, cols],
            send_sem=side_send.at[i],
            recv_sem=side_recv.at[i],
            device_id=side,
            device_id_type=MESH,
        )

    for k in range(width // tile):
        cols = slice(k * tile, (k + 1) * tile)
        part[:, cols] = jnp.dot(
            attended[...], w_big[:, cols], preferred_element_type=f32
        ).astype(bf16)
        if (k + 1) * tile % quarter == 0:
            side_copy((k + 1) * tile // quarter - 1).start()
    step_of(2, third)
    for i in range(4):
        side_copy(i).wait_recv()

    def norm_two(i, carry):
        rows = pl.ds(pl.multiple_of(i * part_rows, part_rows), part_rows)
        x1 = x_in[rows].astype(f32) + (part[rows].astype(f32) + part_side[rows].astype(f32))
        x_mid[rows] = x1
        r2 = lax.rsqrt(jnp.mean(x1 * x1, axis=1, keepdims=True) + eps_norm)
        hidden[rows] = (x1 * r2 * gain_two).astype(bf16)
        return carry

    lax.fori_loop(0, tokens // part_rows, norm_two, 0)
    logits = lax.dot_general(hidden[...], router[...], NT, preferred_element_type=f32)
    on = routed[...] > 0.0
    kept = jnp.where(on, logits, -jnp.inf)
    raised = jnp.where(on, jnp.exp(kept - jnp.max(kept, axis=1, keepdims=True)), 0.0)
    shares = raised / jnp.sum(raised, axis=1, keepdims=True)
    probs[...] = shares
    square[...] = jnp.zeros_like(square)
    square[:, :experts] = jnp.where(on, shares, -1.0)
    marks[...] = jnp.transpose(square[...])[:experts, :]
    step_of(3, third)
    edge_of(third)
    land_of(third)
    drain()
    for i in range(4):
        side_copy(i).wait_send()


def forward_pass(nf, arrays, operands, shapes):
    f32, bf16 = jnp.float32, jnp.bfloat16
    small, w_query, key_projection, value_projection, w_out, grad_out = arrays
    tokens, width, heads_width, kv_width, experts = shapes
    specs = [
        Gather(small, nf, chunks=1),
        Gather(w_query, nf, half=True, chunks=2),
        Gather(key_projection, nf, half=True, chunks=1),
        Gather(value_projection, nf, half=True, chunks=1),
        Gather(w_out, nf, form="col", half=True, chunks=2),
        Gather(grad_out, nf, rep=True, chunks=4),
    ]
    n = len(specs)
    total = sum(s.chunks for s in specs)
    any_spec = pl.BlockSpec(memory_space=pl.ANY)
    vmem = pl.BlockSpec(memory_space=pltpu.VMEM)
    dma = pltpu.SemaphoreType.DMA
    shape = jax.ShapeDtypeStruct
    span = 2 * tokens
    made = [
        shape((tokens, width), bf16),
        shape((nf * tokens, width // nf), bf16),
        shape((experts, tokens), f32),
        shape((tokens, experts), f32),
        shape((tokens, width), f32),
        shape((tokens, heads_width), bf16),
        shape((tokens, heads_width), f32),
        shape((tokens, kv_width), f32),
        shape((tokens, heads_width), bf16),
        shape((span, kv_width), bf16),
        shape((span, kv_width), bf16),
        shape((tokens, span), f32),
        shape((heads_width // HEAD_SIZE, tokens, 1), f32),
        shape((3, width), f32),
        shape((experts, width), bf16),
    ]
    return pl.pallas_call(
        functools.partial(forward_kernel, nf, tuple(specs)),
        out_shape=tuple(shape(s.out_shape(nf), s.array.dtype) for s in specs) + tuple(made),
        in_specs=[any_spec] * n + [vmem] * 4,
        out_specs=tuple([any_spec] * n + [vmem] * len(made)),
        scratch_shapes=[stage_of(s, nf) for s in specs]
        + [dma((2 * nf, total)), dma((5, 2 * nf, total)), dma((2, n))]
        + [
            pltpu.VMEM((width, max(width, heads_width)), bf16),
            pltpu.VMEM((width, kv_width), bf16),
            pltpu.VMEM((width, kv_width), bf16),
            pltpu.VMEM(specs[0].out_shape(nf), bf16),
            pltpu.VMEM((tokens, width), bf16),
            pltpu.VMEM((span, 2 * kv_width + 128), bf16),
            pltpu.VMEM((tokens, width), bf16),
            pltpu.VMEM((tokens, width), bf16),
            pltpu.VMEM((tokens, 128), f32),
            dma((4,)),
            dma((2,)),
            dma((4,)),
            dma((4,)),
        ],
        compiler_params=pltpu.CompilerParams(
            collective_id=9, has_side_effects=True, vmem_limit_bytes=67043328
        ),
    )(*arrays, *operands)


def norm_forward(values, gain_row):
    inverse = lax.rsqrt(jnp.mean(values * values, axis=-1, keepdims=True) + eps_norm)
    normed = values * inverse
    return (normed * gain_row, normed, inverse)


def rms_norm_gradient(grad_scaled, normed, inverse, gain_row):
    grad_normed = grad_scaled * gain_row
    inner_mean = jnp.mean(grad_normed * normed, axis=-1, keepdims=True)
    return inverse * (grad_normed - normed * inner_mean)


def rope_tables(positions):
    half_dim = HEAD_SIZE // 2
    frequencies = rope_base ** (-(jnp.arange(half_dim, dtype=jnp.float32) * 2.0) / HEAD_SIZE)
    angles = positions.astype(jnp.float32)[:, None] * frequencies[None, :]
    return (jnp.cos(angles)[:, None, :], jnp.sin(angles)[:, None, :])


def rotate(values, cosine_table, sine_values):
    half_dim = values.shape[-1] // 2
    first_half = values[..., :half_dim]
    second_half = values[..., half_dim:]
    return jnp.concatenate(
        [
            first_half * cosine_table - second_half * sine_values,
            second_half * cosine_table + first_half * sine_values,
        ],
        axis=-1,
    )


def inverse_rotation(grad_in_rot, cosine_table, sine_values):
    half_dim = grad_in_rot.shape[-1] // 2
    first_half = grad_in_rot[..., :half_dim]
    second_half = grad_in_rot[..., half_dim:]
    return jnp.concatenate(
        [
            first_half * cosine_table + second_half * sine_values,
            second_half * cosine_table - first_half * sine_values,
        ],
        axis=-1,
    )


def masked_scores(query_rotated, key_rotated, allowed):
    scores = jnp.einsum(
        "qkgd,skd->kgqs", query_rotated, key_rotated, preferred_element_type=jnp.float32
    ) * HEAD_SIZE ** (-0.5)
    return jnp.where(allowed[None, None], scores, -jnp.inf)


def swap(value, axis_name):
    return lax.ppermute(value, axis_name, [(0, 1), (1, 0)])


def sum_over_tp(value):
    mine = value.astype(jnp.bfloat16)
    return mine.astype(jnp.float32) + swap(mine, "tp").astype(jnp.float32)


def block_sum(partial, nf):
    return lax.psum_scatter(partial, ("fsdp", "ctx"), scatter_dimension=0, tiled=True)


def by_shard(rows, nf):
    count, width = rows.shape
    return rows.reshape(count, nf, width // nf).transpose(1, 0, 2).reshape(nf * count, width // nf)


def on_device(
    hidden_in,
    segment_ids,
    routes,
    attn_gain,
    qk_gains,
    w_query,
    key_projection,
    value_projection,
    w_out,
    ffn_gain,
    w_router,
    w_gate,
    w_up,
    w_down,
    grad_out,
):
    tokens_dev, width_dim = hidden_in.shape
    nf = lax.axis_size("fsdp")
    devices = nf * lax.axis_size("ctx")
    local_experts = w_gate.shape[0]
    experts = local_experts * devices
    capacity = max(2, 2 * tokens_dev * TOPK // experts)
    query_group_width = QUERY_HEADS // KEY_VALUE_HEADS
    shard_width = attn_gain.shape[0]
    f_index, c_index = lax.axis_index("fsdp"), lax.axis_index("ctx")
    bf16 = jnp.bfloat16
    f32 = jnp.float32

    if nf == 8:
        halves = shard_width // 128
        turned = w_router.T.reshape(experts, halves, 128).transpose(1, 0, 2).reshape(-1, 128)
        qk_row = lax.dynamic_update_slice(
            jnp.zeros((256,), bf16), qk_gains, (f_index * qk_gains.shape[0],)
        )
        small = jnp.concatenate(
            [
                turned,
                attn_gain.reshape(-1, 128),
                ffn_gain.reshape(-1, 128),
                qk_row.reshape(-1, 128),
            ]
        )
        small = jnp.pad(small, ((0, -small.shape[0] % 16), (0, 0)))
        own_positions = c_index * tokens_dev + jnp.arange(tokens_dev, dtype=jnp.int32)
        cosine_table, sine_values = rope_tables(own_positions)
        cosine_row, sine_row = cosine_table[:, 0], sine_values[:, 0]
        trig = jnp.stack(
            [
                jnp.concatenate([cosine_row, cosine_row], axis=1),
                jnp.concatenate([sine_row, -sine_row], axis=1),
            ]
        )
        segment_wide = jnp.broadcast_to(segment_ids.astype(bf16)[:, None], (tokens_dev, 128))
        expert_ids = jnp.arange(experts, dtype=jnp.int32)
        hits = routes[:, :, None] == expert_ids[None, None, :]
        routed = jnp.any(hits, axis=1).astype(f32)
        heads_width, kv_width = w_query.shape[1], key_projection.shape[1]
        shapes = (tokens_dev, width_dim, heads_width, kv_width, experts)
        (
            _,
            query_weight,
            key_weight,
            value_weight,
            out_weight,
            grad_all,
            hidden_two,
            hidden_slices,
            marks,
            probs,
            resid_mid,
            attended,
            query_raw,
            key_projected,
            query_rotated,
            key_all,
            value_all,
            bias,
            log_total,
            gains,
            router_rows,
        ) = forward_pass(
            nf,
            (small, w_query, key_projection, value_projection, w_out, grad_out),
            (hidden_in, segment_wide, routed, trig),
            shapes,
        )
    else:
        pieces = [w_router.reshape(-1), attn_gain, ffn_gain, qk_gains]
        flat = jnp.concatenate(pieces)
        small_rows = -(-flat.shape[0] // 2048) * 16
        small = jnp.pad(flat, (0, small_rows * 128 - flat.shape[0])).reshape(small_rows, 128)
        out_form = "row" if shard_width % 128 else "col"
        small_all, query_weight, key_weight, value_weight, out_weight, grad_all = plane_gather(
            [
                Gather(small, nf, chunks=1),
                Gather(w_query, nf, half=True, chunks=2),
                Gather(key_projection, nf, half=True, chunks=1),
                Gather(value_projection, nf, half=True, chunks=1),
                Gather(w_out, nf, form=out_form, half=True, chunks=2),
                Gather(grad_out, nf, rep=True, chunks=4),
            ],
            1,
            nf,
        )
        if out_form == "row":
            out_weight = out_weight.reshape(nf, -1, shard_width).transpose(1, 0, 2)
            out_weight = out_weight.reshape(-1, width_dim)
        small_all = small_all.reshape(nf, 2, small_rows * 128)[:, 0]
        ends = [0]
        for piece in pieces:
            ends.append(ends[-1] + piece.shape[0])
        router_weight = small_all[:, ends[0] : ends[1]].reshape(width_dim, experts)
        gain_one = small_all[:, ends[1] : ends[2]].reshape(-1).astype(f32)
        gain_two = small_all[:, ends[2] : ends[3]].reshape(-1).astype(f32)
        gain_qk = small_all[:, ends[3] : ends[4]].reshape(-1).astype(f32)
        gain_query, gain_key = gain_qk[:HEAD_SIZE], gain_qk[HEAD_SIZE:]

        kv_local = key_weight.shape[1] // HEAD_SIZE
        head_local = query_weight.shape[1] // HEAD_SIZE
        resid = hidden_in.astype(f32)
        scaled_one, normed_one, inverse_one = norm_forward(resid, gain_one)
        hidden_first = scaled_one.astype(bf16)
        query_raw = jnp.dot(hidden_first, query_weight, preferred_element_type=f32).reshape(
            tokens_dev, head_local, HEAD_SIZE
        )
        key_projected = jnp.dot(hidden_first, key_weight, preferred_element_type=f32).reshape(
            tokens_dev, kv_local, HEAD_SIZE
        )
        value_rows = jnp.dot(hidden_first, value_weight, preferred_element_type=f32).astype(bf16)
        query_normed, query_hat, query_inverse = norm_forward(query_raw, gain_query)
        key_normed, key_unit_rows, key_inverse_norm = norm_forward(key_projected, gain_key)
        own_positions = c_index * tokens_dev + jnp.arange(tokens_dev, dtype=jnp.int32)
        cosine_table, sine_values = rope_tables(own_positions)
        query_rotated = (
            rotate(query_normed, cosine_table, sine_values)
            .astype(bf16)
            .reshape(tokens_dev, kv_local, query_group_width, HEAD_SIZE)
        )
        key_rotated = rotate(key_normed, cosine_table, sine_values).astype(bf16)
        own_segments = segment_ids.astype(bf16)
        packed_kv = jnp.concatenate(
            [
                key_rotated.reshape(tokens_dev, -1),
                value_rows,
                jnp.broadcast_to(own_segments[:, None], (tokens_dev, 128)),
            ],
            axis=1,
        )
        kv_all = lax.all_gather(packed_kv, "ctx", axis=0, tiled=True)
        kv_width = kv_local * HEAD_SIZE
        key_all = kv_all[:, :kv_width].reshape(-1, kv_local, HEAD_SIZE)
        value_all = kv_all[:, kv_width : 2 * kv_width].reshape(-1, kv_local, HEAD_SIZE)
        segment_all = kv_all[:, 2 * kv_width]
        key_positions = jnp.arange(key_all.shape[0], dtype=jnp.int32)
        allowed = (key_positions[None, :] <= own_positions[:, None]) & (
            segment_all[None, :] == own_segments[:, None]
        )
        scores = masked_scores(query_rotated, key_all, allowed)
        top_score = jnp.max(scores, axis=-1, keepdims=True)
        log_total = top_score + jnp.log(jnp.sum(jnp.exp(scores - top_score), axis=-1, keepdims=True))
        weights_att = jnp.exp(scores - log_total).astype(bf16)
        attended = jnp.einsum("kgqs,skd->qkgd", weights_att, value_all, preferred_element_type=f32)
        attended = attended.astype(bf16).reshape(tokens_dev, head_local * HEAD_SIZE)
        out_partial = jnp.dot(attended, out_weight, preferred_element_type=f32)
        resid_mid = resid + sum_over_tp(out_partial)
        scaled_two, normed_two, inverse_two = norm_forward(resid_mid, gain_two)
        hidden_two = scaled_two.astype(bf16)
        logits = jnp.dot(hidden_two, router_weight, preferred_element_type=f32)
        expert_ids = jnp.arange(experts, dtype=jnp.int32)
        hits = routes[:, :, None] == expert_ids[None, None, :]
        routed = jnp.any(hits, axis=1)
        masked_logits = jnp.where(routed, logits, -jnp.inf)
        raised = jnp.where(
            routed, jnp.exp(masked_logits - jnp.max(masked_logits, axis=1, keepdims=True)), 0.0
        )
        probs = raised / jnp.sum(raised, axis=1, keepdims=True)
        marks = jnp.where(routed, probs, -1.0).T
    if nf == 8:
        (
            hidden_all,
            hidden_first_slice,
            moe_partial,
            rows_in,
            grad_prod,
            activated,
            grad_gate_pre,
            grad_up_pre,
            grad_hidden_moe,
            grad_prob,
        ) = expert_pass(
            hidden_two,
            marks,
            hidden_slices,
            grad_all,
            w_gate,
            w_up,
            w_down,
            capacity,
            nf,
        )
        grad_prob = grad_prob.reshape(devices, 8, tokens_dev)[:, :local_experts]
        grad_prob = grad_prob.reshape(experts, tokens_dev).T
    else:
        hidden_all, marks_all, hidden_first_slice = plane_gather(
            [
                Gather(hidden_two, nf, rep=True, chunks=4),
                Gather(marks, nf, chunks=1),
                Gather(by_shard(hidden_first, nf), nf, form="a2a", chunks=1),
            ],
            2,
            nf,
        )
        first_expert = (f_index * 2 + c_index) * local_experts
        marks_here = lax.dynamic_slice_in_dim(
            marks_all.reshape(devices, experts, tokens_dev), first_expert, local_experts, axis=1
        )
        taken = marks_here >= 0.0
        ranks = jnp.cumsum(taken.astype(jnp.int32), axis=2) - 1
        slots = jnp.arange(capacity, dtype=jnp.int32)
        chosen = taken[:, :, None, :] & (ranks[:, :, None, :] == slots[None, None, :, None])
        pick = chosen.astype(bf16)
        weight_slot = jnp.sum(jnp.where(chosen, marks_here[:, :, None, :], 0.0), axis=3)
        weight_slot = weight_slot.transpose(1, 0, 2).reshape(local_experts, devices * capacity)

        def select(rows):
            blocks = rows.reshape(devices, tokens_dev, width_dim)
            out = jnp.einsum("bjst,btd->jbsd", pick, blocks, preferred_element_type=f32)
            return out.astype(bf16).reshape(local_experts, devices * capacity, width_dim)

        def spread(rows):
            blocks = rows.reshape(local_experts, devices, capacity, width_dim)
            out = jnp.einsum("bjst,jbsd->btd", pick, blocks, preferred_element_type=f32)
            return out.astype(bf16).reshape(devices * tokens_dev, width_dim)

        rows_in = select(hidden_all)
        grad_rows_in = select(grad_all)
        gate_pre = jnp.einsum("jrd,jdf->jrf", rows_in, w_gate, preferred_element_type=f32)
        up_pre = jnp.einsum("jrd,jdf->jrf", rows_in, w_up, preferred_element_type=f32)
        sigmoid_gate = jax.nn.sigmoid(gate_pre)
        silu_gate = gate_pre * sigmoid_gate
        activated = (silu_gate * up_pre).astype(bf16)
        produced = jnp.einsum("jrf,jfd->jrd", activated, w_down, preferred_element_type=f32).astype(
            bf16
        )
        wide = produced.astype(f32)
        grad_prob_slot = jnp.sum(wide * grad_rows_in.astype(f32), axis=2)
        grad_prob_part = jnp.sum(
            jnp.where(
                chosen,
                grad_prob_slot.reshape(local_experts, devices, capacity).transpose(1, 0, 2)[..., None],
                0.0,
            ),
            axis=2,
        )
        moe_partial = spread((weight_slot[:, :, None] * wide).astype(bf16))
        grad_prod = (weight_slot[:, :, None] * grad_rows_in.astype(f32)).astype(bf16)
        grad_act = jnp.einsum("jrd,jfd->jrf", grad_prod, w_down, preferred_element_type=f32)
        grad_gate_pre = (
            grad_act * up_pre * (sigmoid_gate * (1.0 + gate_pre * (1.0 - sigmoid_gate)))
        ).astype(bf16)
        grad_up_pre = (grad_act * silu_gate).astype(bf16)
        grad_slots = jnp.einsum("jrf,jdf->jrd", grad_gate_pre, w_gate, preferred_element_type=f32)
        grad_slots = (
            grad_slots + jnp.einsum("jrf,jdf->jrd", grad_up_pre, w_up, preferred_element_type=f32)
        ).astype(bf16)
        hidden_grad_partial = spread(grad_slots)

        grad_hidden_moe = sum_over_tp(block_sum(hidden_grad_partial, nf))
        grad_prob = lax.all_to_all(
            grad_prob_part, ("fsdp", "ctx"), split_axis=0, concat_axis=0, tiled=True
        ).reshape(experts, tokens_dev)
        grad_prob = grad_prob + swap(grad_prob, "tp")
        grad_prob = grad_prob.T
    grad_down = jnp.einsum("jrf,jrd->jfd", activated, grad_prod, preferred_element_type=f32)
    grad_gate = jnp.einsum("jrd,jrf->jdf", rows_in, grad_gate_pre, preferred_element_type=f32)
    grad_up = jnp.einsum("jrd,jrf->jdf", rows_in, grad_up_pre, preferred_element_type=f32)

    if nf == 8:
        operands = (
            grad_hidden_moe,
            grad_prob,
            probs,
            router_rows,
            hidden_in,
            resid_mid,
            gains,
            grad_out,
            out_weight,
            query_weight,
            key_weight,
            value_weight,
            query_raw,
            key_projected,
            query_rotated,
            key_all,
            value_all,
            bias,
            log_total,
            trig,
            moe_partial,
        )
        shapes = (tokens_dev, width_dim, heads_width, kv_width, key_all.shape[0])
        (
            attended_all,
            dq_all,
            dk_all,
            dv_all,
            logits_all,
            tail_all,
            proj_slice,
            grad_in,
            block_out,
        ) = backward_pass(nf, operands, attended, shapes)
        tail_rows = tail_all.shape[0] // devices
    else:
        block_out = (resid_mid + sum_over_tp(block_sum(moe_partial, nf))).astype(bf16)

        grad_rows = grad_out.astype(f32)
        grad_logits = (
            probs * (grad_prob - jnp.sum(probs * grad_prob, axis=1, keepdims=True))
        ).astype(bf16)
        grad_hidden_two = grad_hidden_moe + jnp.einsum(
            "te,de->td", grad_logits, router_weight, preferred_element_type=f32
        )
        grad_ffn_local = jnp.sum(grad_hidden_two * normed_two, axis=0)
        grad_mid = grad_rows + rms_norm_gradient(grad_hidden_two, normed_two, inverse_two, gain_two)
        grad_proj = grad_mid.astype(bf16)
        attended_gradient = jnp.einsum(
            "td,qd->tq", grad_proj, out_weight, preferred_element_type=f32
        ).astype(bf16)
        attended_gradient = attended_gradient.reshape(
            tokens_dev, kv_local, query_group_width, HEAD_SIZE
        )
        probs_att = jnp.exp(scores - log_total)
        grad_value_all = jnp.einsum(
            "kgqs,qkgd->skd", weights_att, attended_gradient, preferred_element_type=f32
        )
        grad_probs = jnp.einsum(
            "qkgd,skd->kgqs", attended_gradient, value_all, preferred_element_type=f32
        )
        delta_row = jnp.sum(probs_att * grad_probs, axis=-1, keepdims=True)
        grad_scores = (probs_att * (grad_probs - delta_row) * HEAD_SIZE ** (-0.5)).astype(bf16)
        grad_query_rot = jnp.einsum(
            "kgqs,skd->qkgd", grad_scores, key_all, preferred_element_type=f32
        ).reshape(tokens_dev, head_local, HEAD_SIZE)
        grad_key_all = jnp.einsum(
            "kgqs,qkgd->skd", grad_scores, query_rotated, preferred_element_type=f32
        )
        grad_kv_all = jnp.concatenate(
            [grad_key_all.reshape(-1, kv_width), grad_value_all.reshape(-1, kv_width)], axis=1
        )
        theirs = lax.dynamic_slice_in_dim(grad_kv_all, (1 - c_index) * tokens_dev, tokens_dev, axis=0)
        mine = lax.dynamic_slice_in_dim(grad_kv_all, c_index * tokens_dev, tokens_dev, axis=0)
        grad_kv = mine + swap(theirs.astype(bf16), "ctx").astype(f32)
        key_rotated_gradient = grad_kv[:, :kv_width].reshape(tokens_dev, kv_local, HEAD_SIZE)
        grad_query_norm = inverse_rotation(grad_query_rot, cosine_table, sine_values)
        key_normed_gradient = inverse_rotation(key_rotated_gradient, cosine_table, sine_values)
        grad_qk_local = jnp.concatenate(
            [
                jnp.sum(grad_query_norm * query_hat, axis=(0, 1)),
                jnp.sum(key_normed_gradient * key_unit_rows, axis=(0, 1)),
            ]
        )
        grad_query_raw = (
            rms_norm_gradient(grad_query_norm, query_hat, query_inverse, gain_query)
            .astype(bf16)
            .reshape(tokens_dev, head_local * HEAD_SIZE)
        )
        key_projected_gradient = (
            rms_norm_gradient(key_normed_gradient, key_unit_rows, key_inverse_norm, gain_key)
            .astype(bf16)
            .reshape(tokens_dev, kv_width)
        )
        value_projected_gradient = grad_kv[:, kv_width:].astype(bf16)
        grad_hidden_part = jnp.einsum(
            "tq,dq->td", grad_query_raw, query_weight, preferred_element_type=f32
        )
        grad_hidden_part = grad_hidden_part + jnp.einsum(
            "tq,dq->td", key_projected_gradient, key_weight, preferred_element_type=f32
        )
        grad_hidden_part = grad_hidden_part + jnp.einsum(
            "tq,dq->td", value_projected_gradient, value_weight, preferred_element_type=f32
        )
        grad_hidden_one = sum_over_tp(grad_hidden_part)
        grad_in = grad_mid + rms_norm_gradient(grad_hidden_one, normed_one, inverse_one, gain_one)
        grad_attn_local = jnp.sum(grad_hidden_one * normed_one, axis=0)
        grad_qk_local = grad_qk_local + swap(grad_qk_local, "tp")
        tail = jnp.concatenate([grad_attn_local, grad_ffn_local, grad_qk_local])
        tail = jnp.pad(tail, (0, -tail.shape[0] % 1024)).reshape(-1, 128)
        tail_rows = tail.shape[0]
        logit_pad = jnp.pad(grad_logits, ((0, 0), (0, -experts % 128)))

        dq_all, dk_all, dv_all, attended_all, proj_slice, logits_all, tail_all = plane_gather(
            [
                Gather(grad_query_raw, nf, chunks=2),
                Gather(key_projected_gradient, nf, chunks=1),
                Gather(value_projected_gradient, nf, chunks=1),
                Gather(attended, nf, chunks=2),
                Gather(by_shard(grad_proj, nf), nf, form="a2a", chunks=1),
                Gather(logit_pad, nf, chunks=1),
                Gather(tail, nf, chunks=1),
            ],
            3,
            nf,
        )
    over_tokens = functools.partial(
        jnp.einsum, "td,tq->dq", preferred_element_type=f32
    )
    grad_query = over_tokens(hidden_first_slice, dq_all)
    grad_key = over_tokens(hidden_first_slice, dk_all)
    grad_value = over_tokens(hidden_first_slice, dv_all)
    grad_out_proj = over_tokens(attended_all, proj_slice)
    hidden_slice = lax.dynamic_slice_in_dim(hidden_all, f_index * shard_width, shard_width, axis=1)
    grad_router = over_tokens(hidden_slice, logits_all)[:, :experts]
    tail_sum = jnp.sum(tail_all.reshape(devices, tail_rows * 128), axis=0)
    grad_attn = lax.dynamic_slice_in_dim(tail_sum, f_index * shard_width, shard_width)
    grad_ffn = lax.dynamic_slice_in_dim(tail_sum, width_dim + f_index * shard_width, shard_width)
    qk_width = qk_gains.shape[0]
    grad_qk = lax.dynamic_slice_in_dim(tail_sum, 2 * width_dim + f_index * qk_width, qk_width)
    return (
        block_out,
        grad_in,
        grad_attn,
        grad_qk,
        grad_query,
        grad_key,
        grad_value,
        grad_out_proj,
        grad_ffn,
        grad_router,
        grad_gate,
        grad_up,
        grad_down,
    )


def solution(mesh):
    return jax.shard_map(
        on_device,
        mesh=mesh,
        in_specs=(
            P(("fsdp", "ctx"), None),
            P(("fsdp", "ctx")),
            P(("fsdp", "ctx"), None),
            P("fsdp"),
            P("fsdp"),
            P("fsdp", "tp"),
            P("fsdp", "tp"),
            P("fsdp", "tp"),
            P("tp", "fsdp"),
            P("fsdp"),
            P("fsdp", None),
            P(("fsdp", "ctx"), None, "tp"),
            P(("fsdp", "ctx"), None, "tp"),
            P(("fsdp", "ctx"), "tp", None),
            P(("fsdp", "ctx"), None),
        ),
        out_specs=(
            P(("fsdp", "ctx"), None),
            P(("fsdp", "ctx"), None),
            P("fsdp"),
            P("fsdp"),
            P("fsdp", "tp"),
            P("fsdp", "tp"),
            P("fsdp", "tp"),
            P("tp", "fsdp"),
            P("fsdp"),
            P("fsdp", None),
            P(("fsdp", "ctx"), None, "tp"),
            P(("fsdp", "ctx"), None, "tp"),
            P(("fsdp", "ctx"), "tp", None),
        ),
        check_vma=False,
    )
```

```python
import functools

import jax
import jax.numpy as jnp
from jax import lax
from jax.experimental import pallas as pl
from jax.experimental.pallas import tpu as pltpu
from jax.sharding import PartitionSpec as P

QUERY_HEADS = 32
KEY_VALUE_HEADS = 4
HEAD_SIZE = 128
TOPK = 8
MESH = pl.DeviceIdType.MESH

eps_norm = 1e-06
rope_base = 1000000.0

UP, DOWN, ACROSS, PARTNER, SIDE = range(5)


class Gather:
    def __init__(self, array, nf, form="row", half=False, rep=False, chunks=2, split=None):
        if nf > 8:
            chunks = 2 if rep else 1
        self.array, self.form, self.half, self.rep, self.chunks = array, form, half, rep, chunks
        self.shape = array.shape
        self.split = nf // 2 - 1 if split is None else split
        self.rows = array.shape[0] // 2 if half else array.shape[0]
        self.step = (self.rows // nf if form == "a2a" else self.rows) // chunks

    def out_shape(self, nf):
        rows, cols = self.rows, self.shape[1]
        if self.form == "col":
            return (2 * rows, nf * cols)
        if self.form == "a2a":
            return (2 * rows, cols)
        return (2 * nf * rows, cols)


def gather_engine(nf, specs, ins, outs, stage, recv, send, local):
    n = len(specs)
    nz = nf // 2
    f, c, t = lax.axis_index("fsdp"), lax.axis_index("ctx"), lax.axis_index("tp")
    z, x = f // 2, lax.rem(f, 2)
    has_up, has_down = z + 1 < nz, z > 0
    device = {
        UP: (f + 2, c, t),
        DOWN: (f - 2, c, t),
        ACROSS: (z * 2 + 1 - x, c, t),
        PARTNER: (f, 1 - c, t),
        SIDE: (f, c, 1 - t),
    }
    first = [sum(s.chunks for s in specs[:a]) for a in range(n)]

    def src(a, q, dest_f=None):
        s = specs[a]
        lo = row_chunk(a, q) * s.step
        if s.half:
            lo = c * s.rows + lo
        if s.form == "a2a":
            lo = dest_f * (s.rows // nf) + lo
        return ins[a].at[pl.ds(lo, s.step)]

    def dst(a, q, bf, bc):
        s = specs[a]
        if s.form == "col":
            width = s.shape[1]
            return outs[a].at[
                pl.ds(bc * s.rows + row_chunk(a, q) * s.step, s.step),
                pl.ds(pl.multiple_of(bf * width, width), width),
            ]
        rows = s.rows // nf if s.form == "a2a" else s.rows
        return outs[a].at[pl.ds((bf * 2 + bc) * rows + row_chunk(a, q) * s.step, s.step)]

    def copy(a, q, bf, bc, source, kind, dev=None, slot=None):
        block = bf * 2 + bc if slot is None else slot
        return pltpu.make_async_remote_copy(
            src_ref=source,
            dst_ref=dst(a, q, bf, bc),
            send_sem=send.at[kind, block, first[a] + row_chunk(a, q)],
            recv_sem=recv.at[bf * 2 + bc, first[a] + row_chunk(a, q)],
            device_id=device[kind] if dev is None else dev,
            device_id_type=MESH,
        )

    def row_chunk(a, q):
        n_chunks = specs[a].chunks
        if not specs[a].rep:
            return q
        return lax.rem(q + t * (n_chunks // 2), n_chunks)

    def in_half(a, q):
        return 2 * q < specs[a].chunks

    def both(*conds):
        if any(k is False for k in conds):
            return False
        conds = [k for k in conds if k is not None and k is not True]
        if not conds:
            return None
        return functools.reduce(lambda u, v: u & v, conds)

    def when(cond, fn):
        if cond is None or cond is True:
            fn()
        elif cond is not False:
            pl.when(cond)(fn)

    def go_up(a, q, dist):
        far = dist + 1 < specs[a].split if specs[a].rep and not in_half(a, q) else None
        return both(has_up, far)

    def go_down(a, q, dist):
        far = dist + 1 < specs[a].split if specs[a].rep and not in_half(a, q) else None
        return both(has_down, far)

    def go_across(a, q):
        return in_half(a, q) if specs[a].rep else None

    relays = [(a, q) for a in range(n) if specs[a].form != "a2a" for q in range(specs[a].chunks)]
    direct = [(a, q) for a in range(n) if specs[a].form == "a2a" for q in range(specs[a].chunks)]

    def start(only=None):
        only = range(n) if only is None else only
        for a, q in relays:
            if a not in only:
                continue
            source = src(a, q)
            when(go_up(a, q, 0), lambda: copy(a, q, f, c, source, UP).start())
            when(go_down(a, q, 0), lambda: copy(a, q, f, c, source, DOWN).start())
            when(go_across(a, q), lambda: copy(a, q, f, c, source, ACROSS).start())
            copy(a, q, f, c, source, PARTNER).start()
        own_start([a for a in only if specs[a].form != "a2a"])

    def own_start(only):
        for a in only:
            own_in(a).start()
        for a in only:
            own_in(a).wait()
            own_out(a).start()

    def start_direct():
        own_start(sorted({a for a, _ in direct}))
        for a, q in direct:
            copy(a, q, f, c, src(a, q, f), PARTNER).start()

            def far_send(d, carry):
                there = lax.rem(f + d, nf)
                copy(a, q, f, c, src(a, q, there), UP, dev=(there, c, t), slot=there).start()
                return carry

            lax.fori_loop(1, nf, far_send, 0)

    def own_in(a):
        s = specs[a]
        if s.form == "a2a":
            view = ins[a].at[pl.ds(f * s.step, s.step)]
        elif s.half:
            view = ins[a].at[pl.ds(c * s.rows, s.rows)]
        else:
            view = ins[a]
        return pltpu.make_async_copy(view, stage[a], local.at[0, a])

    def own_out(a):
        s = specs[a]
        if s.form == "col":
            width = s.shape[1]
            view = outs[a].at[
                pl.ds(c * s.rows, s.rows), pl.ds(pl.multiple_of(f * width, width), width)
            ]
        else:
            rows = s.rows // nf if s.form == "a2a" else s.rows
            view = outs[a].at[pl.ds((f * 2 + c) * rows, rows)]
        return pltpu.make_async_copy(stage[a], view, local.at[1, a])

    def arrived(a, q, bf, bc):
        copy(a, q, bf, bc, dst(a, q, bf, bc), PARTNER).wait_recv()

    def pass_on(a, q, bf, kind, cond=None):
        when(cond, lambda: copy(a, q, bf, c, dst(a, q, bf, c), kind).start())

    pair = z + 1 - 2 * lax.rem(z, 2)
    even = lax.rem(z, 2) == 0

    def shared(a, q):
        return not specs[a].rep and specs[a].chunks > 1 and 2 * q >= specs[a].chunks

    def column(k, a, q):
        rep = specs[a].rep
        came = k < specs[a].split if rep and not in_half(a, q) else None
        far = (k >= specs[a].split) if rep and in_half(a, q) else False

        def take(zz, kind, onward):
            bf = zz * 2 + x
            arrived(a, q, bf, c)
            pass_on(a, q, bf, kind, onward)
            cross = (zz != pair) if shared(a, q) else go_across(a, q)
            pass_on(a, q, bf, ACROSS, cross)
            pass_on(a, q, bf, PARTNER)
            if rep:
                pass_on(a, q, bf, SIDE, far)

        when(both(z - k >= 0, came), lambda: take(z - k, UP, go_up(a, q, k)))
        when(both(z + k < nz, came), lambda: take(z + k, DOWN, go_down(a, q, k)))

    def across(k, a, q):
        rep = specs[a].rep
        mine = in_half(a, q) if rep else None

        def take(zz):
            bf = zz * 2 + 1 - x
            arrived(a, q, bf, c)
            pass_on(a, q, bf, PARTNER)
            if rep:
                pass_on(a, q, bf, SIDE)
            if shared(a, q):
                pass_on(a, q, bf, UP, (zz == z) & even)
                pass_on(a, q, bf, DOWN, (zz == z) & jnp.logical_not(even))

        when(both(z - k >= 0, mine), lambda: take(z - k))
        when(both(z + k < nz, k > 0, mine), lambda: take(z + k))

    def aside(k, a, q):
        if not specs[a].rep:
            return
        if in_half(a, q):
            return

        def take(bf):
            arrived(a, q, bf, c)
            pass_on(a, q, bf, PARTNER)

        when(z - k >= 0, lambda: take((z - k) * 2 + 1 - x))
        when(both(z + k < nz, k > 0), lambda: take((z + k) * 2 + 1 - x))
        far = k >= specs[a].split
        when(both(z - k >= 0, far), lambda: take((z - k) * 2 + x))
        when(both(z + k < nz, far), lambda: take((z + k) * 2 + x))

    count = len(relays)
    lag = 2

    def late(fn, k, i):
        if i >= 0:
            fn(k, *relays[i])
        else:
            pl.when(k > 1)(lambda: fn(k - 1, *relays[count + i]))

    by_chunk = all(specs[a].rep for a, _ in relays)

    def step(k, carry):
        if not by_chunk:
            for a, q in relays:
                column(k, a, q)
            for a, q in relays:
                across(k - 1, a, q)

            @pl.when(k > 1)
            def _():
                for a, q in relays:
                    aside(k - 2, a, q)

            return carry
        for i, (a, q) in enumerate(relays):
            column(k, a, q)
            pl.when(k == 1)(lambda: across(0, a, q))
            late(across, k, i - lag)
            if i >= lag:
                pl.when(k == 1)(lambda: aside(0, *relays[i - lag]))
            late(aside, k, i - 2 * lag)

        @pl.when(k == 1)
        def _():
            for a, q in relays[count - lag :]:
                aside(0, a, q)

        return carry

    def run(hook=None):
        def body(k, carry):
            step(k, carry)
            if hook is not None:
                hook(k)
            return carry

        lax.fori_loop(1, nz, body, 0)
        for a, q in relays[count - lag if by_chunk else 0 :]:
            across(nz - 1, a, q)
        if not by_chunk:
            for a, q in relays:
                aside(nz - 2, a, q)
        for a, q in relays[count - 2 * lag if by_chunk else 0 :]:
            aside(nz - 1, a, q)

    def step_of(k, only):
        some = [(a, q) for a, q in relays if a in only]
        for a, q in some:
            column(k, a, q)
        for a, q in some:
            across(k - 1, a, q)

        if any(specs[a].rep for a, _ in some) and k > 1:
            for a, q in some:
                aside(k - 2, a, q)

    def edge_of(only):
        some = [(a, q) for a, q in relays if a in only]
        for a, q in some:
            across(nz - 1, a, q)
        for a, q in some:
            aside(nz - 2, a, q)
        for a, q in some:
            aside(nz - 1, a, q)

    def land_of(only):
        def take(bf, carry):
            for a, q in relays:
                if a in only:
                    arrived(a, q, bf, 1 - c)
            return carry

        lax.fori_loop(0, nf, take, 0)
        for a in only:
            own_out(a).wait()

    def run_direct():
        for a, q in direct:

            def far_take(d, carry):
                there = lax.rem(f + nf - d, nf)
                arrived(a, q, there, c)
                pass_on(a, q, there, PARTNER)
                return carry

            lax.fori_loop(1, nf, far_take, 0)

    def take_partner(bf, carry):
        for a, q in relays:
            arrived(a, q, bf, 1 - c)
        return carry

    def land():
        lax.fori_loop(0, nf, take_partner, 0)
        for a in range(n):
            if specs[a].form != "a2a":
                own_out(a).wait()

    def finish(bf, carry):
        zz, xx = bf // 2, lax.rem(bf, 2)
        dist = jnp.abs(zz - z)
        here = xx == x
        for a, q in relays:
            rep = specs[a].rep
            view = dst(a, q, bf, c)

            def sent(kind, cond):
                when(cond, lambda: copy(a, q, bf, c, view, kind).wait_send())

            half = in_half(a, q) if rep else None
            by_z = dist < specs[a].split if rep and not half else None
            sent(PARTNER, None)
            sent(UP, both(here, zz <= z, by_z, go_up(a, q, dist)))
            sent(DOWN, both(here, zz >= z, by_z, go_down(a, q, dist)))
            cross = (zz != pair) if shared(a, q) else go_across(a, q)
            sent(ACROSS, both(here, by_z, cross))
            if shared(a, q):
                there = jnp.logical_not(here) & (zz == z)
                sent(UP, there & even)
                sent(DOWN, there & jnp.logical_not(even))
            if rep and half:
                sent(SIDE, jnp.logical_not(here) | (dist >= specs[a].split))
        for a, q in direct:
            arrived(a, q, bf, 1 - c)
            view = dst(a, q, bf, c)
            copy(a, q, bf, c, view, PARTNER).wait_send()

            @pl.when(bf != f)
            def _():
                copy(a, q, bf, c, view, UP, slot=bf).wait_send()

        return carry

    def drain():
        lax.fori_loop(0, nf, finish, 0)
        for a in range(n):
            if specs[a].form == "a2a":
                own_out(a).wait()

    return start, run, land, start_direct, run_direct, drain, step_of, edge_of, land_of


def gather_kernel(nf, specs, *refs):
    n = len(specs)
    ins, outs, scratch = refs[:n], refs[n : 2 * n], refs[2 * n :]
    nz = nf // 2
    f, c, t = lax.axis_index("fsdp"), lax.axis_index("ctx"), lax.axis_index("tp")
    z, x = f // 2, lax.rem(f, 2)
    has_up, has_down = z + 1 < nz, z > 0
    device = {
        UP: (f + 2, c, t),
        DOWN: (f - 2, c, t),
        ACROSS: (z * 2 + 1 - x, c, t),
        PARTNER: (f, 1 - c, t),
        SIDE: (f, c, 1 - t),
    }
    any_a2a = any(s.form == "a2a" for s in specs)
    any_rep = any(s.rep for s in specs)
    barrier = pltpu.get_barrier_semaphore()

    def greet(dev):
        pl.semaphore_signal(barrier, 1, device_id=dev, device_id_type=MESH)

    greeted = 1
    greet(device[PARTNER])
    if any_rep:
        greet(device[SIDE])
        greeted += 1
    if any_a2a:

        def greet_far(d, carry):
            greet((lax.rem(f + d, nf), c, t))
            return carry

        lax.fori_loop(1, nf, greet_far, 0)
        pl.semaphore_wait(barrier, greeted + nf - 1)
    else:
        greet(device[ACROSS])

        @pl.when(has_up)
        def _():
            greet(device[UP])

        @pl.when(has_down)
        def _():
            greet(device[DOWN])

        pl.semaphore_wait(
            barrier, greeted + 1 + has_up.astype(jnp.int32) + has_down.astype(jnp.int32)
        )

    start, run, land, start_direct, run_direct, drain, *_ = gather_engine(
        nf, specs, ins, outs, scratch[:n], *scratch[n:]
    )
    start()
    start_direct()
    run()
    run_direct()
    land()
    drain()


def stage_of(s, nf):
    rows = s.rows // nf if s.form == "a2a" else s.rows
    return pltpu.VMEM((rows, s.shape[1]), s.array.dtype)


def plane_gather(specs, collective_id, nf):
    n = len(specs)
    total = sum(s.chunks for s in specs)

    return pl.pallas_call(
        functools.partial(gather_kernel, nf, tuple(specs)),
        out_shape=tuple(jax.ShapeDtypeStruct(s.out_shape(nf), s.array.dtype) for s in specs),
        in_specs=[pl.BlockSpec(memory_space=pl.ANY)] * n,
        out_specs=tuple(pl.BlockSpec(memory_space=pl.ANY) for _ in specs),
        scratch_shapes=[stage_of(s, nf) for s in specs]
        + [
            pltpu.SemaphoreType.DMA((2 * nf, total)),
            pltpu.SemaphoreType.DMA((5, 2 * nf, total)),
            pltpu.SemaphoreType.DMA((2, n)),
        ],
        compiler_params=pltpu.CompilerParams(
            collective_id=collective_id, has_side_effects=True
        ),
    )(*[s.array for s in specs])


CUT = 4


def expert_kernel(nf, capacity, specs, *refs):
    n = len(specs)
    ins, refs = refs[:n], refs[n:]
    (grad_all, wg_hbm, wu_hbm, wd_hbm), refs = refs[:4], refs[4:]
    gathered, refs = refs[:n], refs[n:]
    (out_part, xs_out, de_out, act_out, dg_out, du_out, grad_tok, prob_tok), refs = (
        refs[:8],
        refs[8:],
    )
    stage, refs = refs[:n], refs[n:]
    (recv, send, local), refs = refs[:3], refs[3:]
    (
        wg,
        wu,
        wd,
        x_buf,
        y_buf,
        xs,
        ys,
        de,
        pe,
        bs,
        act,
        dg,
        du,
        w_slot,
        dp_slot,
        pick,
        mk,
        rk,
        y_out,
        part,
        from_partner,
        from_across,
        from_z,
        from_side,
        dp_send,
        dp_recv,
        dp_side,
        marks_v,
        w_sem,
        load_sem,
        store_sem,
        p_send,
        p_recv,
        x_send,
        x_recv,
        z_send,
        z_recv,
        s_send,
        s_recv,
        d_send,
        d_recv,
    ) = refs
    f32, bf16 = jnp.float32, jnp.bfloat16
    nz = nf // 2
    f, c, t = lax.axis_index("fsdp"), lax.axis_index("ctx"), lax.axis_index("tp")
    z, x = f // 2, lax.rem(f, 2)
    me = f * 2 + c
    up, down = (f + 2, c, t), (f - 2, c, t)
    across_dev, partner, side = (z * 2 + 1 - x, c, t), (f, 1 - c, t), (f, c, 1 - t)
    has_up, has_down = z + 1 < nz, z > 0
    tokens = x_buf.shape[0] // 4
    width = x_buf.shape[1]
    slots = 2 * capacity
    rows_unit = 4 * capacity
    hidden = wg.shape[2]
    experts = specs[1].shape[0]
    step_rows = tokens // CUT

    barrier = pltpu.get_barrier_semaphore()

    def greet(d, carry):
        there = lax.rem(me + d, 2 * nf)
        pl.semaphore_signal(
            barrier, 1, device_id=(there // 2, lax.rem(there, 2), t), device_id_type=MESH
        )
        return carry

    lax.fori_loop(1, 2 * nf, greet, 0)
    pl.semaphore_signal(barrier, 1, device_id=side, device_id_type=MESH)
    pl.semaphore_wait(barrier, 2 * nf)

    start, run, land, start_direct, run_direct, drain, *_ = gather_engine(
        nf, specs, ins, gathered, stage, recv, send, local
    )
    start()
    weight_loads = [
        pltpu.make_async_copy(src, dst, w_sem.at[i])
        for i, (src, dst) in enumerate(((wg_hbm, wg), (wu_hbm, wu), (wd_hbm, wd)))
    ]
    for load in weight_loads:
        load.start()

    order = 0
    for at, seq in enumerate(visiting_order(nz)):
        code = sum(u * nz**i for i, u in enumerate(seq))
        order = order + code * (z == at).astype(jnp.int32)

    def unit_at(i):
        code = order
        for k in range(nz):
            code = jnp.where(i > k, code // nz, code)
        return lax.rem(code, nz)

    def load_rows(u, which):
        rows = pl.ds(pl.multiple_of(u * 4 * tokens, 4 * tokens), 4 * tokens)
        if which == 0:
            return pltpu.make_async_copy(gathered[0].at[rows], x_buf, load_sem.at[0])
        return pltpu.make_async_copy(grad_all.at[rows], y_buf, load_sem.at[1])

    load_rows(unit_at(0), 1).start()
    run()
    land()
    start_direct()
    load_rows(unit_at(0), 0).start()
    marks_in = pltpu.make_async_copy(gathered[1], marks_v, load_sem.at[2])
    marks_in.start()
    marks_in.wait()
    dp_send[...] = jnp.zeros_like(dp_send)
    first_expert = me * 2
    for b in range(2 * nf):
        for j in range(2):
            mk[2 * b + j : 2 * b + j + 1, :] = marks_v[pl.ds(b * experts + first_expert + j, 1), :]
    taken = jnp.where(mk[...] >= 0.0, 1.0, 0.0).astype(bf16)
    before = lax.broadcasted_iota(jnp.int32, (tokens, tokens), 0)
    after = lax.broadcasted_iota(jnp.int32, (tokens, tokens), 1)
    upper = jnp.where(before <= after, 1.0, 0.0).astype(bf16)
    rk[...] = jnp.dot(taken, upper, preferred_element_type=f32) - 1.0
    for load in weight_loads:
        load.wait()

    def store_unit(u):
        rows = pl.ds(pl.multiple_of(u * rows_unit, rows_unit), rows_unit)
        pairs = [(xs, xs_out), (de, de_out), (act, act_out), (dg, dg_out), (du, du_out)]
        copies = [
            pltpu.make_async_copy(src, dst.at[:, rows], store_sem.at[i])
            for i, (src, dst) in enumerate(pairs)
        ]
        out_rows = pl.ds(pl.multiple_of(u * 4 * tokens, 4 * tokens), 4 * tokens)
        copies.append(pltpu.make_async_copy(y_out, out_part.at[out_rows], store_sem.at[5]))
        return copies

    def chunk(q):
        return pl.ds(pl.multiple_of(q * step_rows, step_rows), step_rows)

    def p_copy(u, xx, q):
        return pltpu.make_async_remote_copy(
            src_ref=part.at[u * 4 + xx * 2 + 1 - c, chunk(q)],
            dst_ref=from_partner.at[u * 2 + xx, chunk(q)],
            send_sem=p_send.at[u * 2 + xx, q],
            recv_sem=p_recv.at[u * 2 + xx, q],
            device_id=partner,
            device_id_type=MESH,
        )

    def x_copy(u, q):
        return pltpu.make_async_remote_copy(
            src_ref=part.at[u * 4 + (1 - x) * 2 + c, chunk(q)],
            dst_ref=from_across.at[u, chunk(q)],
            send_sem=x_send.at[u, q],
            recv_sem=x_recv.at[u, q],
            device_id=across_dev,
            device_id_type=MESH,
        )

    def z_copy(u, q, way):
        return pltpu.make_async_remote_copy(
            src_ref=part.at[u * 4 + x * 2 + c, chunk(q)],
            dst_ref=from_z.at[way, u, chunk(q)],
            send_sem=z_send.at[u, q],
            recv_sem=z_recv.at[way, u, q],
            device_id=up if way == 0 else down,
            device_id_type=MESH,
        )

    def z_wait(u, q, way):
        pltpu.make_async_remote_copy(
            src_ref=part.at[me, chunk(q)],
            dst_ref=from_z.at[way, u, chunk(q)],
            send_sem=z_send.at[u, q],
            recv_sem=z_recv.at[way, u, q],
            device_id=partner,
            device_id_type=MESH,
        ).wait_recv()

    def s_copy(q):
        return pltpu.make_async_remote_copy(
            src_ref=part.at[me, chunk(q)],
            dst_ref=from_side.at[chunk(q)],
            send_sem=s_send.at[q],
            recv_sem=s_recv.at[q],
            device_id=side,
            device_id_type=MESH,
        )

    def d_copy(b, source=None):
        return pltpu.make_async_remote_copy(
            src_ref=dp_send.at[b],
            dst_ref=dp_recv.at[me if source is None else source],
            send_sem=d_send.at[b],
            recv_sem=d_recv.at[me if source is None else source],
            device_id=(b // 2, lax.rem(b, 2), t),
            device_id_type=MESH,
        )

    def compute(i, u):
        load_rows(u, 0).wait()
        load_rows(u, 1).wait()

        @pl.when(i > 0)
        def _():
            for cp in store_unit(unit_at(i - 1)):
                cp.wait()

        slot_ids = lax.broadcasted_iota(jnp.int32, (capacity, tokens), 0).astype(f32)
        for b in range(4):
            for j in range(2):
                row = pl.ds(2 * (u * 4 + b) + j, 1)
                mark = mk[row, :]
                hit = (rk[row, :] == slot_ids) & (mark >= 0.0)
                pick[b, j * capacity : (j + 1) * capacity, :] = jnp.where(hit, 1.0, 0.0)
                w_slot[j, b * capacity : (b + 1) * capacity, :] = jnp.sum(
                    jnp.where(hit, mark, 0.0), axis=1, keepdims=True
                )
        tile = 512
        for b in range(4):
            chosen = pick[b].astype(bf16)
            for k in range(width // tile):
                cols = slice(k * tile, (k + 1) * tile)
                got = jnp.dot(
                    chosen, x_buf[b * tokens : (b + 1) * tokens, cols], preferred_element_type=f32
                ).astype(bf16)
                gy = jnp.dot(
                    chosen, y_buf[b * tokens : (b + 1) * tokens, cols], preferred_element_type=f32
                )
                for j in range(2):
                    to = slice(b * capacity, (b + 1) * capacity)
                    of = slice(j * capacity, (j + 1) * capacity)
                    xs[j, to, cols] = got[of]
                    ys[j, to, cols] = gy[of].astype(bf16)
                    de[j, to, cols] = (w_slot[j, to, :] * gy[of]).astype(bf16)

        @pl.when(i + 1 < nz)
        def _():
            load_rows(unit_at(i + 1), 0).start()
            load_rows(unit_at(i + 1), 1).start()

        def expert(j, carry):
            gate = jnp.dot(xs[j], wg[j], preferred_element_type=f32)
            upv = jnp.dot(xs[j], wu[j], preferred_element_type=f32)
            sig = 1.0 / (1.0 + jnp.exp(-gate))
            silu = gate * sig
            act[j] = (silu * upv).astype(bf16)
            grad_act = lax.dot_general(
                de[j], wd[j], (((1,), (1,)), ((), ())), preferred_element_type=f32
            )
            dg[j] = (grad_act * upv * (sig * (1.0 + gate * (1.0 - sig)))).astype(bf16)
            du[j] = (grad_act * silu).astype(bf16)
            total = jnp.zeros((rows_unit, 1), f32)
            for k in range(width // tile):
                cols = slice(k * tile, (k + 1) * tile)
                made = jnp.dot(act[j], wd[j, :, cols], preferred_element_type=f32)
                made = made.astype(bf16).astype(f32)
                total = total + jnp.sum(made * ys[j, :, cols].astype(f32), axis=1, keepdims=True)
                weighted = (w_slot[j] * made).astype(bf16)
                back = lax.dot_general(
                    dg[j], wg[j, cols, :], (((1,), (1,)), ((), ())), preferred_element_type=f32
                ) + lax.dot_general(
                    du[j], wu[j, cols, :], (((1,), (1,)), ((), ())), preferred_element_type=f32
                )
                back = back.astype(bf16)
                for b in range(4):
                    of = slice(b * capacity, (b + 1) * capacity)
                    to = pl.ds(pl.multiple_of(j * capacity, capacity), capacity)
                    pe[b, to, cols] = weighted[of]
                    bs[b, to, cols] = back[of]
            for b in range(4):
                to = pl.ds(pl.multiple_of(j * capacity, capacity), capacity)
                dp_slot[b, to, :] = total[b * capacity : (b + 1) * capacity]
            return carry

        lax.fori_loop(0, 2, expert, 0)

        def spread(b):
            chosen = pick[b]
            back = jnp.transpose(chosen).astype(bf16)
            for k in range(width // tile):
                cols = slice(k * tile, (k + 1) * tile)
                part[u * 4 + b, :, cols] = jnp.dot(
                    back, bs[b, :, cols], preferred_element_type=f32
                ).astype(bf16)

        for b in range(4):
            spread(b)
        for xx in range(2):
            for q in range(CUT):
                p_copy(u, xx, q).start()
        for b in range(4):
            back = jnp.transpose(pick[b]).astype(bf16)
            for k in range(width // tile):
                cols = slice(k * tile, (k + 1) * tile)
                y_out[b * tokens : (b + 1) * tokens, cols] = jnp.dot(
                    back, pe[b, :, cols], preferred_element_type=f32
                ).astype(bf16)
            for j in range(2):
                of = slice(j * capacity, (j + 1) * capacity)
                dp_send[u * 4 + b, j : j + 1, :] = jnp.sum(
                    pick[b, of, :] * dp_slot[b, of, :], axis=0, keepdims=True
                )
        for cp in store_unit(u):
            cp.start()
        for b in range(4):
            bb = u * 4 + b

            @pl.when(bb != me)
            def _():
                d_copy(bb).start()

    def wide(ref):
        return ref.astype(f32)

    def to_across(u):
        @pl.loop(0, CUT)
        def _(q):
            for xx in range(2):
                p_copy(u, xx, q).wait_recv()
            blk = u * 4 + (1 - x) * 2 + c
            part[blk, chunk(q)] = (
                wide(part[blk, chunk(q)]) + wide(from_partner[u * 2 + 1 - x, chunk(q)])
            ).astype(bf16)
            x_copy(u, q).start()

    def along(u):
        blk = u * 4 + x * 2 + c

        @pl.loop(0, CUT)
        def _(q):
            x_copy(u, q).wait_recv()

            def total():
                return (
                    wide(part[blk, chunk(q)])
                    + wide(from_partner[u * 2 + x, chunk(q)])
                    + wide(from_across[u, chunk(q)])
                )

            def hop(way, has_before):
                @pl.when(has_before)
                def _():
                    z_wait(u, q, way)
                    part[blk, chunk(q)] = (total() + wide(from_z[way, u, chunk(q)])).astype(bf16)

                @pl.when(jnp.logical_not(has_before))
                def _():
                    part[blk, chunk(q)] = total().astype(bf16)

                z_copy(u, q, way).start()

            @pl.when(u > z)
            def _():
                hop(0, has_down)

            @pl.when(u < z)
            def _():
                hop(1, has_up)

            @pl.when(u == z)
            def _():
                grad_tok[chunk(q)] = total()

                @pl.when(has_down)
                def _():
                    z_wait(u, q, 0)
                    grad_tok[chunk(q)] = grad_tok[chunk(q)] + wide(from_z[0, u, chunk(q)])

                @pl.when(has_up)
                def _():
                    z_wait(u, q, 1)
                    grad_tok[chunk(q)] = grad_tok[chunk(q)] + wide(from_z[1, u, chunk(q)])

                part[blk, chunk(q)] = grad_tok[chunk(q)].astype(bf16)
                s_copy(q).start()

    def unit(i, carry):
        u = unit_at(i)
        compute(i, u)

        @pl.when(i > 0)
        def _():
            along(unit_at(i - 1))

        to_across(u)
        return carry

    lax.fori_loop(0, nz, unit, 0)
    along(z)

    dp_recv[me] = dp_send[me]

    def take_prob(d, carry):
        d_copy(me, lax.rem(me + d, 2 * nf)).wait_recv()
        return carry

    lax.fori_loop(1, 2 * nf, take_prob, 0)
    swap_prob = pltpu.make_async_remote_copy(
        src_ref=dp_recv,
        dst_ref=dp_side,
        send_sem=s_send.at[CUT],
        recv_sem=s_recv.at[CUT],
        device_id=side,
        device_id_type=MESH,
    )
    swap_prob.start()
    run_direct()
    for q in range(CUT):
        s_copy(q).wait_recv()
        grad_tok[chunk(q)] = wide(part[me, chunk(q)]) + wide(from_side[chunk(q)])
    swap_prob.wait_recv()
    prob_tok[...] = dp_recv[...] + dp_side[...]

    for cp in store_unit(z):
        cp.wait()
    swap_prob.wait_send()

    def ends(u, carry):
        for q in range(CUT):
            for xx in range(2):
                p_copy(u, xx, q).wait_send()
            x_copy(u, q).wait_send()

            @pl.when(u > z)
            def _():
                z_copy(u, q, 0).wait_send()

            @pl.when(u < z)
            def _():
                z_copy(u, q, 1).wait_send()

        for b in range(4):

            @pl.when(u * 4 + b != me)
            def _():
                d_copy(u * 4 + b).wait_send()

        return carry

    lax.fori_loop(0, nz, ends, 0)
    for q in range(CUT):
        s_copy(q).wait_send()

    drain()


def visiting_order(nz):
    rows = []
    for at in range(nz):
        rows.append(sorted(range(nz), key=lambda u: (-abs(u - at), u if at < nz // 2 else -u)))
    return rows


def expert_pass(hidden_two, marks, hidden_slices, grad_all, w_gate, w_up, w_down, capacity, nf):
    specs = [
        Gather(hidden_two, nf, rep=True, chunks=4),
        Gather(marks, nf, rep=True, chunks=2),
        Gather(hidden_slices, nf, form="a2a", chunks=1),
    ]
    n = len(specs)
    f32, bf16 = jnp.float32, jnp.bfloat16
    tokens, width = hidden_two.shape
    nz = nf // 2
    total = sum(s.chunks for s in specs)
    hidden = w_gate.shape[2]
    rows = 2 * nf * capacity
    unit_rows = 4 * capacity
    slots = 2 * capacity
    any_spec = pl.BlockSpec(memory_space=pl.ANY)
    vmem = pl.BlockSpec(memory_space=pltpu.VMEM)
    dma = pltpu.SemaphoreType.DMA
    outs = [jax.ShapeDtypeStruct(s.out_shape(nf), s.array.dtype) for s in specs] + [
        jax.ShapeDtypeStruct((2 * nf * tokens, width), bf16),
        jax.ShapeDtypeStruct((2, rows, width), bf16),
        jax.ShapeDtypeStruct((2, rows, width), bf16),
        jax.ShapeDtypeStruct((2, rows, hidden), bf16),
        jax.ShapeDtypeStruct((2, rows, hidden), bf16),
        jax.ShapeDtypeStruct((2, rows, hidden), bf16),
        jax.ShapeDtypeStruct((tokens, width), f32),
        jax.ShapeDtypeStruct((2 * nf, 8, tokens), f32),
    ]
    result = pl.pallas_call(
        functools.partial(expert_kernel, nf, capacity, tuple(specs)),
        out_shape=tuple(outs),
        in_specs=[any_spec] * (n + 4),
        out_specs=tuple([any_spec] * (n + 6) + [vmem, vmem]),
        scratch_shapes=[stage_of(s, nf) for s in specs]
        + [dma((2 * nf, total)), dma((5, 2 * nf, total)), dma((2, n))]
        + [
            pltpu.VMEM(w_gate.shape, bf16),
            pltpu.VMEM(w_up.shape, bf16),
            pltpu.VMEM(w_down.shape, bf16),
            pltpu.VMEM((4 * tokens, width), bf16),
            pltpu.VMEM((4 * tokens, width), bf16),
            pltpu.VMEM((2, unit_rows, width), bf16),
            pltpu.VMEM((2, unit_rows, width), bf16),
            pltpu.VMEM((2, unit_rows, width), bf16),
            pltpu.VMEM((4, slots, width), bf16),
            pltpu.VMEM((4, slots, width), bf16),
            pltpu.VMEM((2, unit_rows, hidden), bf16),
            pltpu.VMEM((2, unit_rows, hidden), bf16),
            pltpu.VMEM((2, unit_rows, hidden), bf16),
            pltpu.VMEM((2, unit_rows, 1), f32),
            pltpu.VMEM((4, slots, 1), f32),
            pltpu.VMEM((4, slots, tokens), f32),
            pltpu.VMEM((4 * nf, tokens), f32),
            pltpu.VMEM((4 * nf, tokens), f32),
            pltpu.VMEM((4 * tokens, width), bf16),
            pltpu.VMEM((2 * nf, tokens, width), bf16),
            pltpu.VMEM((nf, tokens, width), bf16),
            pltpu.VMEM((nz, tokens, width), bf16),
            pltpu.VMEM((2, nz, tokens, width), bf16),
            pltpu.VMEM((tokens, width), bf16),
            pltpu.VMEM((2 * nf, 8, tokens), f32),
            pltpu.VMEM((2 * nf, 8, tokens), f32),
            pltpu.VMEM((2 * nf, 8, tokens), f32),
            pltpu.VMEM(specs[1].out_shape(nf), f32),
            dma((3,)),
            dma((3,)),
            dma((6,)),
            dma((nf, CUT)),
            dma((nf, CUT)),
            dma((nz, CUT)),
            dma((nz, CUT)),
            dma((nz, CUT)),
            dma((2, nz, CUT)),
            dma((CUT + 1,)),
            dma((CUT + 1,)),
            dma((2 * nf,)),
            dma((2 * nf,)),
        ],
        compiler_params=pltpu.CompilerParams(
            collective_id=7, has_side_effects=True, vmem_limit_bytes=67043328
        ),
    )(*[s.array for s in specs], grad_all, w_gate, w_up, w_down)
    hidden_all, _, hidden_slice = result[:3]
    return (hidden_all, hidden_slice) + tuple(result[3:])


NT = (((1,), (1,)), ((), ()))
TN = (((0,), (0,)), ((), ()))
NN = (((1,), (0,)), ((), ()))


def backward_kernel(nf, specs, *refs):
    n = len(specs)
    (
        attended,
        dh2_moe,
        grad_prob,
        probs,
        router,
        x_in,
        x_mid,
        gains,
        grad_out,
        wo_hbm,
        wq_hbm,
        wkv_hbm,
        q_raw,
        k_raw,
        q_rot,
        keys,
        values,
        bias,
        lse,
        trig,
        out_part,
        xs_hbm,
        de_hbm,
        act_hbm,
        dg_hbm,
        du_hbm,
    ), refs = refs[:26], refs[26:]
    gathered, grad_in, block_out, refs = refs[:n], refs[n], refs[n + 1], refs[n + 2 :]
    (gate_out, up_out, down_out), refs = refs[:3], refs[3:]
    stage, refs = refs[:n], refs[n:]
    (recv, send, local), refs = refs[:3], refs[3:]
    (
        w_big,
        w_kv,
        dx1,
        dh2,
        d_out,
        d_out_slices,
        d_attn,
        d_query,
        d_rest,
        tail,
        dk_acc,
        dv_acc,
        qk_acc,
        kv_send,
        kv_recv,
        dh1,
        dh1_side,
        qk_side,
        row_sum,
        w_sem,
        kv_sem,
        side_send,
        side_recv,
        sum_own,
        sum_total,
        sum_bufs,
        sum_sems,
    ) = refs[:25] + (refs[25:30], refs[30:41])
    act, dg, du, x_tile, d_tile, gate_tile, up_tile, down_tile, e_sem, t_sem, o_sem = refs[41:]
    f32, bf16 = jnp.float32, jnp.bfloat16
    f, c, t = lax.axis_index("fsdp"), lax.axis_index("ctx"), lax.axis_index("tp")
    partner, side = (f, 1 - c, t), (f, c, 1 - t)
    tokens, width = x_in.shape
    experts = probs.shape[1]
    scale = HEAD_SIZE ** (-0.5)

    barrier = pltpu.get_barrier_semaphore()

    def greet(d, carry):
        pl.semaphore_signal(
            barrier, 1, device_id=(lax.rem(f + d, nf), c, t), device_id_type=MESH
        )
        return carry

    lax.fori_loop(1, nf, greet, 0)
    for dev in (partner, side):
        pl.semaphore_signal(barrier, 1, device_id=dev, device_id_type=MESH)
    pl.semaphore_wait(barrier, nf + 1)

    ins = (attended, d_query, d_rest, tail, d_out_slices)
    start, run, land, start_direct, run_direct, drain, step_of, edge_of, _ = gather_engine(
        nf, specs, ins, gathered, stage, recv, send, local
    )
    early, late = (0,), (1, 2, 3)
    kv_width = dk_acc.shape[1]
    nz = nf // 2
    order = visit_code(nz, f // 2)
    own_loads, to_partner, to_side, to_across, along, finish_sum, drain_sum = token_sum(
        nf, out_part, sum_own, sum_total, sum_bufs, sum_sems
    )
    for cp in own_loads:
        cp.start()
    lax.fori_loop(0, nz, lambda i, carry: to_partner(visit(order, nz, i), carry), 0)
    start((0,))

    def load(src, dst, i):
        return pltpu.make_async_copy(src, dst, w_sem.at[i])

    kept_loads = [
        pltpu.make_async_copy(src, dst, e_sem.at[i])
        for i, (src, dst) in enumerate(((act_hbm, act), (dg_hbm, dg), (du_hbm, du)))
    ]
    span = x_tile.shape[2]
    tiles = width // span
    pieces = act.shape[0] * tiles

    def tile_at(p):
        return p // tiles, pl.ds(pl.multiple_of(lax.rem(p, tiles) * span, span), span)

    def tile_loads(p):
        j, cols = tile_at(p)
        slot = lax.rem(p, 2)
        return (
            pltpu.make_async_copy(xs_hbm.at[j, :, cols], x_tile.at[slot], t_sem.at[0, slot]),
            pltpu.make_async_copy(de_hbm.at[j, :, cols], d_tile.at[slot], t_sem.at[1, slot]),
        )

    def tile_stores(p):
        j, cols = tile_at(p)
        slot = lax.rem(p, 2)
        return (
            pltpu.make_async_copy(gate_tile.at[slot], gate_out.at[j, cols], o_sem.at[0, slot]),
            pltpu.make_async_copy(up_tile.at[slot], up_out.at[j, cols], o_sem.at[1, slot]),
            pltpu.make_async_copy(down_tile.at[slot], down_out.at[j, :, cols], o_sem.at[2, slot]),
        )

    def piece(p, carry):
        j, _ = tile_at(p)
        slot = lax.rem(p, 2)
        for cp in tile_loads(p):
            cp.wait()

        @pl.when(p + 1 < pieces)
        def _():
            for cp in tile_loads(p + 1):
                cp.start()

        @pl.when(p >= 2)
        def _():
            for cp in tile_stores(p - 2):
                cp.wait()

        rows = x_tile[slot]
        gate_tile[slot] = lax.dot_general(rows, dg[j], TN, preferred_element_type=f32).astype(bf16)
        up_tile[slot] = lax.dot_general(rows, du[j], TN, preferred_element_type=f32).astype(bf16)
        down_tile[slot] = lax.dot_general(
            act[j], d_tile[slot], TN, preferred_element_type=f32
        ).astype(bf16)
        for cp in tile_stores(p):
            cp.start()
        return carry

    load(wo_hbm, w_big, 0).start()
    for cp in kept_loads:
        cp.start()
    for cp in tile_loads(0):
        cp.start()
    load(wkv_hbm, w_kv, 1).start()

    d_rest[...] = jnp.zeros_like(d_rest)
    pr = probs[...]
    gp = grad_prob[...]
    dl = (pr * (gp - jnp.sum(pr * gp, axis=1, keepdims=True))).astype(bf16)
    d_rest[:, 2 * kv_width : 2 * kv_width + experts] = dl
    tile = 512
    for k in range(width // tile):
        cols = slice(k * tile, (k + 1) * tile)
        dh2[:, cols] = dh2_moe[:, cols] + lax.dot_general(
            dl, router[:, cols], NN, preferred_element_type=f32
        )
    gain_one, gain_two = gains[0:1, :], gains[1:2, :]
    gain_query, gain_key = gains[2:3, :HEAD_SIZE], gains[2:3, HEAD_SIZE : 2 * HEAD_SIZE]
    row_sum[...] = jnp.zeros_like(row_sum)
    part_rows = 16

    def norm_two(i, carry):
        rows = pl.ds(pl.multiple_of(i * part_rows, part_rows), part_rows)
        x1 = x_mid[rows]
        r2 = lax.rsqrt(jnp.mean(x1 * x1, axis=1, keepdims=True) + eps_norm)
        n2 = x1 * r2
        g = dh2[rows]
        row_sum[1:2, :] += jnp.sum(g * n2, axis=0, keepdims=True)
        scaled = g * gain_two
        mean = jnp.mean(scaled * n2, axis=1, keepdims=True)
        out = grad_out[rows].astype(f32) + r2 * (scaled - n2 * mean)
        dx1[rows] = out
        d_out[rows] = out.astype(bf16)
        return carry

    lax.fori_loop(0, tokens // part_rows, norm_two, 0)
    for cp in own_loads:
        cp.wait()
    lax.fori_loop(0, nz, lambda i, carry: to_side(visit(order, nz, i), carry), 0)
    shard = width // nf
    for k in range(nf):
        d_out_slices[k * tokens : (k + 1) * tokens, :] = d_out[:, k * shard : (k + 1) * shard]

    load(wo_hbm, w_big, 0).wait()
    heads_width = d_attn.shape[1]
    tile = 256
    for k in range(heads_width // tile):
        cols = slice(k * tile, (k + 1) * tile)
        d_attn[:, cols] = lax.dot_general(
            d_out[...], w_big[cols, :], NT, preferred_element_type=f32
        ).astype(bf16)
    load(wq_hbm, w_big, 0).start()
    step_of(1, early)
    to_across(visit(order, nz, 0))
    dk_acc[...] = jnp.zeros_like(dk_acc)
    dv_acc[...] = jnp.zeros_like(dv_acc)
    qk_acc[...] = jnp.zeros_like(qk_acc)
    group = QUERY_HEADS // KEY_VALUE_HEADS

    def unrope(g):
        return g * trig[0] + pltpu.roll(g, HEAD_SIZE // 2, 1) * trig[1]

    def norm_back(g, raw, gain):
        inv = lax.rsqrt(jnp.mean(raw * raw, axis=1, keepdims=True) + eps_norm)
        hat = raw * inv
        scaled = g * gain
        mean = jnp.mean(scaled * hat, axis=1, keepdims=True)
        return jnp.sum(g * hat, axis=0, keepdims=True), inv * (scaled - hat * mean)

    def head(h, carry):
        cols = pl.ds(pl.multiple_of(h * HEAD_SIZE, HEAD_SIZE), HEAD_SIZE)
        kv_cols = pl.ds(pl.multiple_of((h // group) * HEAD_SIZE, HEAD_SIZE), HEAD_SIZE)
        q, key, value, da = q_rot[:, cols], keys[:, kv_cols], values[:, kv_cols], d_attn[:, cols]
        s = lax.dot_general(q, key, NT, preferred_element_type=f32) * scale + bias[...]
        prob = jnp.exp(s - lse[h])
        dp = lax.dot_general(da, value, NT, preferred_element_type=f32)
        delta = jnp.sum(prob * dp, axis=1, keepdims=True)
        ds = (prob * (dp - delta) * scale).astype(bf16)
        dk_acc[:, kv_cols] += lax.dot_general(ds, q, TN, preferred_element_type=f32)
        dv_acc[:, kv_cols] += lax.dot_general(
            prob.astype(bf16), da, TN, preferred_element_type=f32
        )
        dq = unrope(jnp.dot(ds, key, preferred_element_type=f32))
        gain_grad, dq = norm_back(dq, q_raw[:, cols], gain_query)
        qk_acc[0:1, :] += gain_grad
        d_query[:, cols] = dq.astype(bf16)
        return carry

    heads = heads_width // HEAD_SIZE
    lax.fori_loop(0, heads // 2, head, 0)
    to_across(visit(order, nz, 1))
    step_of(2, early)
    lax.fori_loop(heads // 2, heads, head, 0)

    theirs = pl.ds(pl.multiple_of((1 - c) * tokens, tokens), tokens)
    mine = pl.ds(pl.multiple_of(c * tokens, tokens), tokens)
    kv_send[:, :kv_width] = dk_acc[theirs].astype(bf16)
    kv_send[:, kv_width:] = dv_acc[theirs].astype(bf16)
    swap_kv = pltpu.make_async_remote_copy(
        src_ref=kv_send,
        dst_ref=kv_recv,
        send_sem=kv_sem.at[0],
        recv_sem=kv_sem.at[1],
        device_id=partner,
        device_id_type=MESH,
    )
    swap_kv.start()
    start((1,))
    start_direct()
    swap_kv.wait()
    for kv in range(kv_width // HEAD_SIZE):
        cols = slice(kv * HEAD_SIZE, (kv + 1) * HEAD_SIZE)
        g = dk_acc[mine, cols] + kv_recv[:, cols].astype(f32)
        gain_grad, dk = norm_back(unrope(g), k_raw[:, cols], gain_key)
        qk_acc[1:2, :] += gain_grad
        d_rest[:, cols] = dk.astype(bf16)
    d_rest[:, kv_width : 2 * kv_width] = (dv_acc[mine] + kv_recv[:, kv_width:].astype(f32)).astype(bf16)
    start((2,))
    to_across(visit(order, nz, 2))
    along(visit(order, nz, 0))

    def to_side(src, dst, i):
        return pltpu.make_async_remote_copy(
            src_ref=src,
            dst_ref=dst,
            send_sem=side_send.at[i],
            recv_sem=side_recv.at[i],
            device_id=side,
            device_id_type=MESH,
        )

    swap_qk = to_side(qk_acc, qk_side, 4)
    swap_qk.start()
    load(wq_hbm, w_big, 0).wait()
    load(wkv_hbm, w_kv, 1).wait()
    quarter = width // 4

    def dh1_copy(i):
        cols = pl.ds(i * quarter, quarter)
        return to_side(dh1.at[:, cols], dh1_side.at[:, cols], i)

    for k in range(width // tile):
        rows = slice(k * tile, (k + 1) * tile)
        total = lax.dot_general(d_query[...], w_big[rows, :], NT, preferred_element_type=f32)
        total = total + lax.dot_general(
            d_rest[:, : 2 * kv_width], w_kv[rows, :], NT, preferred_element_type=f32
        )
        dh1[:, rows] = total.astype(bf16)
        if (k + 1) * tile % quarter == 0:
            dh1_copy((k + 1) * tile // quarter - 1).start()
    to_across(visit(order, nz, 3))
    step_of(3, early)
    along(visit(order, nz, 1))
    for i in range(4):
        dh1_copy(i).wait_recv()
    swap_qk.wait_recv()

    def norm_one(i, carry):
        rows = pl.ds(pl.multiple_of(i * part_rows, part_rows), part_rows)
        x0 = x_in[rows].astype(f32)
        r1 = lax.rsqrt(jnp.mean(x0 * x0, axis=1, keepdims=True) + eps_norm)
        n1 = x0 * r1
        g = dh1[rows].astype(f32) + dh1_side[rows].astype(f32)
        row_sum[0:1, :] += jnp.sum(g * n1, axis=0, keepdims=True)
        scaled = g * gain_one
        mean = jnp.mean(scaled * n1, axis=1, keepdims=True)
        grad_in[rows] = dx1[rows] + r1 * (scaled - n1 * mean)
        return carry

    lax.fori_loop(0, tokens // part_rows, norm_one, 0)
    lanes = width // 128
    tail[...] = jnp.zeros_like(tail)
    for which in range(2):
        for k in range(lanes):
            row = which * lanes + k
            tail[row : row + 1, :] = row_sum[which : which + 1, k * 128 : (k + 1) * 128]
    tail[2 * lanes : 2 * lanes + 2, :] = qk_acc[0:2, :] + qk_side[0:2, :]
    start((3,))
    for cp in kept_loads:
        cp.wait()

    def stage_at(s, carry):
        lax.fori_loop(s * (pieces // nz), (s + 1) * (pieces // nz), piece, 0)

        @pl.when(s + 1 < nz)
        def _():
            step_of(s + 1, late)

        @pl.when(s == 0)
        def _():
            along(visit(order, nz, 2))
            edge_of(early)

        @pl.when(s == 1)
        def _():
            along(f // 2)

        return carry

    lax.fori_loop(0, nz, stage_at, 0)
    edge_of(late)
    run_direct()
    land()

    def put_out(rows, cols, value):
        block_out[rows, cols] = (x_mid[rows, cols] + value).astype(bf16)

    finish_sum(put_out)
    for p in (pieces - 2, pieces - 1):
        for cp in tile_stores(p):
            cp.wait()
    drain()
    drain_sum()
    for i in range(4):
        dh1_copy(i).wait_send()
    swap_qk.wait_send()


def visit_code(nz, z):
    order = 0
    for at, seq in enumerate(visiting_order(nz)):
        code = sum(u * nz**i for i, u in enumerate(seq))
        order = order + code * (z == at).astype(jnp.int32)
    return order


def visit(code, nz, i):
    for k in range(nz):
        code = jnp.where(i > k, code // nz, code)
    return lax.rem(code, nz)


SUM_CUT = 2


def token_sum(nf, partial, own, total_ref, bufs, sems):
    from_partner, from_side, from_across, from_z, last_half = bufs
    (
        load_sem,
        p_send,
        p_recv,
        y_send,
        y_recv,
        x_send,
        x_recv,
        z_send,
        z_recv,
        s_send,
        s_recv,
    ) = sems
    nz = nf // 2
    f, c, t = lax.axis_index("fsdp"), lax.axis_index("ctx"), lax.axis_index("tp")
    z, x = f // 2, lax.rem(f, 2)
    has_up, has_down = z + 1 < nz, z > 0
    up, down = (f + 2, c, t), (f - 2, c, t)
    across_dev, partner, side = (z * 2 + 1 - x, c, t), (f, 1 - c, t), (f, c, 1 - t)
    tokens, half = total_ref.shape
    rows = tokens // SUM_CUT
    bf16 = jnp.bfloat16
    kept = pl.ds(pl.multiple_of(t * half, half), half)
    given = pl.ds(pl.multiple_of((1 - t) * half, half), half)

    def chunk(q):
        return pl.ds(pl.multiple_of(q * rows, rows), rows)

    def remote(src, dst, send, recv, dev):
        return pltpu.make_async_remote_copy(
            src_ref=src,
            dst_ref=dst,
            send_sem=send,
            recv_sem=recv,
            device_id=dev,
            device_id_type=MESH,
        )

    own_loads = [
        pltpu.make_async_copy(
            partial.at[pl.ds((2 * b + c) * tokens, tokens)], own.at[b], load_sem.at[b]
        )
        for b in range(nf)
    ]

    def p_copy(b, q):
        return remote(
            partial.at[pl.ds((2 * b + 1 - c) * tokens + q * rows, rows)],
            from_partner.at[b, chunk(q)],
            p_send.at[b, q],
            p_recv.at[b, q],
            partner,
        )

    def y_copy(b, q):
        return remote(
            own.at[b, chunk(q), given],
            from_side.at[b, chunk(q)],
            y_send.at[b, q],
            y_recv.at[b, q],
            side,
        )

    def x_copy(u, q):
        return remote(
            own.at[u * 2 + 1 - x, chunk(q), kept],
            from_across.at[u, chunk(q)],
            x_send.at[u, q],
            x_recv.at[u, q],
            across_dev,
        )

    def z_copy(u, q, way, dev):
        return remote(
            own.at[u * 2 + x, chunk(q), kept],
            from_z.at[way, u, chunk(q)],
            z_send.at[u, q],
            z_recv.at[way, u, q],
            dev,
        )

    def s_copy(q):
        return remote(
            own.at[f, chunk(q), kept], last_half.at[chunk(q)], s_send.at[q], s_recv.at[q], side
        )

    def wide(value):
        return value.astype(jnp.float32)

    def to_partner(u, carry):
        for xx in range(2):
            for q in range(SUM_CUT):
                p_copy(u * 2 + xx, q).start()
        return carry

    def to_side(u, carry):
        for xx in range(2):
            b = u * 2 + xx

            @pl.loop(0, SUM_CUT)
            def _(q, b=b):
                p_copy(b, q).wait_recv()
                own[b, chunk(q)] = (
                    wide(own[b, chunk(q)]) + wide(from_partner[b, chunk(q)])
                ).astype(bf16)
                y_copy(b, q).start()
        return carry

    def to_across(u):
        b = u * 2 + 1 - x

        @pl.loop(0, SUM_CUT)
        def _(q):
            y_copy(b, q).wait_recv()
            own[b, chunk(q), kept] = (
                wide(own[b, chunk(q), kept]) + wide(from_side[b, chunk(q)])
            ).astype(bf16)
            x_copy(u, q).start()

    def along(u):
        b = u * 2 + x

        @pl.loop(0, SUM_CUT)
        def _(q):
            y_copy(b, q).wait_recv()
            x_copy(u, q).wait_recv()
            total_ref[chunk(q)] = (
                wide(own[b, chunk(q), kept])
                + wide(from_side[b, chunk(q)])
                + wide(from_across[u, chunk(q)])
            )

            @pl.when((u >= z) & has_down)
            def _():
                z_copy(u, q, 0, partner).wait_recv()
                total_ref[chunk(q)] += wide(from_z[0, u, chunk(q)])

            @pl.when((u <= z) & has_up)
            def _():
                z_copy(u, q, 1, partner).wait_recv()
                total_ref[chunk(q)] += wide(from_z[1, u, chunk(q)])

            own[b, chunk(q), kept] = total_ref[chunk(q)].astype(bf16)

            @pl.when(u > z)
            def _():
                z_copy(u, q, 0, up).start()

            @pl.when(u < z)
            def _():
                z_copy(u, q, 1, down).start()

            @pl.when(u == z)
            def _():
                s_copy(q).start()

    def finish_sum(put):
        for q in range(SUM_CUT):
            put(chunk(q), kept, wide(own[f, chunk(q), kept]))
            s_copy(q).wait_recv()
            put(chunk(q), given, wide(last_half[chunk(q)]))

    def drain_sum():
        def ends(u, carry):
            for q in range(SUM_CUT):
                for xx in range(2):
                    p_copy(u * 2 + xx, q).wait_send()
                    y_copy(u * 2 + xx, q).wait_send()
                x_copy(u, q).wait_send()

                @pl.when(u != z)
                def _():
                    z_copy(u, q, 0, partner).wait_send()

            return carry

        lax.fori_loop(0, nz, ends, 0)
        for q in range(SUM_CUT):
            s_copy(q).wait_send()

    return own_loads, to_partner, to_side, to_across, along, finish_sum, drain_sum


def backward_pass(nf, arrays, attended, shapes):
    f32, bf16 = jnp.float32, jnp.bfloat16
    tokens, width, heads_width, kv_width, keys = shapes
    tail_rows = -(-(2 * width // 128 + 2) // 8) * 8
    shape = jax.ShapeDtypeStruct
    specs = [
        Gather(attended, nf, chunks=2),
        Gather(shape((tokens, heads_width), bf16), nf, chunks=2),
        Gather(shape((tokens, 2 * kv_width + 128), bf16), nf, chunks=1),
        Gather(shape((tail_rows, 128), f32), nf, chunks=1),
        Gather(shape((nf * tokens, width // nf), bf16), nf, form="a2a", chunks=1),
    ]
    n = len(specs)
    experts, rows, hidden = arrays[-3].shape
    gate_shape, down_shape = (experts, width, hidden), (experts, hidden, width)
    span = 256
    total = sum(s.chunks for s in specs)
    any_spec = pl.BlockSpec(memory_space=pl.ANY)
    vmem = pl.BlockSpec(memory_space=pltpu.VMEM)
    dma = pltpu.SemaphoreType.DMA
    in_any = {0, 9, 10, 11, 20, 21, 22, 23, 24, 25}
    nz = nf // 2
    return pl.pallas_call(
        functools.partial(backward_kernel, nf, tuple(specs)),
        out_shape=tuple(shape(s.out_shape(nf), s.array.dtype) for s in specs)
        + (shape((tokens, width), f32), shape((tokens, width), bf16))
        + tuple(shape(s, bf16) for s in (gate_shape, gate_shape, down_shape)),
        in_specs=[any_spec if i in in_any else vmem for i in range(26)],
        out_specs=tuple([any_spec] * n + [vmem, vmem] + [any_spec] * 3),
        scratch_shapes=[stage_of(s, nf) for s in specs]
        + [dma((2 * nf, total)), dma((5, 2 * nf, total)), dma((2, n))]
        + [
            pltpu.VMEM((width, max(width, heads_width)), bf16),
            pltpu.VMEM((width, 2 * kv_width), bf16),
            pltpu.VMEM((tokens, width), f32),
            pltpu.VMEM((tokens, width), f32),
            pltpu.VMEM((tokens, width), bf16),
            pltpu.VMEM((nf * tokens, width // nf), bf16),
            pltpu.VMEM((tokens, heads_width), bf16),
            pltpu.VMEM((tokens, heads_width), bf16),
            pltpu.VMEM((tokens, 2 * kv_width + 128), bf16),
            pltpu.VMEM((tail_rows, 128), f32),
            pltpu.VMEM((keys, kv_width), f32),
            pltpu.VMEM((keys, kv_width), f32),
            pltpu.VMEM((8, 128), f32),
            pltpu.VMEM((tokens, 2 * kv_width), bf16),
            pltpu.VMEM((tokens, 2 * kv_width), bf16),
            pltpu.VMEM((tokens, width), bf16),
            pltpu.VMEM((tokens, width), bf16),
            pltpu.VMEM((8, 128), f32),
            pltpu.VMEM((2, width), f32),
            dma((2,)),
            dma((2,)),
            dma((5,)),
            dma((5,)),
            pltpu.VMEM((nf, tokens, width), bf16),
            pltpu.VMEM((tokens, width // 2), f32),
            pltpu.VMEM((nf, tokens, width), bf16),
            pltpu.VMEM((nf, tokens, width // 2), bf16),
            pltpu.VMEM((nz, tokens, width // 2), bf16),
            pltpu.VMEM((2, nz, tokens, width // 2), bf16),
            pltpu.VMEM((tokens, width // 2), bf16),
            dma((nf,)),
            dma((nf, SUM_CUT)),
            dma((nf, SUM_CUT)),
            dma((nf, SUM_CUT)),
            dma((nf, SUM_CUT)),
            dma((nz, SUM_CUT)),
            dma((nz, SUM_CUT)),
            dma((nz, SUM_CUT)),
            dma((2, nz, SUM_CUT)),
            dma((SUM_CUT,)),
            dma((SUM_CUT,)),
            pltpu.VMEM((experts, rows, hidden), bf16),
            pltpu.VMEM((experts, rows, hidden), bf16),
            pltpu.VMEM((experts, rows, hidden), bf16),
            pltpu.VMEM((2, rows, span), bf16),
            pltpu.VMEM((2, rows, span), bf16),
            pltpu.VMEM((2, span, hidden), bf16),
            pltpu.VMEM((2, span, hidden), bf16),
            pltpu.VMEM((2, hidden, span), bf16),
            dma((3,)),
            dma((2, 2)),
            dma((3, 2)),
        ],
        compiler_params=pltpu.CompilerParams(
            collective_id=8, has_side_effects=True, vmem_limit_bytes=67043328
        ),
    )(attended, *arrays)


def forward_kernel(nf, specs, *refs):
    n = len(specs)
    ins, refs = refs[:n], refs[n:]
    (x_in, segments, routed, trig), refs = refs[:4], refs[4:]
    gathered, refs = refs[:n], refs[n:]
    (
        hidden,
        hidden_slices,
        marks,
        probs,
        x_mid,
        attended,
        q_raw,
        k_raw,
        q_rot,
        keys,
        values,
        bias,
        lse,
        gains,
        router,
    ), refs = refs[:15], refs[15:]
    stage, refs = refs[:n], refs[n:]
    (recv, send, local), refs = refs[:3], refs[3:]
    (
        w_big,
        w_kv,
        small,
        hidden_one,
        kv_all,
        part,
        part_side,
        square,
        w_sem,
        kv_sem,
        side_send,
        side_recv,
    ) = refs
    f32, bf16 = jnp.float32, jnp.bfloat16
    nz = nf // 2
    f, c, t = lax.axis_index("fsdp"), lax.axis_index("ctx"), lax.axis_index("tp")
    z, x = f // 2, lax.rem(f, 2)
    partner, side = (f, 1 - c, t), (f, c, 1 - t)
    has_up, has_down = z + 1 < nz, z > 0
    tokens, width = x_in.shape
    experts = routed.shape[1]
    heads_width = q_raw.shape[1]
    kv_width = k_raw.shape[1]
    scale = HEAD_SIZE ** (-0.5)
    barrier = pltpu.get_barrier_semaphore()

    def greet(dev):
        pl.semaphore_signal(barrier, 1, device_id=dev, device_id_type=MESH)

    for dev in (partner, side, (z * 2 + 1 - x, c, t)):
        greet(dev)

    @pl.when(has_up)
    def _():
        greet((f + 2, c, t))

    @pl.when(has_down)
    def _():
        greet((f - 2, c, t))

    pl.semaphore_wait(barrier, 3 + has_up.astype(jnp.int32) + has_down.astype(jnp.int32))
    start, _, _, _, _, drain, step_of, edge_of, land_of = gather_engine(
        nf, specs, ins, gathered, stage, recv, send, local
    )
    first, second, third = (0, 1, 2), (3,), (4,)
    start(first)

    def first_step(k, carry):
        step_of(k, first)
        return carry

    lax.fori_loop(1, nz, first_step, 0)
    start(second)
    edge_of(first)
    land_of(first)

    def load(src, dst, i):
        return pltpu.make_async_copy(src, dst, w_sem.at[i])

    small_load = load(gathered[0], small, 2)
    small_load.start()
    load(gathered[2], w_kv, 1).start()
    load(gathered[1], w_big, 0).start()
    small_load.wait()

    size = specs[0].rows
    halves = width // nf // 128
    qk_sum = [jnp.zeros((1, 128), f32), jnp.zeros((1, 128), f32)]
    for k in range(nf):
        base = 2 * k * size
        for h in range(halves):
            cols = slice((k * halves + h) * 128, (k * halves + h + 1) * 128)
            router[:, cols] = small[base + h * experts : base + (h + 1) * experts, :]
            at = base + halves * experts
            for g in range(2):
                row = at + g * halves + h
                gains[g : g + 1, cols] = small[row : row + 1, :].astype(f32)
        at = base + halves * experts + 2 * halves
        for h in range(2):
            qk_sum[h] = qk_sum[h] + small[at + h : at + h + 1, :].astype(f32)
    gains[2:3, :] = jnp.zeros((1, width), f32)
    for h in range(2):
        gains[2:3, h * 128 : (h + 1) * 128] = qk_sum[h]
    gain_one, gain_two = gains[0:1, :], gains[1:2, :]
    gain_query, gain_key = qk_sum
    part_rows = 16

    def norm_one(i, carry):
        rows = pl.ds(pl.multiple_of(i * part_rows, part_rows), part_rows)
        x0 = x_in[rows].astype(f32)
        r1 = lax.rsqrt(jnp.mean(x0 * x0, axis=1, keepdims=True) + eps_norm)
        hidden_one[rows] = (x0 * r1 * gain_one).astype(bf16)
        return carry

    lax.fori_loop(0, tokens // part_rows, norm_one, 0)
    shard = width // nf
    for k in range(nf):
        hidden_slices[k * tokens : (k + 1) * tokens, :] = hidden_one[:, k * shard : (k + 1) * shard]

    def norm_rope(raw, gain):
        inv = lax.rsqrt(jnp.mean(raw * raw, axis=1, keepdims=True) + eps_norm)
        normed = raw * inv * gain
        turned = normed * trig[0] - pltpu.roll(normed, HEAD_SIZE // 2, 1) * trig[1]
        return turned.astype(bf16)

    load(gathered[2], w_kv, 1).wait()
    mine = pl.ds(pl.multiple_of(c * tokens, tokens), tokens)
    k_raw[...] = jnp.dot(
        hidden_one[...], w_kv[:, :kv_width], preferred_element_type=f32
    )
    kv_all[mine, kv_width : 2 * kv_width] = jnp.dot(
        hidden_one[...], w_kv[:, kv_width:], preferred_element_type=f32
    ).astype(bf16)
    for kv in range(kv_width // HEAD_SIZE):
        cols = slice(kv * HEAD_SIZE, (kv + 1) * HEAD_SIZE)
        kv_all[mine, cols] = norm_rope(k_raw[:, cols], gain_key)
    kv_all[mine, 2 * kv_width :] = segments[...]
    swap_kv = pltpu.make_async_remote_copy(
        src_ref=kv_all.at[mine],
        dst_ref=kv_all.at[mine],
        send_sem=kv_sem.at[0],
        recv_sem=kv_sem.at[1],
        device_id=partner,
        device_id_type=MESH,
    )
    swap_kv.start()
    step_of(1, second)
    load(gathered[1], w_big, 0).wait()
    tile = 256
    for k in range(heads_width // tile):
        cols = slice(k * tile, (k + 1) * tile)
        q_raw[:, cols] = jnp.dot(hidden_one[...], w_big[:, cols], preferred_element_type=f32)
    swap_kv.wait()
    keys[...] = kv_all[:, :kv_width]
    values[...] = kv_all[:, kv_width : 2 * kv_width]
    span = kv_all.shape[0]
    theirs = jnp.transpose(kv_all[:, 2 * kv_width :].astype(f32))
    own = segments[...].astype(f32)
    query_at = c * tokens + lax.broadcasted_iota(jnp.int32, (tokens, 128), 0)
    for h in range(span // 128):
        cols = slice(h * 128, (h + 1) * 128)
        key_at = h * 128 + lax.broadcasted_iota(jnp.int32, (tokens, 128), 1)
        allowed = (key_at <= query_at) & (theirs[:, cols] == own)
        bias[:, cols] = jnp.where(allowed, 0.0, -jnp.inf)
    step_of(2, second)
    group = QUERY_HEADS // KEY_VALUE_HEADS

    def head(h, carry):
        cols = pl.ds(pl.multiple_of(h * HEAD_SIZE, HEAD_SIZE), HEAD_SIZE)
        kv_cols = pl.ds(pl.multiple_of((h // group) * HEAD_SIZE, HEAD_SIZE), HEAD_SIZE)
        q = norm_rope(q_raw[:, cols], gain_query)
        q_rot[:, cols] = q
        s = lax.dot_general(q, keys[:, kv_cols], NT, preferred_element_type=f32) * scale
        s = s + bias[...]
        top = jnp.max(s, axis=1, keepdims=True)
        total = top + jnp.log(jnp.sum(jnp.exp(s - top), axis=1, keepdims=True))
        lse[h] = total
        prob = jnp.exp(s - total).astype(bf16)
        attended[:, cols] = jnp.dot(
            prob, values[:, kv_cols], preferred_element_type=f32
        ).astype(bf16)
        return carry

    heads = heads_width // HEAD_SIZE
    lax.fori_loop(0, heads // 2, head, 0)
    step_of(3, second)
    start(third)
    lax.fori_loop(heads // 2, heads, head, 0)
    edge_of(second)
    land_of(second)
    load(gathered[3], w_big, 0).start()
    step_of(1, third)
    load(gathered[3], w_big, 0).wait()
    quarter = width // 4

    def side_copy(i):
        cols = pl.ds(i * quarter, quarter)
        return pltpu.make_async_remote_copy(
            src_ref=part.at[:, cols],
            dst_ref=part_side.at[:, cols],
            send_sem=side_send.at[i],
            recv_sem=side_recv.at[i],
            device_id=side,
            device_id_type=MESH,
        )

    for k in range(width // tile):
        cols = slice(k * tile, (k + 1) * tile)
        part[:, cols] = jnp.dot(
            attended[...], w_big[:, cols], preferred_element_type=f32
        ).astype(bf16)
        if (k + 1) * tile % quarter == 0:
            side_copy((k + 1) * tile // quarter - 1).start()
    step_of(2, third)
    for i in range(4):
        side_copy(i).wait_recv()

    def norm_two(i, carry):
        rows = pl.ds(pl.multiple_of(i * part_rows, part_rows), part_rows)
        x1 = x_in[rows].astype(f32) + (part[rows].astype(f32) + part_side[rows].astype(f32))
        x_mid[rows] = x1
        r2 = lax.rsqrt(jnp.mean(x1 * x1, axis=1, keepdims=True) + eps_norm)
        hidden[rows] = (x1 * r2 * gain_two).astype(bf16)
        return carry

    lax.fori_loop(0, tokens // part_rows, norm_two, 0)
    logits = lax.dot_general(hidden[...], router[...], NT, preferred_element_type=f32)
    on = routed[...] > 0.0
    kept = jnp.where(on, logits, -jnp.inf)
    raised = jnp.where(on, jnp.exp(kept - jnp.max(kept, axis=1, keepdims=True)), 0.0)
    shares = raised / jnp.sum(raised, axis=1, keepdims=True)
    probs[...] = shares
    square[...] = jnp.zeros_like(square)
    square[:, :experts] = jnp.where(on, shares, -1.0)
    marks[...] = jnp.transpose(square[...])[:experts, :]
    step_of(3, third)
    edge_of(third)
    land_of(third)
    drain()
    for i in range(4):
        side_copy(i).wait_send()


def forward_pass(nf, arrays, operands, shapes):
    f32, bf16 = jnp.float32, jnp.bfloat16
    small, w_query, kv_projection, w_out, grad_out = arrays
    tokens, width, heads_width, kv_width, experts = shapes
    specs = [
        Gather(small, nf, chunks=1),
        Gather(w_query, nf, half=True, chunks=2),
        Gather(kv_projection, nf, half=True, chunks=1),
        Gather(w_out, nf, form="col", half=True, chunks=2),
        Gather(grad_out, nf, chunks=2),
    ]
    n = len(specs)
    total = sum(s.chunks for s in specs)
    any_spec = pl.BlockSpec(memory_space=pl.ANY)
    vmem = pl.BlockSpec(memory_space=pltpu.VMEM)
    dma = pltpu.SemaphoreType.DMA
    shape = jax.ShapeDtypeStruct
    span = 2 * tokens
    made = [
        shape((tokens, width), bf16),
        shape((nf * tokens, width // nf), bf16),
        shape((experts, tokens), f32),
        shape((tokens, experts), f32),
        shape((tokens, width), f32),
        shape((tokens, heads_width), bf16),
        shape((tokens, heads_width), f32),
        shape((tokens, kv_width), f32),
        shape((tokens, heads_width), bf16),
        shape((span, kv_width), bf16),
        shape((span, kv_width), bf16),
        shape((tokens, span), f32),
        shape((heads_width // HEAD_SIZE, tokens, 1), f32),
        shape((3, width), f32),
        shape((experts, width), bf16),
    ]
    return pl.pallas_call(
        functools.partial(forward_kernel, nf, tuple(specs)),
        out_shape=tuple(shape(s.out_shape(nf), s.array.dtype) for s in specs) + tuple(made),
        in_specs=[any_spec] * n + [vmem] * 4,
        out_specs=tuple([any_spec] * n + [vmem] * len(made)),
        scratch_shapes=[stage_of(s, nf) for s in specs]
        + [dma((2 * nf, total)), dma((5, 2 * nf, total)), dma((2, n))]
        + [
            pltpu.VMEM((width, max(width, heads_width)), bf16),
            pltpu.VMEM((width, 2 * kv_width), bf16),
            pltpu.VMEM(specs[0].out_shape(nf), bf16),
            pltpu.VMEM((tokens, width), bf16),
            pltpu.VMEM((span, 2 * kv_width + 128), bf16),
            pltpu.VMEM((tokens, width), bf16),
            pltpu.VMEM((tokens, width), bf16),
            pltpu.VMEM((tokens, 128), f32),
            dma((3,)),
            dma((2,)),
            dma((4,)),
            dma((4,)),
        ],
        compiler_params=pltpu.CompilerParams(
            collective_id=9, has_side_effects=True, vmem_limit_bytes=67043328
        ),
    )(*arrays, *operands)


def norm_forward(values, gain_row):
    inverse = lax.rsqrt(jnp.mean(values * values, axis=-1, keepdims=True) + eps_norm)
    normed = values * inverse
    return (normed * gain_row, normed, inverse)


def rms_norm_gradient(grad_scaled, normed, inverse, gain_row):
    grad_normed = grad_scaled * gain_row
    inner_mean = jnp.mean(grad_normed * normed, axis=-1, keepdims=True)
    return inverse * (grad_normed - normed * inner_mean)


def rope_tables(positions):
    half_dim = HEAD_SIZE // 2
    frequencies = rope_base ** (-(jnp.arange(half_dim, dtype=jnp.float32) * 2.0) / HEAD_SIZE)
    angles = positions.astype(jnp.float32)[:, None] * frequencies[None, :]
    return (jnp.cos(angles)[:, None, :], jnp.sin(angles)[:, None, :])


def rotate(values, cosine_table, sine_values):
    half_dim = values.shape[-1] // 2
    first_half = values[..., :half_dim]
    second_half = values[..., half_dim:]
    return jnp.concatenate(
        [
            first_half * cosine_table - second_half * sine_values,
            second_half * cosine_table + first_half * sine_values,
        ],
        axis=-1,
    )


def inverse_rotation(grad_in_rot, cosine_table, sine_values):
    half_dim = grad_in_rot.shape[-1] // 2
    first_half = grad_in_rot[..., :half_dim]
    second_half = grad_in_rot[..., half_dim:]
    return jnp.concatenate(
        [
            first_half * cosine_table + second_half * sine_values,
            second_half * cosine_table - first_half * sine_values,
        ],
        axis=-1,
    )


def masked_scores(query_rotated, key_rotated, allowed):
    scores = jnp.einsum(
        "qkgd,skd->kgqs", query_rotated, key_rotated, preferred_element_type=jnp.float32
    ) * HEAD_SIZE ** (-0.5)
    return jnp.where(allowed[None, None], scores, -jnp.inf)


def swap(value, axis_name):
    return lax.ppermute(value, axis_name, [(0, 1), (1, 0)])


def sum_over_tp(value):
    mine = value.astype(jnp.bfloat16)
    return mine.astype(jnp.float32) + swap(mine, "tp").astype(jnp.float32)


def block_sum(partial, nf):
    return lax.psum_scatter(partial, ("fsdp", "ctx"), scatter_dimension=0, tiled=True)


def by_shard(rows, nf):
    count, width = rows.shape
    return rows.reshape(count, nf, width // nf).transpose(1, 0, 2).reshape(nf * count, width // nf)


def on_device(
    hidden_in,
    segment_ids,
    routes,
    attn_gain,
    qk_gains,
    w_query,
    key_projection,
    value_projection,
    w_out,
    ffn_gain,
    w_router,
    w_gate,
    w_up,
    w_down,
    grad_out,
):
    tokens_dev, width_dim = hidden_in.shape
    nf = lax.axis_size("fsdp")
    devices = nf * lax.axis_size("ctx")
    local_experts = w_gate.shape[0]
    experts = local_experts * devices
    capacity = max(2, 2 * tokens_dev * TOPK // experts)
    query_group_width = QUERY_HEADS // KEY_VALUE_HEADS
    shard_width = attn_gain.shape[0]
    f_index, c_index = lax.axis_index("fsdp"), lax.axis_index("ctx")
    bf16 = jnp.bfloat16
    f32 = jnp.float32

    if nf == 8:
        halves = shard_width // 128
        turned = w_router.T.reshape(experts, halves, 128).transpose(1, 0, 2).reshape(-1, 128)
        qk_row = lax.dynamic_update_slice(
            jnp.zeros((256,), bf16), qk_gains, (f_index * qk_gains.shape[0],)
        )
        small = jnp.concatenate(
            [
                turned,
                attn_gain.reshape(-1, 128),
                ffn_gain.reshape(-1, 128),
                qk_row.reshape(-1, 128),
            ]
        )
        small = jnp.pad(small, ((0, -small.shape[0] % 16), (0, 0)))
        own_positions = c_index * tokens_dev + jnp.arange(tokens_dev, dtype=jnp.int32)
        cosine_table, sine_values = rope_tables(own_positions)
        cosine_row, sine_row = cosine_table[:, 0], sine_values[:, 0]
        trig = jnp.stack(
            [
                jnp.concatenate([cosine_row, cosine_row], axis=1),
                jnp.concatenate([sine_row, -sine_row], axis=1),
            ]
        )
        segment_wide = jnp.broadcast_to(segment_ids.astype(bf16)[:, None], (tokens_dev, 128))
        expert_ids = jnp.arange(experts, dtype=jnp.int32)
        hits = routes[:, :, None] == expert_ids[None, None, :]
        routed = jnp.any(hits, axis=1).astype(f32)
        heads_width, kv_width = w_query.shape[1], key_projection.shape[1]
        kv_projection = jnp.concatenate([key_projection, value_projection], axis=1)
        shapes = (tokens_dev, width_dim, heads_width, kv_width, experts)
        (
            _,
            query_weight,
            kv_weight,
            out_weight,
            grad_all,
            hidden_two,
            hidden_slices,
            marks,
            probs,
            resid_mid,
            attended,
            query_raw,
            key_projected,
            query_rotated,
            key_all,
            value_all,
            bias,
            log_total,
            gains,
            router_rows,
        ) = forward_pass(
            nf,
            (small, w_query, kv_projection, w_out, grad_out),
            (hidden_in, segment_wide, routed, trig),
            shapes,
        )
    else:
        pieces = [w_router.reshape(-1), attn_gain, ffn_gain, qk_gains]
        flat = jnp.concatenate(pieces)
        small_rows = -(-flat.shape[0] // 2048) * 16
        small = jnp.pad(flat, (0, small_rows * 128 - flat.shape[0])).reshape(small_rows, 128)
        out_form = "row" if shard_width % 128 else "col"
        small_all, query_weight, key_weight, value_weight, out_weight, grad_all = plane_gather(
            [
                Gather(small, nf, chunks=1),
                Gather(w_query, nf, half=True, chunks=2),
                Gather(key_projection, nf, half=True, chunks=1),
                Gather(value_projection, nf, half=True, chunks=1),
                Gather(w_out, nf, form=out_form, half=True, chunks=2),
                Gather(grad_out, nf, rep=True, chunks=4),
            ],
            1,
            nf,
        )
        if out_form == "row":
            out_weight = out_weight.reshape(nf, -1, shard_width).transpose(1, 0, 2)
            out_weight = out_weight.reshape(-1, width_dim)
        small_all = small_all.reshape(nf, 2, small_rows * 128)[:, 0]
        ends = [0]
        for piece in pieces:
            ends.append(ends[-1] + piece.shape[0])
        router_weight = small_all[:, ends[0] : ends[1]].reshape(width_dim, experts)
        gain_one = small_all[:, ends[1] : ends[2]].reshape(-1).astype(f32)
        gain_two = small_all[:, ends[2] : ends[3]].reshape(-1).astype(f32)
        gain_qk = small_all[:, ends[3] : ends[4]].reshape(-1).astype(f32)
        gain_query, gain_key = gain_qk[:HEAD_SIZE], gain_qk[HEAD_SIZE:]

        kv_local = key_weight.shape[1] // HEAD_SIZE
        head_local = query_weight.shape[1] // HEAD_SIZE
        resid = hidden_in.astype(f32)
        scaled_one, normed_one, inverse_one = norm_forward(resid, gain_one)
        hidden_first = scaled_one.astype(bf16)
        query_raw = jnp.dot(hidden_first, query_weight, preferred_element_type=f32).reshape(
            tokens_dev, head_local, HEAD_SIZE
        )
        key_projected = jnp.dot(hidden_first, key_weight, preferred_element_type=f32).reshape(
            tokens_dev, kv_local, HEAD_SIZE
        )
        value_rows = jnp.dot(hidden_first, value_weight, preferred_element_type=f32).astype(bf16)
        query_normed, query_hat, query_inverse = norm_forward(query_raw, gain_query)
        key_normed, key_unit_rows, key_inverse_norm = norm_forward(key_projected, gain_key)
        own_positions = c_index * tokens_dev + jnp.arange(tokens_dev, dtype=jnp.int32)
        cosine_table, sine_values = rope_tables(own_positions)
        query_rotated = (
            rotate(query_normed, cosine_table, sine_values)
            .astype(bf16)
            .reshape(tokens_dev, kv_local, query_group_width, HEAD_SIZE)
        )
        key_rotated = rotate(key_normed, cosine_table, sine_values).astype(bf16)
        own_segments = segment_ids.astype(bf16)
        packed_kv = jnp.concatenate(
            [
                key_rotated.reshape(tokens_dev, -1),
                value_rows,
                jnp.broadcast_to(own_segments[:, None], (tokens_dev, 128)),
            ],
            axis=1,
        )
        kv_all = lax.all_gather(packed_kv, "ctx", axis=0, tiled=True)
        kv_width = kv_local * HEAD_SIZE
        key_all = kv_all[:, :kv_width].reshape(-1, kv_local, HEAD_SIZE)
        value_all = kv_all[:, kv_width : 2 * kv_width].reshape(-1, kv_local, HEAD_SIZE)
        segment_all = kv_all[:, 2 * kv_width]
        key_positions = jnp.arange(key_all.shape[0], dtype=jnp.int32)
        allowed = (key_positions[None, :] <= own_positions[:, None]) & (
            segment_all[None, :] == own_segments[:, None]
        )
        scores = masked_scores(query_rotated, key_all, allowed)
        top_score = jnp.max(scores, axis=-1, keepdims=True)
        log_total = top_score + jnp.log(jnp.sum(jnp.exp(scores - top_score), axis=-1, keepdims=True))
        weights_att = jnp.exp(scores - log_total).astype(bf16)
        attended = jnp.einsum("kgqs,skd->qkgd", weights_att, value_all, preferred_element_type=f32)
        attended = attended.astype(bf16).reshape(tokens_dev, head_local * HEAD_SIZE)
        out_partial = jnp.dot(attended, out_weight, preferred_element_type=f32)
        resid_mid = resid + sum_over_tp(out_partial)
        scaled_two, normed_two, inverse_two = norm_forward(resid_mid, gain_two)
        hidden_two = scaled_two.astype(bf16)
        logits = jnp.dot(hidden_two, router_weight, preferred_element_type=f32)
        expert_ids = jnp.arange(experts, dtype=jnp.int32)
        hits = routes[:, :, None] == expert_ids[None, None, :]
        routed = jnp.any(hits, axis=1)
        masked_logits = jnp.where(routed, logits, -jnp.inf)
        raised = jnp.where(
            routed, jnp.exp(masked_logits - jnp.max(masked_logits, axis=1, keepdims=True)), 0.0
        )
        probs = raised / jnp.sum(raised, axis=1, keepdims=True)
        marks = jnp.where(routed, probs, -1.0).T
    if nf == 8:
        (
            hidden_all,
            hidden_first_slice,
            moe_partial,
            rows_in,
            grad_prod,
            activated,
            grad_gate_pre,
            grad_up_pre,
            grad_hidden_moe,
            grad_prob,
        ) = expert_pass(
            hidden_two,
            marks,
            hidden_slices,
            grad_all,
            w_gate,
            w_up,
            w_down,
            capacity,
            nf,
        )
        grad_prob = grad_prob.reshape(devices, 8, tokens_dev)[:, :local_experts]
        grad_prob = grad_prob.reshape(experts, tokens_dev).T
    else:
        hidden_all, marks_all, hidden_first_slice = plane_gather(
            [
                Gather(hidden_two, nf, rep=True, chunks=4),
                Gather(marks, nf, chunks=1),
                Gather(by_shard(hidden_first, nf), nf, form="a2a", chunks=1),
            ],
            2,
            nf,
        )
        first_expert = (f_index * 2 + c_index) * local_experts
        marks_here = lax.dynamic_slice_in_dim(
            marks_all.reshape(devices, experts, tokens_dev), first_expert, local_experts, axis=1
        )
        taken = marks_here >= 0.0
        ranks = jnp.cumsum(taken.astype(jnp.int32), axis=2) - 1
        slots = jnp.arange(capacity, dtype=jnp.int32)
        chosen = taken[:, :, None, :] & (ranks[:, :, None, :] == slots[None, None, :, None])
        pick = chosen.astype(bf16)
        weight_slot = jnp.sum(jnp.where(chosen, marks_here[:, :, None, :], 0.0), axis=3)
        weight_slot = weight_slot.transpose(1, 0, 2).reshape(local_experts, devices * capacity)

        def select(rows):
            blocks = rows.reshape(devices, tokens_dev, width_dim)
            out = jnp.einsum("bjst,btd->jbsd", pick, blocks, preferred_element_type=f32)
            return out.astype(bf16).reshape(local_experts, devices * capacity, width_dim)

        def spread(rows):
            blocks = rows.reshape(local_experts, devices, capacity, width_dim)
            out = jnp.einsum("bjst,jbsd->btd", pick, blocks, preferred_element_type=f32)
            return out.astype(bf16).reshape(devices * tokens_dev, width_dim)

        rows_in = select(hidden_all)
        grad_rows_in = select(grad_all)
        gate_pre = jnp.einsum("jrd,jdf->jrf", rows_in, w_gate, preferred_element_type=f32)
        up_pre = jnp.einsum("jrd,jdf->jrf", rows_in, w_up, preferred_element_type=f32)
        sigmoid_gate = jax.nn.sigmoid(gate_pre)
        silu_gate = gate_pre * sigmoid_gate
        activated = (silu_gate * up_pre).astype(bf16)
        produced = jnp.einsum("jrf,jfd->jrd", activated, w_down, preferred_element_type=f32).astype(
            bf16
        )
        wide = produced.astype(f32)
        grad_prob_slot = jnp.sum(wide * grad_rows_in.astype(f32), axis=2)
        grad_prob_part = jnp.sum(
            jnp.where(
                chosen,
                grad_prob_slot.reshape(local_experts, devices, capacity).transpose(1, 0, 2)[..., None],
                0.0,
            ),
            axis=2,
        )
        moe_partial = spread((weight_slot[:, :, None] * wide).astype(bf16))
        grad_prod = (weight_slot[:, :, None] * grad_rows_in.astype(f32)).astype(bf16)
        grad_act = jnp.einsum("jrd,jfd->jrf", grad_prod, w_down, preferred_element_type=f32)
        grad_gate_pre = (
            grad_act * up_pre * (sigmoid_gate * (1.0 + gate_pre * (1.0 - sigmoid_gate)))
        ).astype(bf16)
        grad_up_pre = (grad_act * silu_gate).astype(bf16)
        grad_slots = jnp.einsum("jrf,jdf->jrd", grad_gate_pre, w_gate, preferred_element_type=f32)
        grad_slots = (
            grad_slots + jnp.einsum("jrf,jdf->jrd", grad_up_pre, w_up, preferred_element_type=f32)
        ).astype(bf16)
        hidden_grad_partial = spread(grad_slots)

        grad_hidden_moe = sum_over_tp(block_sum(hidden_grad_partial, nf))
        grad_prob = lax.all_to_all(
            grad_prob_part, ("fsdp", "ctx"), split_axis=0, concat_axis=0, tiled=True
        ).reshape(experts, tokens_dev)
        grad_prob = grad_prob + swap(grad_prob, "tp")
        grad_prob = grad_prob.T

    if nf == 8:
        operands = (
            grad_hidden_moe,
            grad_prob,
            probs,
            router_rows,
            hidden_in,
            resid_mid,
            gains,
            grad_out,
            out_weight,
            query_weight,
            kv_weight,
            query_raw,
            key_projected,
            query_rotated,
            key_all,
            value_all,
            bias,
            log_total,
            trig,
            moe_partial,
            rows_in,
            grad_prod,
            activated,
            grad_gate_pre,
            grad_up_pre,
        )
        shapes = (tokens_dev, width_dim, heads_width, kv_width, key_all.shape[0])
        (
            attended_all,
            dq_all,
            rest_all,
            tail_all,
            proj_slice,
            grad_in,
            block_out,
            grad_gate,
            grad_up,
            grad_down,
        ) = backward_pass(nf, operands, attended, shapes)
        grad_gate, grad_up, grad_down = (
            grad_gate.astype(f32),
            grad_up.astype(f32),
            grad_down.astype(f32),
        )
        tail_rows = tail_all.shape[0] // devices
        dk_all, dv_all = rest_all[:, :kv_width], rest_all[:, kv_width : 2 * kv_width]
        logits_all = rest_all[:, 2 * kv_width :]
    else:
        grad_down = jnp.einsum("jrf,jrd->jfd", activated, grad_prod, preferred_element_type=f32)
        grad_gate = jnp.einsum("jrd,jrf->jdf", rows_in, grad_gate_pre, preferred_element_type=f32)
        grad_up = jnp.einsum("jrd,jrf->jdf", rows_in, grad_up_pre, preferred_element_type=f32)
        block_out = (resid_mid + sum_over_tp(block_sum(moe_partial, nf))).astype(bf16)

        grad_rows = grad_out.astype(f32)
        grad_logits = (
            probs * (grad_prob - jnp.sum(probs * grad_prob, axis=1, keepdims=True))
        ).astype(bf16)
        grad_hidden_two = grad_hidden_moe + jnp.einsum(
            "te,de->td", grad_logits, router_weight, preferred_element_type=f32
        )
        grad_ffn_local = jnp.sum(grad_hidden_two * normed_two, axis=0)
        grad_mid = grad_rows + rms_norm_gradient(grad_hidden_two, normed_two, inverse_two, gain_two)
        grad_proj = grad_mid.astype(bf16)
        attended_gradient = jnp.einsum(
            "td,qd->tq", grad_proj, out_weight, preferred_element_type=f32
        ).astype(bf16)
        attended_gradient = attended_gradient.reshape(
            tokens_dev, kv_local, query_group_width, HEAD_SIZE
        )
        probs_att = jnp.exp(scores - log_total)
        grad_value_all = jnp.einsum(
            "kgqs,qkgd->skd", weights_att, attended_gradient, preferred_element_type=f32
        )
        grad_probs = jnp.einsum(
            "qkgd,skd->kgqs", attended_gradient, value_all, preferred_element_type=f32
        )
        delta_row = jnp.sum(probs_att * grad_probs, axis=-1, keepdims=True)
        grad_scores = (probs_att * (grad_probs - delta_row) * HEAD_SIZE ** (-0.5)).astype(bf16)
        grad_query_rot = jnp.einsum(
            "kgqs,skd->qkgd", grad_scores, key_all, preferred_element_type=f32
        ).reshape(tokens_dev, head_local, HEAD_SIZE)
        grad_key_all = jnp.einsum(
            "kgqs,qkgd->skd", grad_scores, query_rotated, preferred_element_type=f32
        )
        grad_kv_all = jnp.concatenate(
            [grad_key_all.reshape(-1, kv_width), grad_value_all.reshape(-1, kv_width)], axis=1
        )
        theirs = lax.dynamic_slice_in_dim(grad_kv_all, (1 - c_index) * tokens_dev, tokens_dev, axis=0)
        mine = lax.dynamic_slice_in_dim(grad_kv_all, c_index * tokens_dev, tokens_dev, axis=0)
        grad_kv = mine + swap(theirs.astype(bf16), "ctx").astype(f32)
        key_rotated_gradient = grad_kv[:, :kv_width].reshape(tokens_dev, kv_local, HEAD_SIZE)
        grad_query_norm = inverse_rotation(grad_query_rot, cosine_table, sine_values)
        key_normed_gradient = inverse_rotation(key_rotated_gradient, cosine_table, sine_values)
        grad_qk_local = jnp.concatenate(
            [
                jnp.sum(grad_query_norm * query_hat, axis=(0, 1)),
                jnp.sum(key_normed_gradient * key_unit_rows, axis=(0, 1)),
            ]
        )
        grad_query_raw = (
            rms_norm_gradient(grad_query_norm, query_hat, query_inverse, gain_query)
            .astype(bf16)
            .reshape(tokens_dev, head_local * HEAD_SIZE)
        )
        key_projected_gradient = (
            rms_norm_gradient(key_normed_gradient, key_unit_rows, key_inverse_norm, gain_key)
            .astype(bf16)
            .reshape(tokens_dev, kv_width)
        )
        value_projected_gradient = grad_kv[:, kv_width:].astype(bf16)
        grad_hidden_part = jnp.einsum(
            "tq,dq->td", grad_query_raw, query_weight, preferred_element_type=f32
        )
        grad_hidden_part = grad_hidden_part + jnp.einsum(
            "tq,dq->td", key_projected_gradient, key_weight, preferred_element_type=f32
        )
        grad_hidden_part = grad_hidden_part + jnp.einsum(
            "tq,dq->td", value_projected_gradient, value_weight, preferred_element_type=f32
        )
        grad_hidden_one = sum_over_tp(grad_hidden_part)
        grad_in = grad_mid + rms_norm_gradient(grad_hidden_one, normed_one, inverse_one, gain_one)
        grad_attn_local = jnp.sum(grad_hidden_one * normed_one, axis=0)
        grad_qk_local = grad_qk_local + swap(grad_qk_local, "tp")
        tail = jnp.concatenate([grad_attn_local, grad_ffn_local, grad_qk_local])
        tail = jnp.pad(tail, (0, -tail.shape[0] % 1024)).reshape(-1, 128)
        tail_rows = tail.shape[0]
        logit_pad = jnp.pad(grad_logits, ((0, 0), (0, -experts % 128)))

        dq_all, dk_all, dv_all, attended_all, proj_slice, logits_all, tail_all = plane_gather(
            [
                Gather(grad_query_raw, nf, chunks=2),
                Gather(key_projected_gradient, nf, chunks=1),
                Gather(value_projected_gradient, nf, chunks=1),
                Gather(attended, nf, chunks=2),
                Gather(by_shard(grad_proj, nf), nf, form="a2a", chunks=1),
                Gather(logit_pad, nf, chunks=1),
                Gather(tail, nf, chunks=1),
            ],
            3,
            nf,
        )
    over_tokens = functools.partial(
        jnp.einsum, "td,tq->dq", preferred_element_type=f32
    )
    grad_query = over_tokens(hidden_first_slice, dq_all)
    grad_key = over_tokens(hidden_first_slice, dk_all)
    grad_value = over_tokens(hidden_first_slice, dv_all)
    grad_out_proj = over_tokens(attended_all, proj_slice)
    hidden_slice = lax.dynamic_slice_in_dim(hidden_all, f_index * shard_width, shard_width, axis=1)
    grad_router = over_tokens(hidden_slice, logits_all)[:, :experts]
    tail_sum = jnp.sum(tail_all.reshape(devices, tail_rows * 128), axis=0)
    grad_attn = lax.dynamic_slice_in_dim(tail_sum, f_index * shard_width, shard_width)
    grad_ffn = lax.dynamic_slice_in_dim(tail_sum, width_dim + f_index * shard_width, shard_width)
    qk_width = qk_gains.shape[0]
    grad_qk = lax.dynamic_slice_in_dim(tail_sum, 2 * width_dim + f_index * qk_width, qk_width)
    return (
        block_out,
        grad_in,
        grad_attn,
        grad_qk,
        grad_query,
        grad_key,
        grad_value,
        grad_out_proj,
        grad_ffn,
        grad_router,
        grad_gate,
        grad_up,
        grad_down,
    )


def solution(mesh):
    return jax.shard_map(
        on_device,
        mesh=mesh,
        in_specs=(
            P(("fsdp", "ctx"), None),
            P(("fsdp", "ctx")),
            P(("fsdp", "ctx"), None),
            P("fsdp"),
            P("fsdp"),
            P("fsdp", "tp"),
            P("fsdp", "tp"),
            P("fsdp", "tp"),
            P("tp", "fsdp"),
            P("fsdp"),
            P("fsdp", None),
            P(("fsdp", "ctx"), None, "tp"),
            P(("fsdp", "ctx"), None, "tp"),
            P(("fsdp", "ctx"), "tp", None),
            P(("fsdp", "ctx"), None),
        ),
        out_specs=(
            P(("fsdp", "ctx"), None),
            P(("fsdp", "ctx"), None),
            P("fsdp"),
            P("fsdp"),
            P("fsdp", "tp"),
            P("fsdp", "tp"),
            P("fsdp", "tp"),
            P("tp", "fsdp"),
            P("fsdp"),
            P("fsdp", None),
            P(("fsdp", "ctx"), None, "tp"),
            P(("fsdp", "ctx"), None, "tp"),
            P(("fsdp", "ctx"), "tp", None),
        ),
        check_vma=False,
    )
```

```python
import functools

import jax
import jax.numpy as jnp
from jax import lax
from jax.experimental import pallas as pl
from jax.experimental.pallas import tpu as pltpu
from jax.sharding import PartitionSpec as P

QUERY_HEADS = 32
KEY_VALUE_HEADS = 4
HEAD_SIZE = 128
TOPK = 8
MESH = pl.DeviceIdType.MESH

eps_norm = 1e-06
rope_base = 1000000.0

UP, DOWN, ACROSS, PARTNER, SIDE = range(5)


class Gather:
    def __init__(self, array, nf, form="row", half=False, rep=False, chunks=2, split=None):
        if nf > 8:
            chunks = 2 if rep else 1
        self.array, self.form, self.half, self.rep, self.chunks = array, form, half, rep, chunks
        self.shape = array.shape
        self.split = nf // 2 - 1 if split is None else split
        self.rows = array.shape[0] // 2 if half else array.shape[0]
        self.step = (self.rows // nf if form == "a2a" else self.rows) // chunks

    def out_shape(self, nf):
        rows, cols = self.rows, self.shape[1]
        if self.form == "col":
            return (2 * rows, nf * cols)
        if self.form == "a2a":
            return (2 * rows, cols)
        return (2 * nf * rows, cols)


def gather_engine(nf, specs, ins, outs, stage, recv, send, local):
    n = len(specs)
    nz = nf // 2
    f, c, t = lax.axis_index("fsdp"), lax.axis_index("ctx"), lax.axis_index("tp")
    z, x = f // 2, lax.rem(f, 2)
    has_up, has_down = z + 1 < nz, z > 0
    device = {
        UP: (f + 2, c, t),
        DOWN: (f - 2, c, t),
        ACROSS: (z * 2 + 1 - x, c, t),
        PARTNER: (f, 1 - c, t),
        SIDE: (f, c, 1 - t),
    }
    first = [sum(s.chunks for s in specs[:a]) for a in range(n)]

    def src(a, q, dest_f=None):
        s = specs[a]
        lo = row_chunk(a, q) * s.step
        if s.half:
            lo = c * s.rows + lo
        if s.form == "a2a":
            lo = dest_f * (s.rows // nf) + lo
        return ins[a].at[pl.ds(lo, s.step)]

    def dst(a, q, bf, bc):
        s = specs[a]
        if s.form == "col":
            width = s.shape[1]
            return outs[a].at[
                pl.ds(bc * s.rows + row_chunk(a, q) * s.step, s.step),
                pl.ds(pl.multiple_of(bf * width, width), width),
            ]
        rows = s.rows // nf if s.form == "a2a" else s.rows
        return outs[a].at[pl.ds((bf * 2 + bc) * rows + row_chunk(a, q) * s.step, s.step)]

    def copy(a, q, bf, bc, source, kind, dev=None, slot=None):
        block = bf * 2 + bc if slot is None else slot
        return pltpu.make_async_remote_copy(
            src_ref=source,
            dst_ref=dst(a, q, bf, bc),
            send_sem=send.at[kind, block, first[a] + row_chunk(a, q)],
            recv_sem=recv.at[bf * 2 + bc, first[a] + row_chunk(a, q)],
            device_id=device[kind] if dev is None else dev,
            device_id_type=MESH,
        )

    def row_chunk(a, q):
        n_chunks = specs[a].chunks
        if not specs[a].rep:
            return q
        return lax.rem(q + t * (n_chunks // 2), n_chunks)

    def in_half(a, q):
        return 2 * q < specs[a].chunks

    def both(*conds):
        if any(k is False for k in conds):
            return False
        conds = [k for k in conds if k is not None and k is not True]
        if not conds:
            return None
        return functools.reduce(lambda u, v: u & v, conds)

    def when(cond, fn):
        if cond is None or cond is True:
            fn()
        elif cond is not False:
            pl.when(cond)(fn)

    def go_up(a, q, dist):
        far = dist + 1 < specs[a].split if specs[a].rep and not in_half(a, q) else None
        return both(has_up, far)

    def go_down(a, q, dist):
        far = dist + 1 < specs[a].split if specs[a].rep and not in_half(a, q) else None
        return both(has_down, far)

    def go_across(a, q):
        return in_half(a, q) if specs[a].rep else None

    relays = [(a, q) for a in range(n) if specs[a].form != "a2a" for q in range(specs[a].chunks)]
    direct = [(a, q) for a in range(n) if specs[a].form == "a2a" for q in range(specs[a].chunks)]

    def start(only=None):
        only = range(n) if only is None else only
        for a, q in relays:
            if a not in only:
                continue
            source = src(a, q)
            when(go_up(a, q, 0), lambda: copy(a, q, f, c, source, UP).start())
            when(go_down(a, q, 0), lambda: copy(a, q, f, c, source, DOWN).start())
            when(go_across(a, q), lambda: copy(a, q, f, c, source, ACROSS).start())
            copy(a, q, f, c, source, PARTNER).start()
        own_start([a for a in only if specs[a].form != "a2a"])

    def own_start(only):
        for a in only:
            own_in(a).start()
        for a in only:
            own_in(a).wait()
            own_out(a).start()

    def start_direct():
        own_start(sorted({a for a, _ in direct}))
        for a, q in direct:
            copy(a, q, f, c, src(a, q, f), PARTNER).start()

            def far_send(d, carry):
                there = lax.rem(f + d, nf)
                copy(a, q, f, c, src(a, q, there), UP, dev=(there, c, t), slot=there).start()
                return carry

            lax.fori_loop(1, nf, far_send, 0)

    def own_in(a):
        s = specs[a]
        if s.form == "a2a":
            view = ins[a].at[pl.ds(f * s.step, s.step)]
        elif s.half:
            view = ins[a].at[pl.ds(c * s.rows, s.rows)]
        else:
            view = ins[a]
        return pltpu.make_async_copy(view, stage[a], local.at[0, a])

    def own_out(a):
        s = specs[a]
        if s.form == "col":
            width = s.shape[1]
            view = outs[a].at[
                pl.ds(c * s.rows, s.rows), pl.ds(pl.multiple_of(f * width, width), width)
            ]
        else:
            rows = s.rows // nf if s.form == "a2a" else s.rows
            view = outs[a].at[pl.ds((f * 2 + c) * rows, rows)]
        return pltpu.make_async_copy(stage[a], view, local.at[1, a])

    def arrived(a, q, bf, bc):
        copy(a, q, bf, bc, dst(a, q, bf, bc), PARTNER).wait_recv()

    def pass_on(a, q, bf, kind, cond=None):
        when(cond, lambda: copy(a, q, bf, c, dst(a, q, bf, c), kind).start())

    pair = z + 1 - 2 * lax.rem(z, 2)
    even = lax.rem(z, 2) == 0

    def shared(a, q):
        return not specs[a].rep and specs[a].chunks > 1 and 2 * q >= specs[a].chunks

    def column(k, a, q):
        rep = specs[a].rep
        came = k < specs[a].split if rep and not in_half(a, q) else None
        far = (k >= specs[a].split) if rep and in_half(a, q) else False

        def take(zz, kind, onward):
            bf = zz * 2 + x
            arrived(a, q, bf, c)
            pass_on(a, q, bf, kind, onward)
            cross = (zz != pair) if shared(a, q) else go_across(a, q)
            pass_on(a, q, bf, ACROSS, cross)
            pass_on(a, q, bf, PARTNER)
            if rep:
                pass_on(a, q, bf, SIDE, far)

        when(both(z - k >= 0, came), lambda: take(z - k, UP, go_up(a, q, k)))
        when(both(z + k < nz, came), lambda: take(z + k, DOWN, go_down(a, q, k)))

    def across(k, a, q):
        rep = specs[a].rep
        mine = in_half(a, q) if rep else None

        def take(zz):
            bf = zz * 2 + 1 - x
            arrived(a, q, bf, c)
            pass_on(a, q, bf, PARTNER)
            if rep:
                pass_on(a, q, bf, SIDE)
            if shared(a, q):
                pass_on(a, q, bf, UP, (zz == z) & even)
                pass_on(a, q, bf, DOWN, (zz == z) & jnp.logical_not(even))

        when(both(z - k >= 0, mine), lambda: take(z - k))
        when(both(z + k < nz, k > 0, mine), lambda: take(z + k))

    def aside(k, a, q):
        if not specs[a].rep:
            return
        if in_half(a, q):
            return

        def take(bf):
            arrived(a, q, bf, c)
            pass_on(a, q, bf, PARTNER)

        when(z - k >= 0, lambda: take((z - k) * 2 + 1 - x))
        when(both(z + k < nz, k > 0), lambda: take((z + k) * 2 + 1 - x))
        far = k >= specs[a].split
        when(both(z - k >= 0, far), lambda: take((z - k) * 2 + x))
        when(both(z + k < nz, far), lambda: take((z + k) * 2 + x))

    count = len(relays)
    lag = 2

    def late(fn, k, i):
        if i >= 0:
            fn(k, *relays[i])
        else:
            pl.when(k > 1)(lambda: fn(k - 1, *relays[count + i]))

    by_chunk = all(specs[a].rep for a, _ in relays)

    def step(k, carry):
        if not by_chunk:
            for a, q in relays:
                column(k, a, q)
            for a, q in relays:
                across(k - 1, a, q)

            @pl.when(k > 1)
            def _():
                for a, q in relays:
                    aside(k - 2, a, q)

            return carry
        for i, (a, q) in enumerate(relays):
            column(k, a, q)
            pl.when(k == 1)(lambda: across(0, a, q))
            late(across, k, i - lag)
            if i >= lag:
                pl.when(k == 1)(lambda: aside(0, *relays[i - lag]))
            late(aside, k, i - 2 * lag)

        @pl.when(k == 1)
        def _():
            for a, q in relays[count - lag :]:
                aside(0, a, q)

        return carry

    def run(hook=None):
        def body(k, carry):
            step(k, carry)
            if hook is not None:
                hook(k)
            return carry

        lax.fori_loop(1, nz, body, 0)
        for a, q in relays[count - lag if by_chunk else 0 :]:
            across(nz - 1, a, q)
        if not by_chunk:
            for a, q in relays:
                aside(nz - 2, a, q)
        for a, q in relays[count - 2 * lag if by_chunk else 0 :]:
            aside(nz - 1, a, q)

    def step_of(k, only):
        some = [(a, q) for a, q in relays if a in only]
        for a, q in some:
            column(k, a, q)
        for a, q in some:
            across(k - 1, a, q)

        if any(specs[a].rep for a, _ in some) and k > 1:
            for a, q in some:
                aside(k - 2, a, q)

    def edge_of(only):
        some = [(a, q) for a, q in relays if a in only]
        for a, q in some:
            across(nz - 1, a, q)
        for a, q in some:
            aside(nz - 2, a, q)
        for a, q in some:
            aside(nz - 1, a, q)

    def land_of(only):
        def take(bf, carry):
            for a, q in relays:
                if a in only:
                    arrived(a, q, bf, 1 - c)
            return carry

        lax.fori_loop(0, nf, take, 0)
        for a in only:
            own_out(a).wait()

    def run_direct():
        for a, q in direct:

            def far_take(d, carry):
                there = lax.rem(f + nf - d, nf)
                arrived(a, q, there, c)
                pass_on(a, q, there, PARTNER)
                return carry

            lax.fori_loop(1, nf, far_take, 0)

    def take_partner(bf, carry):
        for a, q in relays:
            arrived(a, q, bf, 1 - c)
        return carry

    def land():
        lax.fori_loop(0, nf, take_partner, 0)
        for a in range(n):
            if specs[a].form != "a2a":
                own_out(a).wait()

    def finish(bf, carry):
        zz, xx = bf // 2, lax.rem(bf, 2)
        dist = jnp.abs(zz - z)
        here = xx == x
        for a, q in relays:
            rep = specs[a].rep
            view = dst(a, q, bf, c)

            def sent(kind, cond):
                when(cond, lambda: copy(a, q, bf, c, view, kind).wait_send())

            half = in_half(a, q) if rep else None
            by_z = dist < specs[a].split if rep and not half else None
            sent(PARTNER, None)
            sent(UP, both(here, zz <= z, by_z, go_up(a, q, dist)))
            sent(DOWN, both(here, zz >= z, by_z, go_down(a, q, dist)))
            cross = (zz != pair) if shared(a, q) else go_across(a, q)
            sent(ACROSS, both(here, by_z, cross))
            if shared(a, q):
                there = jnp.logical_not(here) & (zz == z)
                sent(UP, there & even)
                sent(DOWN, there & jnp.logical_not(even))
            if rep and half:
                sent(SIDE, jnp.logical_not(here) | (dist >= specs[a].split))
        for a, q in direct:
            arrived(a, q, bf, 1 - c)
            view = dst(a, q, bf, c)
            copy(a, q, bf, c, view, PARTNER).wait_send()

            @pl.when(bf != f)
            def _():
                copy(a, q, bf, c, view, UP, slot=bf).wait_send()

        return carry

    def drain():
        lax.fori_loop(0, nf, finish, 0)
        for a in range(n):
            if specs[a].form == "a2a":
                own_out(a).wait()

    return start, run, land, start_direct, run_direct, drain, step_of, edge_of, land_of


def gather_kernel(nf, specs, *refs):
    n = len(specs)
    ins, outs, scratch = refs[:n], refs[n : 2 * n], refs[2 * n :]
    nz = nf // 2
    f, c, t = lax.axis_index("fsdp"), lax.axis_index("ctx"), lax.axis_index("tp")
    z, x = f // 2, lax.rem(f, 2)
    has_up, has_down = z + 1 < nz, z > 0
    device = {
        UP: (f + 2, c, t),
        DOWN: (f - 2, c, t),
        ACROSS: (z * 2 + 1 - x, c, t),
        PARTNER: (f, 1 - c, t),
        SIDE: (f, c, 1 - t),
    }
    any_a2a = any(s.form == "a2a" for s in specs)
    any_rep = any(s.rep for s in specs)
    barrier = pltpu.get_barrier_semaphore()

    def greet(dev):
        pl.semaphore_signal(barrier, 1, device_id=dev, device_id_type=MESH)

    greeted = 1
    greet(device[PARTNER])
    if any_rep:
        greet(device[SIDE])
        greeted += 1
    if any_a2a:

        def greet_far(d, carry):
            greet((lax.rem(f + d, nf), c, t))
            return carry

        lax.fori_loop(1, nf, greet_far, 0)
        pl.semaphore_wait(barrier, greeted + nf - 1)
    else:
        greet(device[ACROSS])

        @pl.when(has_up)
        def _():
            greet(device[UP])

        @pl.when(has_down)
        def _():
            greet(device[DOWN])

        pl.semaphore_wait(
            barrier, greeted + 1 + has_up.astype(jnp.int32) + has_down.astype(jnp.int32)
        )

    start, run, land, start_direct, run_direct, drain, *_ = gather_engine(
        nf, specs, ins, outs, scratch[:n], *scratch[n:]
    )
    start()
    start_direct()
    run()
    run_direct()
    land()
    drain()


def stage_of(s, nf):
    rows = s.rows // nf if s.form == "a2a" else s.rows
    return pltpu.VMEM((rows, s.shape[1]), s.array.dtype)


def plane_gather(specs, collective_id, nf):
    n = len(specs)
    total = sum(s.chunks for s in specs)

    return pl.pallas_call(
        functools.partial(gather_kernel, nf, tuple(specs)),
        out_shape=tuple(jax.ShapeDtypeStruct(s.out_shape(nf), s.array.dtype) for s in specs),
        in_specs=[pl.BlockSpec(memory_space=pl.ANY)] * n,
        out_specs=tuple(pl.BlockSpec(memory_space=pl.ANY) for _ in specs),
        scratch_shapes=[stage_of(s, nf) for s in specs]
        + [
            pltpu.SemaphoreType.DMA((2 * nf, total)),
            pltpu.SemaphoreType.DMA((5, 2 * nf, total)),
            pltpu.SemaphoreType.DMA((2, n)),
        ],
        compiler_params=pltpu.CompilerParams(
            collective_id=collective_id, has_side_effects=True
        ),
    )(*[s.array for s in specs])


CUT = 4


def expert_kernel(nf, capacity, specs, *refs):
    n = len(specs)
    ins, refs = refs[:n], refs[n:]
    (grad_all, wg_hbm, wu_hbm, wd_hbm), refs = refs[:4], refs[4:]
    gathered, refs = refs[:n], refs[n:]
    (out_part, xs_out, de_out, act_out, dg_out, du_out, grad_tok, prob_tok), refs = (
        refs[:8],
        refs[8:],
    )
    stage, refs = refs[:n], refs[n:]
    (recv, send, local), refs = refs[:3], refs[3:]
    (
        wg,
        wu,
        wd,
        x_buf,
        y_buf,
        xs,
        ys,
        de,
        pe,
        bs,
        act,
        dg,
        du,
        w_slot,
        dp_slot,
        pick,
        mk,
        rk,
        y_out,
        part,
        from_partner,
        from_across,
        from_z,
        from_side,
        dp_send,
        dp_recv,
        dp_side,
        marks_v,
        w_sem,
        load_sem,
        store_sem,
        p_send,
        p_recv,
        x_send,
        x_recv,
        z_send,
        z_recv,
        s_send,
        s_recv,
        d_send,
        d_recv,
    ) = refs
    f32, bf16 = jnp.float32, jnp.bfloat16
    nz = nf // 2
    f, c, t = lax.axis_index("fsdp"), lax.axis_index("ctx"), lax.axis_index("tp")
    z, x = f // 2, lax.rem(f, 2)
    me = f * 2 + c
    up, down = (f + 2, c, t), (f - 2, c, t)
    across_dev, partner, side = (z * 2 + 1 - x, c, t), (f, 1 - c, t), (f, c, 1 - t)
    has_up, has_down = z + 1 < nz, z > 0
    tokens = x_buf.shape[0] // 4
    width = x_buf.shape[1]
    slots = 2 * capacity
    rows_unit = 4 * capacity
    hidden = wg.shape[2]
    experts = specs[1].shape[0]
    step_rows = tokens // CUT

    barrier = pltpu.get_barrier_semaphore()

    def greet(d, carry):
        there = lax.rem(me + d, 2 * nf)
        pl.semaphore_signal(
            barrier, 1, device_id=(there // 2, lax.rem(there, 2), t), device_id_type=MESH
        )
        return carry

    lax.fori_loop(1, 2 * nf, greet, 0)
    pl.semaphore_signal(barrier, 1, device_id=side, device_id_type=MESH)
    pl.semaphore_wait(barrier, 2 * nf)

    start, run, land, start_direct, run_direct, drain, *_ = gather_engine(
        nf, specs, ins, gathered, stage, recv, send, local
    )
    start()
    weight_loads = [
        pltpu.make_async_copy(src, dst, w_sem.at[i])
        for i, (src, dst) in enumerate(((wg_hbm, wg), (wu_hbm, wu), (wd_hbm, wd)))
    ]
    for load in weight_loads:
        load.start()

    order = 0
    for at, seq in enumerate(visiting_order(nz)):
        code = sum(u * nz**i for i, u in enumerate(seq))
        order = order + code * (z == at).astype(jnp.int32)

    def unit_at(i):
        code = order
        for k in range(nz):
            code = jnp.where(i > k, code // nz, code)
        return lax.rem(code, nz)

    def load_rows(u, which):
        rows = pl.ds(pl.multiple_of(u * 4 * tokens, 4 * tokens), 4 * tokens)
        if which == 0:
            return pltpu.make_async_copy(gathered[0].at[rows], x_buf, load_sem.at[0])
        return pltpu.make_async_copy(grad_all.at[rows], y_buf, load_sem.at[1])

    load_rows(unit_at(0), 1).start()
    run()
    land()
    start_direct()
    load_rows(unit_at(0), 0).start()
    marks_in = pltpu.make_async_copy(gathered[1], marks_v, load_sem.at[2])
    marks_in.start()
    marks_in.wait()
    dp_send[...] = jnp.zeros_like(dp_send)
    first_expert = me * 2
    for b in range(2 * nf):
        for j in range(2):
            mk[2 * b + j : 2 * b + j + 1, :] = marks_v[pl.ds(b * experts + first_expert + j, 1), :]
    taken = jnp.where(mk[...] >= 0.0, 1.0, 0.0).astype(bf16)
    before = lax.broadcasted_iota(jnp.int32, (tokens, tokens), 0)
    after = lax.broadcasted_iota(jnp.int32, (tokens, tokens), 1)
    upper = jnp.where(before <= after, 1.0, 0.0).astype(bf16)
    rk[...] = jnp.dot(taken, upper, preferred_element_type=f32) - 1.0
    for load in weight_loads:
        load.wait()

    def store_unit(u):
        rows = pl.ds(pl.multiple_of(u * rows_unit, rows_unit), rows_unit)
        pairs = [(xs, xs_out), (de, de_out), (act, act_out), (dg, dg_out), (du, du_out)]
        copies = [
            pltpu.make_async_copy(src, dst.at[:, rows], store_sem.at[i])
            for i, (src, dst) in enumerate(pairs)
        ]
        out_rows = pl.ds(pl.multiple_of(u * 4 * tokens, 4 * tokens), 4 * tokens)
        copies.append(pltpu.make_async_copy(y_out, out_part.at[out_rows], store_sem.at[5]))
        return copies

    def chunk(q):
        return pl.ds(pl.multiple_of(q * step_rows, step_rows), step_rows)

    def p_copy(u, xx, q):
        return pltpu.make_async_remote_copy(
            src_ref=part.at[u * 4 + xx * 2 + 1 - c, chunk(q)],
            dst_ref=from_partner.at[u * 2 + xx, chunk(q)],
            send_sem=p_send.at[u * 2 + xx, q],
            recv_sem=p_recv.at[u * 2 + xx, q],
            device_id=partner,
            device_id_type=MESH,
        )

    def x_copy(u, q):
        return pltpu.make_async_remote_copy(
            src_ref=part.at[u * 4 + (1 - x) * 2 + c, chunk(q)],
            dst_ref=from_across.at[u, chunk(q)],
            send_sem=x_send.at[u, q],
            recv_sem=x_recv.at[u, q],
            device_id=across_dev,
            device_id_type=MESH,
        )

    def z_copy(u, q, way):
        return pltpu.make_async_remote_copy(
            src_ref=part.at[u * 4 + x * 2 + c, chunk(q)],
            dst_ref=from_z.at[way, u, chunk(q)],
            send_sem=z_send.at[u, q],
            recv_sem=z_recv.at[way, u, q],
            device_id=up if way == 0 else down,
            device_id_type=MESH,
        )

    def z_wait(u, q, way):
        pltpu.make_async_remote_copy(
            src_ref=part.at[me, chunk(q)],
            dst_ref=from_z.at[way, u, chunk(q)],
            send_sem=z_send.at[u, q],
            recv_sem=z_recv.at[way, u, q],
            device_id=partner,
            device_id_type=MESH,
        ).wait_recv()

    def s_copy(q):
        return pltpu.make_async_remote_copy(
            src_ref=part.at[me, chunk(q)],
            dst_ref=from_side.at[chunk(q)],
            send_sem=s_send.at[q],
            recv_sem=s_recv.at[q],
            device_id=side,
            device_id_type=MESH,
        )

    def d_copy(b, source=None):
        return pltpu.make_async_remote_copy(
            src_ref=dp_send.at[b],
            dst_ref=dp_recv.at[me if source is None else source],
            send_sem=d_send.at[b],
            recv_sem=d_recv.at[me if source is None else source],
            device_id=(b // 2, lax.rem(b, 2), t),
            device_id_type=MESH,
        )

    def compute(i, u):
        load_rows(u, 0).wait()
        load_rows(u, 1).wait()

        @pl.when(i > 0)
        def _():
            for cp in store_unit(unit_at(i - 1)):
                cp.wait()

        slot_ids = lax.broadcasted_iota(jnp.int32, (capacity, tokens), 0).astype(f32)
        for b in range(4):
            for j in range(2):
                row = pl.ds(2 * (u * 4 + b) + j, 1)
                mark = mk[row, :]
                hit = (rk[row, :] == slot_ids) & (mark >= 0.0)
                pick[b, j * capacity : (j + 1) * capacity, :] = jnp.where(hit, 1.0, 0.0)
                w_slot[j, b * capacity : (b + 1) * capacity, :] = jnp.sum(
                    jnp.where(hit, mark, 0.0), axis=1, keepdims=True
                )
        tile = 512
        for b in range(4):
            chosen = pick[b].astype(bf16)
            for k in range(width // tile):
                cols = slice(k * tile, (k + 1) * tile)
                got = jnp.dot(
                    chosen, x_buf[b * tokens : (b + 1) * tokens, cols], preferred_element_type=f32
                ).astype(bf16)
                gy = jnp.dot(
                    chosen, y_buf[b * tokens : (b + 1) * tokens, cols], preferred_element_type=f32
                )
                for j in range(2):
                    to = slice(b * capacity, (b + 1) * capacity)
                    of = slice(j * capacity, (j + 1) * capacity)
                    xs[j, to, cols] = got[of]
                    ys[j, to, cols] = gy[of].astype(bf16)
                    de[j, to, cols] = (w_slot[j, to, :] * gy[of]).astype(bf16)

        @pl.when(i + 1 < nz)
        def _():
            load_rows(unit_at(i + 1), 0).start()
            load_rows(unit_at(i + 1), 1).start()

        def expert(j, carry):
            gate = jnp.dot(xs[j], wg[j], preferred_element_type=f32)
            upv = jnp.dot(xs[j], wu[j], preferred_element_type=f32)
            sig = 1.0 / (1.0 + jnp.exp(-gate))
            silu = gate * sig
            act[j] = (silu * upv).astype(bf16)
            grad_act = lax.dot_general(
                de[j], wd[j], (((1,), (1,)), ((), ())), preferred_element_type=f32
            )
            dg[j] = (grad_act * upv * (sig * (1.0 + gate * (1.0 - sig)))).astype(bf16)
            du[j] = (grad_act * silu).astype(bf16)
            total = jnp.zeros((rows_unit, 1), f32)
            for k in range(width // tile):
                cols = slice(k * tile, (k + 1) * tile)
                made = jnp.dot(act[j], wd[j, :, cols], preferred_element_type=f32)
                made = made.astype(bf16).astype(f32)
                total = total + jnp.sum(made * ys[j, :, cols].astype(f32), axis=1, keepdims=True)
                weighted = (w_slot[j] * made).astype(bf16)
                back = lax.dot_general(
                    dg[j], wg[j, cols, :], (((1,), (1,)), ((), ())), preferred_element_type=f32
                ) + lax.dot_general(
                    du[j], wu[j, cols, :], (((1,), (1,)), ((), ())), preferred_element_type=f32
                )
                back = back.astype(bf16)
                for b in range(4):
                    of = slice(b * capacity, (b + 1) * capacity)
                    to = pl.ds(pl.multiple_of(j * capacity, capacity), capacity)
                    pe[b, to, cols] = weighted[of]
                    bs[b, to, cols] = back[of]
            for b in range(4):
                to = pl.ds(pl.multiple_of(j * capacity, capacity), capacity)
                dp_slot[b, to, :] = total[b * capacity : (b + 1) * capacity]
            return carry

        lax.fori_loop(0, 2, expert, 0)

        def spread(b):
            chosen = pick[b]
            back = jnp.transpose(chosen).astype(bf16)
            for k in range(width // tile):
                cols = slice(k * tile, (k + 1) * tile)
                part[u * 4 + b, :, cols] = jnp.dot(
                    back, bs[b, :, cols], preferred_element_type=f32
                ).astype(bf16)

        for b in range(4):
            spread(b)
        for xx in range(2):

            @pl.loop(0, CUT)
            def _(q, xx=xx):
                p_copy(u, xx, q).start()

        for b in range(4):
            back = jnp.transpose(pick[b]).astype(bf16)
            for k in range(width // tile):
                cols = slice(k * tile, (k + 1) * tile)
                y_out[b * tokens : (b + 1) * tokens, cols] = jnp.dot(
                    back, pe[b, :, cols], preferred_element_type=f32
                ).astype(bf16)
            for j in range(2):
                of = slice(j * capacity, (j + 1) * capacity)
                dp_send[u * 4 + b, j : j + 1, :] = jnp.sum(
                    pick[b, of, :] * dp_slot[b, of, :], axis=0, keepdims=True
                )
        for cp in store_unit(u):
            cp.start()
        for b in range(4):
            bb = u * 4 + b

            @pl.when(bb != me)
            def _():
                d_copy(bb).start()

    def wide(ref):
        return ref.astype(f32)

    def to_across(u):
        @pl.loop(0, CUT)
        def _(q):
            for xx in range(2):
                p_copy(u, xx, q).wait_recv()
            blk = u * 4 + (1 - x) * 2 + c
            part[blk, chunk(q)] = (
                wide(part[blk, chunk(q)]) + wide(from_partner[u * 2 + 1 - x, chunk(q)])
            ).astype(bf16)
            x_copy(u, q).start()

    def along(u):
        blk = u * 4 + x * 2 + c

        @pl.loop(0, CUT)
        def _(q):
            x_copy(u, q).wait_recv()

            def total():
                return (
                    wide(part[blk, chunk(q)])
                    + wide(from_partner[u * 2 + x, chunk(q)])
                    + wide(from_across[u, chunk(q)])
                )

            def hop(way, has_before):
                @pl.when(has_before)
                def _():
                    z_wait(u, q, way)
                    part[blk, chunk(q)] = (total() + wide(from_z[way, u, chunk(q)])).astype(bf16)

                @pl.when(jnp.logical_not(has_before))
                def _():
                    part[blk, chunk(q)] = total().astype(bf16)

                z_copy(u, q, way).start()

            @pl.when(u > z)
            def _():
                hop(0, has_down)

            @pl.when(u < z)
            def _():
                hop(1, has_up)

            @pl.when(u == z)
            def _():
                grad_tok[chunk(q)] = total()

                @pl.when(has_down)
                def _():
                    z_wait(u, q, 0)
                    grad_tok[chunk(q)] = grad_tok[chunk(q)] + wide(from_z[0, u, chunk(q)])

                @pl.when(has_up)
                def _():
                    z_wait(u, q, 1)
                    grad_tok[chunk(q)] = grad_tok[chunk(q)] + wide(from_z[1, u, chunk(q)])

                part[blk, chunk(q)] = grad_tok[chunk(q)].astype(bf16)
                s_copy(q).start()

    def unit(i, carry):
        u = unit_at(i)
        compute(i, u)

        @pl.when(i > 0)
        def _():
            along(unit_at(i - 1))

        to_across(u)
        return carry

    lax.fori_loop(0, nz, unit, 0)
    along(z)

    dp_recv[me] = dp_send[me]

    def take_prob(d, carry):
        d_copy(me, lax.rem(me + d, 2 * nf)).wait_recv()
        return carry

    lax.fori_loop(1, 2 * nf, take_prob, 0)
    swap_prob = pltpu.make_async_remote_copy(
        src_ref=dp_recv,
        dst_ref=dp_side,
        send_sem=s_send.at[CUT],
        recv_sem=s_recv.at[CUT],
        device_id=side,
        device_id_type=MESH,
    )
    swap_prob.start()
    run_direct()
    @pl.loop(0, CUT)
    def _(q):
        s_copy(q).wait_recv()
        grad_tok[chunk(q)] = wide(part[me, chunk(q)]) + wide(from_side[chunk(q)])
    swap_prob.wait_recv()
    prob_tok[...] = dp_recv[...] + dp_side[...]

    for cp in store_unit(z):
        cp.wait()
    swap_prob.wait_send()

    def ends(u, carry):
        @pl.loop(0, CUT)
        def _(q):
            for xx in range(2):
                p_copy(u, xx, q).wait_send()
            x_copy(u, q).wait_send()

            @pl.when(u > z)
            def _():
                z_copy(u, q, 0).wait_send()

            @pl.when(u < z)
            def _():
                z_copy(u, q, 1).wait_send()

        for b in range(4):

            @pl.when(u * 4 + b != me)
            def _():
                d_copy(u * 4 + b).wait_send()

        return carry

    lax.fori_loop(0, nz, ends, 0)
    for q in range(CUT):
        s_copy(q).wait_send()

    drain()


def visiting_order(nz):
    rows = []
    for at in range(nz):
        rows.append(sorted(range(nz), key=lambda u: (-abs(u - at), u if at < nz // 2 else -u)))
    return rows


def expert_pass(hidden_two, marks, hidden_slices, grad_all, w_gate, w_up, w_down, capacity, nf):
    specs = [
        Gather(hidden_two, nf, rep=True, chunks=4),
        Gather(marks, nf, rep=True, chunks=2),
        Gather(hidden_slices, nf, form="a2a", chunks=1),
    ]
    n = len(specs)
    f32, bf16 = jnp.float32, jnp.bfloat16
    tokens, width = hidden_two.shape
    nz = nf // 2
    total = sum(s.chunks for s in specs)
    hidden = w_gate.shape[2]
    rows = 2 * nf * capacity
    unit_rows = 4 * capacity
    slots = 2 * capacity
    any_spec = pl.BlockSpec(memory_space=pl.ANY)
    vmem = pl.BlockSpec(memory_space=pltpu.VMEM)
    dma = pltpu.SemaphoreType.DMA
    outs = [jax.ShapeDtypeStruct(s.out_shape(nf), s.array.dtype) for s in specs] + [
        jax.ShapeDtypeStruct((2 * nf * tokens, width), bf16),
        jax.ShapeDtypeStruct((2, rows, width), bf16),
        jax.ShapeDtypeStruct((2, rows, width), bf16),
        jax.ShapeDtypeStruct((2, rows, hidden), bf16),
        jax.ShapeDtypeStruct((2, rows, hidden), bf16),
        jax.ShapeDtypeStruct((2, rows, hidden), bf16),
        jax.ShapeDtypeStruct((tokens, width), f32),
        jax.ShapeDtypeStruct((2 * nf, 8, tokens), f32),
    ]
    result = pl.pallas_call(
        functools.partial(expert_kernel, nf, capacity, tuple(specs)),
        out_shape=tuple(outs),
        in_specs=[any_spec] * (n + 4),
        out_specs=tuple([any_spec] * (n + 6) + [vmem, vmem]),
        scratch_shapes=[stage_of(s, nf) for s in specs]
        + [dma((2 * nf, total)), dma((5, 2 * nf, total)), dma((2, n))]
        + [
            pltpu.VMEM(w_gate.shape, bf16),
            pltpu.VMEM(w_up.shape, bf16),
            pltpu.VMEM(w_down.shape, bf16),
            pltpu.VMEM((4 * tokens, width), bf16),
            pltpu.VMEM((4 * tokens, width), bf16),
            pltpu.VMEM((2, unit_rows, width), bf16),
            pltpu.VMEM((2, unit_rows, width), bf16),
            pltpu.VMEM((2, unit_rows, width), bf16),
            pltpu.VMEM((4, slots, width), bf16),
            pltpu.VMEM((4, slots, width), bf16),
            pltpu.VMEM((2, unit_rows, hidden), bf16),
            pltpu.VMEM((2, unit_rows, hidden), bf16),
            pltpu.VMEM((2, unit_rows, hidden), bf16),
            pltpu.VMEM((2, unit_rows, 1), f32),
            pltpu.VMEM((4, slots, 1), f32),
            pltpu.VMEM((4, slots, tokens), f32),
            pltpu.VMEM((4 * nf, tokens), f32),
            pltpu.VMEM((4 * nf, tokens), f32),
            pltpu.VMEM((4 * tokens, width), bf16),
            pltpu.VMEM((2 * nf, tokens, width), bf16),
            pltpu.VMEM((nf, tokens, width), bf16),
            pltpu.VMEM((nz, tokens, width), bf16),
            pltpu.VMEM((2, nz, tokens, width), bf16),
            pltpu.VMEM((tokens, width), bf16),
            pltpu.VMEM((2 * nf, 8, tokens), f32),
            pltpu.VMEM((2 * nf, 8, tokens), f32),
            pltpu.VMEM((2 * nf, 8, tokens), f32),
            pltpu.VMEM(specs[1].out_shape(nf), f32),
            dma((3,)),
            dma((3,)),
            dma((6,)),
            dma((nf, CUT)),
            dma((nf, CUT)),
            dma((nz, CUT)),
            dma((nz, CUT)),
            dma((nz, CUT)),
            dma((2, nz, CUT)),
            dma((CUT + 1,)),
            dma((CUT + 1,)),
            dma((2 * nf,)),
            dma((2 * nf,)),
        ],
        compiler_params=pltpu.CompilerParams(
            collective_id=7, has_side_effects=True, vmem_limit_bytes=67043328
        ),
    )(*[s.array for s in specs], grad_all, w_gate, w_up, w_down)
    hidden_all, _, hidden_slice = result[:3]
    return (hidden_all, hidden_slice) + tuple(result[3:])


NT = (((1,), (1,)), ((), ()))
TN = (((0,), (0,)), ((), ()))
NN = (((1,), (0,)), ((), ()))


def backward_kernel(nf, specs, *refs):
    n = len(specs)
    (
        attended,
        dh2_moe,
        grad_prob,
        probs,
        router,
        x_in,
        x_mid,
        gains,
        grad_out,
        wo_hbm,
        wq_hbm,
        wkv_hbm,
        q_raw,
        k_raw,
        q_rot,
        keys,
        values,
        bias,
        lse,
        trig,
        out_part,
        xs_hbm,
        de_hbm,
        act_hbm,
        dg_hbm,
        du_hbm,
    ), refs = refs[:26], refs[26:]
    gathered, grad_in, block_out, refs = refs[:n], refs[n], refs[n + 1], refs[n + 2 :]
    (gate_out, up_out, down_out), refs = refs[:3], refs[3:]
    stage, refs = refs[:n], refs[n:]
    (recv, send, local), refs = refs[:3], refs[3:]
    (
        w_big,
        w_kv,
        dx1,
        dh2,
        d_out,
        d_out_slices,
        d_attn,
        d_query,
        d_rest,
        tail,
        dk_acc,
        dv_acc,
        qk_acc,
        kv_send,
        kv_recv,
        dh1,
        dh1_side,
        qk_side,
        row_sum,
        w_sem,
        kv_sem,
        side_send,
        side_recv,
        sum_own,
        sum_total,
        sum_bufs,
        sum_sems,
    ) = refs[:25] + (refs[25:30], refs[30:41])
    act, dg, du, x_tile, d_tile, gate_tile, up_tile, down_tile, e_sem, t_sem, o_sem = refs[41:]
    f32, bf16 = jnp.float32, jnp.bfloat16
    f, c, t = lax.axis_index("fsdp"), lax.axis_index("ctx"), lax.axis_index("tp")
    partner, side = (f, 1 - c, t), (f, c, 1 - t)
    tokens, width = x_in.shape
    experts = probs.shape[1]
    scale = HEAD_SIZE ** (-0.5)

    barrier = pltpu.get_barrier_semaphore()

    def greet(d, carry):
        pl.semaphore_signal(
            barrier, 1, device_id=(lax.rem(f + d, nf), c, t), device_id_type=MESH
        )
        return carry

    lax.fori_loop(1, nf, greet, 0)
    for dev in (partner, side):
        pl.semaphore_signal(barrier, 1, device_id=dev, device_id_type=MESH)
    pl.semaphore_wait(barrier, nf + 1)

    ins = (attended, d_query, d_rest, tail, d_out_slices)
    start, run, land, start_direct, run_direct, drain, step_of, edge_of, _ = gather_engine(
        nf, specs, ins, gathered, stage, recv, send, local
    )
    early, late = (0,), (1, 2, 3)
    kv_width = dk_acc.shape[1]
    nz = nf // 2
    order = visit_code(nz, f // 2)
    own_loads, to_partner, to_side, to_across, along, finish_sum, drain_sum = token_sum(
        nf, out_part, sum_own, sum_total, sum_bufs, sum_sems
    )
    for cp in own_loads:
        cp.start()
    lax.fori_loop(0, nz, lambda i, carry: to_partner(visit(order, nz, i), carry), 0)
    start((0,))

    def load(src, dst, i):
        return pltpu.make_async_copy(src, dst, w_sem.at[i])

    kept_loads = [
        pltpu.make_async_copy(src, dst, e_sem.at[i])
        for i, (src, dst) in enumerate(((act_hbm, act), (dg_hbm, dg), (du_hbm, du)))
    ]
    span = x_tile.shape[2]
    tiles = width // span
    pieces = act.shape[0] * tiles

    def tile_at(p):
        return p // tiles, pl.ds(pl.multiple_of(lax.rem(p, tiles) * span, span), span)

    def tile_loads(p):
        j, cols = tile_at(p)
        slot = lax.rem(p, 2)
        return (
            pltpu.make_async_copy(xs_hbm.at[j, :, cols], x_tile.at[slot], t_sem.at[0, slot]),
            pltpu.make_async_copy(de_hbm.at[j, :, cols], d_tile.at[slot], t_sem.at[1, slot]),
        )

    def tile_stores(p):
        j, cols = tile_at(p)
        slot = lax.rem(p, 2)
        return (
            pltpu.make_async_copy(gate_tile.at[slot], gate_out.at[j, cols], o_sem.at[0, slot]),
            pltpu.make_async_copy(up_tile.at[slot], up_out.at[j, cols], o_sem.at[1, slot]),
            pltpu.make_async_copy(down_tile.at[slot], down_out.at[j, :, cols], o_sem.at[2, slot]),
        )

    def piece(p, carry):
        j, _ = tile_at(p)
        slot = lax.rem(p, 2)
        for cp in tile_loads(p):
            cp.wait()

        @pl.when(p + 1 < pieces)
        def _():
            for cp in tile_loads(p + 1):
                cp.start()

        @pl.when(p >= 2)
        def _():
            for cp in tile_stores(p - 2):
                cp.wait()

        rows = x_tile[slot]
        gate_tile[slot] = lax.dot_general(rows, dg[j], TN, preferred_element_type=f32).astype(bf16)
        up_tile[slot] = lax.dot_general(rows, du[j], TN, preferred_element_type=f32).astype(bf16)
        down_tile[slot] = lax.dot_general(
            act[j], d_tile[slot], TN, preferred_element_type=f32
        ).astype(bf16)
        for cp in tile_stores(p):
            cp.start()
        return carry

    load(wo_hbm, w_big, 0).start()
    for cp in kept_loads:
        cp.start()
    for cp in tile_loads(0):
        cp.start()
    load(wkv_hbm, w_kv, 1).start()

    d_rest[...] = jnp.zeros_like(d_rest)
    pr = probs[...]
    gp = grad_prob[...]
    dl = (pr * (gp - jnp.sum(pr * gp, axis=1, keepdims=True))).astype(bf16)
    d_rest[:, 2 * kv_width : 2 * kv_width + experts] = dl
    tile = 512
    for k in range(width // tile):
        cols = slice(k * tile, (k + 1) * tile)
        dh2[:, cols] = dh2_moe[:, cols] + lax.dot_general(
            dl, router[:, cols], NN, preferred_element_type=f32
        )
    gain_one, gain_two = gains[0:1, :], gains[1:2, :]
    gain_query, gain_key = gains[2:3, :HEAD_SIZE], gains[2:3, HEAD_SIZE : 2 * HEAD_SIZE]
    row_sum[...] = jnp.zeros_like(row_sum)
    part_rows = 16

    def norm_two(i, carry):
        rows = pl.ds(pl.multiple_of(i * part_rows, part_rows), part_rows)
        x1 = x_mid[rows]
        r2 = lax.rsqrt(jnp.mean(x1 * x1, axis=1, keepdims=True) + eps_norm)
        n2 = x1 * r2
        g = dh2[rows]
        row_sum[1:2, :] += jnp.sum(g * n2, axis=0, keepdims=True)
        scaled = g * gain_two
        mean = jnp.mean(scaled * n2, axis=1, keepdims=True)
        out = grad_out[rows].astype(f32) + r2 * (scaled - n2 * mean)
        dx1[rows] = out
        d_out[rows] = out.astype(bf16)
        return carry

    lax.fori_loop(0, tokens // part_rows, norm_two, 0)
    for cp in own_loads:
        cp.wait()
    lax.fori_loop(0, nz, lambda i, carry: to_side(visit(order, nz, i), carry), 0)
    shard = width // nf
    for k in range(nf):
        d_out_slices[k * tokens : (k + 1) * tokens, :] = d_out[:, k * shard : (k + 1) * shard]

    load(wo_hbm, w_big, 0).wait()
    heads_width = d_attn.shape[1]
    tile = 256
    for k in range(heads_width // tile):
        cols = slice(k * tile, (k + 1) * tile)
        d_attn[:, cols] = lax.dot_general(
            d_out[...], w_big[cols, :], NT, preferred_element_type=f32
        ).astype(bf16)
    load(wq_hbm, w_big, 0).start()
    step_of(1, early)
    to_across(visit(order, nz, 0))
    dk_acc[...] = jnp.zeros_like(dk_acc)
    dv_acc[...] = jnp.zeros_like(dv_acc)
    qk_acc[...] = jnp.zeros_like(qk_acc)
    group = QUERY_HEADS // KEY_VALUE_HEADS

    def unrope(g):
        return g * trig[0] + pltpu.roll(g, HEAD_SIZE // 2, 1) * trig[1]

    def norm_back(g, raw, gain):
        inv = lax.rsqrt(jnp.mean(raw * raw, axis=1, keepdims=True) + eps_norm)
        hat = raw * inv
        scaled = g * gain
        mean = jnp.mean(scaled * hat, axis=1, keepdims=True)
        return jnp.sum(g * hat, axis=0, keepdims=True), inv * (scaled - hat * mean)

    def head(h, carry):
        cols = pl.ds(pl.multiple_of(h * HEAD_SIZE, HEAD_SIZE), HEAD_SIZE)
        kv_cols = pl.ds(pl.multiple_of((h // group) * HEAD_SIZE, HEAD_SIZE), HEAD_SIZE)
        q, key, value, da = q_rot[:, cols], keys[:, kv_cols], values[:, kv_cols], d_attn[:, cols]
        s = lax.dot_general(q, key, NT, preferred_element_type=f32) * scale + bias[...]
        prob = jnp.exp(s - lse[h])
        dp = lax.dot_general(da, value, NT, preferred_element_type=f32)
        delta = jnp.sum(prob * dp, axis=1, keepdims=True)
        ds = (prob * (dp - delta) * scale).astype(bf16)
        dk_acc[:, kv_cols] += lax.dot_general(ds, q, TN, preferred_element_type=f32)
        dv_acc[:, kv_cols] += lax.dot_general(
            prob.astype(bf16), da, TN, preferred_element_type=f32
        )
        dq = unrope(jnp.dot(ds, key, preferred_element_type=f32))
        gain_grad, dq = norm_back(dq, q_raw[:, cols], gain_query)
        qk_acc[0:1, :] += gain_grad
        d_query[:, cols] = dq.astype(bf16)
        return carry

    heads = heads_width // HEAD_SIZE
    lax.fori_loop(0, heads // 2, head, 0)
    to_across(visit(order, nz, 1))
    step_of(2, early)
    lax.fori_loop(heads // 2, heads, head, 0)

    theirs = pl.ds(pl.multiple_of((1 - c) * tokens, tokens), tokens)
    mine = pl.ds(pl.multiple_of(c * tokens, tokens), tokens)
    kv_send[:, :kv_width] = dk_acc[theirs].astype(bf16)
    kv_send[:, kv_width:] = dv_acc[theirs].astype(bf16)
    swap_kv = pltpu.make_async_remote_copy(
        src_ref=kv_send,
        dst_ref=kv_recv,
        send_sem=kv_sem.at[0],
        recv_sem=kv_sem.at[1],
        device_id=partner,
        device_id_type=MESH,
    )
    swap_kv.start()
    start((1,))
    start_direct()
    swap_kv.wait()
    for kv in range(kv_width // HEAD_SIZE):
        cols = slice(kv * HEAD_SIZE, (kv + 1) * HEAD_SIZE)
        g = dk_acc[mine, cols] + kv_recv[:, cols].astype(f32)
        gain_grad, dk = norm_back(unrope(g), k_raw[:, cols], gain_key)
        qk_acc[1:2, :] += gain_grad
        d_rest[:, cols] = dk.astype(bf16)
    d_rest[:, kv_width : 2 * kv_width] = (dv_acc[mine] + kv_recv[:, kv_width:].astype(f32)).astype(bf16)
    start((2,))
    to_across(visit(order, nz, 2))
    along(visit(order, nz, 0))

    def to_side(src, dst, i):
        return pltpu.make_async_remote_copy(
            src_ref=src,
            dst_ref=dst,
            send_sem=side_send.at[i],
            recv_sem=side_recv.at[i],
            device_id=side,
            device_id_type=MESH,
        )

    swap_qk = to_side(qk_acc, qk_side, 4)
    swap_qk.start()
    load(wq_hbm, w_big, 0).wait()
    load(wkv_hbm, w_kv, 1).wait()
    quarter = width // 4

    def dh1_copy(i):
        cols = pl.ds(i * quarter, quarter)
        return to_side(dh1.at[:, cols], dh1_side.at[:, cols], i)

    for k in range(width // tile):
        rows = slice(k * tile, (k + 1) * tile)
        total = lax.dot_general(d_query[...], w_big[rows, :], NT, preferred_element_type=f32)
        total = total + lax.dot_general(
            d_rest[:, : 2 * kv_width], w_kv[rows, :], NT, preferred_element_type=f32
        )
        dh1[:, rows] = total.astype(bf16)
        if (k + 1) * tile % quarter == 0:
            dh1_copy((k + 1) * tile // quarter - 1).start()
    to_across(visit(order, nz, 3))
    step_of(3, early)
    along(visit(order, nz, 1))
    for i in range(4):
        dh1_copy(i).wait_recv()
    swap_qk.wait_recv()

    def norm_one(i, carry):
        rows = pl.ds(pl.multiple_of(i * part_rows, part_rows), part_rows)
        x0 = x_in[rows].astype(f32)
        r1 = lax.rsqrt(jnp.mean(x0 * x0, axis=1, keepdims=True) + eps_norm)
        n1 = x0 * r1
        g = dh1[rows].astype(f32) + dh1_side[rows].astype(f32)
        row_sum[0:1, :] += jnp.sum(g * n1, axis=0, keepdims=True)
        scaled = g * gain_one
        mean = jnp.mean(scaled * n1, axis=1, keepdims=True)
        grad_in[rows] = dx1[rows] + r1 * (scaled - n1 * mean)
        return carry

    lax.fori_loop(0, tokens // part_rows, norm_one, 0)
    lanes = width // 128
    tail[...] = jnp.zeros_like(tail)
    for which in range(2):
        for k in range(lanes):
            row = which * lanes + k
            tail[row : row + 1, :] = row_sum[which : which + 1, k * 128 : (k + 1) * 128]
    tail[2 * lanes : 2 * lanes + 2, :] = qk_acc[0:2, :] + qk_side[0:2, :]
    start((3,))
    for cp in kept_loads:
        cp.wait()

    def stage_at(s, carry):
        lax.fori_loop(s * (pieces // nz), (s + 1) * (pieces // nz), piece, 0)

        @pl.when(s + 1 < nz)
        def _():
            step_of(s + 1, late)

        @pl.when(s == 0)
        def _():
            along(visit(order, nz, 2))
            edge_of(early)

        @pl.when(s == 1)
        def _():
            along(f // 2)

        return carry

    lax.fori_loop(0, nz, stage_at, 0)
    edge_of(late)
    run_direct()
    land()

    def put_out(rows, cols, value):
        block_out[rows, cols] = (x_mid[rows, cols] + value).astype(bf16)

    finish_sum(put_out)
    for p in (pieces - 2, pieces - 1):
        for cp in tile_stores(p):
            cp.wait()
    drain()
    drain_sum()
    for i in range(4):
        dh1_copy(i).wait_send()
    swap_qk.wait_send()


def visit_code(nz, z):
    order = 0
    for at, seq in enumerate(visiting_order(nz)):
        code = sum(u * nz**i for i, u in enumerate(seq))
        order = order + code * (z == at).astype(jnp.int32)
    return order


def visit(code, nz, i):
    for k in range(nz):
        code = jnp.where(i > k, code // nz, code)
    return lax.rem(code, nz)


SUM_CUT = 2


def token_sum(nf, partial, own, total_ref, bufs, sems):
    from_partner, from_side, from_across, from_z, last_half = bufs
    (
        load_sem,
        p_send,
        p_recv,
        y_send,
        y_recv,
        x_send,
        x_recv,
        z_send,
        z_recv,
        s_send,
        s_recv,
    ) = sems
    nz = nf // 2
    f, c, t = lax.axis_index("fsdp"), lax.axis_index("ctx"), lax.axis_index("tp")
    z, x = f // 2, lax.rem(f, 2)
    has_up, has_down = z + 1 < nz, z > 0
    up, down = (f + 2, c, t), (f - 2, c, t)
    across_dev, partner, side = (z * 2 + 1 - x, c, t), (f, 1 - c, t), (f, c, 1 - t)
    tokens, half = total_ref.shape
    rows = tokens // SUM_CUT
    bf16 = jnp.bfloat16
    kept = pl.ds(pl.multiple_of(t * half, half), half)
    given = pl.ds(pl.multiple_of((1 - t) * half, half), half)

    def chunk(q):
        return pl.ds(pl.multiple_of(q * rows, rows), rows)

    def remote(src, dst, send, recv, dev):
        return pltpu.make_async_remote_copy(
            src_ref=src,
            dst_ref=dst,
            send_sem=send,
            recv_sem=recv,
            device_id=dev,
            device_id_type=MESH,
        )

    own_loads = [
        pltpu.make_async_copy(
            partial.at[pl.ds((2 * b + c) * tokens, tokens)], own.at[b], load_sem.at[b]
        )
        for b in range(nf)
    ]

    def p_copy(b, q):
        return remote(
            partial.at[pl.ds((2 * b + 1 - c) * tokens + q * rows, rows)],
            from_partner.at[b, chunk(q)],
            p_send.at[b, q],
            p_recv.at[b, q],
            partner,
        )

    def y_copy(b, q):
        return remote(
            own.at[b, chunk(q), given],
            from_side.at[b, chunk(q)],
            y_send.at[b, q],
            y_recv.at[b, q],
            side,
        )

    def x_copy(u, q):
        return remote(
            own.at[u * 2 + 1 - x, chunk(q), kept],
            from_across.at[u, chunk(q)],
            x_send.at[u, q],
            x_recv.at[u, q],
            across_dev,
        )

    def z_copy(u, q, way, dev):
        return remote(
            own.at[u * 2 + x, chunk(q), kept],
            from_z.at[way, u, chunk(q)],
            z_send.at[u, q],
            z_recv.at[way, u, q],
            dev,
        )

    def s_copy(q):
        return remote(
            own.at[f, chunk(q), kept], last_half.at[chunk(q)], s_send.at[q], s_recv.at[q], side
        )

    def wide(value):
        return value.astype(jnp.float32)

    def to_partner(u, carry):
        for xx in range(2):
            for q in range(SUM_CUT):
                p_copy(u * 2 + xx, q).start()
        return carry

    def to_side(u, carry):
        for xx in range(2):
            b = u * 2 + xx

            @pl.loop(0, SUM_CUT)
            def _(q, b=b):
                p_copy(b, q).wait_recv()
                own[b, chunk(q)] = (
                    wide(own[b, chunk(q)]) + wide(from_partner[b, chunk(q)])
                ).astype(bf16)
                y_copy(b, q).start()
        return carry

    def to_across(u):
        b = u * 2 + 1 - x

        @pl.loop(0, SUM_CUT)
        def _(q):
            y_copy(b, q).wait_recv()
            own[b, chunk(q), kept] = (
                wide(own[b, chunk(q), kept]) + wide(from_side[b, chunk(q)])
            ).astype(bf16)
            x_copy(u, q).start()

    def along(u):
        b = u * 2 + x

        @pl.loop(0, SUM_CUT)
        def _(q):
            y_copy(b, q).wait_recv()
            x_copy(u, q).wait_recv()
            total_ref[chunk(q)] = (
                wide(own[b, chunk(q), kept])
                + wide(from_side[b, chunk(q)])
                + wide(from_across[u, chunk(q)])
            )

            @pl.when((u >= z) & has_down)
            def _():
                z_copy(u, q, 0, partner).wait_recv()
                total_ref[chunk(q)] += wide(from_z[0, u, chunk(q)])

            @pl.when((u <= z) & has_up)
            def _():
                z_copy(u, q, 1, partner).wait_recv()
                total_ref[chunk(q)] += wide(from_z[1, u, chunk(q)])

            own[b, chunk(q), kept] = total_ref[chunk(q)].astype(bf16)

            @pl.when(u > z)
            def _():
                z_copy(u, q, 0, up).start()

            @pl.when(u < z)
            def _():
                z_copy(u, q, 1, down).start()

            @pl.when(u == z)
            def _():
                s_copy(q).start()

    def finish_sum(put):
        @pl.loop(0, SUM_CUT)
        def _(q):
            put(chunk(q), kept, wide(own[f, chunk(q), kept]))
            s_copy(q).wait_recv()
            put(chunk(q), given, wide(last_half[chunk(q)]))

    def drain_sum():
        def ends(u, carry):
            @pl.loop(0, SUM_CUT)
            def _(q):
                for xx in range(2):
                    p_copy(u * 2 + xx, q).wait_send()
                    y_copy(u * 2 + xx, q).wait_send()
                x_copy(u, q).wait_send()

                @pl.when(u != z)
                def _():
                    z_copy(u, q, 0, partner).wait_send()

            return carry

        lax.fori_loop(0, nz, ends, 0)
        for q in range(SUM_CUT):
            s_copy(q).wait_send()

    return own_loads, to_partner, to_side, to_across, along, finish_sum, drain_sum


def backward_pass(nf, arrays, attended, shapes):
    f32, bf16 = jnp.float32, jnp.bfloat16
    tokens, width, heads_width, kv_width, keys = shapes
    tail_rows = -(-(2 * width // 128 + 2) // 8) * 8
    shape = jax.ShapeDtypeStruct
    specs = [
        Gather(attended, nf, chunks=2),
        Gather(shape((tokens, heads_width), bf16), nf, chunks=2),
        Gather(shape((tokens, 2 * kv_width + 128), bf16), nf, chunks=1),
        Gather(shape((tail_rows, 128), f32), nf, chunks=1),
        Gather(shape((nf * tokens, width // nf), bf16), nf, form="a2a", chunks=1),
    ]
    n = len(specs)
    experts, rows, hidden = arrays[-3].shape
    gate_shape, down_shape = (experts, width, hidden), (experts, hidden, width)
    span = 256
    total = sum(s.chunks for s in specs)
    any_spec = pl.BlockSpec(memory_space=pl.ANY)
    vmem = pl.BlockSpec(memory_space=pltpu.VMEM)
    dma = pltpu.SemaphoreType.DMA
    in_any = {0, 9, 10, 11, 20, 21, 22, 23, 24, 25}
    nz = nf // 2
    return pl.pallas_call(
        functools.partial(backward_kernel, nf, tuple(specs)),
        out_shape=tuple(shape(s.out_shape(nf), s.array.dtype) for s in specs)
        + (shape((tokens, width), f32), shape((tokens, width), bf16))
        + tuple(shape(s, bf16) for s in (gate_shape, gate_shape, down_shape)),
        in_specs=[any_spec if i in in_any else vmem for i in range(26)],
        out_specs=tuple([any_spec] * n + [vmem, vmem] + [any_spec] * 3),
        scratch_shapes=[stage_of(s, nf) for s in specs]
        + [dma((2 * nf, total)), dma((5, 2 * nf, total)), dma((2, n))]
        + [
            pltpu.VMEM((width, max(width, heads_width)), bf16),
            pltpu.VMEM((width, 2 * kv_width), bf16),
            pltpu.VMEM((tokens, width), f32),
            pltpu.VMEM((tokens, width), f32),
            pltpu.VMEM((tokens, width), bf16),
            pltpu.VMEM((nf * tokens, width // nf), bf16),
            pltpu.VMEM((tokens, heads_width), bf16),
            pltpu.VMEM((tokens, heads_width), bf16),
            pltpu.VMEM((tokens, 2 * kv_width + 128), bf16),
            pltpu.VMEM((tail_rows, 128), f32),
            pltpu.VMEM((keys, kv_width), f32),
            pltpu.VMEM((keys, kv_width), f32),
            pltpu.VMEM((8, 128), f32),
            pltpu.VMEM((tokens, 2 * kv_width), bf16),
            pltpu.VMEM((tokens, 2 * kv_width), bf16),
            pltpu.VMEM((tokens, width), bf16),
            pltpu.VMEM((tokens, width), bf16),
            pltpu.VMEM((8, 128), f32),
            pltpu.VMEM((2, width), f32),
            dma((2,)),
            dma((2,)),
            dma((5,)),
            dma((5,)),
            pltpu.VMEM((nf, tokens, width), bf16),
            pltpu.VMEM((tokens, width // 2), f32),
            pltpu.VMEM((nf, tokens, width), bf16),
            pltpu.VMEM((nf, tokens, width // 2), bf16),
            pltpu.VMEM((nz, tokens, width // 2), bf16),
            pltpu.VMEM((2, nz, tokens, width // 2), bf16),
            pltpu.VMEM((tokens, width // 2), bf16),
            dma((nf,)),
            dma((nf, SUM_CUT)),
            dma((nf, SUM_CUT)),
            dma((nf, SUM_CUT)),
            dma((nf, SUM_CUT)),
            dma((nz, SUM_CUT)),
            dma((nz, SUM_CUT)),
            dma((nz, SUM_CUT)),
            dma((2, nz, SUM_CUT)),
            dma((SUM_CUT,)),
            dma((SUM_CUT,)),
            pltpu.VMEM((experts, rows, hidden), bf16),
            pltpu.VMEM((experts, rows, hidden), bf16),
            pltpu.VMEM((experts, rows, hidden), bf16),
            pltpu.VMEM((2, rows, span), bf16),
            pltpu.VMEM((2, rows, span), bf16),
            pltpu.VMEM((2, span, hidden), bf16),
            pltpu.VMEM((2, span, hidden), bf16),
            pltpu.VMEM((2, hidden, span), bf16),
            dma((3,)),
            dma((2, 2)),
            dma((3, 2)),
        ],
        compiler_params=pltpu.CompilerParams(
            collective_id=8, has_side_effects=True, vmem_limit_bytes=67043328
        ),
    )(attended, *arrays)


def forward_kernel(nf, specs, *refs):
    n = len(specs)
    ins, refs = refs[:n], refs[n:]
    (x_in, segments, routed, trig), refs = refs[:4], refs[4:]
    gathered, refs = refs[:n], refs[n:]
    (
        hidden,
        hidden_slices,
        marks,
        probs,
        x_mid,
        attended,
        q_raw,
        k_raw,
        q_rot,
        keys,
        values,
        bias,
        lse,
        gains,
        router,
    ), refs = refs[:15], refs[15:]
    stage, refs = refs[:n], refs[n:]
    (recv, send, local), refs = refs[:3], refs[3:]
    (
        w_big,
        w_kv,
        small,
        hidden_one,
        kv_all,
        part,
        part_side,
        square,
        w_sem,
        kv_sem,
        side_send,
        side_recv,
    ) = refs
    f32, bf16 = jnp.float32, jnp.bfloat16
    nz = nf // 2
    f, c, t = lax.axis_index("fsdp"), lax.axis_index("ctx"), lax.axis_index("tp")
    z, x = f // 2, lax.rem(f, 2)
    partner, side = (f, 1 - c, t), (f, c, 1 - t)
    has_up, has_down = z + 1 < nz, z > 0
    tokens, width = x_in.shape
    experts = routed.shape[1]
    heads_width = q_raw.shape[1]
    kv_width = k_raw.shape[1]
    scale = HEAD_SIZE ** (-0.5)
    barrier = pltpu.get_barrier_semaphore()

    def greet(dev):
        pl.semaphore_signal(barrier, 1, device_id=dev, device_id_type=MESH)

    for dev in (partner, side, (z * 2 + 1 - x, c, t)):
        greet(dev)

    @pl.when(has_up)
    def _():
        greet((f + 2, c, t))

    @pl.when(has_down)
    def _():
        greet((f - 2, c, t))

    pl.semaphore_wait(barrier, 3 + has_up.astype(jnp.int32) + has_down.astype(jnp.int32))
    start, _, _, _, _, drain, step_of, edge_of, land_of = gather_engine(
        nf, specs, ins, gathered, stage, recv, send, local
    )
    first, second, third = (0, 1, 2), (3,), (4,)
    start(first)

    def first_step(k, carry):
        step_of(k, first)
        return carry

    lax.fori_loop(1, nz, first_step, 0)
    start(second)
    edge_of(first)
    land_of(first)

    def load(src, dst, i):
        return pltpu.make_async_copy(src, dst, w_sem.at[i])

    small_load = load(gathered[0], small, 2)
    small_load.start()
    load(gathered[2], w_kv, 1).start()
    load(gathered[1], w_big, 0).start()
    small_load.wait()

    size = specs[0].rows
    halves = width // nf // 128
    qk_sum = [jnp.zeros((1, 128), f32), jnp.zeros((1, 128), f32)]
    for k in range(nf):
        base = 2 * k * size
        for h in range(halves):
            cols = slice((k * halves + h) * 128, (k * halves + h + 1) * 128)
            router[:, cols] = small[base + h * experts : base + (h + 1) * experts, :]
            at = base + halves * experts
            for g in range(2):
                row = at + g * halves + h
                gains[g : g + 1, cols] = small[row : row + 1, :].astype(f32)
        at = base + halves * experts + 2 * halves
        for h in range(2):
            qk_sum[h] = qk_sum[h] + small[at + h : at + h + 1, :].astype(f32)
    gains[2:3, :] = jnp.zeros((1, width), f32)
    for h in range(2):
        gains[2:3, h * 128 : (h + 1) * 128] = qk_sum[h]
    gain_one, gain_two = gains[0:1, :], gains[1:2, :]
    gain_query, gain_key = qk_sum
    part_rows = 16

    def norm_one(i, carry):
        rows = pl.ds(pl.multiple_of(i * part_rows, part_rows), part_rows)
        x0 = x_in[rows].astype(f32)
        r1 = lax.rsqrt(jnp.mean(x0 * x0, axis=1, keepdims=True) + eps_norm)
        hidden_one[rows] = (x0 * r1 * gain_one).astype(bf16)
        return carry

    lax.fori_loop(0, tokens // part_rows, norm_one, 0)
    shard = width // nf
    for k in range(nf):
        hidden_slices[k * tokens : (k + 1) * tokens, :] = hidden_one[:, k * shard : (k + 1) * shard]

    def norm_rope(raw, gain):
        inv = lax.rsqrt(jnp.mean(raw * raw, axis=1, keepdims=True) + eps_norm)
        normed = raw * inv * gain
        turned = normed * trig[0] - pltpu.roll(normed, HEAD_SIZE // 2, 1) * trig[1]
        return turned.astype(bf16)

    load(gathered[2], w_kv, 1).wait()
    mine = pl.ds(pl.multiple_of(c * tokens, tokens), tokens)
    k_raw[...] = jnp.dot(
        hidden_one[...], w_kv[:, :kv_width], preferred_element_type=f32
    )
    kv_all[mine, kv_width : 2 * kv_width] = jnp.dot(
        hidden_one[...], w_kv[:, kv_width:], preferred_element_type=f32
    ).astype(bf16)
    for kv in range(kv_width // HEAD_SIZE):
        cols = slice(kv * HEAD_SIZE, (kv + 1) * HEAD_SIZE)
        kv_all[mine, cols] = norm_rope(k_raw[:, cols], gain_key)
    kv_all[mine, 2 * kv_width :] = segments[...]
    swap_kv = pltpu.make_async_remote_copy(
        src_ref=kv_all.at[mine],
        dst_ref=kv_all.at[mine],
        send_sem=kv_sem.at[0],
        recv_sem=kv_sem.at[1],
        device_id=partner,
        device_id_type=MESH,
    )
    swap_kv.start()
    step_of(1, second)
    load(gathered[1], w_big, 0).wait()
    tile = 256
    for k in range(heads_width // tile):
        cols = slice(k * tile, (k + 1) * tile)
        q_raw[:, cols] = jnp.dot(hidden_one[...], w_big[:, cols], preferred_element_type=f32)
    swap_kv.wait()
    keys[...] = kv_all[:, :kv_width]
    values[...] = kv_all[:, kv_width : 2 * kv_width]
    span = kv_all.shape[0]
    theirs = jnp.transpose(kv_all[:, 2 * kv_width :].astype(f32))
    own = segments[...].astype(f32)
    query_at = c * tokens + lax.broadcasted_iota(jnp.int32, (tokens, 128), 0)
    for h in range(span // 128):
        cols = slice(h * 128, (h + 1) * 128)
        key_at = h * 128 + lax.broadcasted_iota(jnp.int32, (tokens, 128), 1)
        allowed = (key_at <= query_at) & (theirs[:, cols] == own)
        bias[:, cols] = jnp.where(allowed, 0.0, -jnp.inf)
    step_of(2, second)
    start(third)
    group = QUERY_HEADS // KEY_VALUE_HEADS

    def head(h, carry):
        cols = pl.ds(pl.multiple_of(h * HEAD_SIZE, HEAD_SIZE), HEAD_SIZE)
        kv_cols = pl.ds(pl.multiple_of((h // group) * HEAD_SIZE, HEAD_SIZE), HEAD_SIZE)
        q = norm_rope(q_raw[:, cols], gain_query)
        q_rot[:, cols] = q
        s = lax.dot_general(q, keys[:, kv_cols], NT, preferred_element_type=f32) * scale
        s = s + bias[...]
        top = jnp.max(s, axis=1, keepdims=True)
        total = top + jnp.log(jnp.sum(jnp.exp(s - top), axis=1, keepdims=True))
        lse[h] = total
        prob = jnp.exp(s - total).astype(bf16)
        attended[:, cols] = jnp.dot(
            prob, values[:, kv_cols], preferred_element_type=f32
        ).astype(bf16)
        return carry

    heads = heads_width // HEAD_SIZE
    lax.fori_loop(0, heads // 2, head, 0)
    step_of(3, second)
    lax.fori_loop(heads // 2, heads, head, 0)
    edge_of(second)
    land_of(second)
    load(gathered[3], w_big, 0).start()
    step_of(1, third)
    load(gathered[3], w_big, 0).wait()
    quarter = width // 4

    def side_copy(i):
        cols = pl.ds(i * quarter, quarter)
        return pltpu.make_async_remote_copy(
            src_ref=part.at[:, cols],
            dst_ref=part_side.at[:, cols],
            send_sem=side_send.at[i],
            recv_sem=side_recv.at[i],
            device_id=side,
            device_id_type=MESH,
        )

    for k in range(width // tile):
        cols = slice(k * tile, (k + 1) * tile)
        part[:, cols] = jnp.dot(
            attended[...], w_big[:, cols], preferred_element_type=f32
        ).astype(bf16)
        if (k + 1) * tile % quarter == 0:
            side_copy((k + 1) * tile // quarter - 1).start()
    step_of(2, third)
    for i in range(4):
        side_copy(i).wait_recv()

    def norm_two(i, carry):
        rows = pl.ds(pl.multiple_of(i * part_rows, part_rows), part_rows)
        x1 = x_in[rows].astype(f32) + (part[rows].astype(f32) + part_side[rows].astype(f32))
        x_mid[rows] = x1
        r2 = lax.rsqrt(jnp.mean(x1 * x1, axis=1, keepdims=True) + eps_norm)
        hidden[rows] = (x1 * r2 * gain_two).astype(bf16)
        return carry

    lax.fori_loop(0, tokens // part_rows, norm_two, 0)
    logits = lax.dot_general(hidden[...], router[...], NT, preferred_element_type=f32)
    on = routed[...] > 0.0
    kept = jnp.where(on, logits, -jnp.inf)
    raised = jnp.where(on, jnp.exp(kept - jnp.max(kept, axis=1, keepdims=True)), 0.0)
    shares = raised / jnp.sum(raised, axis=1, keepdims=True)
    probs[...] = shares
    square[...] = jnp.zeros_like(square)
    square[:, :experts] = jnp.where(on, shares, -1.0)
    marks[...] = jnp.transpose(square[...])[:experts, :]
    step_of(3, third)
    edge_of(third)
    land_of(third)
    drain()
    for i in range(4):
        side_copy(i).wait_send()


def forward_pass(nf, arrays, operands, shapes):
    f32, bf16 = jnp.float32, jnp.bfloat16
    small, w_query, kv_projection, w_out, grad_out = arrays
    tokens, width, heads_width, kv_width, experts = shapes
    specs = [
        Gather(small, nf, chunks=1),
        Gather(w_query, nf, half=True, chunks=2),
        Gather(kv_projection, nf, half=True, chunks=1),
        Gather(w_out, nf, form="col", half=True, chunks=2),
        Gather(grad_out, nf, chunks=2),
    ]
    n = len(specs)
    total = sum(s.chunks for s in specs)
    any_spec = pl.BlockSpec(memory_space=pl.ANY)
    vmem = pl.BlockSpec(memory_space=pltpu.VMEM)
    dma = pltpu.SemaphoreType.DMA
    shape = jax.ShapeDtypeStruct
    span = 2 * tokens
    made = [
        shape((tokens, width), bf16),
        shape((nf * tokens, width // nf), bf16),
        shape((experts, tokens), f32),
        shape((tokens, experts), f32),
        shape((tokens, width), f32),
        shape((tokens, heads_width), bf16),
        shape((tokens, heads_width), f32),
        shape((tokens, kv_width), f32),
        shape((tokens, heads_width), bf16),
        shape((span, kv_width), bf16),
        shape((span, kv_width), bf16),
        shape((tokens, span), f32),
        shape((heads_width // HEAD_SIZE, tokens, 1), f32),
        shape((3, width), f32),
        shape((experts, width), bf16),
    ]
    return pl.pallas_call(
        functools.partial(forward_kernel, nf, tuple(specs)),
        out_shape=tuple(shape(s.out_shape(nf), s.array.dtype) for s in specs) + tuple(made),
        in_specs=[any_spec] * n + [vmem] * 4,
        out_specs=tuple([any_spec] * n + [vmem] * len(made)),
        scratch_shapes=[stage_of(s, nf) for s in specs]
        + [dma((2 * nf, total)), dma((5, 2 * nf, total)), dma((2, n))]
        + [
            pltpu.VMEM((width, max(width, heads_width)), bf16),
            pltpu.VMEM((width, 2 * kv_width), bf16),
            pltpu.VMEM(specs[0].out_shape(nf), bf16),
            pltpu.VMEM((tokens, width), bf16),
            pltpu.VMEM((span, 2 * kv_width + 128), bf16),
            pltpu.VMEM((tokens, width), bf16),
            pltpu.VMEM((tokens, width), bf16),
            pltpu.VMEM((tokens, 128), f32),
            dma((3,)),
            dma((2,)),
            dma((4,)),
            dma((4,)),
        ],
        compiler_params=pltpu.CompilerParams(
            collective_id=9, has_side_effects=True, vmem_limit_bytes=67043328
        ),
    )(*arrays, *operands)


def norm_forward(values, gain_row):
    inverse = lax.rsqrt(jnp.mean(values * values, axis=-1, keepdims=True) + eps_norm)
    normed = values * inverse
    return (normed * gain_row, normed, inverse)


def rms_norm_gradient(grad_scaled, normed, inverse, gain_row):
    grad_normed = grad_scaled * gain_row
    inner_mean = jnp.mean(grad_normed * normed, axis=-1, keepdims=True)
    return inverse * (grad_normed - normed * inner_mean)


def rope_tables(positions):
    half_dim = HEAD_SIZE // 2
    frequencies = rope_base ** (-(jnp.arange(half_dim, dtype=jnp.float32) * 2.0) / HEAD_SIZE)
    angles = positions.astype(jnp.float32)[:, None] * frequencies[None, :]
    return (jnp.cos(angles)[:, None, :], jnp.sin(angles)[:, None, :])


def rotate(values, cosine_table, sine_values):
    half_dim = values.shape[-1] // 2
    first_half = values[..., :half_dim]
    second_half = values[..., half_dim:]
    return jnp.concatenate(
        [
            first_half * cosine_table - second_half * sine_values,
            second_half * cosine_table + first_half * sine_values,
        ],
        axis=-1,
    )


def inverse_rotation(grad_in_rot, cosine_table, sine_values):
    half_dim = grad_in_rot.shape[-1] // 2
    first_half = grad_in_rot[..., :half_dim]
    second_half = grad_in_rot[..., half_dim:]
    return jnp.concatenate(
        [
            first_half * cosine_table + second_half * sine_values,
            second_half * cosine_table - first_half * sine_values,
        ],
        axis=-1,
    )


def masked_scores(query_rotated, key_rotated, allowed):
    scores = jnp.einsum(
        "qkgd,skd->kgqs", query_rotated, key_rotated, preferred_element_type=jnp.float32
    ) * HEAD_SIZE ** (-0.5)
    return jnp.where(allowed[None, None], scores, -jnp.inf)


def swap(value, axis_name):
    return lax.ppermute(value, axis_name, [(0, 1), (1, 0)])


def sum_over_tp(value):
    mine = value.astype(jnp.bfloat16)
    return mine.astype(jnp.float32) + swap(mine, "tp").astype(jnp.float32)


def block_sum(partial, nf):
    return lax.psum_scatter(partial, ("fsdp", "ctx"), scatter_dimension=0, tiled=True)


def by_shard(rows, nf):
    count, width = rows.shape
    return rows.reshape(count, nf, width // nf).transpose(1, 0, 2).reshape(nf * count, width // nf)


def on_device(
    hidden_in,
    segment_ids,
    routes,
    attn_gain,
    qk_gains,
    w_query,
    key_projection,
    value_projection,
    w_out,
    ffn_gain,
    w_router,
    w_gate,
    w_up,
    w_down,
    grad_out,
):
    tokens_dev, width_dim = hidden_in.shape
    nf = lax.axis_size("fsdp")
    devices = nf * lax.axis_size("ctx")
    local_experts = w_gate.shape[0]
    experts = local_experts * devices
    capacity = max(2, 2 * tokens_dev * TOPK // experts)
    query_group_width = QUERY_HEADS // KEY_VALUE_HEADS
    shard_width = attn_gain.shape[0]
    f_index, c_index = lax.axis_index("fsdp"), lax.axis_index("ctx")
    bf16 = jnp.bfloat16
    f32 = jnp.float32

    if nf == 8:
        halves = shard_width // 128
        turned = w_router.T.reshape(experts, halves, 128).transpose(1, 0, 2).reshape(-1, 128)
        qk_row = lax.dynamic_update_slice(
            jnp.zeros((256,), bf16), qk_gains, (f_index * qk_gains.shape[0],)
        )
        small = jnp.concatenate(
            [
                turned,
                attn_gain.reshape(-1, 128),
                ffn_gain.reshape(-1, 128),
                qk_row.reshape(-1, 128),
            ]
        )
        small = jnp.pad(small, ((0, -small.shape[0] % 16), (0, 0)))
        own_positions = c_index * tokens_dev + jnp.arange(tokens_dev, dtype=jnp.int32)
        cosine_table, sine_values = rope_tables(own_positions)
        cosine_row, sine_row = cosine_table[:, 0], sine_values[:, 0]
        trig = jnp.stack(
            [
                jnp.concatenate([cosine_row, cosine_row], axis=1),
                jnp.concatenate([sine_row, -sine_row], axis=1),
            ]
        )
        segment_wide = jnp.broadcast_to(segment_ids.astype(bf16)[:, None], (tokens_dev, 128))
        expert_ids = jnp.arange(experts, dtype=jnp.int32)
        hits = routes[:, :, None] == expert_ids[None, None, :]
        routed = jnp.any(hits, axis=1).astype(f32)
        heads_width, kv_width = w_query.shape[1], key_projection.shape[1]
        kv_projection = jnp.concatenate([key_projection, value_projection], axis=1)
        shapes = (tokens_dev, width_dim, heads_width, kv_width, experts)
        (
            _,
            query_weight,
            kv_weight,
            out_weight,
            grad_all,
            hidden_two,
            hidden_slices,
            marks,
            probs,
            resid_mid,
            attended,
            query_raw,
            key_projected,
            query_rotated,
            key_all,
            value_all,
            bias,
            log_total,
            gains,
            router_rows,
        ) = forward_pass(
            nf,
            (small, w_query, kv_projection, w_out, grad_out),
            (hidden_in, segment_wide, routed, trig),
            shapes,
        )
    else:
        pieces = [w_router.reshape(-1), attn_gain, ffn_gain, qk_gains]
        flat = jnp.concatenate(pieces)
        small_rows = -(-flat.shape[0] // 2048) * 16
        small = jnp.pad(flat, (0, small_rows * 128 - flat.shape[0])).reshape(small_rows, 128)
        out_form = "row" if shard_width % 128 else "col"
        small_all, query_weight, key_weight, value_weight, out_weight, grad_all = plane_gather(
            [
                Gather(small, nf, chunks=1),
                Gather(w_query, nf, half=True, chunks=2),
                Gather(key_projection, nf, half=True, chunks=1),
                Gather(value_projection, nf, half=True, chunks=1),
                Gather(w_out, nf, form=out_form, half=True, chunks=2),
                Gather(grad_out, nf, rep=True, chunks=4),
            ],
            1,
            nf,
        )
        if out_form == "row":
            out_weight = out_weight.reshape(nf, -1, shard_width).transpose(1, 0, 2)
            out_weight = out_weight.reshape(-1, width_dim)
        small_all = small_all.reshape(nf, 2, small_rows * 128)[:, 0]
        ends = [0]
        for piece in pieces:
            ends.append(ends[-1] + piece.shape[0])
        router_weight = small_all[:, ends[0] : ends[1]].reshape(width_dim, experts)
        gain_one = small_all[:, ends[1] : ends[2]].reshape(-1).astype(f32)
        gain_two = small_all[:, ends[2] : ends[3]].reshape(-1).astype(f32)
        gain_qk = small_all[:, ends[3] : ends[4]].reshape(-1).astype(f32)
        gain_query, gain_key = gain_qk[:HEAD_SIZE], gain_qk[HEAD_SIZE:]

        kv_local = key_weight.shape[1] // HEAD_SIZE
        head_local = query_weight.shape[1] // HEAD_SIZE
        resid = hidden_in.astype(f32)
        scaled_one, normed_one, inverse_one = norm_forward(resid, gain_one)
        hidden_first = scaled_one.astype(bf16)
        query_raw = jnp.dot(hidden_first, query_weight, preferred_element_type=f32).reshape(
            tokens_dev, head_local, HEAD_SIZE
        )
        key_projected = jnp.dot(hidden_first, key_weight, preferred_element_type=f32).reshape(
            tokens_dev, kv_local, HEAD_SIZE
        )
        value_rows = jnp.dot(hidden_first, value_weight, preferred_element_type=f32).astype(bf16)
        query_normed, query_hat, query_inverse = norm_forward(query_raw, gain_query)
        key_normed, key_unit_rows, key_inverse_norm = norm_forward(key_projected, gain_key)
        own_positions = c_index * tokens_dev + jnp.arange(tokens_dev, dtype=jnp.int32)
        cosine_table, sine_values = rope_tables(own_positions)
        query_rotated = (
            rotate(query_normed, cosine_table, sine_values)
            .astype(bf16)
            .reshape(tokens_dev, kv_local, query_group_width, HEAD_SIZE)
        )
        key_rotated = rotate(key_normed, cosine_table, sine_values).astype(bf16)
        own_segments = segment_ids.astype(bf16)
        packed_kv = jnp.concatenate(
            [
                key_rotated.reshape(tokens_dev, -1),
                value_rows,
                jnp.broadcast_to(own_segments[:, None], (tokens_dev, 128)),
            ],
            axis=1,
        )
        kv_all = lax.all_gather(packed_kv, "ctx", axis=0, tiled=True)
        kv_width = kv_local * HEAD_SIZE
        key_all = kv_all[:, :kv_width].reshape(-1, kv_local, HEAD_SIZE)
        value_all = kv_all[:, kv_width : 2 * kv_width].reshape(-1, kv_local, HEAD_SIZE)
        segment_all = kv_all[:, 2 * kv_width]
        key_positions = jnp.arange(key_all.shape[0], dtype=jnp.int32)
        allowed = (key_positions[None, :] <= own_positions[:, None]) & (
            segment_all[None, :] == own_segments[:, None]
        )
        scores = masked_scores(query_rotated, key_all, allowed)
        top_score = jnp.max(scores, axis=-1, keepdims=True)
        log_total = top_score + jnp.log(jnp.sum(jnp.exp(scores - top_score), axis=-1, keepdims=True))
        weights_att = jnp.exp(scores - log_total).astype(bf16)
        attended = jnp.einsum("kgqs,skd->qkgd", weights_att, value_all, preferred_element_type=f32)
        attended = attended.astype(bf16).reshape(tokens_dev, head_local * HEAD_SIZE)
        out_partial = jnp.dot(attended, out_weight, preferred_element_type=f32)
        resid_mid = resid + sum_over_tp(out_partial)
        scaled_two, normed_two, inverse_two = norm_forward(resid_mid, gain_two)
        hidden_two = scaled_two.astype(bf16)
        logits = jnp.dot(hidden_two, router_weight, preferred_element_type=f32)
        expert_ids = jnp.arange(experts, dtype=jnp.int32)
        hits = routes[:, :, None] == expert_ids[None, None, :]
        routed = jnp.any(hits, axis=1)
        masked_logits = jnp.where(routed, logits, -jnp.inf)
        raised = jnp.where(
            routed, jnp.exp(masked_logits - jnp.max(masked_logits, axis=1, keepdims=True)), 0.0
        )
        probs = raised / jnp.sum(raised, axis=1, keepdims=True)
        marks = jnp.where(routed, probs, -1.0).T
    if nf == 8:
        (
            hidden_all,
            hidden_first_slice,
            moe_partial,
            rows_in,
            grad_prod,
            activated,
            grad_gate_pre,
            grad_up_pre,
            grad_hidden_moe,
            grad_prob,
        ) = expert_pass(
            hidden_two,
            marks,
            hidden_slices,
            grad_all,
            w_gate,
            w_up,
            w_down,
            capacity,
            nf,
        )
        grad_prob = grad_prob.reshape(devices, 8, tokens_dev)[:, :local_experts]
        grad_prob = grad_prob.reshape(experts, tokens_dev).T
    else:
        hidden_all, marks_all, hidden_first_slice = plane_gather(
            [
                Gather(hidden_two, nf, rep=True, chunks=4),
                Gather(marks, nf, chunks=1),
                Gather(by_shard(hidden_first, nf), nf, form="a2a", chunks=1),
            ],
            2,
            nf,
        )
        first_expert = (f_index * 2 + c_index) * local_experts
        marks_here = lax.dynamic_slice_in_dim(
            marks_all.reshape(devices, experts, tokens_dev), first_expert, local_experts, axis=1
        )
        taken = marks_here >= 0.0
        ranks = jnp.cumsum(taken.astype(jnp.int32), axis=2) - 1
        slots = jnp.arange(capacity, dtype=jnp.int32)
        chosen = taken[:, :, None, :] & (ranks[:, :, None, :] == slots[None, None, :, None])
        pick = chosen.astype(bf16)
        weight_slot = jnp.sum(jnp.where(chosen, marks_here[:, :, None, :], 0.0), axis=3)
        weight_slot = weight_slot.transpose(1, 0, 2).reshape(local_experts, devices * capacity)

        def select(rows):
            blocks = rows.reshape(devices, tokens_dev, width_dim)
            out = jnp.einsum("bjst,btd->jbsd", pick, blocks, preferred_element_type=f32)
            return out.astype(bf16).reshape(local_experts, devices * capacity, width_dim)

        def spread(rows):
            blocks = rows.reshape(local_experts, devices, capacity, width_dim)
            out = jnp.einsum("bjst,jbsd->btd", pick, blocks, preferred_element_type=f32)
            return out.astype(bf16).reshape(devices * tokens_dev, width_dim)

        rows_in = select(hidden_all)
        grad_rows_in = select(grad_all)
        gate_pre = jnp.einsum("jrd,jdf->jrf", rows_in, w_gate, preferred_element_type=f32)
        up_pre = jnp.einsum("jrd,jdf->jrf", rows_in, w_up, preferred_element_type=f32)
        sigmoid_gate = jax.nn.sigmoid(gate_pre)
        silu_gate = gate_pre * sigmoid_gate
        activated = (silu_gate * up_pre).astype(bf16)
        produced = jnp.einsum("jrf,jfd->jrd", activated, w_down, preferred_element_type=f32).astype(
            bf16
        )
        wide = produced.astype(f32)
        grad_prob_slot = jnp.sum(wide * grad_rows_in.astype(f32), axis=2)
        grad_prob_part = jnp.sum(
            jnp.where(
                chosen,
                grad_prob_slot.reshape(local_experts, devices, capacity).transpose(1, 0, 2)[..., None],
                0.0,
            ),
            axis=2,
        )
        moe_partial = spread((weight_slot[:, :, None] * wide).astype(bf16))
        grad_prod = (weight_slot[:, :, None] * grad_rows_in.astype(f32)).astype(bf16)
        grad_act = jnp.einsum("jrd,jfd->jrf", grad_prod, w_down, preferred_element_type=f32)
        grad_gate_pre = (
            grad_act * up_pre * (sigmoid_gate * (1.0 + gate_pre * (1.0 - sigmoid_gate)))
        ).astype(bf16)
        grad_up_pre = (grad_act * silu_gate).astype(bf16)
        grad_slots = jnp.einsum("jrf,jdf->jrd", grad_gate_pre, w_gate, preferred_element_type=f32)
        grad_slots = (
            grad_slots + jnp.einsum("jrf,jdf->jrd", grad_up_pre, w_up, preferred_element_type=f32)
        ).astype(bf16)
        hidden_grad_partial = spread(grad_slots)

        grad_hidden_moe = sum_over_tp(block_sum(hidden_grad_partial, nf))
        grad_prob = lax.all_to_all(
            grad_prob_part, ("fsdp", "ctx"), split_axis=0, concat_axis=0, tiled=True
        ).reshape(experts, tokens_dev)
        grad_prob = grad_prob + swap(grad_prob, "tp")
        grad_prob = grad_prob.T

    if nf == 8:
        operands = (
            grad_hidden_moe,
            grad_prob,
            probs,
            router_rows,
            hidden_in,
            resid_mid,
            gains,
            grad_out,
            out_weight,
            query_weight,
            kv_weight,
            query_raw,
            key_projected,
            query_rotated,
            key_all,
            value_all,
            bias,
            log_total,
            trig,
            moe_partial,
            rows_in,
            grad_prod,
            activated,
            grad_gate_pre,
            grad_up_pre,
        )
        shapes = (tokens_dev, width_dim, heads_width, kv_width, key_all.shape[0])
        (
            attended_all,
            dq_all,
            rest_all,
            tail_all,
            proj_slice,
            grad_in,
            block_out,
            grad_gate,
            grad_up,
            grad_down,
        ) = backward_pass(nf, operands, attended, shapes)
        grad_gate, grad_up, grad_down = (
            grad_gate.astype(f32),
            grad_up.astype(f32),
            grad_down.astype(f32),
        )
        tail_rows = tail_all.shape[0] // devices
        dk_all, dv_all = rest_all[:, :kv_width], rest_all[:, kv_width : 2 * kv_width]
        logits_all = rest_all[:, 2 * kv_width :]
    else:
        grad_down = jnp.einsum("jrf,jrd->jfd", activated, grad_prod, preferred_element_type=f32)
        grad_gate = jnp.einsum("jrd,jrf->jdf", rows_in, grad_gate_pre, preferred_element_type=f32)
        grad_up = jnp.einsum("jrd,jrf->jdf", rows_in, grad_up_pre, preferred_element_type=f32)
        block_out = (resid_mid + sum_over_tp(block_sum(moe_partial, nf))).astype(bf16)

        grad_rows = grad_out.astype(f32)
        grad_logits = (
            probs * (grad_prob - jnp.sum(probs * grad_prob, axis=1, keepdims=True))
        ).astype(bf16)
        grad_hidden_two = grad_hidden_moe + jnp.einsum(
            "te,de->td", grad_logits, router_weight, preferred_element_type=f32
        )
        grad_ffn_local = jnp.sum(grad_hidden_two * normed_two, axis=0)
        grad_mid = grad_rows + rms_norm_gradient(grad_hidden_two, normed_two, inverse_two, gain_two)
        grad_proj = grad_mid.astype(bf16)
        attended_gradient = jnp.einsum(
            "td,qd->tq", grad_proj, out_weight, preferred_element_type=f32
        ).astype(bf16)
        attended_gradient = attended_gradient.reshape(
            tokens_dev, kv_local, query_group_width, HEAD_SIZE
        )
        probs_att = jnp.exp(scores - log_total)
        grad_value_all = jnp.einsum(
            "kgqs,qkgd->skd", weights_att, attended_gradient, preferred_element_type=f32
        )
        grad_probs = jnp.einsum(
            "qkgd,skd->kgqs", attended_gradient, value_all, preferred_element_type=f32
        )
        delta_row = jnp.sum(probs_att * grad_probs, axis=-1, keepdims=True)
        grad_scores = (probs_att * (grad_probs - delta_row) * HEAD_SIZE ** (-0.5)).astype(bf16)
        grad_query_rot = jnp.einsum(
            "kgqs,skd->qkgd", grad_scores, key_all, preferred_element_type=f32
        ).reshape(tokens_dev, head_local, HEAD_SIZE)
        grad_key_all = jnp.einsum(
            "kgqs,qkgd->skd", grad_scores, query_rotated, preferred_element_type=f32
        )
        grad_kv_all = jnp.concatenate(
            [grad_key_all.reshape(-1, kv_width), grad_value_all.reshape(-1, kv_width)], axis=1
        )
        theirs = lax.dynamic_slice_in_dim(grad_kv_all, (1 - c_index) * tokens_dev, tokens_dev, axis=0)
        mine = lax.dynamic_slice_in_dim(grad_kv_all, c_index * tokens_dev, tokens_dev, axis=0)
        grad_kv = mine + swap(theirs.astype(bf16), "ctx").astype(f32)
        key_rotated_gradient = grad_kv[:, :kv_width].reshape(tokens_dev, kv_local, HEAD_SIZE)
        grad_query_norm = inverse_rotation(grad_query_rot, cosine_table, sine_values)
        key_normed_gradient = inverse_rotation(key_rotated_gradient, cosine_table, sine_values)
        grad_qk_local = jnp.concatenate(
            [
                jnp.sum(grad_query_norm * query_hat, axis=(0, 1)),
                jnp.sum(key_normed_gradient * key_unit_rows, axis=(0, 1)),
            ]
        )
        grad_query_raw = (
            rms_norm_gradient(grad_query_norm, query_hat, query_inverse, gain_query)
            .astype(bf16)
            .reshape(tokens_dev, head_local * HEAD_SIZE)
        )
        key_projected_gradient = (
            rms_norm_gradient(key_normed_gradient, key_unit_rows, key_inverse_norm, gain_key)
            .astype(bf16)
            .reshape(tokens_dev, kv_width)
        )
        value_projected_gradient = grad_kv[:, kv_width:].astype(bf16)
        grad_hidden_part = jnp.einsum(
            "tq,dq->td", grad_query_raw, query_weight, preferred_element_type=f32
        )
        grad_hidden_part = grad_hidden_part + jnp.einsum(
            "tq,dq->td", key_projected_gradient, key_weight, preferred_element_type=f32
        )
        grad_hidden_part = grad_hidden_part + jnp.einsum(
            "tq,dq->td", value_projected_gradient, value_weight, preferred_element_type=f32
        )
        grad_hidden_one = sum_over_tp(grad_hidden_part)
        grad_in = grad_mid + rms_norm_gradient(grad_hidden_one, normed_one, inverse_one, gain_one)
        grad_attn_local = jnp.sum(grad_hidden_one * normed_one, axis=0)
        grad_qk_local = grad_qk_local + swap(grad_qk_local, "tp")
        tail = jnp.concatenate([grad_attn_local, grad_ffn_local, grad_qk_local])
        tail = jnp.pad(tail, (0, -tail.shape[0] % 1024)).reshape(-1, 128)
        tail_rows = tail.shape[0]
        logit_pad = jnp.pad(grad_logits, ((0, 0), (0, -experts % 128)))

        dq_all, dk_all, dv_all, attended_all, proj_slice, logits_all, tail_all = plane_gather(
            [
                Gather(grad_query_raw, nf, chunks=2),
                Gather(key_projected_gradient, nf, chunks=1),
                Gather(value_projected_gradient, nf, chunks=1),
                Gather(attended, nf, chunks=2),
                Gather(by_shard(grad_proj, nf), nf, form="a2a", chunks=1),
                Gather(logit_pad, nf, chunks=1),
                Gather(tail, nf, chunks=1),
            ],
            3,
            nf,
        )
    over_tokens = functools.partial(
        jnp.einsum, "td,tq->dq", preferred_element_type=f32
    )
    grad_query = over_tokens(hidden_first_slice, dq_all)
    grad_key = over_tokens(hidden_first_slice, dk_all)
    grad_value = over_tokens(hidden_first_slice, dv_all)
    grad_out_proj = over_tokens(attended_all, proj_slice)
    hidden_slice = lax.dynamic_slice_in_dim(hidden_all, f_index * shard_width, shard_width, axis=1)
    grad_router = over_tokens(hidden_slice, logits_all)[:, :experts]
    tail_sum = jnp.sum(tail_all.reshape(devices, tail_rows * 128), axis=0)
    grad_attn = lax.dynamic_slice_in_dim(tail_sum, f_index * shard_width, shard_width)
    grad_ffn = lax.dynamic_slice_in_dim(tail_sum, width_dim + f_index * shard_width, shard_width)
    qk_width = qk_gains.shape[0]
    grad_qk = lax.dynamic_slice_in_dim(tail_sum, 2 * width_dim + f_index * qk_width, qk_width)
    return (
        block_out,
        grad_in,
        grad_attn,
        grad_qk,
        grad_query,
        grad_key,
        grad_value,
        grad_out_proj,
        grad_ffn,
        grad_router,
        grad_gate,
        grad_up,
        grad_down,
    )


def solution(mesh):
    return jax.shard_map(
        on_device,
        mesh=mesh,
        in_specs=(
            P(("fsdp", "ctx"), None),
            P(("fsdp", "ctx")),
            P(("fsdp", "ctx"), None),
            P("fsdp"),
            P("fsdp"),
            P("fsdp", "tp"),
            P("fsdp", "tp"),
            P("fsdp", "tp"),
            P("tp", "fsdp"),
            P("fsdp"),
            P("fsdp", None),
            P(("fsdp", "ctx"), None, "tp"),
            P(("fsdp", "ctx"), None, "tp"),
            P(("fsdp", "ctx"), "tp", None),
            P(("fsdp", "ctx"), None),
        ),
        out_specs=(
            P(("fsdp", "ctx"), None),
            P(("fsdp", "ctx"), None),
            P("fsdp"),
            P("fsdp"),
            P("fsdp", "tp"),
            P("fsdp", "tp"),
            P("fsdp", "tp"),
            P("tp", "fsdp"),
            P("fsdp"),
            P("fsdp", None),
            P(("fsdp", "ctx"), None, "tp"),
            P(("fsdp", "ctx"), None, "tp"),
            P(("fsdp", "ctx"), "tp", None),
        ),
        check_vma=False,
    )
```
